32 devices in a mesh: fsdp: 8 (over z, x), ctx: 2 (over y), tp: 2 (over core).
Axes of the slice: x: 2, y: 2, z: 4, core: 2. Of those that a mesh axis runs over, the one named last changes fastest.
Arguments:
- tokens: bfloat16 [8, 1024, 2048], P('fsdp', 'ctx'), may hold values from -6 to 6
- segment_ids: int32 [8, 1024], P('fsdp'), may hold values from 0 to 3, never falling along the last dimension, each value on 1 to 512 neighbouring positions
- norm_gain: bfloat16 [2048], P('fsdp'), may hold values from 0.5 to 1.5
- query_weight: bfloat16 [2048, 2048], P('fsdp', 'tp'), may hold values from -0.125 to 0.125
- key_matrix: bfloat16 [2048, 1024], P('fsdp', 'tp'), may hold values from -0.125 to 0.125
- value_matrix: bfloat16 [2048, 1024], P('fsdp', 'tp'), may hold values from -0.125 to 0.125
- output_weight: bfloat16 [2048, 2048], P('fsdp', 'tp'), may hold values from -1.5 to 1.5
- query_gain: bfloat16 [128], P('fsdp'), may hold values from 0.7 to 6
- key_gain: bfloat16 [128], P('fsdp'), may hold values from 0.7 to 6
- mlp_gain: bfloat16 [2048], P('fsdp'), may hold values from 0.5 to 1.5
- gate_weight: bfloat16 [2048, 6144], P('fsdp', 'tp'), may hold values from -0.125 to 0.125
- up_weight: bfloat16 [2048, 6144], P('fsdp', 'tp'), may hold values from -0.125 to 0.125
- down_weight: bfloat16 [2048, 6144], P('fsdp', 'tp'), may hold values from -0.078125 to 0.078125
- cotangent: bfloat16 [8, 1024, 2048], P('fsdp', 'ctx'), may hold values from -6 to 6
Outputs:
- layer_out: bfloat16 [8, 1024, 2048], P('fsdp', 'ctx')
- token_grad: bfloat16 [8, 1024, 2048], P('fsdp', 'ctx')
- norm_gain_grad: float32 [2048], P('fsdp')
- query_weight_grad: float32 [2048, 2048], P('fsdp', 'tp')
- key_weight_grad: float32 [2048, 1024], P('fsdp', 'tp')
- value_weight_grad: float32 [2048, 1024], P('fsdp', 'tp')
- output_weight_grad: float32 [2048, 2048], P('fsdp', 'tp')
- query_gain_grad: float32 [128], P('fsdp')
- key_gain_grad: float32 [128], P('fsdp')
- mlp_gain_grad: float32 [2048], P('fsdp')
- gate_weight_grad: float32 [2048, 6144], P('fsdp', 'tp')
- up_weight_grad: float32 [2048, 6144], P('fsdp', 'tp')
- down_weight_grad: float32 [2048, 6144], P('fsdp', 'tp')
The draws below stay inside these ranges and needn't reach their ends.
Inputs may be any that keep to these rules, and one draw needn't show every extreme that they name: `segment_ids`: segment numbers never fall along a sequence; each document has 1 to 512 tokens and one document of each sequence has exactly 512.
All inputs are finite; a program needn't handle non-finite values.
Results may differ from the reference program's by a relative error of at most 0.02.
The reference program's roundings to bfloat16 on the way count: a program that leaves them out, or rounds other values in their place, can miss the bound.
Values may be sent and summed in bfloat16 or wider, within the bound.
A program may use at most 256 MiB of HBM per device.

```python
import math
import jax
import jax.numpy as jnp
import numpy as np
from jax import lax

MODEL_WIDTH = 2048
QUERY_HEADS = 16
KEY_VALUE_HEADS = 8
HEAD_SIZE = 128
FF = 6144
LEN = 1024
DOCS = 4
MOST_DOC = 512
SEQS = 8


def draw_query_gain(key, part):
    stream = jax.random.fold_in(key, 101)
    value = jax.random.uniform(stream, (HEAD_SIZE,), jnp.float32, 0.7, 1.3)
    return value.astype(jnp.bfloat16)


def draw_key_gain(key, part):
    stream = jax.random.fold_in(key, 202)
    value = jax.random.uniform(stream, (HEAD_SIZE,), jnp.float32, 0.7, 1.3)
    return value.astype(jnp.bfloat16)


def levels(key, extent, cuts, low, top_value):
    level, own = 1.0, jax.random.fold_in(key, 6)
    for position, shards_of in cuts:
        steps = jnp.exp(jax.random.uniform(jax.random.fold_in(own, position), (shards_of,), jnp.float32, low / len(cuts), top_value / len(cuts)))
        level = level * jnp.repeat(steps, extent[position] // shards_of).reshape([-1 if axis == position else 1 for axis in range(len(extent))])
    return level


def profile(count, total, bound, skew):
    portions = [(1 << 20) // math.isqrt(grade ** skew) + 1 for grade in range(2, count + 1)]
    rest, holding = total - bound - (count - 1), [1] * (count - 1)
    while rest > 0:
        candidates = [i for i in range(count - 1) if holding[i] < bound]
        mass, remaining = sum([portions[i] for i in candidates]), rest
        for i in candidates:
            extra = min(bound - holding[i], max(1, remaining * portions[i] // mass), rest)
            holding[i] = holding[i] + extra
            rest = rest - extra
    return np.array([bound] + holding)


def ragged(own_key, amount, total, most, slope):
    if amount == 2:
        one = jax.random.randint(own_key, (), max(1, total - most), min(most, total - 1) + 1)
        return jnp.stack([one, total - one])
    sizes = jnp.asarray(profile(amount, total, most, slope), jnp.int32)
    pairs = (amount - 1) // 2
    donor, sink = sizes[1:1 + 2 * pairs:2], sizes[2:2 + 2 * pairs:2]
    room = jnp.minimum(donor - 1, most - sink)
    passed = jax.random.randint(jax.random.fold_in(own_key, 1), (pairs,), 0, 1 << 20) % (room + 1)
    sizes = sizes.at[1:1 + 2 * pairs:2].set(donor - passed).at[2:2 + 2 * pairs:2].set(sink + passed)
    return sizes[jax.random.permutation(jax.random.fold_in(own_key, 2), amount)]


def gaussian(key, dims, spread, reach, pieces=(), held_as=jnp.bfloat16):
    loudness = levels(key, dims, pieces, -0.22, 0.18) if pieces else 1.0
    values = jax.random.normal(key, dims, jnp.float32) * spread * loudness
    return jnp.minimum(jnp.maximum(values, -reach), reach).astype(held_as)


def setup_inputs(seed: int = 0) -> dict:
    splits = jax.random.split(jax.random.key(seed), 15)
    return {
        "tokens": gaussian(splits[0], (SEQS, LEN, MODEL_WIDTH), 1.0, 6.0, ((0, 8), (1, 2))),
        "segment_ids": jax.vmap(lambda own: jnp.searchsorted(jnp.cumsum(ragged(own, DOCS, LEN, MOST_DOC, 0)), jnp.arange(LEN), side="right"))(jax.random.split(splits[1], SEQS)).reshape((SEQS, LEN)).astype(jnp.int32),
        "norm_gain": jnp.clip(1.0 + 0.1 * jax.random.normal(splits[2], (MODEL_WIDTH,), jnp.float32), 0.5, 1.5).astype(jnp.bfloat16),
        "query_weight": gaussian(splits[3], (MODEL_WIDTH, QUERY_HEADS * HEAD_SIZE), MODEL_WIDTH ** -0.5, 0.125, ((0, 8), (1, 2))),
        "key_matrix": gaussian(splits[4], (MODEL_WIDTH, KEY_VALUE_HEADS * HEAD_SIZE), MODEL_WIDTH ** -0.5, 0.125, ((0, 8), (1, 2))),
        "value_matrix": gaussian(splits[5], (MODEL_WIDTH, KEY_VALUE_HEADS * HEAD_SIZE), MODEL_WIDTH ** -0.5, 0.125, ((0, 8), (1, 2))),
        "output_weight": gaussian(splits[6], (MODEL_WIDTH, QUERY_HEADS * HEAD_SIZE), (QUERY_HEADS * HEAD_SIZE // 128) ** -0.5, 1.5, ((0, 8), (1, 2))),
        "query_gain": draw_query_gain(jax.random.fold_in(splits[14], 71), 0),
        "key_gain": draw_key_gain(jax.random.fold_in(splits[14], 71), 0),
        "mlp_gain": jnp.clip(1.0 + 0.1 * jax.random.normal(splits[9], (MODEL_WIDTH,), jnp.float32), 0.5, 1.5).astype(jnp.bfloat16),
        "gate_weight": gaussian(splits[10], (MODEL_WIDTH, FF), MODEL_WIDTH ** -0.5, 0.125, ((0, 8), (1, 2))),
        "up_weight": gaussian(splits[11], (MODEL_WIDTH, FF), MODEL_WIDTH ** -0.5, 0.125, ((0, 8), (1, 2))),
        "down_weight": gaussian(splits[12], (MODEL_WIDTH, FF), FF ** -0.5, 0.078125, ((0, 8), (1, 2))),
        "cotangent": gaussian(splits[13], (SEQS, LEN, MODEL_WIDTH), 1.0, 6.0, ((0, 8), (1, 2))),
    }


EPS = 1e-06
THETA = 1000000.0
MASKED = -1e+30

@jax.custom_vjp
def lower_result(v):
    return lax.optimization_barrier(v.astype(jnp.bfloat16)).astype(jnp.float32)

@jax.custom_vjp
def lower_backward(v):
    return v

def low_keep(v):
    return (lower_result(v), None)

def low_pass(kept, grad):
    return (grad,)

def back_keep(v):
    return (v, None)

def back_low(kept, grad):
    return (lower_result(grad),)
lower_result.defvjp(low_keep, low_pass)
lower_backward.defvjp(back_keep, back_low)

def product_result(form, left, right):
    return jnp.einsum(form, left, right, precision=lax.Precision.HIGHEST)

def rms_norm(value, gain):
    return value * lax.rsqrt(lax.optimization_barrier(jnp.mean(value * value, axis=-1, keepdims=True)) + EPS) * gain

def rope_tables(positions):
    freqs = THETA ** (-(jnp.arange(HEAD_SIZE // 2, dtype=jnp.float32) * 2.0) / HEAD_SIZE)
    angle = positions[:, None] * freqs[None, :]
    cosine = jnp.concatenate([jnp.cos(angle), jnp.cos(angle)], axis=-1)
    sine = jnp.concatenate([jnp.sin(angle), jnp.sin(angle)], axis=-1)
    return (cosine, sine)

def rotate(value, cosine, sine):
    half = value.shape[-1] // 2
    turned = jnp.concatenate([-value[..., half:], value[..., :half]], axis=-1)
    return value * cosine + turned * sine

def attend_one(item):
    query_rows, key_rows, value_rows, segments = item
    length_total = query_rows.shape[0]
    group_size = QUERY_HEADS // KEY_VALUE_HEADS
    scale = 1.0 / math.sqrt(HEAD_SIZE)
    grouped_heads = query_rows.reshape(length_total, KEY_VALUE_HEADS, group_size, HEAD_SIZE)
    scores = lower_backward(product_result('qgrd,kgd->grqk', grouped_heads, key_rows) * scale)
    order = jnp.arange(length_total)
    allowed = (segments[:, None] == segments[None, :]) & (order[None, :] <= order[:, None])
    scores = jnp.where(allowed, scores, MASKED)
    highest = lax.optimization_barrier(jnp.max(scores, axis=-1, keepdims=True))
    weights = jnp.exp(scores - highest)
    probability = weights / lax.optimization_barrier(jnp.sum(weights, axis=-1, keepdims=True))
    mixed = product_result('grqk,kgd->qgrd', lower_result(probability), value_rows)
    return lower_result(lower_backward(mixed)).reshape(length_total, QUERY_HEADS * HEAD_SIZE)

def forward(tokens, segments, params):
    norm_gain, query_weight, key_matrix, value_matrix, output_weight, query_gain, key_gain, mlp_gain, gate_weight, up_weight, down_weight = params
    batch_rows, length_total, width = tokens.shape
    normalized_input = lower_result(rms_norm(tokens, norm_gain))
    query_rows = lower_backward(product_result('zjv,vc->zjc', normalized_input, query_weight)).reshape(batch_rows, length_total, QUERY_HEADS, HEAD_SIZE)
    key_rows = lower_backward(product_result('zjv,vc->zjc', normalized_input, key_matrix)).reshape(batch_rows, length_total, KEY_VALUE_HEADS, HEAD_SIZE)
    value_rows = lower_result(lower_backward(product_result('zjv,vc->zjc', normalized_input, value_matrix))).reshape(batch_rows, length_total, KEY_VALUE_HEADS, HEAD_SIZE)
    cosine, sine = rope_tables(jnp.arange(length_total, dtype=jnp.float32))
    cosine = cosine[:, None, :]
    sine = sine[:, None, :]
    query_rows = lower_result(rotate(rms_norm(query_rows, query_gain), cosine, sine))
    key_rows = lower_result(rotate(rms_norm(key_rows, key_gain), cosine, sine))
    attended = lax.map(jax.checkpoint(attend_one), (query_rows, key_rows, value_rows, segments))
    middle = tokens + lower_backward(product_result('ble,de->bld', attended, output_weight))
    normed_mid = lower_result(rms_norm(middle, mlp_gain))
    gate = lower_backward(product_result('bld,df->blf', normed_mid, gate_weight))
    up_value = lower_backward(product_result('bld,df->blf', normed_mid, up_weight))
    hidden = lower_result(gate * jax.nn.sigmoid(gate) * up_value)
    return middle + lower_backward(product_result('blf,df->bld', hidden, down_weight))

def reference(tokens, segment_ids, norm_gain, query_weight, key_matrix, value_matrix, output_weight, query_gain, key_gain, mlp_gain, gate_weight, up_weight, down_weight, cotangent):
    params = (norm_gain.astype(jnp.float32), query_weight.astype(jnp.float32), key_matrix.astype(jnp.float32), value_matrix.astype(jnp.float32), output_weight.astype(jnp.float32), query_gain.astype(jnp.float32), key_gain.astype(jnp.float32), mlp_gain.astype(jnp.float32), gate_weight.astype(jnp.float32), up_weight.astype(jnp.float32), down_weight.astype(jnp.float32))
    block = math.gcd(SEQS, max(1, 4096 // LEN))
    count = SEQS // block
    inputs = tokens.astype(jnp.float32).reshape(count, block, LEN, MODEL_WIDTH)
    grads_in = cotangent.astype(jnp.float32).reshape(count, block, LEN, MODEL_WIDTH)
    segments = segment_ids.reshape(count, block, LEN)

    def one_block(totals, item):
        piece_in, piece_seg, piece_grad = item
        result, pullback = jax.vjp(lambda value_rows, weights: forward(value_rows, piece_seg, weights), piece_in, params)
        grad_in, grad_params = pullback(piece_grad)
        totals = tuple((left + right for left, right in zip(totals, grad_params)))
        return (totals, (result, grad_in))
    zeros = tuple((jnp.zeros_like(param) for param in params))
    totals, (outputs, grad_tokens) = lax.scan(one_block, zeros, (inputs, segments, grads_in))
    return (outputs.reshape(SEQS, LEN, MODEL_WIDTH).astype(jnp.bfloat16), grad_tokens.reshape(SEQS, LEN, MODEL_WIDTH).astype(jnp.bfloat16), totals[0], totals[1], totals[2], totals[3], totals[4], totals[5], totals[6], totals[7], totals[8], totals[9], totals[10])
```

```python
import math

import jax
import jax.numpy as jnp
from jax import lax
from jax.sharding import PartitionSpec as P

HEAD = 128
EPS = 1e-06
THETA = 1000000.0
MASKED = -1e30
F32 = jnp.float32
BF16 = jnp.bfloat16


def mm(left, right, left_dim, right_dim):
    return lax.dot_general(
        left, right, (((left_dim,), (right_dim,)), ((), ())), preferred_element_type=F32
    )


def swap_core(value):
    return lax.ppermute(value, "tp", [(0, 1), (1, 0)])


def swap_ctx(value):
    return lax.ppermute(value, "ctx", [(0, 1), (1, 0)])


def swap_x(value):
    count = lax.axis_size("fsdp")
    return lax.ppermute(value, "fsdp", [(i, i ^ 1) for i in range(count)])


def lines():
    count = lax.axis_size("fsdp")
    return [[i for i in range(count) if i % 2 == parity] for parity in (0, 1)]


def gather_line(value):
    return lax.all_gather(value, "fsdp", axis=0, tiled=True, axis_index_groups=lines())


def scatter_line(value):
    return lax.psum_scatter(
        value, "fsdp", scatter_dimension=0, tiled=True, axis_index_groups=lines()
    )


def flip_if(flag, value, axis):
    return jnp.where(flag, jnp.flip(value, axis), value)


def col_half(weight, place):
    half = weight.shape[1] // 2
    return lax.dynamic_slice_in_dim(weight, place * half, half, 1)


def reduce4(part, wide_core, wide_ctx):
    rows, cols = part.shape
    quarter = rows // 4
    view = part.reshape(2, 2, quarter, cols)
    kept = view[:, 0] + swap_core(view[:, 1].astype(wide_core)).astype(F32)
    return kept[0] + swap_ctx(kept[1].astype(wide_ctx)).astype(F32)


def gather4(own):
    both = jnp.stack([own, swap_ctx(own)])
    whole = jnp.stack([both, swap_core(both)], axis=1)
    return whole.reshape(4 * own.shape[0], own.shape[1])


def spread_input(rows_pair, core):
    half = rows_pair.shape[0] // 2
    view = flip_if(core == 1, rows_pair.reshape(2, half, -1), 0)
    far = swap_ctx(view[0])
    near = swap_core(far)
    return jnp.concatenate([view[0], view[1], far, near], axis=0)


def rope_tables(positions):
    freqs = THETA ** (-(jnp.arange(HEAD // 2, dtype=F32) * 2.0) / HEAD)
    angle = positions[:, None] * freqs[None, :]
    cosine = jnp.concatenate([jnp.cos(angle), jnp.cos(angle)], axis=-1)
    sine = jnp.concatenate([jnp.sin(angle), jnp.sin(angle)], axis=-1)
    return cosine, sine


def rotate(value, cosine, sine):
    half = value.shape[-1] // 2
    turned = jnp.concatenate([-value[..., half:], value[..., :half]], axis=-1)
    return value * cosine + turned * sine


def rotate_back(value, cosine, sine):
    half = value.shape[-1] // 2
    turned = value * sine
    return value * cosine + jnp.concatenate([turned[..., half:], -turned[..., :half]], axis=-1)


def head_norm(raw, gain):
    inverse = lax.rsqrt(jnp.mean(raw * raw, axis=-1, keepdims=True) + EPS)
    scaled = raw * inverse
    return scaled, inverse, scaled * gain


def norm_back(grad, scaled, inverse, gain):
    weighted = grad * gain
    return inverse * (weighted - scaled * jnp.mean(weighted * scaled, axis=-1, keepdims=True))


def inv_rms(first, second, width):
    total = jnp.sum(first * first, axis=-1, keepdims=True) + jnp.sum(
        second * second, axis=-1, keepdims=True
    )
    return lax.rsqrt(total / width + EPS)


def norm_back_pair(grads, scaled, inverse, gains, width):
    weighted = [g * w for g, w in zip(grads, gains)]
    dots = sum(jnp.sum(w * s, axis=-1, keepdims=True) for w, s in zip(weighted, scaled)) / width
    return [inverse * (w - s * dots) for w, s in zip(weighted, scaled)]


def body(
    tokens,
    segment_ids,
    norm_gain,
    query_weight,
    key_matrix,
    value_matrix,
    output_weight,
    query_gain,
    key_gain,
    mlp_gain,
    gate_weight,
    up_weight,
    down_weight,
    cotangent,
):
    local, width = tokens.shape[1], tokens.shape[2]
    length = 2 * local
    quarter = local // 2
    count = lax.axis_size("fsdp")
    block = width // count
    line = count // 2
    half_width = width // 2
    mine = lax.axis_index("fsdp")
    odd = mine % 2
    place = lax.axis_index("ctx")
    core = lax.axis_index("tp")
    me = 2 * place + core
    scale = 1.0 / math.sqrt(HEAD)

    def split_x(value):
        view = value.reshape(value.shape[0], line, 2, block)
        view = flip_if(odd == 1, view, 2)
        return (
            view[:, :, 0].reshape(value.shape[0], half_width),
            view[:, :, 1].reshape(value.shape[0], half_width),
        )

    def join_x(first, second):
        view = jnp.stack(
            [first.reshape(-1, line, block), second.reshape(-1, line, block)], axis=2
        )
        return flip_if(odd == 1, view, 2).reshape(-1, width)

    q_shard = col_half(query_weight, place)
    k_shard = col_half(key_matrix, place)
    v_shard = col_half(value_matrix, place)
    o_shard = col_half(output_weight, place)
    gate_shard = col_half(gate_weight, place)
    up_shard = col_half(up_weight, place)
    down_shard = col_half(down_weight, place)
    cols_q, cols_k = q_shard.shape[1], k_shard.shape[1]
    heads_q, heads_kv = cols_q // HEAD, cols_k // HEAD
    group = heads_q // heads_kv
    small = query_gain.shape[0]
    gains = jnp.zeros((block, HEAD), BF16)
    gains = gains.at[:, 0].set(norm_gain).at[:, 1].set(mlp_gain)
    gains = gains.at[:small, 2].set(query_gain).at[:small, 3].set(key_gain)
    first_shard = jnp.concatenate([q_shard, k_shard, v_shard, gains], axis=1)

    down_other_shard = swap_x(down_shard)
    first_a = gather_line(first_shard)
    first_b = swap_x(first_a)
    out_a = gather_line(o_shard)
    out_b = swap_x(out_a)
    gate_a = gather_line(gate_shard)
    gate_b = swap_x(gate_a)
    up_a = gather_line(up_shard)
    up_b = swap_x(up_a)
    down_a = gather_line(down_shard)
    down_b = gather_line(down_other_shard)

    tok_a, tok_b = split_x(tokens.reshape(local, width))
    tok_a, tok_b = spread_input(tok_a, core), spread_input(tok_b, core)
    cot_a, cot_b = split_x(cotangent.reshape(local, width))
    cot_a, cot_b = spread_input(cot_a, core), spread_input(cot_b, core)

    order = jnp.arange(4) ^ me
    positions = (order[:, None] * quarter + jnp.arange(quarter)[None, :]).reshape(length)
    segments = jnp.take(segment_ids.reshape(4, quarter), order, axis=0).reshape(length)
    allowed = (segments[:, None] == segments[None, :]) & (
        positions[None, :] <= positions[:, None]
    )
    cosine, sine = rope_tables(positions.astype(F32))
    cosine, sine = cosine[:, None, :], sine[:, None, :]

    cols = cols_q + 2 * cols_k
    qkv_a, qkv_b = first_a[:, :cols], first_b[:, :cols]
    gains_a = first_a[:, cols:].astype(F32)
    gains_b = first_b[:, cols:].astype(F32)
    norm_a, norm_b = gains_a[:, 0][None], gains_b[:, 0][None]
    mid_a, mid_b = gains_a[:, 1][None], gains_b[:, 1][None]
    head_gains = jnp.stack(
        [
            gains_a.reshape(line, block, HEAD)[:, :small, 2:4],
            gains_b.reshape(line, block, HEAD)[:, :small, 2:4],
        ],
        axis=1,
    )
    head_gains = flip_if(odd == 1, head_gains, 1).reshape(HEAD, 2)
    query_gain_f, key_gain_f = head_gains[:, 0], head_gains[:, 1]

    in_a, in_b = tok_a.astype(F32), tok_b.astype(F32)
    inverse_in = inv_rms(in_a, in_b, width)
    x_a = (in_a * inverse_in * norm_a).astype(BF16)
    x_b = (in_b * inverse_in * norm_b).astype(BF16)
    qkv = mm(x_a, qkv_a, 1, 0) + mm(x_b, qkv_b, 1, 0)
    raw_query = qkv[:, :cols_q].reshape(length, heads_q, HEAD)
    raw_key = qkv[:, cols_q : cols_q + cols_k].reshape(length, heads_kv, HEAD)
    values = qkv[:, cols_q + cols_k :].astype(BF16).reshape(length, heads_kv, HEAD)
    query_scaled, query_inverse, query_normed = head_norm(raw_query, query_gain_f)
    key_scaled, key_inverse, key_normed = head_norm(raw_key, key_gain_f)
    queries = rotate(query_normed, cosine, sine).astype(BF16)
    keys = rotate(key_normed, cosine, sine).astype(BF16)
    grouped = queries.reshape(length, heads_kv, group, HEAD)

    def probabilities():
        scores = jnp.einsum("qgrd,kgd->grqk", grouped, keys, preferred_element_type=F32) * scale
        scores = jnp.where(allowed[None, None], scores, MASKED)
        weights = jnp.exp(scores - jnp.max(scores, axis=-1, keepdims=True))
        return weights / jnp.sum(weights, axis=-1, keepdims=True)

    probs = probabilities()
    attended = jnp.einsum(
        "grqk,kgd->qgrd", probs.astype(BF16), values, preferred_element_type=F32
    )
    attended = attended.astype(BF16).reshape(length, cols_q)

    part_a, part_b = mm(attended, out_a, 1, 1), mm(attended, out_b, 1, 1)
    own_in_a, own_in_b = in_a[:quarter], in_b[:quarter]
    middle_a = own_in_a + reduce4(part_a, F32, F32)
    middle_b = own_in_b + reduce4(part_b, F32, F32)
    inverse_mid = inv_rms(middle_a, middle_b, width)
    scaled_mid = (middle_a * inverse_mid, middle_b * inverse_mid)
    y_a = gather4((scaled_mid[0] * mid_a).astype(BF16))
    y_b = gather4((scaled_mid[1] * mid_b).astype(BF16))

    gate = mm(y_a, gate_a, 1, 0) + mm(y_b, gate_b, 1, 0)
    up_value = mm(y_a, up_a, 1, 0) + mm(y_b, up_b, 1, 0)
    sig = jax.nn.sigmoid(gate)
    active = gate * sig
    hidden = (active * up_value).astype(BF16)
    down_grad_b = mm(cot_b, hidden, 0, 0).astype(BF16)
    down_grad_a = mm(cot_a, hidden, 0, 0)
    mlp_a = reduce4(mm(hidden, down_a, 1, 1), BF16, BF16)
    mlp_b = reduce4(mm(hidden, down_b, 1, 1), BF16, BF16)

    def finish_rows(own_a, own_b):
        own = jnp.stack([own_a.astype(BF16), own_b.astype(BF16)])
        both = jnp.stack([own, swap_core(own)], axis=1)
        both = flip_if(core == 1, both, 1).reshape(2, local, half_width)
        return join_x(both[0], both[1]).reshape(tokens.shape)

    layer_out = finish_rows(middle_a + mlp_a, middle_b + mlp_b)

    grad_hidden = mm(cot_a, down_a, 1, 0) + mm(cot_b, down_b, 1, 0)
    grad_up = (grad_hidden * active).astype(BF16)
    grad_gate = (grad_hidden * up_value * (sig * (1.0 + gate * (1.0 - sig)))).astype(BF16)
    gate_grad_b = mm(y_b, grad_gate, 0, 0).astype(BF16)
    up_grad_b = mm(y_b, grad_up, 0, 0).astype(BF16)
    mid_grad_a = reduce4(mm(grad_gate, gate_a, 1, 1) + mm(grad_up, up_a, 1, 1), F32, BF16)
    mid_grad_b = reduce4(mm(grad_gate, gate_b, 1, 1) + mm(grad_up, up_b, 1, 1), F32, BF16)
    gate_grad_a = mm(y_a, grad_gate, 0, 0)
    up_grad_a = mm(y_a, grad_up, 0, 0)

    def owners(kept, sent):
        total = (kept + swap_x(sent).astype(F32)).astype(BF16)
        return scatter_line(total)

    def both_halves(share):
        other = swap_ctx(share)
        pair = jnp.stack([share, other], axis=1)
        pair = flip_if(place == 1, pair, 1)
        return pair.reshape(share.shape[0], 2 * share.shape[1]).astype(F32)

    down_share = both_halves(owners(down_grad_a, down_grad_b))
    gate_share = both_halves(owners(gate_grad_a, gate_grad_b))
    up_share = both_halves(owners(up_grad_a, up_grad_b))

    mlp_gain_part = jnp.stack(
        [
            jnp.sum(mid_grad_a * scaled_mid[0], axis=0),
            jnp.sum(mid_grad_b * scaled_mid[1], axis=0),
        ]
    )
    back_a, back_b = norm_back_pair(
        (mid_grad_a, mid_grad_b), scaled_mid, inverse_mid, (mid_a, mid_b), width
    )
    grad_middle_a = cot_a[:quarter].astype(F32) + back_a
    grad_middle_b = cot_b[:quarter].astype(F32) + back_b
    ga_a = gather4(grad_middle_a.astype(BF16))
    ga_b = gather4(grad_middle_b.astype(BF16))
    out_grad_b = mm(ga_b, attended, 0, 0).astype(BF16)
    out_grad_a = mm(ga_a, attended, 0, 0)
    out_share = both_halves(owners(out_grad_a, out_grad_b))
    grad_att = (mm(ga_a, out_a, 1, 0) + mm(ga_b, out_b, 1, 0)).astype(BF16)
    grad_grouped = grad_att.reshape(length, heads_kv, group, HEAD)

    grad_probs = jnp.einsum("qgrd,kgd->grqk", grad_grouped, values, preferred_element_type=F32)
    delta = jnp.sum(probs * grad_probs, axis=-1, keepdims=True)
    grad_scores = (probs * (grad_probs - delta)).astype(BF16)
    grad_queries = (
        jnp.einsum("grqk,kgd->qgrd", grad_scores, keys, preferred_element_type=F32) * scale
    )
    grad_keys = (
        jnp.einsum("grqk,qgrd->kgd", grad_scores, grouped, preferred_element_type=F32) * scale
    )
    grad_values = jnp.einsum(
        "grqk,qgrd->kgd", probs.astype(BF16), grad_grouped, preferred_element_type=F32
    ).astype(BF16)
    grad_queries = rotate_back(
        grad_queries.reshape(length, heads_q, HEAD), cosine, sine
    )
    grad_keys = rotate_back(grad_keys, cosine, sine)
    query_gain_part = jnp.sum(grad_queries * query_scaled, axis=(0, 1))
    key_gain_part = jnp.sum(grad_keys * key_scaled, axis=(0, 1))
    raw_grad_q = norm_back(grad_queries, query_scaled, query_inverse, query_gain_f).astype(BF16)
    raw_grad_k = norm_back(grad_keys, key_scaled, key_inverse, key_gain_f).astype(BF16)
    raw_grads = jnp.concatenate(
        [
            raw_grad_q.reshape(length, cols_q),
            raw_grad_k.reshape(length, cols_k),
            grad_values.reshape(length, cols_k),
        ],
        axis=1,
    )
    first_grad_b = mm(x_b, raw_grads, 0, 0).astype(BF16)
    first_grad_a = mm(x_a, raw_grads, 0, 0)
    in_grad_a = reduce4(mm(raw_grads, qkv_a, 1, 1), F32, BF16)
    in_grad_b = reduce4(mm(raw_grads, qkv_b, 1, 1), F32, BF16)
    first_own = owners(first_grad_a, first_grad_b)
    first_other = swap_ctx(first_own)

    def whole_columns(start, stop):
        pair = jnp.stack([first_own[:, start:stop], first_other[:, start:stop]], axis=1)
        pair = flip_if(place == 1, pair, 1)
        return pair.reshape(block, 2 * (stop - start)).astype(F32)

    query_share = whole_columns(0, cols_q)
    key_share = whole_columns(cols_q, cols_q + cols_k)
    value_share = whole_columns(cols_q + cols_k, cols)

    own_inverse = inverse_in[:quarter]
    scaled_in = (own_in_a * own_inverse, own_in_b * own_inverse)
    norm_gain_part = jnp.stack(
        [jnp.sum(in_grad_a * scaled_in[0], axis=0), jnp.sum(in_grad_b * scaled_in[1], axis=0)]
    )
    back_a, back_b = norm_back_pair(
        (in_grad_a, in_grad_b), scaled_in, own_inverse, (norm_a, norm_b), width
    )
    token_grad = finish_rows(grad_middle_a + back_a, grad_middle_b + back_b)

    pair_parts = flip_if(odd == 1, jnp.stack([norm_gain_part, mlp_gain_part], axis=1), 0)
    sums = lax.psum(
        (pair_parts, query_gain_part, key_gain_part), ("fsdp", "ctx", "tp")
    )
    own_pair = lax.dynamic_index_in_dim(
        sums[0].reshape(2, 2, line, block), odd, 0, keepdims=False
    )
    own_pair = lax.dynamic_index_in_dim(own_pair, mine // 2, 1, keepdims=False)
    query_gain_grad = lax.dynamic_slice_in_dim(sums[1], mine * small, small, 0)
    key_gain_grad = lax.dynamic_slice_in_dim(sums[2], mine * small, small, 0)
    return (
        layer_out,
        token_grad,
        own_pair[0],
        query_share,
        key_share,
        value_share,
        out_share,
        query_gain_grad,
        key_gain_grad,
        own_pair[1],
        gate_share,
        up_share,
        down_share,
    )


def solution(mesh):
    in_specs = (
        P("fsdp", "ctx", None),
        P("fsdp", None),
        P("fsdp"),
        P("fsdp", "tp"),
        P("fsdp", "tp"),
        P("fsdp", "tp"),
        P("fsdp", "tp"),
        P("fsdp"),
        P("fsdp"),
        P("fsdp"),
        P("fsdp", "tp"),
        P("fsdp", "tp"),
        P("fsdp", "tp"),
        P("fsdp", "ctx", None),
    )
    out_specs = (
        P("fsdp", "ctx", None),
        P("fsdp", "ctx", None),
        P("fsdp"),
        P("fsdp", "tp"),
        P("fsdp", "tp"),
        P("fsdp", "tp"),
        P("fsdp", "tp"),
        P("fsdp"),
        P("fsdp"),
        P("fsdp"),
        P("fsdp", "tp"),
        P("fsdp", "tp"),
        P("fsdp", "tp"),
    )
    return jax.shard_map(body, mesh=mesh, in_specs=in_specs, out_specs=out_specs, check_vma=False)
```

```python
import functools
import math

import jax
import jax.numpy as jnp
from jax import lax
from jax.experimental import pallas as pl
from jax.experimental.pallas import tpu as pltpu
from jax.sharding import PartitionSpec as P

HEAD = 128
EPS = 1e-06
THETA = 1000000.0
MASKED = -1e30
MOST_DOC = 512
F32 = jnp.float32
BF16 = jnp.bfloat16


def mm(left, right, left_dim, right_dim):
    return lax.dot_general(
        left, right, (((left_dim,), (right_dim,)), ((), ())), preferred_element_type=F32
    )


def swap_core(value):
    return lax.ppermute(value, "tp", [(0, 1), (1, 0)])


def swap_ctx(value):
    return lax.ppermute(value, "ctx", [(0, 1), (1, 0)])


def swap_x(value):
    count = lax.axis_size("fsdp")
    return lax.ppermute(value, "fsdp", [(i, i ^ 1) for i in range(count)])


def lines():
    count = lax.axis_size("fsdp")
    return [[i for i in range(count) if i % 2 == parity] for parity in (0, 1)]


def gather_line(value):
    return lax.all_gather(value, "fsdp", axis=0, tiled=True, axis_index_groups=lines())


def scatter_line(value):
    return lax.psum_scatter(
        value, "fsdp", scatter_dimension=0, tiled=True, axis_index_groups=lines()
    )


def flip_if(flag, value, axis):
    return jnp.where(flag, jnp.flip(value, axis), value)


def gather8(own):
    rows = own.shape[0] // 2
    first, second = own[:rows], own[rows:]
    first = jnp.concatenate([first, swap_x(first)])
    second = jnp.concatenate([second, swap_ctx(second)])
    side = jnp.concatenate([first, swap_ctx(first), second, swap_x(second)])
    return jnp.concatenate([side, swap_core(side)])


def reduce8(near, far, wide):
    total = near + swap_core(far).astype(F32)
    rows = total.shape[0] // 8
    first, second = total[: 4 * rows], total[4 * rows :]
    first = first[: 2 * rows] + swap_ctx(first[2 * rows :].astype(wide)).astype(F32)
    second = second[: 2 * rows] + swap_x(second[2 * rows :].astype(wide)).astype(F32)
    first = first[:rows] + swap_x(first[rows:].astype(wide)).astype(F32)
    second = second[:rows] + swap_ctx(second[rows:].astype(wide)).astype(F32)
    return jnp.concatenate([first, second])


def rope_tables(positions):
    freqs = THETA ** (-(jnp.arange(HEAD // 2, dtype=F32) * 2.0) / HEAD)
    angle = positions[:, None] * freqs[None, :]
    cosine = jnp.concatenate([jnp.cos(angle), jnp.cos(angle)], axis=-1)
    sine = jnp.concatenate([-jnp.sin(angle), jnp.sin(angle)], axis=-1)
    return cosine, sine


def norm_back(grad, scaled, inverse, gain):
    weighted = grad * gain
    return inverse * (weighted - scaled * jnp.mean(weighted * scaled, axis=-1, keepdims=True))


def inv_rms(value):
    return lax.rsqrt(jnp.mean(value * value, axis=-1, keepdims=True) + EPS)


def block_row(meta_ref, seq, index, rows):
    away_c = lax.rem(meta_ref[0] + index // 4, 2)
    away_t = lax.rem(meta_ref[1] + (index // 2) % 2, 2)
    if index % 2 == 0:
        inner = away_c * 2 + seq
    else:
        inner = seq * 2 + away_c + 4
    return pl.multiple_of((away_t * 8 + inner) * rows, rows)


def scaled_of(raw):
    inverse = lax.rsqrt(jnp.mean(raw * raw, axis=-1, keepdims=True) + EPS)
    return raw * inverse, inverse


def load_heads(meta_ref, qkv_ref, cos_ref, sin_ref, gain_ref, q_scr, k_scr, v_scr, heads):
    seq = pl.program_id(0)
    rows = q_scr.shape[1] // 8
    for index in range(8):
        start = block_row(meta_ref, seq, index, rows)
        here = slice(index * rows, (index + 1) * rows)
        cosine, sine = cos_ref[here, :], sin_ref[here, :]
        for head in range(heads + 1):
            raw = qkv_ref[pl.ds(start, rows), head * HEAD : (head + 1) * HEAD]
            scaled, _ = scaled_of(raw)
            which = 0 if head < heads else 1
            value = scaled * gain_ref[which : which + 1, :]
            turned = value * cosine + pltpu.roll(value, HEAD // 2, 1) * sine
            if head < heads:
                q_scr[head, here, :] = turned.astype(BF16)
            else:
                k_scr[here, :] = turned.astype(BF16)
        v_scr[here, :] = qkv_ref[
            pl.ds(start, rows), (heads + 1) * HEAD : (heads + 2) * HEAD
        ].astype(BF16)


def key_span(index, tile):
    low = max(0, (index * tile - (MOST_DOC - 1)) // tile) * tile
    return low, (index + 1) * tile


def allowed_mask(segc_ref, segr_ref, index, tile):
    low, high = key_span(index, tile)
    shape = (tile, high - low)
    rows = lax.broadcasted_iota(jnp.int32, shape, 0) + index * tile
    cols = lax.broadcasted_iota(jnp.int32, shape, 1) + low
    same = segc_ref[0, index * tile : (index + 1) * tile, :] == segr_ref[0, :, low:high]
    return same & (cols <= rows)


def probs_of(query, keys, allowed, scale):
    scores = jnp.where(allowed, mm(query, keys, 1, 1) * scale, MASKED)
    weights = jnp.exp(scores - jnp.max(scores, axis=-1, keepdims=True))
    return weights * (1.0 / jnp.sum(weights, axis=-1, keepdims=True))


def attend_kernel(
    heads, tile, meta_ref, qkv_ref, segc_ref, segr_ref, cos_ref, sin_ref, gain_ref, out_ref, q_scr, k_scr, v_scr
):
    seq = pl.program_id(0)
    length = k_scr.shape[0]
    rows = length // 8
    scale = 1.0 / math.sqrt(HEAD)
    load_heads(meta_ref, qkv_ref, cos_ref, sin_ref, gain_ref, q_scr, k_scr, v_scr, heads)
    for index in range(length // tile):
        low, high = key_span(index, tile)
        allowed = allowed_mask(segc_ref, segr_ref, index, tile)
        for head in range(heads):
            query = q_scr[head, index * tile : (index + 1) * tile, :]
            probs = probs_of(query, k_scr[low:high, :], allowed, scale)
            mixed = mm(probs.astype(BF16), v_scr[low:high, :], 1, 0).astype(BF16)
            for piece in range(tile // rows):
                start = block_row(meta_ref, seq, index * (tile // rows) + piece, rows)
                out_ref[pl.ds(start, rows), head * HEAD : (head + 1) * HEAD] = mixed[
                    piece * rows : (piece + 1) * rows
                ]


def attend_back_kernel(
    heads,
    tile,
    meta_ref,
    qkv_ref,
    grad_ref,
    segc_ref,
    segr_ref,
    cos_ref,
    sin_ref,
    gain_ref,
    out_ref,
    gain_out_ref,
    q_scr,
    k_scr,
    v_scr,
    g_scr,
    dk_scr,
    dv_scr,
):
    seq = pl.program_id(0)
    length = k_scr.shape[0]
    rows = length // 8
    scale = 1.0 / math.sqrt(HEAD)
    load_heads(meta_ref, qkv_ref, cos_ref, sin_ref, gain_ref, q_scr, k_scr, v_scr, heads)
    for index in range(8):
        start = block_row(meta_ref, seq, index, rows)
        g_scr[index * rows : (index + 1) * rows, :] = grad_ref[pl.ds(start, rows), :]
    dk_scr[...] = jnp.zeros_like(dk_scr)
    dv_scr[...] = jnp.zeros_like(dv_scr)

    @pl.when(seq == 0)
    def _():
        gain_out_ref[...] = jnp.zeros_like(gain_out_ref)

    def finish(grad, index, head, which):
        here = slice(index * rows, (index + 1) * rows)
        start = block_row(meta_ref, seq, index, rows)
        grad = grad * cos_ref[here, :] - pltpu.roll(grad, HEAD // 2, 1) * sin_ref[here, :]
        raw = qkv_ref[pl.ds(start, rows), head * HEAD : (head + 1) * HEAD]
        scaled, inverse = scaled_of(raw)
        gain_out_ref[which : which + 1, :] += jnp.sum(grad * scaled, axis=0, keepdims=True)
        out = norm_back(grad, scaled, inverse, gain_ref[which : which + 1, :])
        out_ref[pl.ds(start, rows), head * HEAD : (head + 1) * HEAD] = out.astype(BF16)

    per = tile // rows
    for index in range(length // tile):
        low, high = key_span(index, tile)
        mine = slice(index * tile, (index + 1) * tile)
        allowed = allowed_mask(segc_ref, segr_ref, index, tile)
        for head in range(heads):
            query = q_scr[head, mine, :]
            keys = k_scr[low:high, :]
            probs = probs_of(query, keys, allowed, scale)
            grad = g_scr[mine, head * HEAD : (head + 1) * HEAD]
            grad_probs = mm(grad, v_scr[low:high, :], 1, 1)
            delta = jnp.sum(probs * grad_probs, axis=-1, keepdims=True)
            grad_scores = (probs * (grad_probs - delta)).astype(BF16)
            dv_scr[low:high, :] += mm(probs.astype(BF16), grad, 0, 0)
            dk_scr[low:high, :] += mm(grad_scores, query, 0, 0) * scale
            grad_query = mm(grad_scores, keys, 1, 0) * scale
            for piece in range(per):
                finish(
                    grad_query[piece * rows : (piece + 1) * rows], index * per + piece, head, 0
                )
    for index in range(8):
        here = slice(index * rows, (index + 1) * rows)
        start = block_row(meta_ref, seq, index, rows)
        finish(dk_scr[here, :], index, heads, 1)
        out_ref[pl.ds(start, rows), (heads + 1) * HEAD : (heads + 2) * HEAD] = dv_scr[
            here, :
        ].astype(BF16)


def whole(shape):
    return pl.BlockSpec(shape, lambda seq, meta: (0,) * len(shape))


def seg_specs(length):
    return [
        pl.BlockSpec((1, length, 1), lambda seq, meta: (seq, 0, 0)),
        pl.BlockSpec((1, 1, length), lambda seq, meta: (seq, 0, 0)),
    ]


def attend(meta, qkv, seg_cols, seg_rows, cosine, sine, gains):
    length = cosine.shape[0]
    tile = length // 4
    heads = qkv.shape[1] // HEAD - 2
    pairs = 2 * heads * length * length // 2
    return pl.pallas_call(
        functools.partial(attend_kernel, heads, tile),
        out_shape=jax.ShapeDtypeStruct((qkv.shape[0], heads * HEAD), BF16),
        grid_spec=pltpu.PrefetchScalarGridSpec(
            num_scalar_prefetch=1,
            grid=(2,),
            in_specs=[whole(qkv.shape)]
            + seg_specs(length)
            + [whole(cosine.shape), whole(sine.shape), whole(gains.shape)],
            out_specs=whole((qkv.shape[0], heads * HEAD)),
            scratch_shapes=[
                pltpu.VMEM((heads, length, HEAD), BF16),
                pltpu.VMEM((length, HEAD), BF16),
                pltpu.VMEM((length, HEAD), BF16),
            ],
        ),
        cost_estimate=pl.CostEstimate(
            flops=4 * pairs * HEAD, bytes_accessed=qkv.size * 4 + qkv.size, transcendentals=pairs
        ),
        name="attend",
    )(meta, qkv, seg_cols, seg_rows, cosine, sine, gains)


def attend_back(meta, qkv, grad, seg_cols, seg_rows, cosine, sine, gains):
    length = cosine.shape[0]
    tile = length // 4
    heads = qkv.shape[1] // HEAD - 2
    pairs = 2 * heads * length * length // 2
    return pl.pallas_call(
        functools.partial(attend_back_kernel, heads, tile),
        out_shape=(
            jax.ShapeDtypeStruct(qkv.shape, BF16),
            jax.ShapeDtypeStruct(gains.shape, F32),
        ),
        grid_spec=pltpu.PrefetchScalarGridSpec(
            num_scalar_prefetch=1,
            grid=(2,),
            in_specs=[whole(qkv.shape), whole(grad.shape)]
            + seg_specs(length)
            + [whole(cosine.shape), whole(sine.shape), whole(gains.shape)],
            out_specs=(whole(qkv.shape), whole(gains.shape)),
            scratch_shapes=[
                pltpu.VMEM((heads, length, HEAD), BF16),
                pltpu.VMEM((length, HEAD), BF16),
                pltpu.VMEM((length, HEAD), BF16),
                pltpu.VMEM((length, heads * HEAD), BF16),
                pltpu.VMEM((length, HEAD), F32),
                pltpu.VMEM((length, HEAD), F32),
            ],
        ),
        cost_estimate=pl.CostEstimate(
            flops=10 * pairs * HEAD, bytes_accessed=qkv.size * 8, transcendentals=pairs
        ),
        name="attend_back",
    )(meta, qkv, grad, seg_cols, seg_rows, cosine, sine, gains)


def body(
    tokens,
    segment_ids,
    norm_gain,
    query_weight,
    key_matrix,
    value_matrix,
    output_weight,
    query_gain,
    key_gain,
    mlp_gain,
    gate_weight,
    up_weight,
    down_weight,
    cotangent,
):
    local, width = tokens.shape[1], tokens.shape[2]
    length = 2 * local
    quarter = local // 2
    count = lax.axis_size("fsdp")
    block = width // count
    line = count // 2
    mine = lax.axis_index("fsdp")
    odd = mine % 2
    place = lax.axis_index("ctx")
    core = lax.axis_index("tp")
    column = 2 * place + odd

    def cut(weight, which):
        size = weight.shape[1] // 4
        return lax.dynamic_slice_in_dim(weight, which * size, size, 1)

    def shard(weights, extra=()):
        own = [cut(weight, column) for weight in weights] + list(extra)
        peer = [cut(weight, column ^ 1) for weight in weights] + list(extra)
        own = own[0] if len(own) == 1 else jnp.concatenate(own, axis=1)
        peer = peer[0] if len(peer) == 1 else jnp.concatenate(peer, axis=1)
        pair = flip_if(odd == 1, jnp.stack([own, swap_x(peer)]), 0)
        return gather_line(pair.reshape(2 * block, own.shape[1]))

    small = query_gain.shape[0]
    lanes = jnp.arange(HEAD)[None, :]

    def pad_rows(vector):
        return jnp.concatenate([vector, jnp.zeros((block - small,), BF16)])

    gains = jnp.where(
        lanes == 0,
        norm_gain[:, None],
        jnp.where(
            lanes == 1,
            mlp_gain[:, None],
            jnp.where(
                lanes == 2, pad_rows(query_gain)[:, None], pad_rows(key_gain)[:, None]
            ),
        ),
    )
    first = shard((query_weight, key_matrix, value_matrix), (gains,))
    out_w = shard((output_weight,))
    gate_up_w = shard((gate_weight, up_weight))
    down_w = shard((down_weight,))

    def own_quarter(value):
        return lax.dynamic_slice_in_dim(value.reshape(local, width), core * quarter, quarter, 0)

    own_tok, own_cot = own_quarter(tokens), own_quarter(cotangent)
    tok = gather8(own_tok)
    cot = gather8(own_cot)
    segments = jnp.concatenate([segment_ids, swap_x(segment_ids)])
    seg_cols, seg_rows = segments[:, :, None], segments[:, None, :]
    cosine, sine = rope_tables(jnp.arange(length).astype(F32))
    meta = jnp.stack([place, core]).astype(jnp.int32)

    heads_q = query_weight.shape[1] // 4 // HEAD
    cols = (heads_q + 2) * HEAD
    qkv_w = first[:, :cols]
    gain_cols = first[:, cols:].astype(F32)
    in_gain, mid_gain = gain_cols[:, 0][None], gain_cols[:, 1][None]
    head_gains = gain_cols.reshape(count, block, HEAD)[:, :small, 2:4].reshape(HEAD, 2).T

    in_f = tok.astype(F32)
    x_all = (in_f * inv_rms(in_f) * in_gain).astype(BF16)
    qkv = mm(x_all, qkv_w, 1, 0)
    attended = attend(meta, qkv, seg_cols, seg_rows, cosine, sine, head_gains)
    half = 4 * quarter
    middle = own_tok.astype(F32) + reduce8(
        mm(attended[:half], out_w, 1, 1), mm(attended[half:], out_w, 1, 1), BF16
    )
    inverse_mid = inv_rms(middle)
    scaled_mid = middle * inverse_mid
    y_all = gather8((scaled_mid * mid_gain).astype(BF16))

    ff = gate_up_w.shape[1] // 2
    gate_up = mm(y_all, gate_up_w, 1, 0)
    gate, up_value = gate_up[:, :ff], gate_up[:, ff:]
    sig = jax.nn.sigmoid(gate)
    active = gate * sig
    hidden = (active * up_value).astype(BF16)
    down_grad = mm(cot, hidden, 0, 0).astype(BF16)
    mlp = reduce8(
        mm(hidden[:half], down_w, 1, 1), mm(hidden[half:], down_w, 1, 1).astype(BF16), BF16
    )

    def finish_rows(own):
        pair = jnp.stack([own, swap_core(own)])
        return flip_if(core == 1, pair, 0).reshape(tokens.shape)

    layer_out = finish_rows((middle + mlp).astype(BF16))

    grad_hidden = mm(cot, down_w, 1, 0)
    grad_up = (grad_hidden * active).astype(BF16)
    grad_gate = (grad_hidden * up_value * (sig * (1.0 + gate * (1.0 - sig)))).astype(BF16)
    grad_gate_up = jnp.concatenate([grad_gate, grad_up], axis=1)
    mid_grad = reduce8(
        mm(grad_gate_up[:half], gate_up_w, 1, 1),
        mm(grad_gate_up[half:], gate_up_w, 1, 1).astype(BF16),
        BF16,
    )
    gate_up_grad = mm(y_all, grad_gate_up, 0, 0).astype(BF16)

    mlp_gain_part = jnp.sum(mid_grad * scaled_mid, axis=0)
    grad_middle = own_cot.astype(F32) + norm_back(mid_grad, scaled_mid, inverse_mid, mid_gain)
    grad_attn = gather8(grad_middle.astype(BF16))
    out_grad = mm(grad_attn, attended, 0, 0).astype(BF16)
    grad_att = mm(grad_attn, out_w, 1, 0).astype(BF16)
    raw_grads, head_gain_parts = attend_back(
        meta, qkv, grad_att, seg_cols, seg_rows, cosine, sine, head_gains
    )
    first_grad = mm(x_all, raw_grads, 0, 0).astype(BF16)
    in_grad = reduce8(
        mm(raw_grads[:half], qkv_w, 1, 1),
        mm(raw_grads[half:], qkv_w, 1, 1).astype(BF16),
        BF16,
    )

    def owners(grad, sizes):
        mine_rows = scatter_line(grad).reshape(2, block, grad.shape[1])
        kept = lax.dynamic_index_in_dim(mine_rows, odd, 0, keepdims=False)
        sent = lax.dynamic_index_in_dim(mine_rows, 1 - odd, 0, keepdims=False)
        pair = flip_if(odd == 1, jnp.stack([kept, swap_x(sent)]), 0)
        four = flip_if(place == 1, jnp.stack([pair, swap_ctx(pair)]), 0)
        four = four.reshape(4, block, grad.shape[1])
        shares, start = [], 0
        for size in sizes:
            piece = four[:, :, start : start + size]
            shares.append(jnp.moveaxis(piece, 0, 1).reshape(block, 4 * size).astype(F32))
            start += size
        return shares

    (down_share,) = owners(down_grad, (ff,))
    gate_share, up_share = owners(gate_up_grad, (ff, ff))
    (out_share,) = owners(out_grad, (out_grad.shape[1],))
    query_share, key_share, value_share = owners(first_grad, (heads_q * HEAD, HEAD, HEAD))

    own_in = own_tok.astype(F32)
    inverse_in = inv_rms(own_in)
    scaled_in = own_in * inverse_in
    norm_gain_part = jnp.sum(in_grad * scaled_in, axis=0)
    token_grad = finish_rows(
        (grad_middle + norm_back(in_grad, scaled_in, inverse_in, in_gain)).astype(BF16)
    )

    parts = jnp.concatenate([norm_gain_part, mlp_gain_part, head_gain_parts.reshape(-1)])
    sums = lax.psum(parts, ("fsdp", "ctx", "tp"))
    norm_gain_grad = lax.dynamic_slice_in_dim(sums, mine * block, block, 0)
    mlp_gain_grad = lax.dynamic_slice_in_dim(sums, width + mine * block, block, 0)
    query_gain_grad = lax.dynamic_slice_in_dim(sums, 2 * width + mine * small, small, 0)
    key_gain_grad = lax.dynamic_slice_in_dim(sums, 2 * width + HEAD + mine * small, small, 0)
    return (
        layer_out,
        token_grad,
        norm_gain_grad,
        query_share,
        key_share,
        value_share,
        out_share,
        query_gain_grad,
        key_gain_grad,
        mlp_gain_grad,
        gate_share,
        up_share,
        down_share,
    )


def solution(mesh):
    in_specs = (
        P("fsdp", "ctx", None),
        P("fsdp", None),
        P("fsdp"),
        P("fsdp", "tp"),
        P("fsdp", "tp"),
        P("fsdp", "tp"),
        P("fsdp", "tp"),
        P("fsdp"),
        P("fsdp"),
        P("fsdp"),
        P("fsdp", "tp"),
        P("fsdp", "tp"),
        P("fsdp", "tp"),
        P("fsdp", "ctx", None),
    )
    out_specs = (
        P("fsdp", "ctx", None),
        P("fsdp", "ctx", None),
        P("fsdp"),
        P("fsdp", "tp"),
        P("fsdp", "tp"),
        P("fsdp", "tp"),
        P("fsdp", "tp"),
        P("fsdp"),
        P("fsdp"),
        P("fsdp"),
        P("fsdp", "tp"),
        P("fsdp", "tp"),
        P("fsdp", "tp"),
    )
    return jax.shard_map(body, mesh=mesh, in_specs=in_specs, out_specs=out_specs, check_vma=False)
```

```python
import functools
import math

import jax
import jax.numpy as jnp
from jax import lax
from jax.experimental import pallas as pl
from jax.experimental.pallas import tpu as pltpu
from jax.sharding import PartitionSpec as P


HEAD = 128
EPS = 1e-06
THETA = 1000000.0
MASKED = -1e30
MOST_DOC = 512
MESH = pl.DeviceIdType.MESH
F32 = jnp.float32
BF16 = jnp.bfloat16


def mm(left, right, left_dim, right_dim):
    return lax.dot_general(
        left, right, (((left_dim,), (right_dim,)), ((), ())), preferred_element_type=F32
    )


def swap_core(value):
    return lax.ppermute(value, "tp", [(0, 1), (1, 0)])


def swap_ctx(value):
    return lax.ppermute(value, "ctx", [(0, 1), (1, 0)])


def swap_x(value):
    count = lax.axis_size("fsdp")
    return lax.ppermute(value, "fsdp", [(i, i ^ 1) for i in range(count)])


def lines():
    count = lax.axis_size("fsdp")
    return [[i for i in range(count) if i % 2 == parity] for parity in (0, 1)]


def gather_line(value):
    return lax.all_gather(value, "fsdp", axis=0, tiled=True, axis_index_groups=lines())


def scatter_line(value):
    return lax.psum_scatter(
        value, "fsdp", scatter_dimension=0, tiled=True, axis_index_groups=lines()
    )


def flip_if(flag, value, axis):
    return jnp.where(flag, jnp.flip(value, axis), value)


def neighbours():
    mine = lax.axis_index("fsdp")
    return (
        {"fsdp": mine + 1 - 2 * lax.rem(mine, 2)},
        {"ctx": 1 - lax.axis_index("ctx")},
        {"tp": 1 - lax.axis_index("tp")},
    )


def greet(peers):
    barrier = pltpu.get_barrier_semaphore()
    for peer in peers:
        pl.semaphore_signal(barrier, inc=1, device_id=peer, device_id_type=MESH)
    pl.semaphore_wait(barrier, len(peers))


def remote_params(number, limit=None):
    return pltpu.CompilerParams(
        collective_id=number, has_side_effects=True, vmem_limit_bytes=limit
    )


def gather8_kernel(rows, own_ref, out_ref, send_sem, recv_sem, local_sem):
    x_peer, y_peer, c_peer = neighbours()
    greet((x_peer, y_peer, c_peer))

    def slot(away_t, half, outer, inner):
        return out_ref.at[pl.ds((away_t * 8 + half * 4 + outer * 2 + inner) * rows, rows)]

    number = iter(range(14))

    def send(source, target, peer):
        index = next(number)
        copy = pltpu.make_async_remote_copy(
            src_ref=source,
            dst_ref=target,
            send_sem=send_sem.at[index],
            recv_sem=recv_sem.at[index],
            device_id=peer,
            device_id_type=MESH,
        )
        copy.start()
        return copy

    first, second = own_ref.at[pl.ds(0, rows)], own_ref.at[pl.ds(rows, rows)]
    x1 = send(first, slot(0, 0, 0, 1), x_peer)
    y1 = send(second, slot(0, 1, 0, 1), y_peer)
    x2 = send(second, slot(0, 1, 1, 0), x_peer)
    y2 = send(first, slot(0, 0, 1, 0), y_peer)
    rest = [send(first, slot(1, 0, 0, 0), c_peer), send(second, slot(1, 1, 0, 0), c_peer)]
    kept = [
        pltpu.make_async_copy(first, slot(0, 0, 0, 0), local_sem.at[0]),
        pltpu.make_async_copy(second, slot(0, 1, 0, 0), local_sem.at[1]),
    ]
    for copy in kept:
        copy.start()
    x1.wait_recv()
    y3 = send(slot(0, 0, 0, 1), slot(0, 0, 1, 1), y_peer)
    y1.wait_recv()
    x3 = send(slot(0, 1, 0, 1), slot(0, 1, 1, 1), x_peer)
    rest.append(send(slot(0, 0, 0, 1), slot(1, 0, 0, 1), c_peer))
    rest.append(send(slot(0, 1, 0, 1), slot(1, 1, 0, 1), c_peer))
    x2.wait_recv()
    rest.append(send(slot(0, 1, 1, 0), slot(1, 1, 1, 0), c_peer))
    y2.wait_recv()
    rest.append(send(slot(0, 0, 1, 0), slot(1, 0, 1, 0), c_peer))
    y3.wait_recv()
    rest.append(send(slot(0, 0, 1, 1), slot(1, 0, 1, 1), c_peer))
    x3.wait_recv()
    rest.append(send(slot(0, 1, 1, 1), slot(1, 1, 1, 1), c_peer))
    for copy in (x1, y1, x2, y2, y3, x3):
        copy.wait_send()
    for copy in rest:
        copy.wait()
    for copy in kept:
        copy.wait()


def gather8(own):
    rows, width = own.shape[0] // 2, own.shape[1]
    return pl.pallas_call(
        functools.partial(gather8_kernel, rows),
        out_shape=jax.ShapeDtypeStruct((16 * rows, width), own.dtype),
        in_specs=[pl.BlockSpec(memory_space=pltpu.VMEM)],
        out_specs=pl.BlockSpec(memory_space=pl.ANY),
        scratch_shapes=[
            pltpu.SemaphoreType.DMA((14,)),
            pltpu.SemaphoreType.DMA((14,)),
            pltpu.SemaphoreType.DMA((2,)),
        ],
        compiler_params=remote_params(1),
        name="gather8",
    )(own)


def reduce8_kernel(
    rows,
    near_ref,
    far_ref,
    out_ref,
    near,
    core_in,
    link_in,
    link_out,
    send_sem,
    recv_sem,
    local_sem,
):
    x_peer, y_peer, c_peer = neighbours()
    greet((x_peer, y_peer, c_peer))
    order = [(h, o, i) for o, i in ((1, 1), (1, 0), (0, 1), (0, 0)) for h in (0, 1)]
    core_copies, local_copies = {}, {}
    for number, (half, outer, inner) in enumerate(order):
        place = pl.ds((half * 4 + outer * 2 + inner) * rows, rows)
        core_copies[half, outer, inner] = pltpu.make_async_remote_copy(
            src_ref=far_ref.at[place],
            dst_ref=core_in.at[place],
            send_sem=send_sem.at[number],
            recv_sem=recv_sem.at[number],
            device_id=c_peer,
            device_id_type=MESH,
        )
        local_copies[half, outer, inner] = pltpu.make_async_copy(
            near_ref.at[place], near.at[place], local_sem.at[number]
        )
    for block in order:
        core_copies[block].start()
        local_copies[block].start()

    def partial_sum(block):
        half, outer, inner = block
        place = pl.ds((half * 4 + outer * 2 + inner) * rows, rows)
        core_copies[block].wait_recv()
        local_copies[block].wait()
        return near[place, :] + core_in[place, :].astype(F32)

    def link(index, value, peer):
        link_out[index] = value.astype(BF16)
        copy = pltpu.make_async_remote_copy(
            src_ref=link_out.at[index],
            dst_ref=link_in.at[index],
            send_sem=send_sem.at[8 + index],
            recv_sem=recv_sem.at[8 + index],
            device_id=peer,
            device_id_type=MESH,
        )
        copy.start()
        return copy

    y11 = link(0, partial_sum((0, 1, 1)), y_peer)
    x11 = link(1, partial_sum((1, 1, 1)), x_peer)
    y10 = link(2, partial_sum((0, 1, 0)), y_peer)
    x10 = link(3, partial_sum((1, 1, 0)), x_peer)
    first01, second01 = partial_sum((0, 0, 1)), partial_sum((1, 0, 1))
    y11.wait_recv()
    x01 = link(4, first01 + link_in[0].astype(F32), x_peer)
    x11.wait_recv()
    y01 = link(5, second01 + link_in[1].astype(F32), y_peer)
    first = partial_sum((0, 0, 0))
    second = partial_sum((1, 0, 0))
    y10.wait_recv()
    out_ref[pl.ds(0, rows), :] = first + link_in[2].astype(F32)
    x10.wait_recv()
    out_ref[pl.ds(rows, rows), :] = second + link_in[3].astype(F32)
    x01.wait_recv()
    out_ref[pl.ds(0, rows), :] += link_in[4].astype(F32)
    y01.wait_recv()
    out_ref[pl.ds(rows, rows), :] += link_in[5].astype(F32)
    for copy in (y11, x11, y10, x10, x01, y01):
        copy.wait_send()
    for copy in core_copies.values():
        copy.wait_send()


def reduce8(near, far):
    rows, width = near.shape[0] // 8, near.shape[1]
    return pl.pallas_call(
        functools.partial(reduce8_kernel, rows),
        out_shape=jax.ShapeDtypeStruct((2 * rows, width), F32),
        in_specs=[pl.BlockSpec(memory_space=pl.ANY), pl.BlockSpec(memory_space=pl.ANY)],
        out_specs=pl.BlockSpec(memory_space=pltpu.VMEM),
        scratch_shapes=[
            pltpu.VMEM(near.shape, F32),
            pltpu.VMEM(near.shape, BF16),
            pltpu.VMEM((6, rows, width), BF16),
            pltpu.VMEM((6, rows, width), BF16),
            pltpu.SemaphoreType.DMA((14,)),
            pltpu.SemaphoreType.DMA((14,)),
            pltpu.SemaphoreType.DMA((8,)),
        ],
        compiler_params=remote_params(2, 48 * 1024 * 1024),
        name="reduce8",
    )(near, far)


def shard_kernel(plan, outs, *refs):
    ins, out_refs = refs[: len(plan)], refs[len(plan) : len(plan) + outs]
    stage = refs[len(plan) + outs : 2 * len(plan) + outs]
    send_sem, recv_sem, load_sem, store_sem = refs[2 * len(plan) + outs :]
    x_peer, _, _ = neighbours()
    odd = lax.rem(lax.axis_index("fsdp"), 2)
    column = 2 * lax.axis_index("ctx") + odd
    other = 2 * lax.axis_index("ctx") + 1 - odd
    greet((x_peer,))
    remote, loads, stores = [], [], []
    for number, (which, start, size, cut) in enumerate(plan):
        target = out_refs[which].at[odd, :, pl.ds(start, size)]

        def source(index, ref=ins[number], size=size, cut=cut):
            if not cut:
                return ref
            return ref.at[:, pl.ds(pl.multiple_of(index * size, HEAD), size)]

        remote.append(
            pltpu.make_async_remote_copy(
                src_ref=source(other),
                dst_ref=target,
                send_sem=send_sem.at[number],
                recv_sem=recv_sem.at[number],
                device_id=x_peer,
                device_id_type=MESH,
            )
        )
        loads.append(pltpu.make_async_copy(source(column), stage[number], load_sem.at[number]))
        stores.append(pltpu.make_async_copy(stage[number], target, store_sem.at[number]))
    for copy in remote:
        copy.start()
    for copy in loads:
        copy.start()
    for load, store in zip(loads, stores):
        load.wait()
        store.start()
    for copy in stores:
        copy.wait()
    for copy in remote:
        copy.wait()


def shards(groups, number):
    plan, arrays, shapes = [], [], []
    for which, group in enumerate(groups):
        start = 0
        for array, cut in group:
            size = array.shape[1] // 4 if cut else array.shape[1]
            plan.append((which, start, size, cut))
            arrays.append(array)
            start += size
        shapes.append((2, group[0][0].shape[0], start))
    hbm = pl.BlockSpec(memory_space=pl.ANY)
    pairs = pl.pallas_call(
        functools.partial(shard_kernel, tuple(plan), len(groups)),
        out_shape=[jax.ShapeDtypeStruct(shape, BF16) for shape in shapes],
        in_specs=[hbm] * len(arrays),
        out_specs=[hbm] * len(groups),
        scratch_shapes=[
            pltpu.VMEM((array.shape[0], size), BF16)
            for array, (_, _, size, _) in zip(arrays, plan)
        ]
        + [pltpu.SemaphoreType.DMA((len(plan),))] * 4,
        compiler_params=remote_params(number),
        name="shards",
    )(*arrays)
    return [pair.reshape(2 * pair.shape[1], pair.shape[2]) for pair in pairs]


def total_kernel(stages, part_ref, out_ref, inbox, outbox, send_sem, recv_sem):
    peers = []
    for axis, bit in stages:
        mine = lax.axis_index(axis)
        peers.append({axis: mine + bit * (1 - 2 * lax.rem(mine // bit, 2))})
    greet(peers)
    value = part_ref[...]
    copies = []
    for index, peer in enumerate(peers):
        outbox[index] = value
        copy = pltpu.make_async_remote_copy(
            src_ref=outbox.at[index],
            dst_ref=inbox.at[index],
            send_sem=send_sem.at[index],
            recv_sem=recv_sem.at[index],
            device_id=peer,
            device_id_type=MESH,
        )
        copy.start()
        copies.append(copy)
        copy.wait_recv()
        value = value + inbox[index]
    out_ref[...] = value
    for copy in copies:
        copy.wait_send()


def total(part):
    stages = [("tp", 1), ("ctx", 1)]
    bit = 1
    while bit < lax.axis_size("fsdp"):
        stages.append(("fsdp", bit))
        bit *= 2
    return pl.pallas_call(
        functools.partial(total_kernel, tuple(stages)),
        out_shape=jax.ShapeDtypeStruct(part.shape, F32),
        in_specs=[pl.BlockSpec(memory_space=pltpu.VMEM)],
        out_specs=pl.BlockSpec(memory_space=pltpu.VMEM),
        scratch_shapes=[
            pltpu.VMEM((len(stages),) + part.shape, F32),
            pltpu.VMEM((len(stages),) + part.shape, F32),
            pltpu.SemaphoreType.DMA((len(stages),)),
            pltpu.SemaphoreType.DMA((len(stages),)),
        ],
        compiler_params=remote_params(5),
        name="total",
    )(part)


def after(value, *others):
    return lax.optimization_barrier((value,) + others)[0]


def reduce4_links(total_rows, *others):
    rows = total_rows.shape[0] // 8
    first, second = total_rows[: 4 * rows], total_rows[4 * rows :]
    came_first = swap_ctx(first[2 * rows :].astype(BF16))
    came_second = swap_x(second[2 * rows :].astype(BF16))
    first = first[: 2 * rows] + after(came_first, *others).astype(F32)
    second = second[: 2 * rows] + after(came_second, *others).astype(F32)
    came_first = swap_x(first[rows:].astype(BF16))
    came_second = swap_ctx(second[rows:].astype(BF16))
    first = first[:rows] + came_first.astype(F32)
    second = second[:rows] + came_second.astype(F32)
    return jnp.concatenate([first, second])


def rope_tables(positions):
    freqs = THETA ** (-(jnp.arange(HEAD // 2, dtype=F32) * 2.0) / HEAD)
    angle = positions[:, None] * freqs[None, :]
    cosine = jnp.concatenate([jnp.cos(angle), jnp.cos(angle)], axis=-1)
    sine = jnp.concatenate([-jnp.sin(angle), jnp.sin(angle)], axis=-1)
    return cosine, sine


def norm_back(grad, scaled, inverse, gain):
    weighted = grad * gain
    return inverse * (weighted - scaled * jnp.mean(weighted * scaled, axis=-1, keepdims=True))


def inv_rms(value):
    return lax.rsqrt(jnp.mean(value * value, axis=-1, keepdims=True) + EPS)


def block_row(meta_ref, seq, index, rows):
    away_c = lax.rem(meta_ref[0] + index // 4, 2)
    away_t = lax.rem(meta_ref[1] + (index // 2) % 2, 2)
    if index % 2 == 0:
        inner = away_c * 2 + seq
    else:
        inner = seq * 2 + away_c + 4
    return pl.multiple_of((away_t * 8 + inner) * rows, rows)


def scaled_of(raw):
    inverse = lax.rsqrt(jnp.mean(raw * raw, axis=-1, keepdims=True) + EPS)
    return raw * inverse, inverse


def load_heads(meta_ref, qkv_ref, cos_ref, sin_ref, gain_ref, q_scr, k_scr, v_scr, heads):
    seq = pl.program_id(0)
    rows = q_scr.shape[1] // 8
    for index in range(8):
        start = block_row(meta_ref, seq, index, rows)
        here = slice(index * rows, (index + 1) * rows)
        cosine, sine = cos_ref[here, :], sin_ref[here, :]
        for head in range(heads + 1):
            raw = qkv_ref[pl.ds(start, rows), head * HEAD : (head + 1) * HEAD]
            scaled, _ = scaled_of(raw)
            which = 0 if head < heads else 1
            value = scaled * gain_ref[which : which + 1, :]
            turned = value * cosine + pltpu.roll(value, HEAD // 2, 1) * sine
            if head < heads:
                q_scr[head, here, :] = turned.astype(BF16)
            else:
                k_scr[here, :] = turned.astype(BF16)
        v_scr[here, :] = qkv_ref[
            pl.ds(start, rows), (heads + 1) * HEAD : (heads + 2) * HEAD
        ].astype(BF16)


def key_span(index, tile):
    low = max(0, (index * tile - (MOST_DOC - 1)) // tile) * tile
    return low, (index + 1) * tile


def allowed_mask(segc_ref, segr_ref, index, tile):
    low, high = key_span(index, tile)
    shape = (tile, high - low)
    rows = lax.broadcasted_iota(jnp.int32, shape, 0) + index * tile
    cols = lax.broadcasted_iota(jnp.int32, shape, 1) + low
    same = segc_ref[0, index * tile : (index + 1) * tile, :] == segr_ref[0, :, low:high]
    return same & (cols <= rows)


def probs_of(query, keys, allowed, scale):
    scores = jnp.where(allowed, mm(query, keys, 1, 1) * scale, MASKED)
    weights = jnp.exp(scores - jnp.max(scores, axis=-1, keepdims=True))
    return weights * (1.0 / jnp.sum(weights, axis=-1, keepdims=True))


def attend_kernel(
    heads, tile, meta_ref, qkv_ref, segc_ref, segr_ref, cos_ref, sin_ref, gain_ref, out_ref, q_scr, k_scr, v_scr
):
    seq = pl.program_id(0)
    length = k_scr.shape[0]
    rows = length // 8
    scale = 1.0 / math.sqrt(HEAD)
    load_heads(meta_ref, qkv_ref, cos_ref, sin_ref, gain_ref, q_scr, k_scr, v_scr, heads)
    for index in range(length // tile):
        low, high = key_span(index, tile)
        allowed = allowed_mask(segc_ref, segr_ref, index, tile)
        for head in range(heads):
            query = q_scr[head, index * tile : (index + 1) * tile, :]
            probs = probs_of(query, k_scr[low:high, :], allowed, scale)
            mixed = mm(probs.astype(BF16), v_scr[low:high, :], 1, 0).astype(BF16)
            for piece in range(tile // rows):
                start = block_row(meta_ref, seq, index * (tile // rows) + piece, rows)
                out_ref[pl.ds(start, rows), head * HEAD : (head + 1) * HEAD] = mixed[
                    piece * rows : (piece + 1) * rows
                ]


def attend_back_kernel(
    heads,
    tile,
    meta_ref,
    qkv_ref,
    grad_ref,
    segc_ref,
    segr_ref,
    cos_ref,
    sin_ref,
    gain_ref,
    out_ref,
    gain_out_ref,
    q_scr,
    k_scr,
    v_scr,
    g_scr,
    dk_scr,
    dv_scr,
):
    seq = pl.program_id(0)
    length = k_scr.shape[0]
    rows = length // 8
    scale = 1.0 / math.sqrt(HEAD)
    load_heads(meta_ref, qkv_ref, cos_ref, sin_ref, gain_ref, q_scr, k_scr, v_scr, heads)
    for index in range(8):
        start = block_row(meta_ref, seq, index, rows)
        g_scr[index * rows : (index + 1) * rows, :] = grad_ref[pl.ds(start, rows), :]
    dk_scr[...] = jnp.zeros_like(dk_scr)
    dv_scr[...] = jnp.zeros_like(dv_scr)

    @pl.when(seq == 0)
    def _():
        gain_out_ref[...] = jnp.zeros_like(gain_out_ref)

    def finish(grad, index, head, which):
        here = slice(index * rows, (index + 1) * rows)
        start = block_row(meta_ref, seq, index, rows)
        grad = grad * cos_ref[here, :] - pltpu.roll(grad, HEAD // 2, 1) * sin_ref[here, :]
        raw = qkv_ref[pl.ds(start, rows), head * HEAD : (head + 1) * HEAD]
        scaled, inverse = scaled_of(raw)
        gain_out_ref[which : which + 1, :] += jnp.sum(grad * scaled, axis=0, keepdims=True)
        out = norm_back(grad, scaled, inverse, gain_ref[which : which + 1, :])
        out_ref[pl.ds(start, rows), head * HEAD : (head + 1) * HEAD] = out.astype(BF16)

    per = tile // rows
    for index in range(length // tile):
        low, high = key_span(index, tile)
        mine = slice(index * tile, (index + 1) * tile)
        allowed = allowed_mask(segc_ref, segr_ref, index, tile)
        for head in range(heads):
            query = q_scr[head, mine, :]
            keys = k_scr[low:high, :]
            probs = probs_of(query, keys, allowed, scale)
            grad = g_scr[mine, head * HEAD : (head + 1) * HEAD]
            grad_probs = mm(grad, v_scr[low:high, :], 1, 1)
            delta = jnp.sum(probs * grad_probs, axis=-1, keepdims=True)
            grad_scores = (probs * (grad_probs - delta)).astype(BF16)
            dv_scr[low:high, :] += mm(probs.astype(BF16), grad, 0, 0)
            dk_scr[low:high, :] += mm(grad_scores, query, 0, 0) * scale
            grad_query = mm(grad_scores, keys, 1, 0) * scale
            for piece in range(per):
                finish(
                    grad_query[piece * rows : (piece + 1) * rows], index * per + piece, head, 0
                )
    for index in range(8):
        here = slice(index * rows, (index + 1) * rows)
        start = block_row(meta_ref, seq, index, rows)
        finish(dk_scr[here, :], index, heads, 1)
        out_ref[pl.ds(start, rows), (heads + 1) * HEAD : (heads + 2) * HEAD] = dv_scr[
            here, :
        ].astype(BF16)


def whole(shape):
    return pl.BlockSpec(shape, lambda seq, meta: (0,) * len(shape))


def seg_specs(length):
    return [
        pl.BlockSpec((1, length, 1), lambda seq, meta: (seq, 0, 0)),
        pl.BlockSpec((1, 1, length), lambda seq, meta: (seq, 0, 0)),
    ]


def attend(meta, qkv, seg_cols, seg_rows, cosine, sine, gains):
    length = cosine.shape[0]
    tile = length // 4
    heads = qkv.shape[1] // HEAD - 2
    pairs = 2 * heads * length * length // 2
    return pl.pallas_call(
        functools.partial(attend_kernel, heads, tile),
        out_shape=jax.ShapeDtypeStruct((qkv.shape[0], heads * HEAD), BF16),
        grid_spec=pltpu.PrefetchScalarGridSpec(
            num_scalar_prefetch=1,
            grid=(2,),
            in_specs=[whole(qkv.shape)]
            + seg_specs(length)
            + [whole(cosine.shape), whole(sine.shape), whole(gains.shape)],
            out_specs=whole((qkv.shape[0], heads * HEAD)),
            scratch_shapes=[
                pltpu.VMEM((heads, length, HEAD), BF16),
                pltpu.VMEM((length, HEAD), BF16),
                pltpu.VMEM((length, HEAD), BF16),
            ],
        ),
        cost_estimate=pl.CostEstimate(
            flops=4 * pairs * HEAD, bytes_accessed=qkv.size * 4 + qkv.size, transcendentals=pairs
        ),
        name="attend",
    )(meta, qkv, seg_cols, seg_rows, cosine, sine, gains)


def attend_back(meta, qkv, grad, seg_cols, seg_rows, cosine, sine, gains):
    length = cosine.shape[0]
    tile = length // 4
    heads = qkv.shape[1] // HEAD - 2
    pairs = 2 * heads * length * length // 2
    return pl.pallas_call(
        functools.partial(attend_back_kernel, heads, tile),
        out_shape=(
            jax.ShapeDtypeStruct(qkv.shape, BF16),
            jax.ShapeDtypeStruct(gains.shape, F32),
        ),
        grid_spec=pltpu.PrefetchScalarGridSpec(
            num_scalar_prefetch=1,
            grid=(2,),
            in_specs=[whole(qkv.shape), whole(grad.shape)]
            + seg_specs(length)
            + [whole(cosine.shape), whole(sine.shape), whole(gains.shape)],
            out_specs=(whole(qkv.shape), whole(gains.shape)),
            scratch_shapes=[
                pltpu.VMEM((heads, length, HEAD), BF16),
                pltpu.VMEM((length, HEAD), BF16),
                pltpu.VMEM((length, HEAD), BF16),
                pltpu.VMEM((length, heads * HEAD), BF16),
                pltpu.VMEM((length, HEAD), F32),
                pltpu.VMEM((length, HEAD), F32),
            ],
        ),
        cost_estimate=pl.CostEstimate(
            flops=10 * pairs * HEAD, bytes_accessed=qkv.size * 8, transcendentals=pairs
        ),
        name="attend_back",
    )(meta, qkv, grad, seg_cols, seg_rows, cosine, sine, gains)


def body(
    tokens,
    segment_ids,
    norm_gain,
    query_weight,
    key_matrix,
    value_matrix,
    output_weight,
    query_gain,
    key_gain,
    mlp_gain,
    gate_weight,
    up_weight,
    down_weight,
    cotangent,
):
    local, width = tokens.shape[1], tokens.shape[2]
    length = 2 * local
    quarter = local // 2
    count = lax.axis_size("fsdp")
    block = width // count
    mine = lax.axis_index("fsdp")
    odd = mine % 2
    place = lax.axis_index("ctx")
    core = lax.axis_index("tp")

    small = query_gain.shape[0]
    lanes = jnp.arange(HEAD)[None, :]

    def pad_rows(vector):
        return jnp.concatenate([vector, jnp.zeros((block - small,), BF16)])

    gains = jnp.where(
        lanes == 0,
        norm_gain[:, None],
        jnp.where(
            lanes == 1,
            mlp_gain[:, None],
            jnp.where(
                lanes == 2, pad_rows(query_gain)[:, None], pad_rows(key_gain)[:, None]
            ),
        ),
    )
    (first_pair,) = shards(
        [
            [
                (query_weight, True),
                (key_matrix, True),
                (value_matrix, True),
                (output_weight, True),
                (gains, False),
            ]
        ],
        3,
    )
    first = gather_line(first_pair)
    gate_up_pair, down_pair = shards(
        [
            [(after(gate_weight, first_pair), True), (up_weight, True)],
            [(down_weight, True)],
        ],
        4,
    )
    gate_up_w = gather_line(gate_up_pair)
    down_w = gather_line(down_pair)

    def own_quarter(value):
        return lax.dynamic_slice_in_dim(value.reshape(local, width), core * quarter, quarter, 0)

    own_tok, own_cot = own_quarter(tokens), own_quarter(cotangent)
    tok = gather8(after(own_tok, gate_up_pair))
    segments = jnp.concatenate([segment_ids, swap_x(segment_ids)])
    seg_cols, seg_rows = segments[:, :, None], segments[:, None, :]
    cosine, sine = rope_tables(jnp.arange(length).astype(F32))
    meta = jnp.stack([place, core]).astype(jnp.int32)

    heads_q = query_weight.shape[1] // 4 // HEAD
    cols = (heads_q + 2) * HEAD
    qkv_w = first[:, :cols]
    out_w = first[:, cols : cols + heads_q * HEAD]
    gain_cols = first[:, cols + heads_q * HEAD :].astype(F32)
    in_gain, mid_gain = gain_cols[:, 0][None], gain_cols[:, 1][None]
    head_gains = gain_cols.reshape(count, block, HEAD)[:, :small, 2:4].reshape(HEAD, 2).T

    in_f = tok.astype(F32)
    inverse_all = inv_rms(in_f)
    cot = gather8(after(own_cot, inverse_all))
    x_all = (in_f * inverse_all * in_gain).astype(BF16)
    qkv = mm(x_all, qkv_w, 1, 0)
    attended = attend(meta, qkv, seg_cols, seg_rows, cosine, sine, head_gains)
    half = 4 * quarter
    middle = own_tok.astype(F32) + reduce8(
        mm(attended[:half], out_w, 1, 1), mm(attended[half:], out_w, 1, 1).astype(BF16)
    )
    inverse_mid = inv_rms(middle)
    scaled_mid = middle * inverse_mid
    y_all = gather8((scaled_mid * mid_gain).astype(BF16))

    ff = gate_up_w.shape[1] // 2
    gate_up = mm(y_all, gate_up_w, 1, 0)
    gate, up_value = gate_up[:, :ff], gate_up[:, ff:]
    sig = jax.nn.sigmoid(gate)
    active = gate * sig
    hidden = (active * up_value).astype(BF16)
    down_grad = mm(cot, hidden, 0, 0).astype(BF16)

    def finish_rows(own):
        pair = jnp.stack([own, swap_core(own)])
        return flip_if(core == 1, pair, 0).reshape(tokens.shape)

    grad_hidden = mm(after(cot, down_grad), down_w, 1, 0)
    grad_up = (grad_hidden * active).astype(BF16)
    grad_gate = (grad_hidden * up_value * (sig * (1.0 + gate * (1.0 - sig)))).astype(BF16)
    grad_gate_up = jnp.concatenate([grad_gate, grad_up], axis=1)
    gate_up_grad = mm(y_all, grad_gate_up, 0, 0).astype(BF16)
    mid_near = mm(grad_gate_up[:half], gate_up_w, 1, 1)
    mid_far = mm(grad_gate_up[half:], gate_up_w, 1, 1).astype(BF16)
    mid_grad = reduce8(mid_near, after(mid_far, gate_up_grad))

    mlp_gain_part = jnp.sum(mid_grad * scaled_mid, axis=0)
    grad_middle = own_cot.astype(F32) + norm_back(mid_grad, scaled_mid, inverse_mid, mid_gain)
    grad_attn = gather8(grad_middle.astype(BF16))
    out_grad = mm(grad_attn, attended, 0, 0).astype(BF16)
    grad_att = mm(grad_attn, out_w, 1, 0).astype(BF16)
    mlp_hidden = after(hidden, grad_attn)
    mlp_far = mm(mlp_hidden[half:], down_w, 1, 1).astype(BF16)
    mlp_came = swap_core(mlp_far)
    mlp_rows = mm(mlp_hidden[:half], down_w, 1, 1) + mlp_came.astype(F32)
    raw_grads, head_gain_parts = attend_back(
        meta, qkv, after(grad_att, mlp_rows), seg_cols, seg_rows, cosine, sine, head_gains
    )
    first_grad = mm(x_all, raw_grads, 0, 0).astype(BF16)
    mlp = reduce4_links(mlp_rows, raw_grads)
    layer_out = finish_rows((middle + mlp).astype(BF16))
    in_near = mm(raw_grads[:half], qkv_w, 1, 1)
    in_far = mm(raw_grads[half:], qkv_w, 1, 1).astype(BF16)
    in_grad = reduce8(in_near, after(in_far, first_grad))

    def owners(grad, sizes, *others):
        rows = scatter_line(grad)
        rows = after(rows, *others).reshape(2, block, grad.shape[1])
        kept = lax.dynamic_index_in_dim(rows, odd, 0, keepdims=False)
        sent = lax.dynamic_index_in_dim(rows, 1 - odd, 0, keepdims=False)
        came = swap_x(sent)
        pair = flip_if(odd == 1, jnp.stack([kept, came]), 0)
        far = swap_ctx(pair)
        four = flip_if(place == 1, jnp.stack([pair, far]), 0)
        four = four.reshape(4, block, grad.shape[1])
        shares, start = [], 0
        for size in sizes:
            piece = four[:, :, start : start + size]
            shares.append(jnp.moveaxis(piece, 0, 1).reshape(block, 4 * size).astype(F32))
            start += size
        return shares

    (down_share,) = owners(down_grad, (ff,), grad_attn)
    gate_share, up_share = owners(gate_up_grad, (ff, ff), raw_grads)
    (out_share,) = owners(out_grad, (out_grad.shape[1],), raw_grads)
    query_share, key_share, value_share = owners(first_grad, (heads_q * HEAD, HEAD, HEAD))

    own_in = own_tok.astype(F32)
    inverse_in = inv_rms(own_in)
    scaled_in = own_in * inverse_in
    norm_gain_part = jnp.sum(in_grad * scaled_in, axis=0)
    token_grad = finish_rows(
        (grad_middle + norm_back(in_grad, scaled_in, inverse_in, in_gain)).astype(BF16)
    )

    parts = jnp.concatenate([norm_gain_part, mlp_gain_part, head_gain_parts.reshape(-1)])
    sums = total(parts.reshape(-1, HEAD)).reshape(-1)
    norm_gain_grad = lax.dynamic_slice_in_dim(sums, mine * block, block, 0)
    mlp_gain_grad = lax.dynamic_slice_in_dim(sums, width + mine * block, block, 0)
    query_gain_grad = lax.dynamic_slice_in_dim(sums, 2 * width + mine * small, small, 0)
    key_gain_grad = lax.dynamic_slice_in_dim(sums, 2 * width + HEAD + mine * small, small, 0)
    return (
        layer_out,
        token_grad,
        norm_gain_grad,
        query_share,
        key_share,
        value_share,
        out_share,
        query_gain_grad,
        key_gain_grad,
        mlp_gain_grad,
        gate_share,
        up_share,
        down_share,
    )


def solution(mesh):
    in_specs = (
        P("fsdp", "ctx", None),
        P("fsdp", None),
        P("fsdp"),
        P("fsdp", "tp"),
        P("fsdp", "tp"),
        P("fsdp", "tp"),
        P("fsdp", "tp"),
        P("fsdp"),
        P("fsdp"),
        P("fsdp"),
        P("fsdp", "tp"),
        P("fsdp", "tp"),
        P("fsdp", "tp"),
        P("fsdp", "ctx", None),
    )
    out_specs = (
        P("fsdp", "ctx", None),
        P("fsdp", "ctx", None),
        P("fsdp"),
        P("fsdp", "tp"),
        P("fsdp", "tp"),
        P("fsdp", "tp"),
        P("fsdp", "tp"),
        P("fsdp"),
        P("fsdp"),
        P("fsdp"),
        P("fsdp", "tp"),
        P("fsdp", "tp"),
        P("fsdp", "tp"),
    )

    return jax.shard_map(body, mesh=mesh, in_specs=in_specs, out_specs=out_specs, check_vma=False)
```

```python
import functools
import math

import jax
import jax.numpy as jnp
from jax import lax
from jax.experimental import pallas as pl
from jax.experimental.pallas import tpu as pltpu
from jax.sharding import PartitionSpec as P


HEAD = 128
EPS = 1e-06
THETA = 1000000.0
MASKED = -1e30
MOST_DOC = 512
MESH = pl.DeviceIdType.MESH
F32 = jnp.float32
BF16 = jnp.bfloat16


def mm(left, right, left_dim, right_dim):
    return lax.dot_general(
        left, right, (((left_dim,), (right_dim,)), ((), ())), preferred_element_type=F32
    )


def swap_core(value):
    return lax.ppermute(value, "tp", [(0, 1), (1, 0)])


def swap_ctx(value):
    return lax.ppermute(value, "ctx", [(0, 1), (1, 0)])


def swap_x(value):
    count = lax.axis_size("fsdp")
    return lax.ppermute(value, "fsdp", [(i, i ^ 1) for i in range(count)])


def lines():
    count = lax.axis_size("fsdp")
    return [[i for i in range(count) if i % 2 == parity] for parity in (0, 1)]


def gather_line(value):
    return lax.all_gather(value, "fsdp", axis=0, tiled=True, axis_index_groups=lines())


def scatter_line(value):
    return lax.psum_scatter(
        value, "fsdp", scatter_dimension=0, tiled=True, axis_index_groups=lines()
    )


def flip_if(flag, value, axis):
    return jnp.where(flag, jnp.flip(value, axis), value)


def neighbours():
    mine = lax.axis_index("fsdp")
    return (
        {"fsdp": mine + 1 - 2 * lax.rem(mine, 2)},
        {"ctx": 1 - lax.axis_index("ctx")},
        {"tp": 1 - lax.axis_index("tp")},
    )


def greet(peers):
    barrier = pltpu.get_barrier_semaphore()
    for peer in peers:
        pl.semaphore_signal(barrier, inc=1, device_id=peer, device_id_type=MESH)
    pl.semaphore_wait(barrier, len(peers))


def remote_params(number, limit=None):
    return pltpu.CompilerParams(
        collective_id=number, has_side_effects=True, vmem_limit_bytes=limit
    )


def gather8_kernel(rows, own_ref, out_ref, send_sem, recv_sem, local_sem):
    x_peer, y_peer, c_peer = neighbours()
    greet((x_peer, y_peer, c_peer))

    def slot(away_t, half, outer, inner):
        return out_ref.at[pl.ds((away_t * 8 + half * 4 + outer * 2 + inner) * rows, rows)]

    number = iter(range(14))

    def send(source, target, peer):
        index = next(number)
        copy = pltpu.make_async_remote_copy(
            src_ref=source,
            dst_ref=target,
            send_sem=send_sem.at[index],
            recv_sem=recv_sem.at[index],
            device_id=peer,
            device_id_type=MESH,
        )
        copy.start()
        return copy

    first, second = own_ref.at[pl.ds(0, rows)], own_ref.at[pl.ds(rows, rows)]
    x1 = send(first, slot(0, 0, 0, 1), x_peer)
    y1 = send(second, slot(0, 1, 0, 1), y_peer)
    x2 = send(second, slot(0, 1, 1, 0), x_peer)
    y2 = send(first, slot(0, 0, 1, 0), y_peer)
    rest = [send(first, slot(1, 0, 0, 0), c_peer), send(second, slot(1, 1, 0, 0), c_peer)]
    kept = [
        pltpu.make_async_copy(first, slot(0, 0, 0, 0), local_sem.at[0]),
        pltpu.make_async_copy(second, slot(0, 1, 0, 0), local_sem.at[1]),
    ]
    for copy in kept:
        copy.start()
    x1.wait_recv()
    y3 = send(slot(0, 0, 0, 1), slot(0, 0, 1, 1), y_peer)
    y1.wait_recv()
    x3 = send(slot(0, 1, 0, 1), slot(0, 1, 1, 1), x_peer)
    rest.append(send(slot(0, 0, 0, 1), slot(1, 0, 0, 1), c_peer))
    rest.append(send(slot(0, 1, 0, 1), slot(1, 1, 0, 1), c_peer))
    x2.wait_recv()
    rest.append(send(slot(0, 1, 1, 0), slot(1, 1, 1, 0), c_peer))
    y2.wait_recv()
    rest.append(send(slot(0, 0, 1, 0), slot(1, 0, 1, 0), c_peer))
    y3.wait_recv()
    rest.append(send(slot(0, 0, 1, 1), slot(1, 0, 1, 1), c_peer))
    x3.wait_recv()
    rest.append(send(slot(0, 1, 1, 1), slot(1, 1, 1, 1), c_peer))
    for copy in (x1, y1, x2, y2, y3, x3):
        copy.wait_send()
    for copy in rest:
        copy.wait()
    for copy in kept:
        copy.wait()


def gather8(own):
    rows, width = own.shape[0] // 2, own.shape[1]
    return pl.pallas_call(
        functools.partial(gather8_kernel, rows),
        out_shape=jax.ShapeDtypeStruct((16 * rows, width), own.dtype),
        in_specs=[pl.BlockSpec(memory_space=pltpu.VMEM)],
        out_specs=pl.BlockSpec(memory_space=pl.ANY),
        scratch_shapes=[
            pltpu.SemaphoreType.DMA((14,)),
            pltpu.SemaphoreType.DMA((14,)),
            pltpu.SemaphoreType.DMA((2,)),
        ],
        compiler_params=remote_params(1),
        name="gather8",
    )(own)


def reduce8_kernel(
    rows,
    near_ref,
    far_ref,
    out_ref,
    near,
    core_in,
    link_in,
    link_out,
    send_sem,
    recv_sem,
    local_sem,
):
    x_peer, y_peer, c_peer = neighbours()
    greet((x_peer, y_peer, c_peer))
    order = [(h, o, i) for o, i in ((1, 1), (1, 0), (0, 1), (0, 0)) for h in (0, 1)]
    core_copies, local_copies = {}, {}
    for number, (half, outer, inner) in enumerate(order):
        place = pl.ds((half * 4 + outer * 2 + inner) * rows, rows)
        core_copies[half, outer, inner] = pltpu.make_async_remote_copy(
            src_ref=far_ref.at[place],
            dst_ref=core_in.at[place],
            send_sem=send_sem.at[number],
            recv_sem=recv_sem.at[number],
            device_id=c_peer,
            device_id_type=MESH,
        )
        local_copies[half, outer, inner] = pltpu.make_async_copy(
            near_ref.at[place], near.at[place], local_sem.at[number]
        )
    for block in order:
        core_copies[block].start()
        local_copies[block].start()

    def partial_sum(block):
        half, outer, inner = block
        place = pl.ds((half * 4 + outer * 2 + inner) * rows, rows)
        core_copies[block].wait_recv()
        local_copies[block].wait()
        return near[place, :] + core_in[place, :].astype(F32)

    def link(index, value, peer):
        link_out[index] = value.astype(BF16)
        copy = pltpu.make_async_remote_copy(
            src_ref=link_out.at[index],
            dst_ref=link_in.at[index],
            send_sem=send_sem.at[8 + index],
            recv_sem=recv_sem.at[8 + index],
            device_id=peer,
            device_id_type=MESH,
        )
        copy.start()
        return copy

    y11 = link(0, partial_sum((0, 1, 1)), y_peer)
    x11 = link(1, partial_sum((1, 1, 1)), x_peer)
    y10 = link(2, partial_sum((0, 1, 0)), y_peer)
    x10 = link(3, partial_sum((1, 1, 0)), x_peer)
    first01, second01 = partial_sum((0, 0, 1)), partial_sum((1, 0, 1))
    y11.wait_recv()
    x01 = link(4, first01 + link_in[0].astype(F32), x_peer)
    x11.wait_recv()
    y01 = link(5, second01 + link_in[1].astype(F32), y_peer)
    first = partial_sum((0, 0, 0))
    second = partial_sum((1, 0, 0))
    y10.wait_recv()
    out_ref[pl.ds(0, rows), :] = first + link_in[2].astype(F32)
    x10.wait_recv()
    out_ref[pl.ds(rows, rows), :] = second + link_in[3].astype(F32)
    x01.wait_recv()
    out_ref[pl.ds(0, rows), :] += link_in[4].astype(F32)
    y01.wait_recv()
    out_ref[pl.ds(rows, rows), :] += link_in[5].astype(F32)
    for copy in (y11, x11, y10, x10, x01, y01):
        copy.wait_send()
    for copy in core_copies.values():
        copy.wait_send()


def reduce8(near, far):
    rows, width = near.shape[0] // 8, near.shape[1]
    return pl.pallas_call(
        functools.partial(reduce8_kernel, rows),
        out_shape=jax.ShapeDtypeStruct((2 * rows, width), F32),
        in_specs=[pl.BlockSpec(memory_space=pl.ANY), pl.BlockSpec(memory_space=pl.ANY)],
        out_specs=pl.BlockSpec(memory_space=pltpu.VMEM),
        scratch_shapes=[
            pltpu.VMEM(near.shape, F32),
            pltpu.VMEM(near.shape, BF16),
            pltpu.VMEM((6, rows, width), BF16),
            pltpu.VMEM((6, rows, width), BF16),
            pltpu.SemaphoreType.DMA((14,)),
            pltpu.SemaphoreType.DMA((14,)),
            pltpu.SemaphoreType.DMA((8,)),
        ],
        compiler_params=remote_params(2, 48 * 1024 * 1024),
        name="reduce8",
    )(near, far)


def shard_kernel(plan, outs, *refs):
    ins, out_refs = refs[: len(plan)], refs[len(plan) : len(plan) + outs]
    stage = refs[len(plan) + outs : 2 * len(plan) + outs]
    send_sem, recv_sem, load_sem, store_sem = refs[2 * len(plan) + outs :]
    x_peer, _, _ = neighbours()
    odd = lax.rem(lax.axis_index("fsdp"), 2)
    column = 2 * lax.axis_index("ctx") + odd
    other = 2 * lax.axis_index("ctx") + 1 - odd
    greet((x_peer,))
    remote, loads, stores = [], [], []
    for number, (which, start, size, cut) in enumerate(plan):
        target = out_refs[which].at[odd, :, pl.ds(start, size)]

        def source(index, ref=ins[number], size=size, cut=cut):
            if not cut:
                return ref
            return ref.at[:, pl.ds(pl.multiple_of(index * size, HEAD), size)]

        remote.append(
            pltpu.make_async_remote_copy(
                src_ref=source(other),
                dst_ref=target,
                send_sem=send_sem.at[number],
                recv_sem=recv_sem.at[number],
                device_id=x_peer,
                device_id_type=MESH,
            )
        )
        loads.append(pltpu.make_async_copy(source(column), stage[number], load_sem.at[number]))
        stores.append(pltpu.make_async_copy(stage[number], target, store_sem.at[number]))
    for copy in remote:
        copy.start()
    for copy in loads:
        copy.start()
    for load, store in zip(loads, stores):
        load.wait()
        store.start()
    for copy in stores:
        copy.wait()
    for copy in remote:
        copy.wait()


def shards(groups, number):
    plan, arrays, shapes = [], [], []
    for which, group in enumerate(groups):
        start = 0
        for array, cut in group:
            size = array.shape[1] // 4 if cut else array.shape[1]
            plan.append((which, start, size, cut))
            arrays.append(array)
            start += size
        shapes.append((2, group[0][0].shape[0], start))
    hbm = pl.BlockSpec(memory_space=pl.ANY)
    pairs = pl.pallas_call(
        functools.partial(shard_kernel, tuple(plan), len(groups)),
        out_shape=[jax.ShapeDtypeStruct(shape, BF16) for shape in shapes],
        in_specs=[hbm] * len(arrays),
        out_specs=[hbm] * len(groups),
        scratch_shapes=[
            pltpu.VMEM((array.shape[0], size), BF16)
            for array, (_, _, size, _) in zip(arrays, plan)
        ]
        + [pltpu.SemaphoreType.DMA((len(plan),))] * 4,
        compiler_params=remote_params(number),
        name="shards",
    )(*arrays)
    return [pair.reshape(2 * pair.shape[1], pair.shape[2]) for pair in pairs]


def total_kernel(stages, part_ref, out_ref, inbox, outbox, send_sem, recv_sem):
    peers = []
    for axis, bit in stages:
        mine = lax.axis_index(axis)
        peers.append({axis: mine + bit * (1 - 2 * lax.rem(mine // bit, 2))})
    greet(peers)
    value = part_ref[...]
    copies = []
    for index, peer in enumerate(peers):
        outbox[index] = value
        copy = pltpu.make_async_remote_copy(
            src_ref=outbox.at[index],
            dst_ref=inbox.at[index],
            send_sem=send_sem.at[index],
            recv_sem=recv_sem.at[index],
            device_id=peer,
            device_id_type=MESH,
        )
        copy.start()
        copies.append(copy)
        copy.wait_recv()
        value = value + inbox[index]
    out_ref[...] = value
    for copy in copies:
        copy.wait_send()


def total(part):
    stages = [("tp", 1), ("ctx", 1)]
    bit = 1
    while bit < lax.axis_size("fsdp"):
        stages.append(("fsdp", bit))
        bit *= 2
    return pl.pallas_call(
        functools.partial(total_kernel, tuple(stages)),
        out_shape=jax.ShapeDtypeStruct(part.shape, F32),
        in_specs=[pl.BlockSpec(memory_space=pltpu.VMEM)],
        out_specs=pl.BlockSpec(memory_space=pltpu.VMEM),
        scratch_shapes=[
            pltpu.VMEM((len(stages),) + part.shape, F32),
            pltpu.VMEM((len(stages),) + part.shape, F32),
            pltpu.SemaphoreType.DMA((len(stages),)),
            pltpu.SemaphoreType.DMA((len(stages),)),
        ],
        compiler_params=remote_params(5),
        name="total",
    )(part)


def join_kernel(sizes, spot_ref, kept_ref, x_ref, y_ref, both_ref, *out_refs):
    place, odd = spot_ref[0], spot_ref[1]
    parts = (
        (kept_ref, 2 * place + odd),
        (x_ref, 2 * place + 1 - odd),
        (y_ref, 2 - 2 * place + odd),
        (both_ref, 3 - 2 * place - odd),
    )
    for part, column in parts:
        start = 0
        for size, out_ref in zip(sizes, out_refs):
            target = pl.ds(pl.multiple_of(column * size, HEAD), size)
            out_ref[:, target] = part[:, start : start + size].astype(F32)
            start += size


def join_columns(spot, parts, sizes):
    rows = parts[0].shape[0]
    tile = min(rows, 64)
    return pl.pallas_call(
        functools.partial(join_kernel, sizes),
        out_shape=[jax.ShapeDtypeStruct((rows, 4 * size), F32) for size in sizes],
        grid_spec=pltpu.PrefetchScalarGridSpec(
            num_scalar_prefetch=1,
            grid=(rows // tile,),
            in_specs=[
                pl.BlockSpec((tile, part.shape[1]), lambda i, spot: (i, 0)) for part in parts
            ],
            out_specs=[pl.BlockSpec((tile, 4 * size), lambda i, spot: (i, 0)) for size in sizes],
        ),
        name="join",
    )(spot, *parts)


def after(value, *others):
    return lax.optimization_barrier((value,) + others)[0]


def reduce4_links(total_rows, *others):
    rows = total_rows.shape[0] // 8
    first, second = total_rows[: 4 * rows], total_rows[4 * rows :]
    came_first = swap_ctx(first[2 * rows :].astype(BF16))
    came_second = swap_x(second[2 * rows :].astype(BF16))
    first = first[: 2 * rows] + after(came_first, *others).astype(F32)
    second = second[: 2 * rows] + after(came_second, *others).astype(F32)
    came_first = swap_x(first[rows:].astype(BF16))
    came_second = swap_ctx(second[rows:].astype(BF16))
    first = first[:rows] + came_first.astype(F32)
    second = second[:rows] + came_second.astype(F32)
    return jnp.concatenate([first, second])


def rope_tables(positions):
    freqs = THETA ** (-(jnp.arange(HEAD // 2, dtype=F32) * 2.0) / HEAD)
    angle = positions[:, None] * freqs[None, :]
    cosine = jnp.concatenate([jnp.cos(angle), jnp.cos(angle)], axis=-1)
    sine = jnp.concatenate([-jnp.sin(angle), jnp.sin(angle)], axis=-1)
    return cosine, sine


def norm_back(grad, scaled, inverse, gain):
    weighted = grad * gain
    return inverse * (weighted - scaled * jnp.mean(weighted * scaled, axis=-1, keepdims=True))


def inv_rms(value):
    return lax.rsqrt(jnp.mean(value * value, axis=-1, keepdims=True) + EPS)


def block_row(meta_ref, seq, index, rows):
    away_c = lax.rem(meta_ref[0] + index // 4, 2)
    away_t = lax.rem(meta_ref[1] + (index // 2) % 2, 2)
    if index % 2 == 0:
        inner = away_c * 2 + seq
    else:
        inner = seq * 2 + away_c + 4
    return pl.multiple_of((away_t * 8 + inner) * rows, rows)


def scaled_of(raw):
    inverse = lax.rsqrt(jnp.mean(raw * raw, axis=-1, keepdims=True) + EPS)
    return raw * inverse, inverse


def load_heads(meta_ref, qkv_ref, cos_ref, sin_ref, gain_ref, q_scr, k_scr, v_scr, heads):
    seq = pl.program_id(0)
    rows = q_scr.shape[1] // 8
    for index in range(8):
        start = block_row(meta_ref, seq, index, rows)
        here = slice(index * rows, (index + 1) * rows)
        cosine, sine = cos_ref[here, :], sin_ref[here, :]
        for head in range(heads + 1):
            raw = qkv_ref[pl.ds(start, rows), head * HEAD : (head + 1) * HEAD]
            scaled, _ = scaled_of(raw)
            which = 0 if head < heads else 1
            value = scaled * gain_ref[which : which + 1, :]
            turned = value * cosine + pltpu.roll(value, HEAD // 2, 1) * sine
            if head < heads:
                q_scr[head, here, :] = turned.astype(BF16)
            else:
                k_scr[here, :] = turned.astype(BF16)
        v_scr[here, :] = qkv_ref[
            pl.ds(start, rows), (heads + 1) * HEAD : (heads + 2) * HEAD
        ].astype(BF16)


def key_span(index, tile):
    low = max(0, (index * tile - (MOST_DOC - 1)) // tile) * tile
    return low, (index + 1) * tile


def allowed_mask(segc_ref, segr_ref, index, tile):
    low, high = key_span(index, tile)
    shape = (tile, high - low)
    rows = lax.broadcasted_iota(jnp.int32, shape, 0) + index * tile
    cols = lax.broadcasted_iota(jnp.int32, shape, 1) + low
    same = segc_ref[0, index * tile : (index + 1) * tile, :] == segr_ref[0, :, low:high]
    return same & (cols <= rows)


def probs_of(query, keys, allowed, scale):
    scores = jnp.where(allowed, mm(query, keys, 1, 1) * scale, MASKED)
    weights = jnp.exp(scores - jnp.max(scores, axis=-1, keepdims=True))
    return weights * (1.0 / jnp.sum(weights, axis=-1, keepdims=True))


def attend_kernel(
    heads, tile, meta_ref, qkv_ref, segc_ref, segr_ref, cos_ref, sin_ref, gain_ref, out_ref, q_scr, k_scr, v_scr
):
    seq = pl.program_id(0)
    length = k_scr.shape[0]
    rows = length // 8
    scale = 1.0 / math.sqrt(HEAD)
    load_heads(meta_ref, qkv_ref, cos_ref, sin_ref, gain_ref, q_scr, k_scr, v_scr, heads)
    for index in range(length // tile):
        low, high = key_span(index, tile)
        allowed = allowed_mask(segc_ref, segr_ref, index, tile)
        for head in range(heads):
            query = q_scr[head, index * tile : (index + 1) * tile, :]
            probs = probs_of(query, k_scr[low:high, :], allowed, scale)
            mixed = mm(probs.astype(BF16), v_scr[low:high, :], 1, 0).astype(BF16)
            for piece in range(tile // rows):
                start = block_row(meta_ref, seq, index * (tile // rows) + piece, rows)
                out_ref[pl.ds(start, rows), head * HEAD : (head + 1) * HEAD] = mixed[
                    piece * rows : (piece + 1) * rows
                ]


def attend_back_kernel(
    heads,
    tile,
    meta_ref,
    qkv_ref,
    grad_ref,
    segc_ref,
    segr_ref,
    cos_ref,
    sin_ref,
    gain_ref,
    out_ref,
    gain_out_ref,
    q_scr,
    k_scr,
    v_scr,
    g_scr,
    dk_scr,
    dv_scr,
):
    seq = pl.program_id(0)
    length = k_scr.shape[0]
    rows = length // 8
    scale = 1.0 / math.sqrt(HEAD)
    load_heads(meta_ref, qkv_ref, cos_ref, sin_ref, gain_ref, q_scr, k_scr, v_scr, heads)
    for index in range(8):
        start = block_row(meta_ref, seq, index, rows)
        g_scr[index * rows : (index + 1) * rows, :] = grad_ref[pl.ds(start, rows), :]
    dk_scr[...] = jnp.zeros_like(dk_scr)
    dv_scr[...] = jnp.zeros_like(dv_scr)

    @pl.when(seq == 0)
    def _():
        gain_out_ref[...] = jnp.zeros_like(gain_out_ref)

    def finish(grad, index, head, which):
        here = slice(index * rows, (index + 1) * rows)
        start = block_row(meta_ref, seq, index, rows)
        grad = grad * cos_ref[here, :] - pltpu.roll(grad, HEAD // 2, 1) * sin_ref[here, :]
        raw = qkv_ref[pl.ds(start, rows), head * HEAD : (head + 1) * HEAD]
        scaled, inverse = scaled_of(raw)
        gain_out_ref[which : which + 1, :] += jnp.sum(grad * scaled, axis=0, keepdims=True)
        out = norm_back(grad, scaled, inverse, gain_ref[which : which + 1, :])
        out_ref[pl.ds(start, rows), head * HEAD : (head + 1) * HEAD] = out.astype(BF16)

    per = tile // rows
    for index in range(length // tile):
        low, high = key_span(index, tile)
        mine = slice(index * tile, (index + 1) * tile)
        allowed = allowed_mask(segc_ref, segr_ref, index, tile)
        for head in range(heads):
            query = q_scr[head, mine, :]
            keys = k_scr[low:high, :]
            probs = probs_of(query, keys, allowed, scale)
            grad = g_scr[mine, head * HEAD : (head + 1) * HEAD]
            grad_probs = mm(grad, v_scr[low:high, :], 1, 1)
            delta = jnp.sum(probs * grad_probs, axis=-1, keepdims=True)
            grad_scores = (probs * (grad_probs - delta)).astype(BF16)
            dv_scr[low:high, :] += mm(probs.astype(BF16), grad, 0, 0)
            dk_scr[low:high, :] += mm(grad_scores, query, 0, 0) * scale
            grad_query = mm(grad_scores, keys, 1, 0) * scale
            for piece in range(per):
                finish(
                    grad_query[piece * rows : (piece + 1) * rows], index * per + piece, head, 0
                )
    for index in range(8):
        here = slice(index * rows, (index + 1) * rows)
        start = block_row(meta_ref, seq, index, rows)
        finish(dk_scr[here, :], index, heads, 1)
        out_ref[pl.ds(start, rows), (heads + 1) * HEAD : (heads + 2) * HEAD] = dv_scr[
            here, :
        ].astype(BF16)


def whole(shape):
    return pl.BlockSpec(shape, lambda seq, meta: (0,) * len(shape))


def seg_specs(length):
    return [
        pl.BlockSpec((1, length, 1), lambda seq, meta: (seq, 0, 0)),
        pl.BlockSpec((1, 1, length), lambda seq, meta: (seq, 0, 0)),
    ]


def attend(meta, qkv, seg_cols, seg_rows, cosine, sine, gains):
    length = cosine.shape[0]
    tile = length // 4
    heads = qkv.shape[1] // HEAD - 2
    pairs = 2 * heads * length * length // 2
    return pl.pallas_call(
        functools.partial(attend_kernel, heads, tile),
        out_shape=jax.ShapeDtypeStruct((qkv.shape[0], heads * HEAD), BF16),
        grid_spec=pltpu.PrefetchScalarGridSpec(
            num_scalar_prefetch=1,
            grid=(2,),
            in_specs=[whole(qkv.shape)]
            + seg_specs(length)
            + [whole(cosine.shape), whole(sine.shape), whole(gains.shape)],
            out_specs=whole((qkv.shape[0], heads * HEAD)),
            scratch_shapes=[
                pltpu.VMEM((heads, length, HEAD), BF16),
                pltpu.VMEM((length, HEAD), BF16),
                pltpu.VMEM((length, HEAD), BF16),
            ],
        ),
        cost_estimate=pl.CostEstimate(
            flops=4 * pairs * HEAD, bytes_accessed=qkv.size * 4 + qkv.size, transcendentals=pairs
        ),
        name="attend",
    )(meta, qkv, seg_cols, seg_rows, cosine, sine, gains)


def attend_back(meta, qkv, grad, seg_cols, seg_rows, cosine, sine, gains):
    length = cosine.shape[0]
    tile = length // 4
    heads = qkv.shape[1] // HEAD - 2
    pairs = 2 * heads * length * length // 2
    return pl.pallas_call(
        functools.partial(attend_back_kernel, heads, tile),
        out_shape=(
            jax.ShapeDtypeStruct(qkv.shape, BF16),
            jax.ShapeDtypeStruct(gains.shape, F32),
        ),
        grid_spec=pltpu.PrefetchScalarGridSpec(
            num_scalar_prefetch=1,
            grid=(2,),
            in_specs=[whole(qkv.shape), whole(grad.shape)]
            + seg_specs(length)
            + [whole(cosine.shape), whole(sine.shape), whole(gains.shape)],
            out_specs=(whole(qkv.shape), whole(gains.shape)),
            scratch_shapes=[
                pltpu.VMEM((heads, length, HEAD), BF16),
                pltpu.VMEM((length, HEAD), BF16),
                pltpu.VMEM((length, HEAD), BF16),
                pltpu.VMEM((length, heads * HEAD), BF16),
                pltpu.VMEM((length, HEAD), F32),
                pltpu.VMEM((length, HEAD), F32),
            ],
        ),
        cost_estimate=pl.CostEstimate(
            flops=10 * pairs * HEAD, bytes_accessed=qkv.size * 8, transcendentals=pairs
        ),
        name="attend_back",
    )(meta, qkv, grad, seg_cols, seg_rows, cosine, sine, gains)


def body(
    tokens,
    segment_ids,
    norm_gain,
    query_weight,
    key_matrix,
    value_matrix,
    output_weight,
    query_gain,
    key_gain,
    mlp_gain,
    gate_weight,
    up_weight,
    down_weight,
    cotangent,
):
    local, width = tokens.shape[1], tokens.shape[2]
    length = 2 * local
    quarter = local // 2
    count = lax.axis_size("fsdp")
    block = width // count
    mine = lax.axis_index("fsdp")
    odd = mine % 2
    place = lax.axis_index("ctx")
    core = lax.axis_index("tp")

    small = query_gain.shape[0]
    lanes = jnp.arange(HEAD)[None, :]

    def pad_rows(vector):
        return jnp.concatenate([vector, jnp.zeros((block - small,), BF16)])

    gains = jnp.where(
        lanes == 0,
        norm_gain[:, None],
        jnp.where(
            lanes == 1,
            mlp_gain[:, None],
            jnp.where(
                lanes == 2, pad_rows(query_gain)[:, None], pad_rows(key_gain)[:, None]
            ),
        ),
    )
    (first_pair,) = shards(
        [
            [
                (query_weight, True),
                (key_matrix, True),
                (value_matrix, True),
                (output_weight, True),
                (gains, False),
            ]
        ],
        3,
    )
    first = gather_line(first_pair)
    gate_up_pair, down_pair = shards(
        [
            [(after(gate_weight, first_pair), True), (up_weight, True)],
            [(down_weight, True)],
        ],
        4,
    )
    gate_up_w = gather_line(gate_up_pair)
    down_w = gather_line(down_pair)

    def own_quarter(value):
        return lax.dynamic_slice_in_dim(value.reshape(local, width), core * quarter, quarter, 0)

    own_tok, own_cot = own_quarter(tokens), own_quarter(cotangent)
    tok = gather8(after(own_tok, gate_up_pair))
    segments = jnp.concatenate([segment_ids, swap_x(segment_ids)])
    seg_cols, seg_rows = segments[:, :, None], segments[:, None, :]
    cosine, sine = rope_tables(jnp.arange(length).astype(F32))
    meta = jnp.stack([place, core]).astype(jnp.int32)

    heads_q = query_weight.shape[1] // 4 // HEAD
    cols = (heads_q + 2) * HEAD
    qkv_w = first[:, :cols]
    out_w = first[:, cols : cols + heads_q * HEAD]
    gain_cols = first[:, cols + heads_q * HEAD :].astype(F32)
    in_gain, mid_gain = gain_cols[:, 0][None], gain_cols[:, 1][None]
    head_gains = gain_cols.reshape(count, block, HEAD)[:, :small, 2:4].reshape(HEAD, 2).T

    in_f = tok.astype(F32)
    cot_from = after(own_cot, tok)
    cot_x, cot_y = swap_x(cot_from), swap_ctx(cot_from)
    x_all = (in_f * inv_rms(in_f) * in_gain).astype(BF16)
    qkv = mm(x_all, qkv_w, 1, 0)
    attended = attend(meta, qkv, seg_cols, seg_rows, cosine, sine, head_gains)
    half = 4 * quarter
    cot_x, cot_y = after(cot_x, attended), after(cot_y, attended)
    eighth = quarter // 2
    cot_first, cot_second = swap_ctx(cot_x[:eighth]), swap_x(cot_y[eighth:])
    out_far = mm(attended[half:], out_w, 1, 1).astype(BF16)
    out_near = mm(attended[:half], out_w, 1, 1)
    cot_first = after(cot_first, out_near, out_far)
    cot_second = after(cot_second, out_near, out_far)
    cot_side = jnp.concatenate(
        [
            cot_from[:eighth],
            cot_x[:eighth],
            cot_y[:eighth],
            cot_first,
            cot_from[eighth:],
            cot_y[eighth:],
            cot_x[eighth:],
            cot_second,
        ]
    )
    cot_far = swap_core(cot_side)
    middle = own_tok.astype(F32) + reduce8(out_near, out_far)
    inverse_mid = inv_rms(middle)
    scaled_mid = middle * inverse_mid
    y_all = gather8((scaled_mid * mid_gain).astype(BF16))
    cot = jnp.concatenate([cot_side, after(cot_far, y_all)])

    ff = gate_up_w.shape[1] // 2
    gate_up = mm(y_all, gate_up_w, 1, 0)
    gate, up_value = gate_up[:, :ff], gate_up[:, ff:]
    sig = jax.nn.sigmoid(gate)
    active = gate * sig
    hidden = (active * up_value).astype(BF16)
    down_grad = mm(cot, hidden, 0, 0).astype(BF16)

    def finish_rows(own):
        pair = jnp.stack([own, swap_core(own)])
        return flip_if(core == 1, pair, 0).reshape(tokens.shape)

    grad_hidden = mm(after(cot, down_grad), down_w, 1, 0)
    grad_up = (grad_hidden * active).astype(BF16)
    grad_gate = (grad_hidden * up_value * (sig * (1.0 + gate * (1.0 - sig)))).astype(BF16)
    grad_gate_up = jnp.concatenate([grad_gate, grad_up], axis=1)
    gate_up_grad = mm(y_all, grad_gate_up, 0, 0).astype(BF16)
    mid_near = mm(grad_gate_up[:half], gate_up_w, 1, 1)
    mid_far = mm(grad_gate_up[half:], gate_up_w, 1, 1).astype(BF16)
    mid_grad = reduce8(mid_near, after(mid_far, gate_up_grad))

    mlp_gain_part = jnp.sum(mid_grad * scaled_mid, axis=0)
    grad_middle = own_cot.astype(F32) + norm_back(mid_grad, scaled_mid, inverse_mid, mid_gain)
    grad_attn = gather8(grad_middle.astype(BF16))
    out_grad = mm(grad_attn, attended, 0, 0).astype(BF16)
    grad_att = mm(grad_attn, out_w, 1, 0).astype(BF16)
    mlp_hidden = after(hidden, grad_attn)
    mlp_far = mm(mlp_hidden[half:], down_w, 1, 1).astype(BF16)
    mlp_came = swap_core(mlp_far)
    mlp_rows = mm(mlp_hidden[:half], down_w, 1, 1) + mlp_came.astype(F32)
    raw_grads, head_gain_parts = attend_back(
        meta, qkv, after(grad_att, mlp_rows), seg_cols, seg_rows, cosine, sine, head_gains
    )
    first_grad = jnp.concatenate([mm(x_all, raw_grads, 0, 0).astype(BF16), out_grad], axis=1)
    mlp = reduce4_links(mlp_rows, raw_grads)
    layer_out = finish_rows((middle + mlp).astype(BF16))
    in_near = mm(raw_grads[:half], qkv_w, 1, 1)
    in_far = mm(raw_grads[half:], qkv_w, 1, 1).astype(BF16)
    in_grad = reduce8(in_near, after(in_far, first_grad))

    spot = jnp.stack([place, odd]).astype(jnp.int32)

    def owners(grad, sizes, *others):
        rows = scatter_line(grad)
        rows = after(rows, *others)
        kept = lax.dynamic_slice_in_dim(rows, odd * block, block, 0)
        sent = lax.dynamic_slice_in_dim(rows, (1 - odd) * block, block, 0)
        by_x, by_y = swap_x(sent), swap_ctx(kept)
        by_both = swap_ctx(by_x)
        return join_columns(spot, (kept, by_x, by_y, by_both), sizes)

    (down_share,) = owners(down_grad, (ff,))
    gate_share, up_share = owners(gate_up_grad, (ff, ff))
    query_share, key_share, value_share, out_share = owners(
        first_grad, (heads_q * HEAD, HEAD, HEAD, heads_q * HEAD)
    )

    own_in = own_tok.astype(F32)
    inverse_in = inv_rms(own_in)
    scaled_in = own_in * inverse_in
    norm_gain_part = jnp.sum(in_grad * scaled_in, axis=0)
    token_grad = finish_rows(
        (grad_middle + norm_back(in_grad, scaled_in, inverse_in, in_gain)).astype(BF16)
    )

    parts = jnp.concatenate([norm_gain_part, mlp_gain_part, head_gain_parts.reshape(-1)])
    sums = total(parts.reshape(-1, HEAD)).reshape(-1)
    norm_gain_grad = lax.dynamic_slice_in_dim(sums, mine * block, block, 0)
    mlp_gain_grad = lax.dynamic_slice_in_dim(sums, width + mine * block, block, 0)
    query_gain_grad = lax.dynamic_slice_in_dim(sums, 2 * width + mine * small, small, 0)
    key_gain_grad = lax.dynamic_slice_in_dim(sums, 2 * width + HEAD + mine * small, small, 0)
    return (
        layer_out,
        token_grad,
        norm_gain_grad,
        query_share,
        key_share,
        value_share,
        out_share,
        query_gain_grad,
        key_gain_grad,
        mlp_gain_grad,
        gate_share,
        up_share,
        down_share,
    )


def solution(mesh):
    in_specs = (
        P("fsdp", "ctx", None),
        P("fsdp", None),
        P("fsdp"),
        P("fsdp", "tp"),
        P("fsdp", "tp"),
        P("fsdp", "tp"),
        P("fsdp", "tp"),
        P("fsdp"),
        P("fsdp"),
        P("fsdp"),
        P("fsdp", "tp"),
        P("fsdp", "tp"),
        P("fsdp", "tp"),
        P("fsdp", "ctx", None),
    )
    out_specs = (
        P("fsdp", "ctx", None),
        P("fsdp", "ctx", None),
        P("fsdp"),
        P("fsdp", "tp"),
        P("fsdp", "tp"),
        P("fsdp", "tp"),
        P("fsdp", "tp"),
        P("fsdp"),
        P("fsdp"),
        P("fsdp"),
        P("fsdp", "tp"),
        P("fsdp", "tp"),
        P("fsdp", "tp"),
    )

    return jax.shard_map(body, mesh=mesh, in_specs=in_specs, out_specs=out_specs, check_vma=False)
```

```python
import functools
import math

import jax
import jax.numpy as jnp
from jax import lax
from jax.experimental import pallas as pl
from jax.experimental.pallas import tpu as pltpu
from jax.sharding import PartitionSpec as P


HEAD = 128
EPS = 1e-06
THETA = 1000000.0
MASKED = -1e30
MOST_DOC = 512
MESH = pl.DeviceIdType.MESH
F32 = jnp.float32
BF16 = jnp.bfloat16


def mm(left, right, left_dim, right_dim):
    return lax.dot_general(
        left, right, (((left_dim,), (right_dim,)), ((), ())), preferred_element_type=F32
    )


def swap_core(value):
    return lax.ppermute(value, "tp", [(0, 1), (1, 0)])


def swap_ctx(value):
    return lax.ppermute(value, "ctx", [(0, 1), (1, 0)])


def swap_x(value):
    count = lax.axis_size("fsdp")
    return lax.ppermute(value, "fsdp", [(i, i ^ 1) for i in range(count)])


def lines():
    count = lax.axis_size("fsdp")
    return [[i for i in range(count) if i % 2 == parity] for parity in (0, 1)]


def gather_line(value):
    return lax.all_gather(value, "fsdp", axis=0, tiled=True, axis_index_groups=lines())


def scatter_line(value):
    return lax.psum_scatter(
        value, "fsdp", scatter_dimension=0, tiled=True, axis_index_groups=lines()
    )


def flip_if(flag, value, axis):
    return jnp.where(flag, jnp.flip(value, axis), value)


def neighbours():
    mine = lax.axis_index("fsdp")
    return (
        {"fsdp": mine + 1 - 2 * lax.rem(mine, 2)},
        {"ctx": 1 - lax.axis_index("ctx")},
        {"tp": 1 - lax.axis_index("tp")},
    )


def greet(peers):
    barrier = pltpu.get_barrier_semaphore()
    for peer in peers:
        pl.semaphore_signal(barrier, inc=1, device_id=peer, device_id_type=MESH)
    pl.semaphore_wait(barrier, len(peers))


def remote_params(number, limit=None):
    return pltpu.CompilerParams(
        collective_id=number, has_side_effects=True, vmem_limit_bytes=limit
    )


def gather8_kernel(rows, spread, *refs):
    if spread:
        own_ref, kept_ref, x_ref, y_ref, first_ref, second_ref, out_ref, also_ref = refs[:8]
        send_sem, recv_sem, local_sem, stage, also_send, also_recv, also_in, also_out = refs[8:]
    else:
        own_ref, out_ref, send_sem, recv_sem, local_sem = refs
    x_peer, y_peer, c_peer = neighbours()

    def start_of(away_t, half, outer, inner):
        return pl.ds((away_t * 8 + half * 4 + outer * 2 + inner) * rows, rows)

    def slot(*block):
        return out_ref.at[start_of(*block)]

    also_loads, also_remote, also_stores = [], [], []
    if spread:
        top, low = pl.ds(0, rows), pl.ds(rows, rows)
        pieces = [
            ((0, 0, 0), kept_ref.at[top]),
            ((0, 0, 1), x_ref.at[top]),
            ((0, 1, 0), y_ref.at[top]),
            ((0, 1, 1), first_ref),
            ((1, 0, 0), kept_ref.at[low]),
            ((1, 0, 1), y_ref.at[low]),
            ((1, 1, 0), x_ref.at[low]),
            ((1, 1, 1), second_ref),
        ]
        for index, (block, source) in enumerate(pieces):
            also_loads.append(pltpu.make_async_copy(source, stage.at[index], also_in.at[index]))
            also_stores.append(
                pltpu.make_async_copy(
                    stage.at[index], also_ref.at[start_of(0, *block)], also_out.at[index]
                )
            )
            also_remote.append(
                pltpu.make_async_remote_copy(
                    src_ref=source,
                    dst_ref=also_ref.at[start_of(1, *block)],
                    send_sem=also_send.at[index],
                    recv_sem=also_recv.at[index],
                    device_id=c_peer,
                    device_id_type=MESH,
                )
            )
        for copy in also_loads:
            copy.start()
    greet((x_peer, y_peer, c_peer))

    number = iter(range(14))

    def send(source, target, peer):
        index = next(number)
        copy = pltpu.make_async_remote_copy(
            src_ref=source,
            dst_ref=target,
            send_sem=send_sem.at[index],
            recv_sem=recv_sem.at[index],
            device_id=peer,
            device_id_type=MESH,
        )
        copy.start()
        return copy

    first, second = own_ref.at[pl.ds(0, rows)], own_ref.at[pl.ds(rows, rows)]
    x1 = send(first, slot(0, 0, 0, 1), x_peer)
    y1 = send(second, slot(0, 1, 0, 1), y_peer)
    x2 = send(second, slot(0, 1, 1, 0), x_peer)
    y2 = send(first, slot(0, 0, 1, 0), y_peer)
    rest = [send(first, slot(1, 0, 0, 0), c_peer), send(second, slot(1, 1, 0, 0), c_peer)]
    kept = [
        pltpu.make_async_copy(first, slot(0, 0, 0, 0), local_sem.at[0]),
        pltpu.make_async_copy(second, slot(0, 1, 0, 0), local_sem.at[1]),
    ]
    for copy in kept:
        copy.start()
    for copy in also_remote:
        copy.start()
    for load, store in zip(also_loads, also_stores):
        load.wait()
        store.start()
    x1.wait_recv()
    y3 = send(slot(0, 0, 0, 1), slot(0, 0, 1, 1), y_peer)
    y1.wait_recv()
    x3 = send(slot(0, 1, 0, 1), slot(0, 1, 1, 1), x_peer)
    rest.append(send(slot(0, 0, 0, 1), slot(1, 0, 0, 1), c_peer))
    rest.append(send(slot(0, 1, 0, 1), slot(1, 1, 0, 1), c_peer))
    x2.wait_recv()
    rest.append(send(slot(0, 1, 1, 0), slot(1, 1, 1, 0), c_peer))
    y2.wait_recv()
    rest.append(send(slot(0, 0, 1, 0), slot(1, 0, 1, 0), c_peer))
    y3.wait_recv()
    rest.append(send(slot(0, 0, 1, 1), slot(1, 0, 1, 1), c_peer))
    x3.wait_recv()
    rest.append(send(slot(0, 1, 1, 1), slot(1, 1, 1, 1), c_peer))
    for copy in (x1, y1, x2, y2, y3, x3):
        copy.wait_send()
    for copy in rest + also_remote + kept + also_stores:
        copy.wait()


def gather8(own, also=()):
    rows, width = own.shape[0] // 2, own.shape[1]
    hbm = pl.BlockSpec(memory_space=pl.ANY)
    whole_shape = jax.ShapeDtypeStruct((16 * rows, width), own.dtype)
    sems = [
        pltpu.SemaphoreType.DMA((14,)),
        pltpu.SemaphoreType.DMA((14,)),
        pltpu.SemaphoreType.DMA((2,)),
    ]
    if also:
        sems += [pltpu.VMEM((8, rows, width), own.dtype)] + [pltpu.SemaphoreType.DMA((8,))] * 4
    outs = pl.pallas_call(
        functools.partial(gather8_kernel, rows, bool(also)),
        out_shape=[whole_shape] * (2 if also else 1),
        in_specs=[pl.BlockSpec(memory_space=pltpu.VMEM)] + [hbm] * len(also),
        out_specs=[hbm] * (2 if also else 1),
        scratch_shapes=sems,
        compiler_params=remote_params(6 if also else 1),
        name="gather8_also" if also else "gather8",
    )(own, *also)
    return outs if also else outs[0]


def reduce8_kernel(
    rows,
    near_ref,
    far_ref,
    out_ref,
    near,
    core_in,
    link_in,
    link_out,
    send_sem,
    recv_sem,
    local_sem,
):
    x_peer, y_peer, c_peer = neighbours()
    greet((x_peer, y_peer, c_peer))
    order = [(h, o, i) for o, i in ((1, 1), (1, 0), (0, 1), (0, 0)) for h in (0, 1)]
    core_copies, local_copies = {}, {}
    for number, (half, outer, inner) in enumerate(order):
        place = pl.ds((half * 4 + outer * 2 + inner) * rows, rows)
        core_copies[half, outer, inner] = pltpu.make_async_remote_copy(
            src_ref=far_ref.at[place],
            dst_ref=core_in.at[place],
            send_sem=send_sem.at[number],
            recv_sem=recv_sem.at[number],
            device_id=c_peer,
            device_id_type=MESH,
        )
        local_copies[half, outer, inner] = pltpu.make_async_copy(
            near_ref.at[place], near.at[place], local_sem.at[number]
        )
    for block in order:
        core_copies[block].start()
        local_copies[block].start()

    def partial_sum(block):
        half, outer, inner = block
        place = pl.ds((half * 4 + outer * 2 + inner) * rows, rows)
        core_copies[block].wait_recv()
        local_copies[block].wait()
        return near[place, :] + core_in[place, :].astype(F32)

    def link(index, value, peer):
        link_out[index] = value.astype(BF16)
        copy = pltpu.make_async_remote_copy(
            src_ref=link_out.at[index],
            dst_ref=link_in.at[index],
            send_sem=send_sem.at[8 + index],
            recv_sem=recv_sem.at[8 + index],
            device_id=peer,
            device_id_type=MESH,
        )
        copy.start()
        return copy

    y11 = link(0, partial_sum((0, 1, 1)), y_peer)
    x11 = link(1, partial_sum((1, 1, 1)), x_peer)
    y10 = link(2, partial_sum((0, 1, 0)), y_peer)
    x10 = link(3, partial_sum((1, 1, 0)), x_peer)
    first01, second01 = partial_sum((0, 0, 1)), partial_sum((1, 0, 1))
    y11.wait_recv()
    x01 = link(4, first01 + link_in[0].astype(F32), x_peer)
    x11.wait_recv()
    y01 = link(5, second01 + link_in[1].astype(F32), y_peer)
    first = partial_sum((0, 0, 0))
    second = partial_sum((1, 0, 0))
    y10.wait_recv()
    out_ref[pl.ds(0, rows), :] = first + link_in[2].astype(F32)
    x10.wait_recv()
    out_ref[pl.ds(rows, rows), :] = second + link_in[3].astype(F32)
    x01.wait_recv()
    out_ref[pl.ds(0, rows), :] += link_in[4].astype(F32)
    y01.wait_recv()
    out_ref[pl.ds(rows, rows), :] += link_in[5].astype(F32)
    for copy in (y11, x11, y10, x10, x01, y01):
        copy.wait_send()
    for copy in core_copies.values():
        copy.wait_send()


def reduce8(near, far):
    rows, width = near.shape[0] // 8, near.shape[1]
    return pl.pallas_call(
        functools.partial(reduce8_kernel, rows),
        out_shape=jax.ShapeDtypeStruct((2 * rows, width), F32),
        in_specs=[pl.BlockSpec(memory_space=pl.ANY), pl.BlockSpec(memory_space=pl.ANY)],
        out_specs=pl.BlockSpec(memory_space=pltpu.VMEM),
        scratch_shapes=[
            pltpu.VMEM(near.shape, F32),
            pltpu.VMEM(near.shape, BF16),
            pltpu.VMEM((6, rows, width), BF16),
            pltpu.VMEM((6, rows, width), BF16),
            pltpu.SemaphoreType.DMA((14,)),
            pltpu.SemaphoreType.DMA((14,)),
            pltpu.SemaphoreType.DMA((8,)),
        ],
        compiler_params=remote_params(2, 48 * 1024 * 1024),
        name="reduce8",
    )(near, far)


def shard_kernel(plan, outs, *refs):
    ins, out_refs = refs[: len(plan)], refs[len(plan) : len(plan) + outs]
    stage = refs[len(plan) + outs : 2 * len(plan) + outs]
    send_sem, recv_sem, load_sem, store_sem = refs[2 * len(plan) + outs :]
    x_peer, _, _ = neighbours()
    odd = lax.rem(lax.axis_index("fsdp"), 2)
    column = 2 * lax.axis_index("ctx") + odd
    other = 2 * lax.axis_index("ctx") + 1 - odd
    greet((x_peer,))
    remote, loads, stores = [], [], []
    for number, (which, start, size, cut) in enumerate(plan):
        rows = ins[number].shape[0]
        place = pl.ds(pl.multiple_of(odd * rows, rows), rows)
        target = out_refs[which].at[place, pl.ds(start, size)]

        def source(index, ref=ins[number], size=size, cut=cut):
            if not cut:
                return ref
            return ref.at[:, pl.ds(pl.multiple_of(index * size, HEAD), size)]

        remote.append(
            pltpu.make_async_remote_copy(
                src_ref=source(other),
                dst_ref=target,
                send_sem=send_sem.at[number],
                recv_sem=recv_sem.at[number],
                device_id=x_peer,
                device_id_type=MESH,
            )
        )
        loads.append(pltpu.make_async_copy(source(column), stage[number], load_sem.at[number]))
        stores.append(pltpu.make_async_copy(stage[number], target, store_sem.at[number]))
    for copy in remote:
        copy.start()
    for copy in loads:
        copy.start()
    for load, store in zip(loads, stores):
        load.wait()
        store.start()
    for copy in stores:
        copy.wait()
    for copy in remote:
        copy.wait()


def shards(groups, number):
    plan, arrays, shapes = [], [], []
    for which, group in enumerate(groups):
        start = 0
        for array, cut in group:
            size = array.shape[1] // 4 if cut else array.shape[1]
            plan.append((which, start, size, cut))
            arrays.append(array)
            start += size
        shapes.append((2 * group[0][0].shape[0], start))
    hbm = pl.BlockSpec(memory_space=pl.ANY)
    return pl.pallas_call(
        functools.partial(shard_kernel, tuple(plan), len(groups)),
        out_shape=[jax.ShapeDtypeStruct(shape, BF16) for shape in shapes],
        in_specs=[hbm] * len(arrays),
        out_specs=[hbm] * len(groups),
        scratch_shapes=[
            pltpu.VMEM((array.shape[0], size), BF16)
            for array, (_, _, size, _) in zip(arrays, plan)
        ]
        + [pltpu.SemaphoreType.DMA((len(plan),))] * 4,
        compiler_params=remote_params(number),
        name="shards",
    )(*arrays)


def total_kernel(stages, part_ref, out_ref, inbox, outbox, send_sem, recv_sem):
    peers = []
    for axis, bit in stages:
        mine = lax.axis_index(axis)
        peers.append({axis: mine + bit * (1 - 2 * lax.rem(mine // bit, 2))})
    greet(peers)
    value = part_ref[...]
    copies = []
    for index, peer in enumerate(peers):
        outbox[index] = value
        copy = pltpu.make_async_remote_copy(
            src_ref=outbox.at[index],
            dst_ref=inbox.at[index],
            send_sem=send_sem.at[index],
            recv_sem=recv_sem.at[index],
            device_id=peer,
            device_id_type=MESH,
        )
        copy.start()
        copies.append(copy)
        copy.wait_recv()
        value = value + inbox[index]
    out_ref[...] = value
    for copy in copies:
        copy.wait_send()


def total(part):
    stages = [("tp", 1), ("ctx", 1)]
    bit = 1
    while bit < lax.axis_size("fsdp"):
        stages.append(("fsdp", bit))
        bit *= 2
    return pl.pallas_call(
        functools.partial(total_kernel, tuple(stages)),
        out_shape=jax.ShapeDtypeStruct(part.shape, F32),
        in_specs=[pl.BlockSpec(memory_space=pltpu.VMEM)],
        out_specs=pl.BlockSpec(memory_space=pltpu.VMEM),
        scratch_shapes=[
            pltpu.VMEM((len(stages),) + part.shape, F32),
            pltpu.VMEM((len(stages),) + part.shape, F32),
            pltpu.SemaphoreType.DMA((len(stages),)),
            pltpu.SemaphoreType.DMA((len(stages),)),
        ],
        compiler_params=remote_params(5),
        name="total",
    )(part)


def join_kernel(sizes, spot_ref, kept_ref, x_ref, y_ref, both_ref, *out_refs):
    place, odd = spot_ref[0], spot_ref[1]
    parts = (
        (kept_ref, 2 * place + odd),
        (x_ref, 2 * place + 1 - odd),
        (y_ref, 2 - 2 * place + odd),
        (both_ref, 3 - 2 * place - odd),
    )
    for part, column in parts:
        start = 0
        for size, out_ref in zip(sizes, out_refs):
            target = pl.ds(pl.multiple_of(column * size, HEAD), size)
            out_ref[:, target] = part[:, start : start + size].astype(F32)
            start += size


def join_columns(spot, parts, sizes):
    rows = parts[0].shape[0]
    tile = min(rows, 64)
    return pl.pallas_call(
        functools.partial(join_kernel, sizes),
        out_shape=[jax.ShapeDtypeStruct((rows, 4 * size), F32) for size in sizes],
        grid_spec=pltpu.PrefetchScalarGridSpec(
            num_scalar_prefetch=1,
            grid=(rows // tile,),
            in_specs=[
                pl.BlockSpec((tile, part.shape[1]), lambda i, spot: (i, 0)) for part in parts
            ],
            out_specs=[pl.BlockSpec((tile, 4 * size), lambda i, spot: (i, 0)) for size in sizes],
        ),
        name="join",
    )(spot, *parts)


def after(value, *others):
    return lax.optimization_barrier((value,) + others)[0]


def reduce4_links(total_rows, *others):
    rows = total_rows.shape[0] // 8
    first, second = total_rows[: 4 * rows], total_rows[4 * rows :]
    came_first = swap_ctx(first[2 * rows :].astype(BF16))
    came_second = swap_x(second[2 * rows :].astype(BF16))
    first = first[: 2 * rows] + after(came_first, *others).astype(F32)
    second = second[: 2 * rows] + after(came_second, *others).astype(F32)
    came_first = swap_x(first[rows:].astype(BF16))
    came_second = swap_ctx(second[rows:].astype(BF16))
    return first[:rows], second[:rows], came_first, came_second


def rope_tables(positions):
    freqs = THETA ** (-(jnp.arange(HEAD // 2, dtype=F32) * 2.0) / HEAD)
    angle = positions[:, None] * freqs[None, :]
    cosine = jnp.concatenate([jnp.cos(angle), jnp.cos(angle)], axis=-1)
    sine = jnp.concatenate([-jnp.sin(angle), jnp.sin(angle)], axis=-1)
    return cosine, sine


def norm_back(grad, scaled, inverse, gain):
    weighted = grad * gain
    return inverse * (weighted - scaled * jnp.mean(weighted * scaled, axis=-1, keepdims=True))


def inv_rms(value):
    return lax.rsqrt(jnp.mean(value * value, axis=-1, keepdims=True) + EPS)


def block_row(meta_ref, seq, index, rows):
    away_c = lax.rem(meta_ref[0] + index // 4, 2)
    away_t = lax.rem(meta_ref[1] + (index // 2) % 2, 2)
    if index % 2 == 0:
        inner = away_c * 2 + seq
    else:
        inner = seq * 2 + away_c + 4
    return pl.multiple_of((away_t * 8 + inner) * rows, rows)


def scaled_of(raw):
    inverse = lax.rsqrt(jnp.mean(raw * raw, axis=-1, keepdims=True) + EPS)
    return raw * inverse, inverse


def load_heads(meta_ref, qkv_ref, cos_ref, sin_ref, gain_ref, q_scr, k_scr, v_scr, heads):
    seq = pl.program_id(0)
    rows = q_scr.shape[1] // 8
    for index in range(8):
        start = block_row(meta_ref, seq, index, rows)
        here = slice(index * rows, (index + 1) * rows)
        cosine, sine = cos_ref[here, :], sin_ref[here, :]
        for head in range(heads + 1):
            raw = qkv_ref[pl.ds(start, rows), head * HEAD : (head + 1) * HEAD]
            scaled, _ = scaled_of(raw)
            which = 0 if head < heads else 1
            value = scaled * gain_ref[which : which + 1, :]
            turned = value * cosine + pltpu.roll(value, HEAD // 2, 1) * sine
            if head < heads:
                q_scr[head, here, :] = turned.astype(BF16)
            else:
                k_scr[here, :] = turned.astype(BF16)
        v_scr[here, :] = qkv_ref[
            pl.ds(start, rows), (heads + 1) * HEAD : (heads + 2) * HEAD
        ].astype(BF16)


def key_span(index, tile):
    low = max(0, (index * tile - (MOST_DOC - 1)) // tile) * tile
    return low, (index + 1) * tile


def allowed_mask(segc_ref, segr_ref, index, tile):
    low, high = key_span(index, tile)
    shape = (tile, high - low)
    rows = lax.broadcasted_iota(jnp.int32, shape, 0) + index * tile
    cols = lax.broadcasted_iota(jnp.int32, shape, 1) + low
    same = segc_ref[0, index * tile : (index + 1) * tile, :] == segr_ref[0, :, low:high]
    return same & (cols <= rows)


def probs_of(query, keys, allowed, scale):
    scores = jnp.where(allowed, mm(query, keys, 1, 1) * scale, MASKED)
    weights = jnp.exp(scores - jnp.max(scores, axis=-1, keepdims=True))
    return weights * (1.0 / jnp.sum(weights, axis=-1, keepdims=True))


def attend_kernel(
    heads, tile, meta_ref, qkv_ref, segc_ref, segr_ref, cos_ref, sin_ref, gain_ref, out_ref, q_scr, k_scr, v_scr
):
    seq = pl.program_id(0)
    length = k_scr.shape[0]
    rows = length // 8
    scale = 1.0 / math.sqrt(HEAD)
    load_heads(meta_ref, qkv_ref, cos_ref, sin_ref, gain_ref, q_scr, k_scr, v_scr, heads)
    for index in range(length // tile):
        low, high = key_span(index, tile)
        allowed = allowed_mask(segc_ref, segr_ref, index, tile)
        for head in range(heads):
            query = q_scr[head, index * tile : (index + 1) * tile, :]
            probs = probs_of(query, k_scr[low:high, :], allowed, scale)
            mixed = mm(probs.astype(BF16), v_scr[low:high, :], 1, 0).astype(BF16)
            for piece in range(tile // rows):
                start = block_row(meta_ref, seq, index * (tile // rows) + piece, rows)
                out_ref[pl.ds(start, rows), head * HEAD : (head + 1) * HEAD] = mixed[
                    piece * rows : (piece + 1) * rows
                ]


def attend_back_kernel(
    heads,
    tile,
    meta_ref,
    qkv_ref,
    grad_ref,
    segc_ref,
    segr_ref,
    cos_ref,
    sin_ref,
    gain_ref,
    out_ref,
    gain_out_ref,
    q_scr,
    k_scr,
    v_scr,
    g_scr,
    dk_scr,
    dv_scr,
):
    seq = pl.program_id(0)
    length = k_scr.shape[0]
    rows = length // 8
    scale = 1.0 / math.sqrt(HEAD)
    load_heads(meta_ref, qkv_ref, cos_ref, sin_ref, gain_ref, q_scr, k_scr, v_scr, heads)
    for index in range(8):
        start = block_row(meta_ref, seq, index, rows)
        g_scr[index * rows : (index + 1) * rows, :] = grad_ref[pl.ds(start, rows), :]
    dk_scr[...] = jnp.zeros_like(dk_scr)
    dv_scr[...] = jnp.zeros_like(dv_scr)

    @pl.when(seq == 0)
    def _():
        gain_out_ref[...] = jnp.zeros_like(gain_out_ref)

    def finish(grad, index, head, which):
        here = slice(index * rows, (index + 1) * rows)
        start = block_row(meta_ref, seq, index, rows)
        grad = grad * cos_ref[here, :] - pltpu.roll(grad, HEAD // 2, 1) * sin_ref[here, :]
        raw = qkv_ref[pl.ds(start, rows), head * HEAD : (head + 1) * HEAD]
        scaled, inverse = scaled_of(raw)
        gain_out_ref[which : which + 1, :] += jnp.sum(grad * scaled, axis=0, keepdims=True)
        out = norm_back(grad, scaled, inverse, gain_ref[which : which + 1, :])
        out_ref[pl.ds(start, rows), head * HEAD : (head + 1) * HEAD] = out.astype(BF16)

    per = tile // rows
    for index in range(length // tile):
        low, high = key_span(index, tile)
        mine = slice(index * tile, (index + 1) * tile)
        allowed = allowed_mask(segc_ref, segr_ref, index, tile)
        for head in range(heads):
            query = q_scr[head, mine, :]
            keys = k_scr[low:high, :]
            probs = probs_of(query, keys, allowed, scale)
            grad = g_scr[mine, head * HEAD : (head + 1) * HEAD]
            grad_probs = mm(grad, v_scr[low:high, :], 1, 1)
            delta = jnp.sum(probs * grad_probs, axis=-1, keepdims=True)
            grad_scores = (probs * (grad_probs - delta)).astype(BF16)
            dv_scr[low:high, :] += mm(probs.astype(BF16), grad, 0, 0)
            dk_scr[low:high, :] += mm(grad_scores, query, 0, 0) * scale
            grad_query = mm(grad_scores, keys, 1, 0) * scale
            for piece in range(per):
                finish(
                    grad_query[piece * rows : (piece + 1) * rows], index * per + piece, head, 0
                )
    for index in range(8):
        here = slice(index * rows, (index + 1) * rows)
        start = block_row(meta_ref, seq, index, rows)
        finish(dk_scr[here, :], index, heads, 1)
        out_ref[pl.ds(start, rows), (heads + 1) * HEAD : (heads + 2) * HEAD] = dv_scr[
            here, :
        ].astype(BF16)


def whole(shape):
    return pl.BlockSpec(shape, lambda seq, meta: (0,) * len(shape))


def seg_specs(length):
    return [
        pl.BlockSpec((1, length, 1), lambda seq, meta: (seq, 0, 0)),
        pl.BlockSpec((1, 1, length), lambda seq, meta: (seq, 0, 0)),
    ]


def attend(meta, qkv, seg_cols, seg_rows, cosine, sine, gains):
    length = cosine.shape[0]
    tile = length // 4
    heads = qkv.shape[1] // HEAD - 2
    pairs = 2 * heads * length * length // 2
    return pl.pallas_call(
        functools.partial(attend_kernel, heads, tile),
        out_shape=jax.ShapeDtypeStruct((qkv.shape[0], heads * HEAD), BF16),
        grid_spec=pltpu.PrefetchScalarGridSpec(
            num_scalar_prefetch=1,
            grid=(2,),
            in_specs=[whole(qkv.shape)]
            + seg_specs(length)
            + [whole(cosine.shape), whole(sine.shape), whole(gains.shape)],
            out_specs=whole((qkv.shape[0], heads * HEAD)),
            scratch_shapes=[
                pltpu.VMEM((heads, length, HEAD), BF16),
                pltpu.VMEM((length, HEAD), BF16),
                pltpu.VMEM((length, HEAD), BF16),
            ],
        ),
        cost_estimate=pl.CostEstimate(
            flops=4 * pairs * HEAD, bytes_accessed=qkv.size * 4 + qkv.size, transcendentals=pairs
        ),
        name="attend",
    )(meta, qkv, seg_cols, seg_rows, cosine, sine, gains)


def attend_back(meta, qkv, grad, seg_cols, seg_rows, cosine, sine, gains):
    length = cosine.shape[0]
    tile = length // 4
    heads = qkv.shape[1] // HEAD - 2
    pairs = 2 * heads * length * length // 2
    return pl.pallas_call(
        functools.partial(attend_back_kernel, heads, tile),
        out_shape=(
            jax.ShapeDtypeStruct(qkv.shape, BF16),
            jax.ShapeDtypeStruct(gains.shape, F32),
        ),
        grid_spec=pltpu.PrefetchScalarGridSpec(
            num_scalar_prefetch=1,
            grid=(2,),
            in_specs=[whole(qkv.shape), whole(grad.shape)]
            + seg_specs(length)
            + [whole(cosine.shape), whole(sine.shape), whole(gains.shape)],
            out_specs=(whole(qkv.shape), whole(gains.shape)),
            scratch_shapes=[
                pltpu.VMEM((heads, length, HEAD), BF16),
                pltpu.VMEM((length, HEAD), BF16),
                pltpu.VMEM((length, HEAD), BF16),
                pltpu.VMEM((length, heads * HEAD), BF16),
                pltpu.VMEM((length, HEAD), F32),
                pltpu.VMEM((length, HEAD), F32),
            ],
        ),
        cost_estimate=pl.CostEstimate(
            flops=10 * pairs * HEAD, bytes_accessed=qkv.size * 8, transcendentals=pairs
        ),
        name="attend_back",
    )(meta, qkv, grad, seg_cols, seg_rows, cosine, sine, gains)


def body(
    tokens,
    segment_ids,
    norm_gain,
    query_weight,
    key_matrix,
    value_matrix,
    output_weight,
    query_gain,
    key_gain,
    mlp_gain,
    gate_weight,
    up_weight,
    down_weight,
    cotangent,
):
    local, width = tokens.shape[1], tokens.shape[2]
    length = 2 * local
    quarter = local // 2
    count = lax.axis_size("fsdp")
    block = width // count
    mine = lax.axis_index("fsdp")
    odd = mine % 2
    place = lax.axis_index("ctx")
    core = lax.axis_index("tp")

    small = query_gain.shape[0]
    lanes = jnp.arange(HEAD)[None, :]

    def pad_rows(vector):
        return jnp.concatenate([vector, jnp.zeros((block - small,), BF16)])

    gains = jnp.where(
        lanes == 0,
        norm_gain[:, None],
        jnp.where(
            lanes == 1,
            mlp_gain[:, None],
            jnp.where(
                lanes == 2, pad_rows(query_gain)[:, None], pad_rows(key_gain)[:, None]
            ),
        ),
    )
    far_segments = swap_x(segment_ids)
    (first_pair,) = shards(
        [
            [
                (query_weight, True),
                (key_matrix, True),
                (value_matrix, True),
                (output_weight, True),
                (gains, False),
            ]
        ],
        3,
    )
    first = gather_line(first_pair)
    gate_up_pair, down_pair = shards(
        [
            [(after(gate_weight, first_pair), True), (up_weight, True)],
            [(down_weight, True)],
        ],
        4,
    )
    gate_up_w = gather_line(gate_up_pair)
    down_w = gather_line(down_pair)

    def own_quarter(value):
        return lax.dynamic_slice_in_dim(value.reshape(local, width), core * quarter, quarter, 0)

    own_tok, own_cot = own_quarter(tokens), own_quarter(cotangent)
    tok = gather8(after(own_tok, gate_up_pair))
    segments = jnp.concatenate([segment_ids, far_segments])
    seg_cols, seg_rows = segments[:, :, None], segments[:, None, :]
    cosine, sine = rope_tables(jnp.arange(length).astype(F32))
    meta = jnp.stack([place, core]).astype(jnp.int32)

    heads_q = query_weight.shape[1] // 4 // HEAD
    cols = (heads_q + 2) * HEAD
    qkv_w = first[:, :cols]
    out_w = first[:, cols : cols + heads_q * HEAD]
    gain_cols = first[:, cols + heads_q * HEAD :].astype(F32)
    in_gain, mid_gain = gain_cols[:, 0][None], gain_cols[:, 1][None]
    head_gains = gain_cols.reshape(count, block, HEAD)[:, :small, 2:4].reshape(HEAD, 2).T

    in_f = tok.astype(F32)
    cot_from = after(own_cot, tok)
    cot_x, cot_y = swap_x(cot_from), swap_ctx(cot_from)
    x_all = (in_f * inv_rms(in_f) * in_gain).astype(BF16)
    qkv = mm(x_all, qkv_w, 1, 0)
    attended = attend(meta, qkv, seg_cols, seg_rows, cosine, sine, head_gains)
    half = 4 * quarter
    cot_x, cot_y = after(cot_x, attended), after(cot_y, attended)
    eighth = quarter // 2
    cot_first, cot_second = swap_ctx(cot_x[:eighth]), swap_x(cot_y[eighth:])
    out_far = mm(attended[half:], out_w, 1, 1).astype(BF16)
    out_near = mm(attended[:half], out_w, 1, 1)
    middle = own_tok.astype(F32) + reduce8(out_near, out_far)
    inverse_mid = inv_rms(middle)
    scaled_mid = middle * inverse_mid
    y_own = (scaled_mid * mid_gain).astype(BF16)
    cot_first, cot_second = after(cot_first, y_own), after(cot_second, y_own)
    y_all, cot = gather8(y_own, (cot_from, cot_x, cot_y, cot_first, cot_second))

    ff = gate_up_w.shape[1] // 2
    gate_up = mm(y_all, gate_up_w, 1, 0)
    gate, up_value = gate_up[:, :ff], gate_up[:, ff:]
    sig = jax.nn.sigmoid(gate)
    active = gate * sig
    hidden = (active * up_value).astype(BF16)
    down_grad = mm(cot, hidden, 0, 0).astype(BF16)

    def finish_rows(own):
        pair = jnp.stack([own, swap_core(own)])
        return flip_if(core == 1, pair, 0).reshape(tokens.shape)

    grad_hidden = mm(after(cot, down_grad), down_w, 1, 0)
    grad_up = (grad_hidden * active).astype(BF16)
    grad_gate = (grad_hidden * up_value * (sig * (1.0 + gate * (1.0 - sig)))).astype(BF16)
    grad_gate_up = jnp.concatenate([grad_gate, grad_up], axis=1)
    gate_up_grad = mm(y_all, grad_gate_up, 0, 0).astype(BF16)
    mid_near = mm(grad_gate_up[:half], gate_up_w, 1, 1)
    mid_far = mm(grad_gate_up[half:], gate_up_w, 1, 1).astype(BF16)
    mid_grad = reduce8(mid_near, after(mid_far, gate_up_grad))

    mlp_gain_part = jnp.sum(mid_grad * scaled_mid, axis=0)
    grad_middle = own_cot.astype(F32) + norm_back(mid_grad, scaled_mid, inverse_mid, mid_gain)
    grad_attn = gather8(grad_middle.astype(BF16))
    out_grad = mm(grad_attn, attended, 0, 0).astype(BF16)
    grad_att = mm(grad_attn, out_w, 1, 0).astype(BF16)
    mlp_hidden = after(hidden, grad_attn)
    mlp_far = mm(mlp_hidden[half:], down_w, 1, 1).astype(BF16)
    mlp_came = swap_core(mlp_far)
    mlp_rows = mm(mlp_hidden[:half], down_w, 1, 1) + mlp_came.astype(F32)
    raw_grads, head_gain_parts = attend_back(
        meta, qkv, after(grad_att, mlp_rows), seg_cols, seg_rows, cosine, sine, head_gains
    )
    first_grad = jnp.concatenate([mm(x_all, raw_grads, 0, 0).astype(BF16), out_grad], axis=1)
    mlp_first, mlp_second, mlp_came1, mlp_came2 = reduce4_links(mlp_rows, raw_grads)
    in_near = mm(raw_grads[:half], qkv_w, 1, 1)
    in_far = mm(raw_grads[half:], qkv_w, 1, 1).astype(BF16)
    in_grad = reduce8(in_near, after(in_far, first_grad))

    mlp_first = mlp_first + after(mlp_came1, in_grad).astype(F32)
    mlp_second = mlp_second + after(mlp_came2, in_grad).astype(F32)
    layer_out = finish_rows((middle + jnp.concatenate([mlp_first, mlp_second])).astype(BF16))

    spot = jnp.stack([place, odd]).astype(jnp.int32)

    def owners(grad, sizes, *others):
        rows = scatter_line(grad)
        rows = after(rows, *others)
        kept = lax.dynamic_slice_in_dim(rows, odd * block, block, 0)
        sent = lax.dynamic_slice_in_dim(rows, (1 - odd) * block, block, 0)
        by_x, by_y = swap_x(sent), swap_ctx(kept)
        by_both = swap_ctx(by_x)
        return join_columns(spot, (kept, by_x, by_y, by_both), sizes)

    (down_share,) = owners(down_grad, (ff,))
    gate_share, up_share = owners(gate_up_grad, (ff, ff))
    query_share, key_share, value_share, out_share = owners(
        first_grad, (heads_q * HEAD, HEAD, HEAD, heads_q * HEAD)
    )

    own_in = own_tok.astype(F32)
    inverse_in = inv_rms(own_in)
    scaled_in = own_in * inverse_in
    norm_gain_part = jnp.sum(in_grad * scaled_in, axis=0)
    token_grad = finish_rows(
        (grad_middle + norm_back(in_grad, scaled_in, inverse_in, in_gain)).astype(BF16)
    )

    parts = jnp.concatenate([norm_gain_part, mlp_gain_part, head_gain_parts.reshape(-1)])
    sums = total(parts.reshape(-1, HEAD)).reshape(-1)
    norm_gain_grad = lax.dynamic_slice_in_dim(sums, mine * block, block, 0)
    mlp_gain_grad = lax.dynamic_slice_in_dim(sums, width + mine * block, block, 0)
    query_gain_grad = lax.dynamic_slice_in_dim(sums, 2 * width + mine * small, small, 0)
    key_gain_grad = lax.dynamic_slice_in_dim(sums, 2 * width + HEAD + mine * small, small, 0)
    return (
        layer_out,
        token_grad,
        norm_gain_grad,
        query_share,
        key_share,
        value_share,
        out_share,
        query_gain_grad,
        key_gain_grad,
        mlp_gain_grad,
        gate_share,
        up_share,
        down_share,
    )


def solution(mesh):
    in_specs = (
        P("fsdp", "ctx", None),
        P("fsdp", None),
        P("fsdp"),
        P("fsdp", "tp"),
        P("fsdp", "tp"),
        P("fsdp", "tp"),
        P("fsdp", "tp"),
        P("fsdp"),
        P("fsdp"),
        P("fsdp"),
        P("fsdp", "tp"),
        P("fsdp", "tp"),
        P("fsdp", "tp"),
        P("fsdp", "ctx", None),
    )
    out_specs = (
        P("fsdp", "ctx", None),
        P("fsdp", "ctx", None),
        P("fsdp"),
        P("fsdp", "tp"),
        P("fsdp", "tp"),
        P("fsdp", "tp"),
        P("fsdp", "tp"),
        P("fsdp"),
        P("fsdp"),
        P("fsdp"),
        P("fsdp", "tp"),
        P("fsdp", "tp"),
        P("fsdp", "tp"),
    )

    return jax.shard_map(body, mesh=mesh, in_specs=in_specs, out_specs=out_specs, check_vma=False)
```

```python
import functools
import math

import jax
import jax.numpy as jnp
from jax import lax
from jax.experimental import pallas as pl
from jax.experimental.pallas import tpu as pltpu
from jax.sharding import PartitionSpec as P


HEAD = 128
EPS = 1e-06
THETA = 1000000.0
MASKED = -1e30
MOST_DOC = 512
MESH = pl.DeviceIdType.MESH
F32 = jnp.float32
BF16 = jnp.bfloat16


def mm(left, right, left_dim, right_dim):
    return lax.dot_general(
        left, right, (((left_dim,), (right_dim,)), ((), ())), preferred_element_type=F32
    )


def swap_core(value):
    return lax.ppermute(value, "tp", [(0, 1), (1, 0)])


def swap_ctx(value):
    return lax.ppermute(value, "ctx", [(0, 1), (1, 0)])


def swap_x(value):
    count = lax.axis_size("fsdp")
    return lax.ppermute(value, "fsdp", [(i, i ^ 1) for i in range(count)])


def lines():
    count = lax.axis_size("fsdp")
    return [[i for i in range(count) if i % 2 == parity] for parity in (0, 1)]


def gather_line(value):
    return lax.all_gather(value, "fsdp", axis=0, tiled=True, axis_index_groups=lines())


def scatter_line(value):
    return lax.psum_scatter(
        value, "fsdp", scatter_dimension=0, tiled=True, axis_index_groups=lines()
    )


def flip_if(flag, value, axis):
    return jnp.where(flag, jnp.flip(value, axis), value)


def neighbours():
    mine = lax.axis_index("fsdp")
    return (
        {"fsdp": mine + 1 - 2 * lax.rem(mine, 2)},
        {"ctx": 1 - lax.axis_index("ctx")},
        {"tp": 1 - lax.axis_index("tp")},
    )


def greet(peers):
    barrier = pltpu.get_barrier_semaphore()
    for peer in peers:
        pl.semaphore_signal(barrier, inc=1, device_id=peer, device_id_type=MESH)
    pl.semaphore_wait(barrier, len(peers))


def remote_params(number, limit=None):
    return pltpu.CompilerParams(
        collective_id=number, has_side_effects=True, vmem_limit_bytes=limit
    )


def gather8_kernel(rows, spread, *refs):
    if spread:
        own_ref, kept_ref, x_ref, y_ref, first_ref, second_ref, out_ref, also_ref = refs[:8]
        send_sem, recv_sem, local_sem, stage, also_send, also_recv, also_in, also_out = refs[8:]
    else:
        own_ref, out_ref, send_sem, recv_sem, local_sem = refs
    x_peer, y_peer, c_peer = neighbours()

    def start_of(away_t, half, outer, inner):
        return pl.ds((away_t * 8 + half * 4 + outer * 2 + inner) * rows, rows)

    def slot(*block):
        return out_ref.at[start_of(*block)]

    also_loads, also_remote, also_stores = [], [], []
    if spread:
        top, low = pl.ds(0, rows), pl.ds(rows, rows)
        pieces = [
            ((0, 0, 0), kept_ref.at[top]),
            ((0, 0, 1), x_ref.at[top]),
            ((0, 1, 0), y_ref.at[top]),
            ((0, 1, 1), first_ref),
            ((1, 0, 0), kept_ref.at[low]),
            ((1, 0, 1), y_ref.at[low]),
            ((1, 1, 0), x_ref.at[low]),
            ((1, 1, 1), second_ref),
        ]
        for index, (block, source) in enumerate(pieces):
            also_loads.append(pltpu.make_async_copy(source, stage.at[index], also_in.at[index]))
            also_stores.append(
                pltpu.make_async_copy(
                    stage.at[index], also_ref.at[start_of(0, *block)], also_out.at[index]
                )
            )
            also_remote.append(
                pltpu.make_async_remote_copy(
                    src_ref=source,
                    dst_ref=also_ref.at[start_of(1, *block)],
                    send_sem=also_send.at[index],
                    recv_sem=also_recv.at[index],
                    device_id=c_peer,
                    device_id_type=MESH,
                )
            )
        for copy in also_loads:
            copy.start()
    greet((x_peer, y_peer, c_peer))

    number = iter(range(14))

    def send(source, target, peer):
        index = next(number)
        copy = pltpu.make_async_remote_copy(
            src_ref=source,
            dst_ref=target,
            send_sem=send_sem.at[index],
            recv_sem=recv_sem.at[index],
            device_id=peer,
            device_id_type=MESH,
        )
        copy.start()
        return copy

    first, second = own_ref.at[pl.ds(0, rows)], own_ref.at[pl.ds(rows, rows)]
    x1 = send(first, slot(0, 0, 0, 1), x_peer)
    y1 = send(second, slot(0, 1, 0, 1), y_peer)
    x2 = send(second, slot(0, 1, 1, 0), x_peer)
    y2 = send(first, slot(0, 0, 1, 0), y_peer)
    rest = [send(first, slot(1, 0, 0, 0), c_peer), send(second, slot(1, 1, 0, 0), c_peer)]
    kept = [
        pltpu.make_async_copy(first, slot(0, 0, 0, 0), local_sem.at[0]),
        pltpu.make_async_copy(second, slot(0, 1, 0, 0), local_sem.at[1]),
    ]
    for copy in kept:
        copy.start()
    for copy in also_remote:
        copy.start()
    for load, store in zip(also_loads, also_stores):
        load.wait()
        store.start()
    x1.wait_recv()
    y3 = send(slot(0, 0, 0, 1), slot(0, 0, 1, 1), y_peer)
    y1.wait_recv()
    x3 = send(slot(0, 1, 0, 1), slot(0, 1, 1, 1), x_peer)
    rest.append(send(slot(0, 0, 0, 1), slot(1, 0, 0, 1), c_peer))
    rest.append(send(slot(0, 1, 0, 1), slot(1, 1, 0, 1), c_peer))
    x2.wait_recv()
    rest.append(send(slot(0, 1, 1, 0), slot(1, 1, 1, 0), c_peer))
    y2.wait_recv()
    rest.append(send(slot(0, 0, 1, 0), slot(1, 0, 1, 0), c_peer))
    y3.wait_recv()
    rest.append(send(slot(0, 0, 1, 1), slot(1, 0, 1, 1), c_peer))
    x3.wait_recv()
    rest.append(send(slot(0, 1, 1, 1), slot(1, 1, 1, 1), c_peer))
    for copy in (x1, y1, x2, y2, y3, x3):
        copy.wait_send()
    for copy in rest + also_remote + kept + also_stores:
        copy.wait()


def gather8_product_kernel(
    rows,
    own_ref,
    acts_ref,
    weight_ref,
    out_ref,
    kept_ref,
    to_y_ref,
    to_x_ref,
    send_sem,
    recv_sem,
    local_sem,
    acts,
    weight,
    far,
    core_in,
    core_send,
    core_recv,
    load_sem,
):
    x_peer, y_peer, c_peer = neighbours()
    width = weight.shape[0]
    wide = 2 * rows
    loads = [
        pltpu.make_async_copy(weight_ref, weight, load_sem.at[0]),
        pltpu.make_async_copy(acts_ref, acts, load_sem.at[1]),
    ]
    for copy in loads:
        copy.start()
    greet((x_peer, y_peer, c_peer))

    def slot(away_t, half, outer, inner):
        return out_ref.at[pl.ds((away_t * 8 + half * 4 + outer * 2 + inner) * rows, rows)]

    number = iter(range(14))

    def send(source, target, peer):
        index = next(number)
        copy = pltpu.make_async_remote_copy(
            src_ref=source,
            dst_ref=target,
            send_sem=send_sem.at[index],
            recv_sem=recv_sem.at[index],
            device_id=peer,
            device_id_type=MESH,
        )
        copy.start()
        return copy

    core_copies = []

    def far_chunk(index):
        place = pl.ds(index * wide, wide)
        source = pl.ds(4 * wide + index * wide, wide)

        def step(cols):
            far[place, cols] = mm(acts[source, :], weight[cols, :], 1, 1).astype(BF16)
            return 0

        tiled(width, width // 2, step)
        copy = pltpu.make_async_remote_copy(
            src_ref=far.at[place],
            dst_ref=core_in.at[place],
            send_sem=core_send.at[index],
            recv_sem=core_recv.at[index],
            device_id=c_peer,
            device_id_type=MESH,
        )
        copy.start()
        core_copies.append(copy)

    def near_chunk(index, target_ref, start):
        core_copies[index].wait_recv()
        place = pl.ds(index * wide, wide)
        target = pl.ds(start, wide)

        def step(cols):
            value = mm(acts[place, :], weight[cols, :], 1, 1) + core_in[place, cols].astype(F32)
            target_ref[target, cols] = value.astype(target_ref.dtype)
            return 0

        tiled(width, width // 2, step)

    first, second = own_ref.at[pl.ds(0, rows)], own_ref.at[pl.ds(rows, rows)]
    x1 = send(first, slot(0, 0, 0, 1), x_peer)
    y1 = send(second, slot(0, 1, 0, 1), y_peer)
    x2 = send(second, slot(0, 1, 1, 0), x_peer)
    y2 = send(first, slot(0, 0, 1, 0), y_peer)
    rest = [send(first, slot(1, 0, 0, 0), c_peer), send(second, slot(1, 1, 0, 0), c_peer)]
    kept = [
        pltpu.make_async_copy(first, slot(0, 0, 0, 0), local_sem.at[0]),
        pltpu.make_async_copy(second, slot(0, 1, 0, 0), local_sem.at[1]),
    ]
    for copy in kept:
        copy.start()
    for copy in loads:
        copy.wait()
    for index in range(4):
        far_chunk(index)
    x1.wait_recv()
    y3 = send(slot(0, 0, 0, 1), slot(0, 0, 1, 1), y_peer)
    y1.wait_recv()
    x3 = send(slot(0, 1, 0, 1), slot(0, 1, 1, 1), x_peer)
    rest.append(send(slot(0, 0, 0, 1), slot(1, 0, 0, 1), c_peer))
    rest.append(send(slot(0, 1, 0, 1), slot(1, 1, 0, 1), c_peer))
    near_chunk(0, kept_ref, 0)
    near_chunk(1, to_y_ref, 0)
    near_chunk(2, kept_ref, wide)
    near_chunk(3, to_x_ref, 0)
    x2.wait_recv()
    rest.append(send(slot(0, 1, 1, 0), slot(1, 1, 1, 0), c_peer))
    y2.wait_recv()
    rest.append(send(slot(0, 0, 1, 0), slot(1, 0, 1, 0), c_peer))
    y3.wait_recv()
    rest.append(send(slot(0, 0, 1, 1), slot(1, 0, 1, 1), c_peer))
    x3.wait_recv()
    rest.append(send(slot(0, 1, 1, 1), slot(1, 1, 1, 1), c_peer))
    for copy in (x1, y1, x2, y2, y3, x3):
        copy.wait_send()
    for copy in core_copies:
        copy.wait_send()
    for copy in rest + kept:
        copy.wait()


def gather8_product(own, acts, weight):
    rows, width = own.shape[0] // 2, own.shape[1]
    hbm = pl.BlockSpec(memory_space=pl.ANY)
    vmem = pl.BlockSpec(memory_space=pltpu.VMEM)
    return pl.pallas_call(
        functools.partial(gather8_product_kernel, rows),
        out_shape=[
            jax.ShapeDtypeStruct((16 * rows, width), own.dtype),
            jax.ShapeDtypeStruct((4 * rows, width), F32),
            jax.ShapeDtypeStruct((2 * rows, width), BF16),
            jax.ShapeDtypeStruct((2 * rows, width), BF16),
        ],
        in_specs=[vmem, hbm, hbm],
        out_specs=[hbm, vmem, vmem, vmem],
        scratch_shapes=[
            pltpu.SemaphoreType.DMA((14,)),
            pltpu.SemaphoreType.DMA((14,)),
            pltpu.SemaphoreType.DMA((2,)),
            pltpu.VMEM(acts.shape, BF16),
            pltpu.VMEM(weight.shape, BF16),
            pltpu.VMEM((8 * rows, width), BF16),
            pltpu.VMEM((8 * rows, width), BF16),
            pltpu.SemaphoreType.DMA((4,)),
            pltpu.SemaphoreType.DMA((4,)),
            pltpu.SemaphoreType.DMA((2,)),
        ],
        compiler_params=remote_params(9, 48 * 1024 * 1024),
        cost_estimate=pl.CostEstimate(
            flops=2 * acts.size * width, bytes_accessed=16 * own.size, transcendentals=0
        ),
        name="gather8_product",
    )(own, acts, weight)


def gather8(own, also=()):
    rows, width = own.shape[0] // 2, own.shape[1]
    hbm = pl.BlockSpec(memory_space=pl.ANY)
    whole_shape = jax.ShapeDtypeStruct((16 * rows, width), own.dtype)
    sems = [
        pltpu.SemaphoreType.DMA((14,)),
        pltpu.SemaphoreType.DMA((14,)),
        pltpu.SemaphoreType.DMA((2,)),
    ]
    if also:
        sems += [pltpu.VMEM((8, rows, width), own.dtype)] + [pltpu.SemaphoreType.DMA((8,))] * 4
    outs = pl.pallas_call(
        functools.partial(gather8_kernel, rows, bool(also)),
        out_shape=[whole_shape] * (2 if also else 1),
        in_specs=[pl.BlockSpec(memory_space=pltpu.VMEM)] + [hbm] * len(also),
        out_specs=[hbm] * (2 if also else 1),
        scratch_shapes=sems,
        compiler_params=remote_params(6 if also else 1),
        name="gather8_also" if also else "gather8",
    )(own, *also)
    return outs if also else outs[0]


def reduce8_kernel(
    rows,
    near_ref,
    far_ref,
    out_ref,
    near,
    core_in,
    link_in,
    link_out,
    send_sem,
    recv_sem,
    local_sem,
):
    x_peer, y_peer, c_peer = neighbours()
    greet((x_peer, y_peer, c_peer))
    order = [(h, o, i) for o, i in ((1, 1), (1, 0), (0, 1), (0, 0)) for h in (0, 1)]
    core_copies, local_copies = {}, {}
    for number, (half, outer, inner) in enumerate(order):
        place = pl.ds((half * 4 + outer * 2 + inner) * rows, rows)
        core_copies[half, outer, inner] = pltpu.make_async_remote_copy(
            src_ref=far_ref.at[place],
            dst_ref=core_in.at[place],
            send_sem=send_sem.at[number],
            recv_sem=recv_sem.at[number],
            device_id=c_peer,
            device_id_type=MESH,
        )
        local_copies[half, outer, inner] = pltpu.make_async_copy(
            near_ref.at[place], near.at[place], local_sem.at[number]
        )
    for block in order:
        core_copies[block].start()
        local_copies[block].start()

    def partial_sum(block):
        half, outer, inner = block
        place = pl.ds((half * 4 + outer * 2 + inner) * rows, rows)
        core_copies[block].wait_recv()
        local_copies[block].wait()
        return near[place, :] + core_in[place, :].astype(F32)

    def link(index, value, peer):
        link_out[index] = value.astype(BF16)
        copy = pltpu.make_async_remote_copy(
            src_ref=link_out.at[index],
            dst_ref=link_in.at[index],
            send_sem=send_sem.at[8 + index],
            recv_sem=recv_sem.at[8 + index],
            device_id=peer,
            device_id_type=MESH,
        )
        copy.start()
        return copy

    y11 = link(0, partial_sum((0, 1, 1)), y_peer)
    x11 = link(1, partial_sum((1, 1, 1)), x_peer)
    y10 = link(2, partial_sum((0, 1, 0)), y_peer)
    x10 = link(3, partial_sum((1, 1, 0)), x_peer)
    first01, second01 = partial_sum((0, 0, 1)), partial_sum((1, 0, 1))
    y11.wait_recv()
    x01 = link(4, first01 + link_in[0].astype(F32), x_peer)
    x11.wait_recv()
    y01 = link(5, second01 + link_in[1].astype(F32), y_peer)
    first = partial_sum((0, 0, 0))
    second = partial_sum((1, 0, 0))
    y10.wait_recv()
    out_ref[pl.ds(0, rows), :] = first + link_in[2].astype(F32)
    x10.wait_recv()
    out_ref[pl.ds(rows, rows), :] = second + link_in[3].astype(F32)
    x01.wait_recv()
    out_ref[pl.ds(0, rows), :] += link_in[4].astype(F32)
    y01.wait_recv()
    out_ref[pl.ds(rows, rows), :] += link_in[5].astype(F32)
    for copy in (y11, x11, y10, x10, x01, y01):
        copy.wait_send()
    for copy in core_copies.values():
        copy.wait_send()


def reduce8(near, far):
    rows, width = near.shape[0] // 8, near.shape[1]
    return pl.pallas_call(
        functools.partial(reduce8_kernel, rows),
        out_shape=jax.ShapeDtypeStruct((2 * rows, width), F32),
        in_specs=[pl.BlockSpec(memory_space=pl.ANY), pl.BlockSpec(memory_space=pl.ANY)],
        out_specs=pl.BlockSpec(memory_space=pltpu.VMEM),
        scratch_shapes=[
            pltpu.VMEM(near.shape, F32),
            pltpu.VMEM(near.shape, BF16),
            pltpu.VMEM((6, rows, width), BF16),
            pltpu.VMEM((6, rows, width), BF16),
            pltpu.SemaphoreType.DMA((14,)),
            pltpu.SemaphoreType.DMA((14,)),
            pltpu.SemaphoreType.DMA((8,)),
        ],
        compiler_params=remote_params(2, 48 * 1024 * 1024),
        name="reduce8",
    )(near, far)


def tiled(count, tile, step):
    lax.fori_loop(0, count // tile, lambda i, _: step(pl.ds(pl.multiple_of(i * tile, tile), tile)), 0)


def product_reduce8_kernel(rows, filler, *refs):
    if filler:
        acts_ref, weight_ref, lhs_ref, out_ref, grad_ref, *refs = refs
    else:
        acts_ref, weight_ref, out_ref, *refs = refs
    acts, weight, far, near, core_in, link_in, link_out, send_sem, recv_sem, load_sem, *refs = refs
    x_peer, y_peer, c_peer = neighbours()
    width = weight.shape[0]
    wide = 2 * rows
    chunks = [(0, 1), (1, 1), (0, 0), (1, 0)]

    def where(chunk):
        return chunk[0] * 2 * wide + chunk[1] * wide

    load_weight = pltpu.make_async_copy(weight_ref, weight, load_sem.at[8])
    loads = {}
    for number, chunk in enumerate(chunks):
        for side in (1, 0):
            place = pl.ds(side * 4 * wide + where(chunk), wide)
            loads[side, chunk] = pltpu.make_async_copy(
                acts_ref.at[place], acts.at[place], load_sem.at[2 * number + side]
            )
    loads[1, chunks[0]].start()
    load_weight.start()
    for chunk in chunks:
        for side in (1, 0):
            if (side, chunk) != (1, chunks[0]):
                loads[side, chunk].start()
    if filler:
        lhs, grad, grad_sem = refs
        load_lhs = pltpu.make_async_copy(lhs_ref, lhs, load_sem.at[9])
        load_lhs.start()
    greet((x_peer, y_peer, c_peer))

    core_copies = {}

    def product(chunk, side, target):
        loads[side, chunk].wait()
        place = pl.ds(where(chunk), wide)
        source = pl.ds(side * 4 * wide + where(chunk), wide)

        def step(cols):
            target[place, cols] = mm(acts[source, :], weight[cols, :], 1, 1).astype(target.dtype)
            return 0

        tiled(width, width // 2, step)

    def send_core(chunk):
        product(chunk, 1, far)
        number = chunks.index(chunk)
        place = pl.ds(where(chunk), wide)
        core_copies[chunk] = pltpu.make_async_remote_copy(
            src_ref=far.at[place],
            dst_ref=core_in.at[place],
            send_sem=send_sem.at[number],
            recv_sem=recv_sem.at[number],
            device_id=c_peer,
            device_id_type=MESH,
        )
        core_copies[chunk].start()

    def partial_sum(half, outer, inner):
        place = pl.ds(where((half, outer)) + inner * rows, rows)
        return near[place, :] + core_in[place, :].astype(F32)

    def link(index, value, peer):
        link_out[index] = value.astype(BF16)
        copy = pltpu.make_async_remote_copy(
            src_ref=link_out.at[index],
            dst_ref=link_in.at[index],
            send_sem=send_sem.at[4 + index],
            recv_sem=recv_sem.at[4 + index],
            device_id=peer,
            device_id_type=MESH,
        )
        copy.start()
        return copy

    load_weight.wait()
    send_core((0, 1))
    product((0, 1), 0, near)
    core_copies[0, 1].wait_recv()
    y11 = link(0, partial_sum(0, 1, 1), y_peer)
    send_core((1, 1))
    y10 = link(2, partial_sum(0, 1, 0), y_peer)
    product((1, 1), 0, near)
    core_copies[1, 1].wait_recv()
    x11 = link(1, partial_sum(1, 1, 1), x_peer)
    x10 = link(3, partial_sum(1, 1, 0), x_peer)
    send_core((0, 0))
    product((0, 0), 0, near)
    send_core((1, 0))
    product((1, 0), 0, near)
    core_copies[0, 0].wait_recv()
    core_copies[1, 0].wait_recv()
    grad_copies = []
    parts = grad_sem.shape[0] if filler else 0

    def fill(index):
        size = width // parts
        cols = pl.ds(index * size, size)

        def step(columns):
            grad[cols, columns] = mm(lhs[:, cols], acts[:, columns], 0, 0).astype(BF16)
            return 0

        tiled(acts.shape[1], acts.shape[1] // 3, step)
        copy = pltpu.make_async_copy(grad.at[cols], grad_ref.at[cols], grad_sem.at[index])
        copy.start()
        grad_copies.append(copy)

    if filler:
        load_lhs.wait()
    y11.wait_recv()
    x01 = link(4, partial_sum(0, 0, 1) + link_in[0].astype(F32), x_peer)
    if filler:
        fill(0)
    x11.wait_recv()
    y01 = link(5, partial_sum(1, 0, 1) + link_in[1].astype(F32), y_peer)
    for index in range(1, parts):
        fill(index)
    y10.wait_recv()
    out_ref[pl.ds(0, rows), :] = partial_sum(0, 0, 0) + link_in[2].astype(F32)
    x10.wait_recv()
    out_ref[pl.ds(rows, rows), :] = partial_sum(1, 0, 0) + link_in[3].astype(F32)
    x01.wait_recv()
    out_ref[pl.ds(0, rows), :] += link_in[4].astype(F32)
    y01.wait_recv()
    out_ref[pl.ds(rows, rows), :] += link_in[5].astype(F32)
    for copy in (y11, x11, y10, x10, x01, y01):
        copy.wait_send()
    for copy in core_copies.values():
        copy.wait_send()
    for copy in grad_copies:
        copy.wait()


def product_reduce8(acts, weight, number, lhs=None):
    rows, width, depth = acts.shape[0] // 16, weight.shape[0], weight.shape[1]
    filler = lhs is not None
    hbm = pl.BlockSpec(memory_space=pl.ANY)
    parts = 4
    scratch = [
        pltpu.VMEM(acts.shape, BF16),
        pltpu.VMEM(weight.shape, BF16),
        pltpu.VMEM((8 * rows, width), BF16),
        pltpu.VMEM((8 * rows, width), F32),
        pltpu.VMEM((8 * rows, width), BF16),
        pltpu.VMEM((6, rows, width), BF16),
        pltpu.VMEM((6, rows, width), BF16),
        pltpu.SemaphoreType.DMA((10,)),
        pltpu.SemaphoreType.DMA((10,)),
        pltpu.SemaphoreType.DMA((10,)),
    ]
    out_shape = [jax.ShapeDtypeStruct((2 * rows, width), F32)]
    out_specs = [pl.BlockSpec(memory_space=pltpu.VMEM)]
    flops = 2 * acts.shape[0] * width * depth
    if filler:
        scratch += [
            pltpu.VMEM(lhs.shape, BF16),
            pltpu.VMEM((width, depth), BF16),
            pltpu.SemaphoreType.DMA((parts,)),
        ]
        out_shape.append(jax.ShapeDtypeStruct((width, depth), BF16))
        out_specs.append(hbm)
        flops *= 2
    outs = pl.pallas_call(
        functools.partial(product_reduce8_kernel, rows, filler),
        out_shape=out_shape,
        in_specs=[hbm] * (3 if filler else 2),
        out_specs=out_specs,
        scratch_shapes=scratch,
        compiler_params=remote_params(number, 63 * 1024 * 1024),
        cost_estimate=pl.CostEstimate(
            flops=flops, bytes_accessed=4 * (acts.size + weight.size), transcendentals=0
        ),
        name="product_reduce8",
    )(acts, weight, *((lhs,) if filler else ()))
    return outs if filler else outs[0]


def shard_kernel(plan, outs, *refs):
    ins, out_refs = refs[: len(plan)], refs[len(plan) : len(plan) + outs]
    stage = refs[len(plan) + outs : 2 * len(plan) + outs]
    send_sem, recv_sem, load_sem, store_sem = refs[2 * len(plan) + outs :]
    x_peer, _, _ = neighbours()
    odd = lax.rem(lax.axis_index("fsdp"), 2)
    column = 2 * lax.axis_index("ctx") + odd
    other = 2 * lax.axis_index("ctx") + 1 - odd
    greet((x_peer,))
    remote, loads, stores = [], [], []
    for number, (which, start, size, cut) in enumerate(plan):
        rows = ins[number].shape[0]
        place = pl.ds(pl.multiple_of(odd * rows, rows), rows)
        target = out_refs[which].at[place, pl.ds(start, size)]

        def source(index, ref=ins[number], size=size, cut=cut):
            if not cut:
                return ref
            return ref.at[:, pl.ds(pl.multiple_of(index * size, HEAD), size)]

        remote.append(
            pltpu.make_async_remote_copy(
                src_ref=source(other),
                dst_ref=target,
                send_sem=send_sem.at[number],
                recv_sem=recv_sem.at[number],
                device_id=x_peer,
                device_id_type=MESH,
            )
        )
        loads.append(pltpu.make_async_copy(source(column), stage[number], load_sem.at[number]))
        stores.append(pltpu.make_async_copy(stage[number], target, store_sem.at[number]))
    for copy in remote:
        copy.start()
    for copy in loads:
        copy.start()
    for load, store in zip(loads, stores):
        load.wait()
        store.start()
    for copy in stores:
        copy.wait()
    for copy in remote:
        copy.wait()


def shards(groups, number):
    plan, arrays, shapes = [], [], []
    for which, group in enumerate(groups):
        start = 0
        for array, cut in group:
            size = array.shape[1] // 4 if cut else array.shape[1]
            plan.append((which, start, size, cut))
            arrays.append(array)
            start += size
        shapes.append((2 * group[0][0].shape[0], start))
    hbm = pl.BlockSpec(memory_space=pl.ANY)
    return pl.pallas_call(
        functools.partial(shard_kernel, tuple(plan), len(groups)),
        out_shape=[jax.ShapeDtypeStruct(shape, BF16) for shape in shapes],
        in_specs=[hbm] * len(arrays),
        out_specs=[hbm] * len(groups),
        scratch_shapes=[
            pltpu.VMEM((array.shape[0], size), BF16)
            for array, (_, _, size, _) in zip(arrays, plan)
        ]
        + [pltpu.SemaphoreType.DMA((len(plan),))] * 4,
        compiler_params=remote_params(number),
        name="shards",
    )(*arrays)


def total_kernel(stages, part_ref, out_ref, inbox, outbox, send_sem, recv_sem):
    peers = []
    for axis, bit in stages:
        mine = lax.axis_index(axis)
        peers.append({axis: mine + bit * (1 - 2 * lax.rem(mine // bit, 2))})
    greet(peers)
    value = part_ref[...]
    copies = []
    for index, peer in enumerate(peers):
        outbox[index] = value
        copy = pltpu.make_async_remote_copy(
            src_ref=outbox.at[index],
            dst_ref=inbox.at[index],
            send_sem=send_sem.at[index],
            recv_sem=recv_sem.at[index],
            device_id=peer,
            device_id_type=MESH,
        )
        copy.start()
        copies.append(copy)
        copy.wait_recv()
        value = value + inbox[index]
    out_ref[...] = value
    for copy in copies:
        copy.wait_send()


def total(part):
    stages, bit = [], 2
    while bit < lax.axis_size("fsdp"):
        stages.append(("fsdp", bit))
        bit *= 2
    stages += [("tp", 1), ("fsdp", 1), ("ctx", 1)]
    return pl.pallas_call(
        functools.partial(total_kernel, tuple(stages)),
        out_shape=jax.ShapeDtypeStruct(part.shape, F32),
        in_specs=[pl.BlockSpec(memory_space=pltpu.VMEM)],
        out_specs=pl.BlockSpec(memory_space=pltpu.VMEM),
        scratch_shapes=[
            pltpu.VMEM((len(stages),) + part.shape, F32),
            pltpu.VMEM((len(stages),) + part.shape, F32),
            pltpu.SemaphoreType.DMA((len(stages),)),
            pltpu.SemaphoreType.DMA((len(stages),)),
        ],
        compiler_params=remote_params(5),
        name="total",
    )(part)


def join_kernel(sizes, spot_ref, kept_ref, x_ref, y_ref, both_ref, *out_refs):
    place, odd = spot_ref[0], spot_ref[1]
    parts = (
        (kept_ref, 2 * place + odd),
        (x_ref, 2 * place + 1 - odd),
        (y_ref, 2 - 2 * place + odd),
        (both_ref, 3 - 2 * place - odd),
    )
    for part, column in parts:
        start = 0
        for size, out_ref in zip(sizes, out_refs):
            target = pl.ds(pl.multiple_of(column * size, HEAD), size)
            out_ref[:, target] = part[:, start : start + size].astype(F32)
            start += size


def join_columns(spot, parts, sizes):
    rows = parts[0].shape[0]
    tile = min(rows, 64)
    return pl.pallas_call(
        functools.partial(join_kernel, sizes),
        out_shape=[jax.ShapeDtypeStruct((rows, 4 * size), F32) for size in sizes],
        grid_spec=pltpu.PrefetchScalarGridSpec(
            num_scalar_prefetch=1,
            grid=(rows // tile,),
            in_specs=[
                pl.BlockSpec((tile, part.shape[1]), lambda i, spot: (i, 0)) for part in parts
            ],
            out_specs=[pl.BlockSpec((tile, 4 * size), lambda i, spot: (i, 0)) for size in sizes],
        ),
        name="join",
    )(spot, *parts)


def after(value, *others):
    return lax.optimization_barrier((value,) + others)[0]


def reduce4_links(kept, to_y, to_x, *others):
    rows = kept.shape[0] // 4
    came_first, came_second = swap_ctx(to_y), swap_x(to_x)
    first = kept[: 2 * rows] + after(came_first, *others).astype(F32)
    second = kept[2 * rows :] + after(came_second, *others).astype(F32)
    came_first = swap_x(first[rows:].astype(BF16))
    came_second = swap_ctx(second[rows:].astype(BF16))
    return first[:rows], second[:rows], came_first, came_second


def rope_tables(positions):
    freqs = THETA ** (-(jnp.arange(HEAD // 2, dtype=F32) * 2.0) / HEAD)
    angle = positions[:, None] * freqs[None, :]
    cosine = jnp.concatenate([jnp.cos(angle), jnp.cos(angle)], axis=-1)
    sine = jnp.concatenate([-jnp.sin(angle), jnp.sin(angle)], axis=-1)
    return cosine, sine


def norm_back(grad, scaled, inverse, gain):
    weighted = grad * gain
    return inverse * (weighted - scaled * jnp.mean(weighted * scaled, axis=-1, keepdims=True))


def inv_rms(value):
    return lax.rsqrt(jnp.mean(value * value, axis=-1, keepdims=True) + EPS)


def block_row(meta_ref, seq, index, rows):
    away_c = lax.rem(meta_ref[0] + index // 4, 2)
    away_t = lax.rem(meta_ref[1] + (index // 2) % 2, 2)
    if index % 2 == 0:
        inner = away_c * 2 + seq
    else:
        inner = seq * 2 + away_c + 4
    return pl.multiple_of((away_t * 8 + inner) * rows, rows)


def scaled_of(raw):
    inverse = lax.rsqrt(jnp.mean(raw * raw, axis=-1, keepdims=True) + EPS)
    return raw * inverse, inverse


def load_heads(meta_ref, qkv_ref, cos_ref, sin_ref, gain_ref, q_scr, k_scr, v_scr, heads):
    seq = pl.program_id(0)
    rows = q_scr.shape[1] // 8
    for index in range(8):
        start = block_row(meta_ref, seq, index, rows)
        here = slice(index * rows, (index + 1) * rows)
        cosine, sine = cos_ref[here, :], sin_ref[here, :]
        for head in range(heads + 1):
            raw = qkv_ref[pl.ds(start, rows), head * HEAD : (head + 1) * HEAD]
            scaled, _ = scaled_of(raw)
            which = 0 if head < heads else 1
            value = scaled * gain_ref[which : which + 1, :]
            turned = value * cosine + pltpu.roll(value, HEAD // 2, 1) * sine
            if head < heads:
                q_scr[head, here, :] = turned.astype(BF16)
            else:
                k_scr[here, :] = turned.astype(BF16)
        v_scr[here, :] = qkv_ref[
            pl.ds(start, rows), (heads + 1) * HEAD : (heads + 2) * HEAD
        ].astype(BF16)


def key_span(index, tile):
    low = max(0, (index * tile - (MOST_DOC - 1)) // tile) * tile
    return low, (index + 1) * tile


def allowed_mask(segc_ref, segr_ref, index, tile):
    low, high = key_span(index, tile)
    shape = (tile, high - low)
    rows = lax.broadcasted_iota(jnp.int32, shape, 0) + index * tile
    cols = lax.broadcasted_iota(jnp.int32, shape, 1) + low
    same = segc_ref[0, index * tile : (index + 1) * tile, :] == segr_ref[0, :, low:high]
    return same & (cols <= rows)


def probs_of(query, keys, allowed, scale):
    scores = jnp.where(allowed, mm(query, keys, 1, 1) * scale, MASKED)
    weights = jnp.exp(scores - jnp.max(scores, axis=-1, keepdims=True))
    return weights * (1.0 / jnp.sum(weights, axis=-1, keepdims=True))


def attend_kernel(
    heads, tile, meta_ref, qkv_ref, segc_ref, segr_ref, cos_ref, sin_ref, gain_ref, out_ref, q_scr, k_scr, v_scr
):
    seq = pl.program_id(0)
    length = k_scr.shape[0]
    rows = length // 8
    scale = 1.0 / math.sqrt(HEAD)
    load_heads(meta_ref, qkv_ref, cos_ref, sin_ref, gain_ref, q_scr, k_scr, v_scr, heads)
    for index in range(length // tile):
        low, high = key_span(index, tile)
        allowed = allowed_mask(segc_ref, segr_ref, index, tile)
        for head in range(heads):
            query = q_scr[head, index * tile : (index + 1) * tile, :]
            probs = probs_of(query, k_scr[low:high, :], allowed, scale)
            mixed = mm(probs.astype(BF16), v_scr[low:high, :], 1, 0).astype(BF16)
            for piece in range(tile // rows):
                start = block_row(meta_ref, seq, index * (tile // rows) + piece, rows)
                out_ref[pl.ds(start, rows), head * HEAD : (head + 1) * HEAD] = mixed[
                    piece * rows : (piece + 1) * rows
                ]


def attend_back_kernel(
    heads,
    tile,
    meta_ref,
    qkv_ref,
    grad_ref,
    segc_ref,
    segr_ref,
    cos_ref,
    sin_ref,
    gain_ref,
    out_ref,
    gain_out_ref,
    q_scr,
    k_scr,
    v_scr,
    g_scr,
    dk_scr,
    dv_scr,
):
    seq = pl.program_id(0)
    length = k_scr.shape[0]
    rows = length // 8
    scale = 1.0 / math.sqrt(HEAD)
    load_heads(meta_ref, qkv_ref, cos_ref, sin_ref, gain_ref, q_scr, k_scr, v_scr, heads)
    for index in range(8):
        start = block_row(meta_ref, seq, index, rows)
        g_scr[index * rows : (index + 1) * rows, :] = grad_ref[pl.ds(start, rows), :]
    dk_scr[...] = jnp.zeros_like(dk_scr)
    dv_scr[...] = jnp.zeros_like(dv_scr)

    @pl.when(seq == 0)
    def _():
        gain_out_ref[...] = jnp.zeros_like(gain_out_ref)

    def finish(grad, index, head, which):
        here = slice(index * rows, (index + 1) * rows)
        start = block_row(meta_ref, seq, index, rows)
        grad = grad * cos_ref[here, :] - pltpu.roll(grad, HEAD // 2, 1) * sin_ref[here, :]
        raw = qkv_ref[pl.ds(start, rows), head * HEAD : (head + 1) * HEAD]
        scaled, inverse = scaled_of(raw)
        gain_out_ref[which : which + 1, :] += jnp.sum(grad * scaled, axis=0, keepdims=True)
        out = norm_back(grad, scaled, inverse, gain_ref[which : which + 1, :])
        out_ref[pl.ds(start, rows), head * HEAD : (head + 1) * HEAD] = out.astype(BF16)

    per = tile // rows
    for index in range(length // tile):
        low, high = key_span(index, tile)
        mine = slice(index * tile, (index + 1) * tile)
        allowed = allowed_mask(segc_ref, segr_ref, index, tile)
        for head in range(heads):
            query = q_scr[head, mine, :]
            keys = k_scr[low:high, :]
            probs = probs_of(query, keys, allowed, scale)
            grad = g_scr[mine, head * HEAD : (head + 1) * HEAD]
            grad_probs = mm(grad, v_scr[low:high, :], 1, 1)
            delta = jnp.sum(probs * grad_probs, axis=-1, keepdims=True)
            grad_scores = (probs * (grad_probs - delta)).astype(BF16)
            dv_scr[low:high, :] += mm(probs.astype(BF16), grad, 0, 0)
            dk_scr[low:high, :] += mm(grad_scores, query, 0, 0) * scale
            grad_query = mm(grad_scores, keys, 1, 0) * scale
            for piece in range(per):
                finish(
                    grad_query[piece * rows : (piece + 1) * rows], index * per + piece, head, 0
                )
    for index in range(8):
        here = slice(index * rows, (index + 1) * rows)
        start = block_row(meta_ref, seq, index, rows)
        finish(dk_scr[here, :], index, heads, 1)
        out_ref[pl.ds(start, rows), (heads + 1) * HEAD : (heads + 2) * HEAD] = dv_scr[
            here, :
        ].astype(BF16)


def whole(shape):
    return pl.BlockSpec(shape, lambda seq, meta: (0,) * len(shape))


def seg_specs(length):
    return [
        pl.BlockSpec((1, length, 1), lambda seq, meta: (seq, 0, 0)),
        pl.BlockSpec((1, 1, length), lambda seq, meta: (seq, 0, 0)),
    ]


def attend(meta, qkv, seg_cols, seg_rows, cosine, sine, gains):
    length = cosine.shape[0]
    tile = length // 4
    heads = qkv.shape[1] // HEAD - 2
    pairs = 2 * heads * length * length // 2
    return pl.pallas_call(
        functools.partial(attend_kernel, heads, tile),
        out_shape=jax.ShapeDtypeStruct((qkv.shape[0], heads * HEAD), BF16),
        grid_spec=pltpu.PrefetchScalarGridSpec(
            num_scalar_prefetch=1,
            grid=(2,),
            in_specs=[whole(qkv.shape)]
            + seg_specs(length)
            + [whole(cosine.shape), whole(sine.shape), whole(gains.shape)],
            out_specs=whole((qkv.shape[0], heads * HEAD)),
            scratch_shapes=[
                pltpu.VMEM((heads, length, HEAD), BF16),
                pltpu.VMEM((length, HEAD), BF16),
                pltpu.VMEM((length, HEAD), BF16),
            ],
        ),
        cost_estimate=pl.CostEstimate(
            flops=4 * pairs * HEAD, bytes_accessed=qkv.size * 4 + qkv.size, transcendentals=pairs
        ),
        name="attend",
    )(meta, qkv, seg_cols, seg_rows, cosine, sine, gains)


def attend_back(meta, qkv, grad, seg_cols, seg_rows, cosine, sine, gains):
    length = cosine.shape[0]
    tile = length // 4
    heads = qkv.shape[1] // HEAD - 2
    pairs = 2 * heads * length * length // 2
    return pl.pallas_call(
        functools.partial(attend_back_kernel, heads, tile),
        out_shape=(
            jax.ShapeDtypeStruct(qkv.shape, BF16),
            jax.ShapeDtypeStruct(gains.shape, F32),
        ),
        grid_spec=pltpu.PrefetchScalarGridSpec(
            num_scalar_prefetch=1,
            grid=(2,),
            in_specs=[whole(qkv.shape), whole(grad.shape)]
            + seg_specs(length)
            + [whole(cosine.shape), whole(sine.shape), whole(gains.shape)],
            out_specs=(whole(qkv.shape), whole(gains.shape)),
            scratch_shapes=[
                pltpu.VMEM((heads, length, HEAD), BF16),
                pltpu.VMEM((length, HEAD), BF16),
                pltpu.VMEM((length, HEAD), BF16),
                pltpu.VMEM((length, heads * HEAD), BF16),
                pltpu.VMEM((length, HEAD), F32),
                pltpu.VMEM((length, HEAD), F32),
            ],
        ),
        cost_estimate=pl.CostEstimate(
            flops=10 * pairs * HEAD, bytes_accessed=qkv.size * 8, transcendentals=pairs
        ),
        name="attend_back",
    )(meta, qkv, grad, seg_cols, seg_rows, cosine, sine, gains)


def body(
    tokens,
    segment_ids,
    norm_gain,
    query_weight,
    key_matrix,
    value_matrix,
    output_weight,
    query_gain,
    key_gain,
    mlp_gain,
    gate_weight,
    up_weight,
    down_weight,
    cotangent,
):
    local, width = tokens.shape[1], tokens.shape[2]
    length = 2 * local
    quarter = local // 2
    count = lax.axis_size("fsdp")
    block = width // count
    mine = lax.axis_index("fsdp")
    odd = mine % 2
    place = lax.axis_index("ctx")
    core = lax.axis_index("tp")

    small = query_gain.shape[0]
    lanes = jnp.arange(HEAD)[None, :]

    def pad_rows(vector):
        return jnp.concatenate([vector, jnp.zeros((block - small,), BF16)])

    gains = jnp.where(
        lanes == 0,
        norm_gain[:, None],
        jnp.where(
            lanes == 1,
            mlp_gain[:, None],
            jnp.where(
                lanes == 2, pad_rows(query_gain)[:, None], pad_rows(key_gain)[:, None]
            ),
        ),
    )
    far_segments = swap_x(segment_ids)
    (first_pair,) = shards(
        [
            [
                (query_weight, True),
                (key_matrix, True),
                (value_matrix, True),
                (output_weight, True),
                (gains, False),
            ]
        ],
        3,
    )
    first = gather_line(first_pair)
    gate_up_pair, down_pair = shards(
        [
            [(after(gate_weight, first_pair), True), (up_weight, True)],
            [(down_weight, True)],
        ],
        4,
    )
    gate_up_w = gather_line(gate_up_pair)
    down_w = gather_line(down_pair)

    def own_quarter(value):
        return lax.dynamic_slice_in_dim(value.reshape(local, width), core * quarter, quarter, 0)

    own_tok, own_cot = own_quarter(tokens), own_quarter(cotangent)
    tok = gather8(after(own_tok, gate_up_pair))
    segments = jnp.concatenate([segment_ids, far_segments])
    seg_cols, seg_rows = segments[:, :, None], segments[:, None, :]
    cosine, sine = rope_tables(jnp.arange(length).astype(F32))
    meta = jnp.stack([place, core]).astype(jnp.int32)

    heads_q = query_weight.shape[1] // 4 // HEAD
    cols = (heads_q + 2) * HEAD
    qkv_w = first[:, :cols]
    out_w = first[:, cols : cols + heads_q * HEAD]
    gain_cols = first[:, cols + heads_q * HEAD :].astype(F32)
    in_gain, mid_gain = gain_cols[:, 0][None], gain_cols[:, 1][None]
    head_gains = gain_cols.reshape(count, block, HEAD)[:, :small, 2:4].reshape(HEAD, 2).T

    in_f = tok.astype(F32)
    cot_from = after(own_cot, tok)
    cot_x, cot_y = swap_x(cot_from), swap_ctx(cot_from)
    x_all = (in_f * inv_rms(in_f) * in_gain).astype(BF16)
    qkv = mm(x_all, qkv_w, 1, 0)
    attended = attend(meta, qkv, seg_cols, seg_rows, cosine, sine, head_gains)
    half = 4 * quarter
    cot_x, cot_y = after(cot_x, attended), after(cot_y, attended)
    eighth = quarter // 2
    cot_first, cot_second = swap_ctx(cot_x[:eighth]), swap_x(cot_y[eighth:])
    out_far = mm(attended[half:], out_w, 1, 1).astype(BF16)
    out_near = mm(attended[:half], out_w, 1, 1)
    middle = own_tok.astype(F32) + reduce8(out_near, out_far)
    inverse_mid = inv_rms(middle)
    scaled_mid = middle * inverse_mid
    y_own = (scaled_mid * mid_gain).astype(BF16)
    cot_first, cot_second = after(cot_first, y_own), after(cot_second, y_own)
    y_all, cot = gather8(y_own, (cot_from, cot_x, cot_y, cot_first, cot_second))

    ff = gate_up_w.shape[1] // 2
    gate_up = mm(y_all, gate_up_w, 1, 0)
    gate, up_value = gate_up[:, :ff], gate_up[:, ff:]
    sig = jax.nn.sigmoid(gate)
    active = gate * sig
    hidden = (active * up_value).astype(BF16)
    down_grad = mm(cot, hidden, 0, 0).astype(BF16)

    def finish_rows(own):
        pair = jnp.stack([own, swap_core(own)])
        return flip_if(core == 1, pair, 0).reshape(tokens.shape)

    grad_hidden = mm(after(cot, down_grad), down_w, 1, 0)
    grad_up = (grad_hidden * active).astype(BF16)
    grad_gate = (grad_hidden * up_value * (sig * (1.0 + gate * (1.0 - sig)))).astype(BF16)
    grad_gate_up = jnp.concatenate([grad_gate, grad_up], axis=1)
    mid_grad, gate_up_grad = product_reduce8(grad_gate_up, gate_up_w, 7, y_all)

    mlp_gain_part = jnp.sum(mid_grad * scaled_mid, axis=0)
    grad_middle = own_cot.astype(F32) + norm_back(mid_grad, scaled_mid, inverse_mid, mid_gain)
    grad_attn, mlp_kept, mlp_to_y, mlp_to_x = gather8_product(
        grad_middle.astype(BF16), hidden, down_w
    )
    out_grad = mm(grad_attn, attended, 0, 0).astype(BF16)
    grad_att = mm(grad_attn, out_w, 1, 0).astype(BF16)
    raw_grads, head_gain_parts = attend_back(
        meta, qkv, grad_att, seg_cols, seg_rows, cosine, sine, head_gains
    )
    first_grad = jnp.concatenate([mm(x_all, raw_grads, 0, 0).astype(BF16), out_grad], axis=1)
    mlp_first, mlp_second, mlp_came1, mlp_came2 = reduce4_links(mlp_kept, mlp_to_y, mlp_to_x, raw_grads)
    in_grad = product_reduce8(after(raw_grads, first_grad), qkv_w, 8)

    mlp_first = mlp_first + after(mlp_came1, in_grad).astype(F32)
    mlp_second = mlp_second + after(mlp_came2, in_grad).astype(F32)
    layer_out = finish_rows((middle + jnp.concatenate([mlp_first, mlp_second])).astype(BF16))

    spot = jnp.stack([place, odd]).astype(jnp.int32)

    def owners(grad, sizes, *others):
        rows = scatter_line(grad)
        rows = after(rows, *others)
        kept = lax.dynamic_slice_in_dim(rows, odd * block, block, 0)
        sent = lax.dynamic_slice_in_dim(rows, (1 - odd) * block, block, 0)
        by_x, by_y = swap_x(sent), swap_ctx(kept)
        by_both = swap_ctx(by_x)
        return join_columns(spot, (kept, by_x, by_y, by_both), sizes)

    (down_share,) = owners(down_grad, (ff,))
    gate_share, up_share = owners(gate_up_grad, (ff, ff))
    query_share, key_share, value_share, out_share = owners(
        first_grad, (heads_q * HEAD, HEAD, HEAD, heads_q * HEAD)
    )

    own_in = own_tok.astype(F32)
    inverse_in = inv_rms(own_in)
    scaled_in = own_in * inverse_in
    norm_gain_part = jnp.sum(in_grad * scaled_in, axis=0)
    token_grad = finish_rows(
        (grad_middle + norm_back(in_grad, scaled_in, inverse_in, in_gain)).astype(BF16)
    )

    parts = jnp.concatenate([norm_gain_part, mlp_gain_part, head_gain_parts.reshape(-1)])
    sums = total(parts.reshape(-1, HEAD)).reshape(-1)
    norm_gain_grad = lax.dynamic_slice_in_dim(sums, mine * block, block, 0)
    mlp_gain_grad = lax.dynamic_slice_in_dim(sums, width + mine * block, block, 0)
    query_gain_grad = lax.dynamic_slice_in_dim(sums, 2 * width + mine * small, small, 0)
    key_gain_grad = lax.dynamic_slice_in_dim(sums, 2 * width + HEAD + mine * small, small, 0)
    return (
        layer_out,
        token_grad,
        norm_gain_grad,
        query_share,
        key_share,
        value_share,
        out_share,
        query_gain_grad,
        key_gain_grad,
        mlp_gain_grad,
        gate_share,
        up_share,
        down_share,
    )


def solution(mesh):
    in_specs = (
        P("fsdp", "ctx", None),
        P("fsdp", None),
        P("fsdp"),
        P("fsdp", "tp"),
        P("fsdp", "tp"),
        P("fsdp", "tp"),
        P("fsdp", "tp"),
        P("fsdp"),
        P("fsdp"),
        P("fsdp"),
        P("fsdp", "tp"),
        P("fsdp", "tp"),
        P("fsdp", "tp"),
        P("fsdp", "ctx", None),
    )
    out_specs = (
        P("fsdp", "ctx", None),
        P("fsdp", "ctx", None),
        P("fsdp"),
        P("fsdp", "tp"),
        P("fsdp", "tp"),
        P("fsdp", "tp"),
        P("fsdp", "tp"),
        P("fsdp"),
        P("fsdp"),
        P("fsdp"),
        P("fsdp", "tp"),
        P("fsdp", "tp"),
        P("fsdp", "tp"),
    )

    return jax.shard_map(body, mesh=mesh, in_specs=in_specs, out_specs=out_specs, check_vma=False)
```

```python
import functools
import math

import jax
import jax.numpy as jnp
from jax import lax
from jax.experimental import pallas as pl
from jax.experimental.pallas import tpu as pltpu
from jax.sharding import PartitionSpec as P


HEAD = 128
EPS = 1e-06
THETA = 1000000.0
MASKED = -1e30
MOST_DOC = 512
MESH = pl.DeviceIdType.MESH
F32 = jnp.float32
BF16 = jnp.bfloat16


def mm(left, right, left_dim, right_dim):
    return lax.dot_general(
        left, right, (((left_dim,), (right_dim,)), ((), ())), preferred_element_type=F32
    )


def swap_core(value):
    return lax.ppermute(value, "tp", [(0, 1), (1, 0)])


def swap_ctx(value):
    return lax.ppermute(value, "ctx", [(0, 1), (1, 0)])


def swap_x(value):
    count = lax.axis_size("fsdp")
    return lax.ppermute(value, "fsdp", [(i, i ^ 1) for i in range(count)])


def lines():
    count = lax.axis_size("fsdp")
    return [[i for i in range(count) if i % 2 == parity] for parity in (0, 1)]


def gather_line(value):
    return lax.all_gather(value, "fsdp", axis=0, tiled=True, axis_index_groups=lines())


def scatter_line(value):
    return lax.psum_scatter(
        value, "fsdp", scatter_dimension=0, tiled=True, axis_index_groups=lines()
    )


def flip_if(flag, value, axis):
    return jnp.where(flag, jnp.flip(value, axis), value)


def neighbours():
    mine = lax.axis_index("fsdp")
    return (
        {"fsdp": mine + 1 - 2 * lax.rem(mine, 2)},
        {"ctx": 1 - lax.axis_index("ctx")},
        {"tp": 1 - lax.axis_index("tp")},
    )


def greet(peers):
    barrier = pltpu.get_barrier_semaphore()
    for peer in peers:
        pl.semaphore_signal(barrier, inc=1, device_id=peer, device_id_type=MESH)
    pl.semaphore_wait(barrier, len(peers))


def remote_params(number, limit=None):
    return pltpu.CompilerParams(
        collective_id=number, has_side_effects=True, vmem_limit_bytes=limit
    )


def gather8_kernel(rows, spread, *refs):
    if spread:
        own_ref, kept_ref, x_ref, y_ref, first_ref, second_ref, out_ref, also_ref = refs[:8]
        send_sem, recv_sem, local_sem, stage, also_send, also_recv, also_in, also_out = refs[8:]
    else:
        own_ref, out_ref, send_sem, recv_sem, local_sem = refs
    x_peer, y_peer, c_peer = neighbours()

    def start_of(away_t, half, outer, inner):
        return pl.ds((away_t * 8 + half * 4 + outer * 2 + inner) * rows, rows)

    def slot(*block):
        return out_ref.at[start_of(*block)]

    also_loads, also_remote, also_stores = [], [], []
    if spread:
        top, low = pl.ds(0, rows), pl.ds(rows, rows)
        pieces = [
            ((0, 0, 0), kept_ref.at[top]),
            ((0, 0, 1), x_ref.at[top]),
            ((0, 1, 0), y_ref.at[top]),
            ((0, 1, 1), first_ref),
            ((1, 0, 0), kept_ref.at[low]),
            ((1, 0, 1), y_ref.at[low]),
            ((1, 1, 0), x_ref.at[low]),
            ((1, 1, 1), second_ref),
        ]
        for index, (block, source) in enumerate(pieces):
            also_loads.append(pltpu.make_async_copy(source, stage.at[index], also_in.at[index]))
            also_stores.append(
                pltpu.make_async_copy(
                    stage.at[index], also_ref.at[start_of(0, *block)], also_out.at[index]
                )
            )
            also_remote.append(
                pltpu.make_async_remote_copy(
                    src_ref=source,
                    dst_ref=also_ref.at[start_of(1, *block)],
                    send_sem=also_send.at[index],
                    recv_sem=also_recv.at[index],
                    device_id=c_peer,
                    device_id_type=MESH,
                )
            )
        for copy in also_loads:
            copy.start()
    greet((x_peer, y_peer, c_peer))

    number = iter(range(14))

    def send(source, target, peer):
        index = next(number)
        copy = pltpu.make_async_remote_copy(
            src_ref=source,
            dst_ref=target,
            send_sem=send_sem.at[index],
            recv_sem=recv_sem.at[index],
            device_id=peer,
            device_id_type=MESH,
        )
        copy.start()
        return copy

    first, second = own_ref.at[pl.ds(0, rows)], own_ref.at[pl.ds(rows, rows)]
    x1 = send(first, slot(0, 0, 0, 1), x_peer)
    y1 = send(second, slot(0, 1, 0, 1), y_peer)
    x2 = send(second, slot(0, 1, 1, 0), x_peer)
    y2 = send(first, slot(0, 0, 1, 0), y_peer)
    rest = [send(first, slot(1, 0, 0, 0), c_peer), send(second, slot(1, 1, 0, 0), c_peer)]
    kept = [
        pltpu.make_async_copy(first, slot(0, 0, 0, 0), local_sem.at[0]),
        pltpu.make_async_copy(second, slot(0, 1, 0, 0), local_sem.at[1]),
    ]
    for copy in kept:
        copy.start()
    for copy in also_remote:
        copy.start()
    for load, store in zip(also_loads, also_stores):
        load.wait()
        store.start()
    x1.wait_recv()
    y3 = send(slot(0, 0, 0, 1), slot(0, 0, 1, 1), y_peer)
    y1.wait_recv()
    x3 = send(slot(0, 1, 0, 1), slot(0, 1, 1, 1), x_peer)
    rest.append(send(slot(0, 0, 0, 1), slot(1, 0, 0, 1), c_peer))
    rest.append(send(slot(0, 1, 0, 1), slot(1, 1, 0, 1), c_peer))
    x2.wait_recv()
    rest.append(send(slot(0, 1, 1, 0), slot(1, 1, 1, 0), c_peer))
    y2.wait_recv()
    rest.append(send(slot(0, 0, 1, 0), slot(1, 0, 1, 0), c_peer))
    y3.wait_recv()
    rest.append(send(slot(0, 0, 1, 1), slot(1, 0, 1, 1), c_peer))
    x3.wait_recv()
    rest.append(send(slot(0, 1, 1, 1), slot(1, 1, 1, 1), c_peer))
    for copy in (x1, y1, x2, y2, y3, x3):
        copy.wait_send()
    for copy in rest + also_remote + kept + also_stores:
        copy.wait()


def gather8_product_kernel(
    rows,
    own_ref,
    acts_ref,
    weight_ref,
    out_ref,
    kept_ref,
    to_y_ref,
    to_x_ref,
    send_sem,
    recv_sem,
    local_sem,
    acts,
    weight,
    far,
    core_in,
    core_send,
    core_recv,
    load_sem,
):
    x_peer, y_peer, c_peer = neighbours()
    width = weight.shape[0]
    wide = 2 * rows
    loads = [
        pltpu.make_async_copy(weight_ref, weight, load_sem.at[0]),
        pltpu.make_async_copy(acts_ref, acts, load_sem.at[1]),
    ]
    for copy in loads:
        copy.start()
    greet((x_peer, y_peer, c_peer))

    def slot(away_t, half, outer, inner):
        return out_ref.at[pl.ds((away_t * 8 + half * 4 + outer * 2 + inner) * rows, rows)]

    number = iter(range(14))

    def send(source, target, peer):
        index = next(number)
        copy = pltpu.make_async_remote_copy(
            src_ref=source,
            dst_ref=target,
            send_sem=send_sem.at[index],
            recv_sem=recv_sem.at[index],
            device_id=peer,
            device_id_type=MESH,
        )
        copy.start()
        return copy

    core_copies = []

    def far_chunk(index):
        place = pl.ds(index * wide, wide)
        source = pl.ds(4 * wide + index * wide, wide)

        def step(cols):
            far[place, cols] = mm(acts[source, :], weight[cols, :], 1, 1).astype(BF16)
            return 0

        tiled(width, width // 2, step)
        copy = pltpu.make_async_remote_copy(
            src_ref=far.at[place],
            dst_ref=core_in.at[place],
            send_sem=core_send.at[index],
            recv_sem=core_recv.at[index],
            device_id=c_peer,
            device_id_type=MESH,
        )
        copy.start()
        core_copies.append(copy)

    def near_chunk(index, target_ref, start):
        core_copies[index].wait_recv()
        place = pl.ds(index * wide, wide)
        target = pl.ds(start, wide)

        def step(cols):
            value = mm(acts[place, :], weight[cols, :], 1, 1) + core_in[place, cols].astype(F32)
            target_ref[target, cols] = value.astype(target_ref.dtype)
            return 0

        tiled(width, width // 2, step)

    first, second = own_ref.at[pl.ds(0, rows)], own_ref.at[pl.ds(rows, rows)]
    x1 = send(first, slot(0, 0, 0, 1), x_peer)
    y1 = send(second, slot(0, 1, 0, 1), y_peer)
    x2 = send(second, slot(0, 1, 1, 0), x_peer)
    y2 = send(first, slot(0, 0, 1, 0), y_peer)
    rest = [send(first, slot(1, 0, 0, 0), c_peer), send(second, slot(1, 1, 0, 0), c_peer)]
    kept = [
        pltpu.make_async_copy(first, slot(0, 0, 0, 0), local_sem.at[0]),
        pltpu.make_async_copy(second, slot(0, 1, 0, 0), local_sem.at[1]),
    ]
    for copy in kept:
        copy.start()
    for copy in loads:
        copy.wait()
    for index in range(4):
        far_chunk(index)
    x1.wait_recv()
    y3 = send(slot(0, 0, 0, 1), slot(0, 0, 1, 1), y_peer)
    y1.wait_recv()
    x3 = send(slot(0, 1, 0, 1), slot(0, 1, 1, 1), x_peer)
    rest.append(send(slot(0, 0, 0, 1), slot(1, 0, 0, 1), c_peer))
    rest.append(send(slot(0, 1, 0, 1), slot(1, 1, 0, 1), c_peer))
    near_chunk(0, kept_ref, 0)
    near_chunk(1, to_y_ref, 0)
    near_chunk(2, kept_ref, wide)
    near_chunk(3, to_x_ref, 0)
    x2.wait_recv()
    rest.append(send(slot(0, 1, 1, 0), slot(1, 1, 1, 0), c_peer))
    y2.wait_recv()
    rest.append(send(slot(0, 0, 1, 0), slot(1, 0, 1, 0), c_peer))
    y3.wait_recv()
    rest.append(send(slot(0, 0, 1, 1), slot(1, 0, 1, 1), c_peer))
    x3.wait_recv()
    rest.append(send(slot(0, 1, 1, 1), slot(1, 1, 1, 1), c_peer))
    for copy in (x1, y1, x2, y2, y3, x3):
        copy.wait_send()
    for copy in core_copies:
        copy.wait_send()
    for copy in rest + kept:
        copy.wait()


def gather8_product(own, acts, weight):
    rows, width = own.shape[0] // 2, own.shape[1]
    hbm = pl.BlockSpec(memory_space=pl.ANY)
    vmem = pl.BlockSpec(memory_space=pltpu.VMEM)
    return pl.pallas_call(
        functools.partial(gather8_product_kernel, rows),
        out_shape=[
            jax.ShapeDtypeStruct((16 * rows, width), own.dtype),
            jax.ShapeDtypeStruct((4 * rows, width), F32),
            jax.ShapeDtypeStruct((2 * rows, width), BF16),
            jax.ShapeDtypeStruct((2 * rows, width), BF16),
        ],
        in_specs=[vmem, hbm, hbm],
        out_specs=[hbm, vmem, vmem, vmem],
        scratch_shapes=[
            pltpu.SemaphoreType.DMA((14,)),
            pltpu.SemaphoreType.DMA((14,)),
            pltpu.SemaphoreType.DMA((2,)),
            pltpu.VMEM(acts.shape, BF16),
            pltpu.VMEM(weight.shape, BF16),
            pltpu.VMEM((8 * rows, width), BF16),
            pltpu.VMEM((8 * rows, width), BF16),
            pltpu.SemaphoreType.DMA((4,)),
            pltpu.SemaphoreType.DMA((4,)),
            pltpu.SemaphoreType.DMA((2,)),
        ],
        compiler_params=remote_params(9, 48 * 1024 * 1024),
        cost_estimate=pl.CostEstimate(
            flops=2 * acts.size * width, bytes_accessed=16 * own.size, transcendentals=0
        ),
        name="gather8_product",
    )(own, acts, weight)


def gather8(own, also=()):
    rows, width = own.shape[0] // 2, own.shape[1]
    hbm = pl.BlockSpec(memory_space=pl.ANY)
    whole_shape = jax.ShapeDtypeStruct((16 * rows, width), own.dtype)
    sems = [
        pltpu.SemaphoreType.DMA((14,)),
        pltpu.SemaphoreType.DMA((14,)),
        pltpu.SemaphoreType.DMA((2,)),
    ]
    if also:
        sems += [pltpu.VMEM((8, rows, width), own.dtype)] + [pltpu.SemaphoreType.DMA((8,))] * 4
    outs = pl.pallas_call(
        functools.partial(gather8_kernel, rows, bool(also)),
        out_shape=[whole_shape] * (2 if also else 1),
        in_specs=[pl.BlockSpec(memory_space=pltpu.VMEM)] + [hbm] * len(also),
        out_specs=[hbm] * (2 if also else 1),
        scratch_shapes=sems,
        compiler_params=remote_params(6 if also else 1),
        name="gather8_also" if also else "gather8",
    )(own, *also)
    return outs if also else outs[0]


def reduce8_kernel(
    rows,
    near_ref,
    far_ref,
    out_ref,
    near,
    core_in,
    link_in,
    link_out,
    send_sem,
    recv_sem,
    local_sem,
):
    x_peer, y_peer, c_peer = neighbours()
    greet((x_peer, y_peer, c_peer))
    order = [(h, o, i) for o, i in ((1, 1), (1, 0), (0, 1), (0, 0)) for h in (0, 1)]
    core_copies, local_copies = {}, {}
    for number, (half, outer, inner) in enumerate(order):
        place = pl.ds((half * 4 + outer * 2 + inner) * rows, rows)
        core_copies[half, outer, inner] = pltpu.make_async_remote_copy(
            src_ref=far_ref.at[place],
            dst_ref=core_in.at[place],
            send_sem=send_sem.at[number],
            recv_sem=recv_sem.at[number],
            device_id=c_peer,
            device_id_type=MESH,
        )
        local_copies[half, outer, inner] = pltpu.make_async_copy(
            near_ref.at[place], near.at[place], local_sem.at[number]
        )
    for block in order:
        core_copies[block].start()
        local_copies[block].start()

    def partial_sum(block):
        half, outer, inner = block
        place = pl.ds((half * 4 + outer * 2 + inner) * rows, rows)
        core_copies[block].wait_recv()
        local_copies[block].wait()
        return near[place, :] + core_in[place, :].astype(F32)

    def link(index, value, peer):
        link_out[index] = value.astype(BF16)
        copy = pltpu.make_async_remote_copy(
            src_ref=link_out.at[index],
            dst_ref=link_in.at[index],
            send_sem=send_sem.at[8 + index],
            recv_sem=recv_sem.at[8 + index],
            device_id=peer,
            device_id_type=MESH,
        )
        copy.start()
        return copy

    y11 = link(0, partial_sum((0, 1, 1)), y_peer)
    x11 = link(1, partial_sum((1, 1, 1)), x_peer)
    y10 = link(2, partial_sum((0, 1, 0)), y_peer)
    x10 = link(3, partial_sum((1, 1, 0)), x_peer)
    first01, second01 = partial_sum((0, 0, 1)), partial_sum((1, 0, 1))
    y11.wait_recv()
    x01 = link(4, first01 + link_in[0].astype(F32), x_peer)
    x11.wait_recv()
    y01 = link(5, second01 + link_in[1].astype(F32), y_peer)
    first = partial_sum((0, 0, 0))
    second = partial_sum((1, 0, 0))
    y10.wait_recv()
    out_ref[pl.ds(0, rows), :] = first + link_in[2].astype(F32)
    x10.wait_recv()
    out_ref[pl.ds(rows, rows), :] = second + link_in[3].astype(F32)
    x01.wait_recv()
    out_ref[pl.ds(0, rows), :] += link_in[4].astype(F32)
    y01.wait_recv()
    out_ref[pl.ds(rows, rows), :] += link_in[5].astype(F32)
    for copy in (y11, x11, y10, x10, x01, y01):
        copy.wait_send()
    for copy in core_copies.values():
        copy.wait_send()


def reduce8(near, far):
    rows, width = near.shape[0] // 8, near.shape[1]
    return pl.pallas_call(
        functools.partial(reduce8_kernel, rows),
        out_shape=jax.ShapeDtypeStruct((2 * rows, width), F32),
        in_specs=[pl.BlockSpec(memory_space=pl.ANY), pl.BlockSpec(memory_space=pl.ANY)],
        out_specs=pl.BlockSpec(memory_space=pltpu.VMEM),
        scratch_shapes=[
            pltpu.VMEM(near.shape, F32),
            pltpu.VMEM(near.shape, BF16),
            pltpu.VMEM((6, rows, width), BF16),
            pltpu.VMEM((6, rows, width), BF16),
            pltpu.SemaphoreType.DMA((14,)),
            pltpu.SemaphoreType.DMA((14,)),
            pltpu.SemaphoreType.DMA((8,)),
        ],
        compiler_params=remote_params(2, 48 * 1024 * 1024),
        name="reduce8",
    )(near, far)


def tiled(count, tile, step):
    lax.fori_loop(0, count // tile, lambda i, _: step(pl.ds(pl.multiple_of(i * tile, tile), tile)), 0)


def product_reduce8_kernel(rows, groups, filler, *refs):
    acts_refs, refs = refs[:groups], refs[groups:]
    if filler:
        weight_ref, lhs_ref, out_ref, grad_ref, *refs = refs
    else:
        weight_ref, out_ref, *refs = refs
    acts, weight, far, near, core_in, link_in, link_out, send_sem, recv_sem, load_sem, *refs = refs
    x_peer, y_peer, c_peer = neighbours()
    width = weight.shape[0]
    wide = 2 * rows
    chunks = [(0, 1), (1, 1), (0, 0), (1, 0)]

    def where(chunk):
        return chunk[0] * 2 * wide + chunk[1] * wide

    load_weight = pltpu.make_async_copy(weight_ref, weight, load_sem.at[8])
    loads = {}
    depth = weight.shape[1] // groups
    for number, chunk in enumerate(chunks):
        for side in (1, 0):
            place = pl.ds(side * 4 * wide + where(chunk), wide)
            loads[side, chunk] = [
                pltpu.make_async_copy(
                    acts_refs[group].at[place],
                    acts.at[place, pl.ds(group * depth, depth)],
                    load_sem.at[10 + (2 * number + side) * groups + group],
                )
                for group in range(groups)
            ]
    for copy in loads[1, chunks[0]]:
        copy.start()
    load_weight.start()
    for chunk in chunks:
        for side in (1, 0):
            if (side, chunk) != (1, chunks[0]):
                for copy in loads[side, chunk]:
                    copy.start()
    if filler:
        lhs, grad, grad_sem = refs
        load_lhs = pltpu.make_async_copy(lhs_ref, lhs, load_sem.at[9])
        load_lhs.start()
    greet((x_peer, y_peer, c_peer))

    core_copies = {}

    def product(chunk, side, target):
        for copy in loads[side, chunk]:
            copy.wait()
        place = pl.ds(where(chunk), wide)
        source = pl.ds(side * 4 * wide + where(chunk), wide)

        def step(cols):
            target[place, cols] = mm(acts[source, :], weight[cols, :], 1, 1).astype(target.dtype)
            return 0

        tiled(width, width // 2, step)

    def send_core(chunk):
        product(chunk, 1, far)
        number = chunks.index(chunk)
        place = pl.ds(where(chunk), wide)
        core_copies[chunk] = pltpu.make_async_remote_copy(
            src_ref=far.at[place],
            dst_ref=core_in.at[place],
            send_sem=send_sem.at[number],
            recv_sem=recv_sem.at[number],
            device_id=c_peer,
            device_id_type=MESH,
        )
        core_copies[chunk].start()

    def partial_sum(half, outer, inner):
        place = pl.ds(where((half, outer)) + inner * rows, rows)
        return near[place, :] + core_in[place, :].astype(F32)

    def link(index, value, peer):
        link_out[index] = value.astype(BF16)
        copy = pltpu.make_async_remote_copy(
            src_ref=link_out.at[index],
            dst_ref=link_in.at[index],
            send_sem=send_sem.at[4 + index],
            recv_sem=recv_sem.at[4 + index],
            device_id=peer,
            device_id_type=MESH,
        )
        copy.start()
        return copy

    load_weight.wait()
    send_core((0, 1))
    product((0, 1), 0, near)
    core_copies[0, 1].wait_recv()
    y11 = link(0, partial_sum(0, 1, 1), y_peer)
    send_core((1, 1))
    y10 = link(2, partial_sum(0, 1, 0), y_peer)
    product((1, 1), 0, near)
    core_copies[1, 1].wait_recv()
    x11 = link(1, partial_sum(1, 1, 1), x_peer)
    x10 = link(3, partial_sum(1, 1, 0), x_peer)
    send_core((0, 0))
    product((0, 0), 0, near)
    send_core((1, 0))
    product((1, 0), 0, near)
    core_copies[0, 0].wait_recv()
    core_copies[1, 0].wait_recv()
    grad_copies = []
    parts = grad_sem.shape[0] if filler else 0

    def fill(index):
        size = width // parts
        cols = pl.ds(index * size, size)

        def step(columns):
            grad[cols, columns] = mm(lhs[:, cols], acts[:, columns], 0, 0).astype(BF16)
            return 0

        tiled(acts.shape[1], acts.shape[1] // 3, step)
        copy = pltpu.make_async_copy(grad.at[cols], grad_ref.at[cols], grad_sem.at[index])
        copy.start()
        grad_copies.append(copy)

    if filler:
        load_lhs.wait()
    y11.wait_recv()
    x01 = link(4, partial_sum(0, 0, 1) + link_in[0].astype(F32), x_peer)
    if filler:
        fill(0)
    x11.wait_recv()
    y01 = link(5, partial_sum(1, 0, 1) + link_in[1].astype(F32), y_peer)
    for index in range(1, parts):
        fill(index)
    y10.wait_recv()
    out_ref[pl.ds(0, rows), :] = partial_sum(0, 0, 0) + link_in[2].astype(F32)
    x10.wait_recv()
    out_ref[pl.ds(rows, rows), :] = partial_sum(1, 0, 0) + link_in[3].astype(F32)
    x01.wait_recv()
    out_ref[pl.ds(0, rows), :] += link_in[4].astype(F32)
    y01.wait_recv()
    out_ref[pl.ds(rows, rows), :] += link_in[5].astype(F32)
    for copy in (y11, x11, y10, x10, x01, y01):
        copy.wait_send()
    for copy in core_copies.values():
        copy.wait_send()
    for copy in grad_copies:
        copy.wait()


def product_reduce8(columns, weight, number, lhs=None):
    acts = jax.ShapeDtypeStruct((columns[0].shape[0], weight.shape[1]), BF16)
    rows, width, depth = acts.shape[0] // 16, weight.shape[0], weight.shape[1]
    groups = len(columns)
    filler = lhs is not None
    hbm = pl.BlockSpec(memory_space=pl.ANY)
    parts = 4
    scratch = [
        pltpu.VMEM(acts.shape, BF16),
        pltpu.VMEM(weight.shape, BF16),
        pltpu.VMEM((8 * rows, width), BF16),
        pltpu.VMEM((8 * rows, width), F32),
        pltpu.VMEM((8 * rows, width), BF16),
        pltpu.VMEM((6, rows, width), BF16),
        pltpu.VMEM((6, rows, width), BF16),
        pltpu.SemaphoreType.DMA((10,)),
        pltpu.SemaphoreType.DMA((10,)),
        pltpu.SemaphoreType.DMA((10 + 8 * groups,)),
    ]
    out_shape = [jax.ShapeDtypeStruct((2 * rows, width), F32)]
    out_specs = [pl.BlockSpec(memory_space=pltpu.VMEM)]
    flops = 2 * acts.shape[0] * width * depth
    if filler:
        scratch += [
            pltpu.VMEM(lhs.shape, BF16),
            pltpu.VMEM((width, depth), BF16),
            pltpu.SemaphoreType.DMA((parts,)),
        ]
        out_shape.append(jax.ShapeDtypeStruct((width, depth), BF16))
        out_specs.append(hbm)
        flops *= 2
    outs = pl.pallas_call(
        functools.partial(product_reduce8_kernel, rows, groups, filler),
        out_shape=out_shape,
        in_specs=[hbm] * (groups + (2 if filler else 1)),
        out_specs=out_specs,
        scratch_shapes=scratch,
        compiler_params=remote_params(number, 63 * 1024 * 1024),
        cost_estimate=pl.CostEstimate(
            flops=flops, bytes_accessed=4 * (acts.size + weight.size), transcendentals=0
        ),
        name="product_reduce8",
    )(*columns, weight, *((lhs,) if filler else ()))
    return outs if filler else outs[0]


def shard_kernel(plan, outs, *refs):
    ins, out_refs = refs[: len(plan)], refs[len(plan) : len(plan) + outs]
    stage = refs[len(plan) + outs : 2 * len(plan) + outs]
    send_sem, recv_sem, load_sem, store_sem = refs[2 * len(plan) + outs :]
    x_peer, _, _ = neighbours()
    odd = lax.rem(lax.axis_index("fsdp"), 2)
    column = 2 * lax.axis_index("ctx") + odd
    other = 2 * lax.axis_index("ctx") + 1 - odd
    greet((x_peer,))
    remote, loads, stores = [], [], []
    for number, (which, start, size, cut) in enumerate(plan):
        rows = ins[number].shape[0]
        place = pl.ds(pl.multiple_of(odd * rows, rows), rows)
        target = out_refs[which].at[place, pl.ds(start, size)]

        def source(index, ref=ins[number], size=size, cut=cut):
            if not cut:
                return ref
            return ref.at[:, pl.ds(pl.multiple_of(index * size, HEAD), size)]

        remote.append(
            pltpu.make_async_remote_copy(
                src_ref=source(other),
                dst_ref=target,
                send_sem=send_sem.at[number],
                recv_sem=recv_sem.at[number],
                device_id=x_peer,
                device_id_type=MESH,
            )
        )
        loads.append(pltpu.make_async_copy(source(column), stage[number], load_sem.at[number]))
        stores.append(pltpu.make_async_copy(stage[number], target, store_sem.at[number]))
    for copy in remote:
        copy.start()
    for copy in loads:
        copy.start()
    for load, store in zip(loads, stores):
        load.wait()
        store.start()
    for copy in stores:
        copy.wait()
    for copy in remote:
        copy.wait()


def shards(groups, number):
    plan, arrays, shapes = [], [], []
    for which, group in enumerate(groups):
        start = 0
        for array, cut in group:
            size = array.shape[1] // 4 if cut else array.shape[1]
            plan.append((which, start, size, cut))
            arrays.append(array)
            start += size
        shapes.append((2 * group[0][0].shape[0], start))
    hbm = pl.BlockSpec(memory_space=pl.ANY)
    return pl.pallas_call(
        functools.partial(shard_kernel, tuple(plan), len(groups)),
        out_shape=[jax.ShapeDtypeStruct(shape, BF16) for shape in shapes],
        in_specs=[hbm] * len(arrays),
        out_specs=[hbm] * len(groups),
        scratch_shapes=[
            pltpu.VMEM((array.shape[0], size), BF16)
            for array, (_, _, size, _) in zip(arrays, plan)
        ]
        + [pltpu.SemaphoreType.DMA((len(plan),))] * 4,
        compiler_params=remote_params(number),
        name="shards",
    )(*arrays)


def total_kernel(stages, part_ref, out_ref, inbox, outbox, send_sem, recv_sem):
    peers = []
    for axis, bit in stages:
        mine = lax.axis_index(axis)
        peers.append({axis: mine + bit * (1 - 2 * lax.rem(mine // bit, 2))})
    greet(peers)
    value = part_ref[...]
    copies = []
    for index, peer in enumerate(peers):
        outbox[index] = value
        copy = pltpu.make_async_remote_copy(
            src_ref=outbox.at[index],
            dst_ref=inbox.at[index],
            send_sem=send_sem.at[index],
            recv_sem=recv_sem.at[index],
            device_id=peer,
            device_id_type=MESH,
        )
        copy.start()
        copies.append(copy)
        copy.wait_recv()
        value = value + inbox[index]
    out_ref[...] = value
    for copy in copies:
        copy.wait_send()


def total(part):
    stages, bit = [], 2
    while bit < lax.axis_size("fsdp"):
        stages.append(("fsdp", bit))
        bit *= 2
    stages += [("tp", 1), ("fsdp", 1), ("ctx", 1)]
    return pl.pallas_call(
        functools.partial(total_kernel, tuple(stages)),
        out_shape=jax.ShapeDtypeStruct(part.shape, F32),
        in_specs=[pl.BlockSpec(memory_space=pltpu.VMEM)],
        out_specs=pl.BlockSpec(memory_space=pltpu.VMEM),
        scratch_shapes=[
            pltpu.VMEM((len(stages),) + part.shape, F32),
            pltpu.VMEM((len(stages),) + part.shape, F32),
            pltpu.SemaphoreType.DMA((len(stages),)),
            pltpu.SemaphoreType.DMA((len(stages),)),
        ],
        compiler_params=remote_params(5),
        name="total",
    )(part)


def join_kernel(sizes, spot_ref, kept_ref, x_ref, y_ref, both_ref, *out_refs):
    place, odd = spot_ref[0], spot_ref[1]
    parts = (
        (kept_ref, 2 * place + odd),
        (x_ref, 2 * place + 1 - odd),
        (y_ref, 2 - 2 * place + odd),
        (both_ref, 3 - 2 * place - odd),
    )
    for part, column in parts:
        start = 0
        for size, out_ref in zip(sizes, out_refs):
            target = pl.ds(pl.multiple_of(column * size, HEAD), size)
            out_ref[:, target] = part[:, start : start + size].astype(F32)
            start += size


def join_columns(spot, parts, sizes):
    rows = parts[0].shape[0]
    tile = min(rows, 64)
    return pl.pallas_call(
        functools.partial(join_kernel, sizes),
        out_shape=[jax.ShapeDtypeStruct((rows, 4 * size), F32) for size in sizes],
        grid_spec=pltpu.PrefetchScalarGridSpec(
            num_scalar_prefetch=1,
            grid=(rows // tile,),
            in_specs=[
                pl.BlockSpec((tile, part.shape[1]), lambda i, spot: (i, 0)) for part in parts
            ],
            out_specs=[pl.BlockSpec((tile, 4 * size), lambda i, spot: (i, 0)) for size in sizes],
        ),
        name="join",
    )(spot, *parts)


def after(value, *others):
    return lax.optimization_barrier((value,) + others)[0]


def reduce4_links(kept, to_y, to_x, *others):
    rows = kept.shape[0] // 4
    came_first, came_second = swap_ctx(to_y), swap_x(to_x)
    first = kept[: 2 * rows] + after(came_first, *others).astype(F32)
    second = kept[2 * rows :] + after(came_second, *others).astype(F32)
    came_first = swap_x(first[rows:].astype(BF16))
    came_second = swap_ctx(second[rows:].astype(BF16))
    return first[:rows], second[:rows], came_first, came_second


def rope_tables(positions):
    freqs = THETA ** (-(jnp.arange(HEAD // 2, dtype=F32) * 2.0) / HEAD)
    angle = positions[:, None] * freqs[None, :]
    cosine = jnp.concatenate([jnp.cos(angle), jnp.cos(angle)], axis=-1)
    sine = jnp.concatenate([-jnp.sin(angle), jnp.sin(angle)], axis=-1)
    return cosine, sine


def norm_back(grad, scaled, inverse, gain):
    weighted = grad * gain
    return inverse * (weighted - scaled * jnp.mean(weighted * scaled, axis=-1, keepdims=True))


def inv_rms(value):
    return lax.rsqrt(jnp.mean(value * value, axis=-1, keepdims=True) + EPS)


def block_row(meta_ref, seq, index, rows):
    away_c = lax.rem(meta_ref[0] + index // 4, 2)
    away_t = lax.rem(meta_ref[1] + (index // 2) % 2, 2)
    if index % 2 == 0:
        inner = away_c * 2 + seq
    else:
        inner = seq * 2 + away_c + 4
    return pl.multiple_of((away_t * 8 + inner) * rows, rows)


def scaled_of(raw):
    inverse = lax.rsqrt(jnp.mean(raw * raw, axis=-1, keepdims=True) + EPS)
    return raw * inverse, inverse


def load_heads(meta_ref, qkv_ref, cos_ref, sin_ref, gain_ref, q_scr, k_scr, v_scr, heads):
    seq = pl.program_id(0)
    rows = q_scr.shape[1] // 8
    for index in range(8):
        start = block_row(meta_ref, seq, index, rows)
        here = slice(index * rows, (index + 1) * rows)
        cosine, sine = cos_ref[here, :], sin_ref[here, :]
        for head in range(heads + 1):
            raw = qkv_ref[pl.ds(start, rows), head * HEAD : (head + 1) * HEAD]
            scaled, _ = scaled_of(raw)
            which = 0 if head < heads else 1
            value = scaled * gain_ref[which : which + 1, :]
            turned = value * cosine + pltpu.roll(value, HEAD // 2, 1) * sine
            if head < heads:
                q_scr[head, here, :] = turned.astype(BF16)
            else:
                k_scr[here, :] = turned.astype(BF16)
        v_scr[here, :] = qkv_ref[
            pl.ds(start, rows), (heads + 1) * HEAD : (heads + 2) * HEAD
        ].astype(BF16)


def key_span(index, tile):
    low = max(0, (index * tile - (MOST_DOC - 1)) // tile) * tile
    return low, (index + 1) * tile


def allowed_mask(segc_ref, segr_ref, index, tile):
    low, high = key_span(index, tile)
    shape = (tile, high - low)
    rows = lax.broadcasted_iota(jnp.int32, shape, 0) + index * tile
    cols = lax.broadcasted_iota(jnp.int32, shape, 1) + low
    same = segc_ref[0, index * tile : (index + 1) * tile, :] == segr_ref[0, :, low:high]
    return same & (cols <= rows)


def probs_of(query, keys, allowed, scale):
    scores = jnp.where(allowed, mm(query, keys, 1, 1) * scale, MASKED)
    weights = jnp.exp(scores - jnp.max(scores, axis=-1, keepdims=True))
    return weights * (1.0 / jnp.sum(weights, axis=-1, keepdims=True))


def attend_kernel(
    heads, tile, meta_ref, qkv_ref, segc_ref, segr_ref, cos_ref, sin_ref, gain_ref, out_ref, q_scr, k_scr, v_scr
):
    seq = pl.program_id(0)
    length = k_scr.shape[0]
    rows = length // 8
    scale = 1.0 / math.sqrt(HEAD)
    load_heads(meta_ref, qkv_ref, cos_ref, sin_ref, gain_ref, q_scr, k_scr, v_scr, heads)
    for index in range(length // tile):
        low, high = key_span(index, tile)
        allowed = allowed_mask(segc_ref, segr_ref, index, tile)
        for head in range(heads):
            query = q_scr[head, index * tile : (index + 1) * tile, :]
            probs = probs_of(query, k_scr[low:high, :], allowed, scale)
            mixed = mm(probs.astype(BF16), v_scr[low:high, :], 1, 0).astype(BF16)
            for piece in range(tile // rows):
                start = block_row(meta_ref, seq, index * (tile // rows) + piece, rows)
                out_ref[pl.ds(start, rows), head * HEAD : (head + 1) * HEAD] = mixed[
                    piece * rows : (piece + 1) * rows
                ]


def attend_back_kernel(
    heads,
    tile,
    meta_ref,
    qkv_ref,
    grad_ref,
    segc_ref,
    segr_ref,
    cos_ref,
    sin_ref,
    gain_ref,
    out_ref,
    gain_out_ref,
    q_scr,
    k_scr,
    v_scr,
    g_scr,
    dk_scr,
    dv_scr,
):
    seq = pl.program_id(0)
    length = k_scr.shape[0]
    rows = length // 8
    scale = 1.0 / math.sqrt(HEAD)
    load_heads(meta_ref, qkv_ref, cos_ref, sin_ref, gain_ref, q_scr, k_scr, v_scr, heads)
    for index in range(8):
        start = block_row(meta_ref, seq, index, rows)
        g_scr[index * rows : (index + 1) * rows, :] = grad_ref[pl.ds(start, rows), :]
    dk_scr[...] = jnp.zeros_like(dk_scr)
    dv_scr[...] = jnp.zeros_like(dv_scr)

    @pl.when(seq == 0)
    def _():
        gain_out_ref[...] = jnp.zeros_like(gain_out_ref)

    def finish(grad, index, head, which):
        here = slice(index * rows, (index + 1) * rows)
        start = block_row(meta_ref, seq, index, rows)
        grad = grad * cos_ref[here, :] - pltpu.roll(grad, HEAD // 2, 1) * sin_ref[here, :]
        raw = qkv_ref[pl.ds(start, rows), head * HEAD : (head + 1) * HEAD]
        scaled, inverse = scaled_of(raw)
        gain_out_ref[which : which + 1, :] += jnp.sum(grad * scaled, axis=0, keepdims=True)
        out = norm_back(grad, scaled, inverse, gain_ref[which : which + 1, :])
        out_ref[pl.ds(start, rows), head * HEAD : (head + 1) * HEAD] = out.astype(BF16)

    per = tile // rows
    for index in range(length // tile):
        low, high = key_span(index, tile)
        mine = slice(index * tile, (index + 1) * tile)
        allowed = allowed_mask(segc_ref, segr_ref, index, tile)
        for head in range(heads):
            query = q_scr[head, mine, :]
            keys = k_scr[low:high, :]
            probs = probs_of(query, keys, allowed, scale)
            grad = g_scr[mine, head * HEAD : (head + 1) * HEAD]
            grad_probs = mm(grad, v_scr[low:high, :], 1, 1)
            delta = jnp.sum(probs * grad_probs, axis=-1, keepdims=True)
            grad_scores = (probs * (grad_probs - delta)).astype(BF16)
            dv_scr[low:high, :] += mm(probs.astype(BF16), grad, 0, 0)
            dk_scr[low:high, :] += mm(grad_scores, query, 0, 0) * scale
            grad_query = mm(grad_scores, keys, 1, 0) * scale
            for piece in range(per):
                finish(
                    grad_query[piece * rows : (piece + 1) * rows], index * per + piece, head, 0
                )
    for index in range(8):
        here = slice(index * rows, (index + 1) * rows)
        start = block_row(meta_ref, seq, index, rows)
        finish(dk_scr[here, :], index, heads, 1)
        out_ref[pl.ds(start, rows), (heads + 1) * HEAD : (heads + 2) * HEAD] = dv_scr[
            here, :
        ].astype(BF16)


def whole(shape):
    return pl.BlockSpec(shape, lambda seq, meta: (0,) * len(shape))


def seg_specs(length):
    return [
        pl.BlockSpec((1, length, 1), lambda seq, meta: (seq, 0, 0)),
        pl.BlockSpec((1, 1, length), lambda seq, meta: (seq, 0, 0)),
    ]


def attend(meta, qkv, seg_cols, seg_rows, cosine, sine, gains):
    length = cosine.shape[0]
    tile = length // 4
    heads = qkv.shape[1] // HEAD - 2
    pairs = 2 * heads * length * length // 2
    return pl.pallas_call(
        functools.partial(attend_kernel, heads, tile),
        out_shape=jax.ShapeDtypeStruct((qkv.shape[0], heads * HEAD), BF16),
        grid_spec=pltpu.PrefetchScalarGridSpec(
            num_scalar_prefetch=1,
            grid=(2,),
            in_specs=[whole(qkv.shape)]
            + seg_specs(length)
            + [whole(cosine.shape), whole(sine.shape), whole(gains.shape)],
            out_specs=whole((qkv.shape[0], heads * HEAD)),
            scratch_shapes=[
                pltpu.VMEM((heads, length, HEAD), BF16),
                pltpu.VMEM((length, HEAD), BF16),
                pltpu.VMEM((length, HEAD), BF16),
            ],
        ),
        cost_estimate=pl.CostEstimate(
            flops=4 * pairs * HEAD, bytes_accessed=qkv.size * 4 + qkv.size, transcendentals=pairs
        ),
        name="attend",
    )(meta, qkv, seg_cols, seg_rows, cosine, sine, gains)


def attend_back(meta, qkv, grad, seg_cols, seg_rows, cosine, sine, gains):
    length = cosine.shape[0]
    tile = length // 4
    heads = qkv.shape[1] // HEAD - 2
    pairs = 2 * heads * length * length // 2
    return pl.pallas_call(
        functools.partial(attend_back_kernel, heads, tile),
        out_shape=(
            jax.ShapeDtypeStruct(qkv.shape, BF16),
            jax.ShapeDtypeStruct(gains.shape, F32),
        ),
        grid_spec=pltpu.PrefetchScalarGridSpec(
            num_scalar_prefetch=1,
            grid=(2,),
            in_specs=[whole(qkv.shape), whole(grad.shape)]
            + seg_specs(length)
            + [whole(cosine.shape), whole(sine.shape), whole(gains.shape)],
            out_specs=(whole(qkv.shape), whole(gains.shape)),
            scratch_shapes=[
                pltpu.VMEM((heads, length, HEAD), BF16),
                pltpu.VMEM((length, HEAD), BF16),
                pltpu.VMEM((length, HEAD), BF16),
                pltpu.VMEM((length, heads * HEAD), BF16),
                pltpu.VMEM((length, HEAD), F32),
                pltpu.VMEM((length, HEAD), F32),
            ],
        ),
        cost_estimate=pl.CostEstimate(
            flops=10 * pairs * HEAD, bytes_accessed=qkv.size * 8, transcendentals=pairs
        ),
        name="attend_back",
    )(meta, qkv, grad, seg_cols, seg_rows, cosine, sine, gains)


def body(
    tokens,
    segment_ids,
    norm_gain,
    query_weight,
    key_matrix,
    value_matrix,
    output_weight,
    query_gain,
    key_gain,
    mlp_gain,
    gate_weight,
    up_weight,
    down_weight,
    cotangent,
):
    local, width = tokens.shape[1], tokens.shape[2]
    length = 2 * local
    quarter = local // 2
    count = lax.axis_size("fsdp")
    block = width // count
    mine = lax.axis_index("fsdp")
    odd = mine % 2
    place = lax.axis_index("ctx")
    core = lax.axis_index("tp")

    small = query_gain.shape[0]
    lanes = jnp.arange(HEAD)[None, :]

    def pad_rows(vector):
        return jnp.concatenate([vector, jnp.zeros((block - small,), BF16)])

    gains = jnp.where(
        lanes == 0,
        norm_gain[:, None],
        jnp.where(
            lanes == 1,
            mlp_gain[:, None],
            jnp.where(
                lanes == 2, pad_rows(query_gain)[:, None], pad_rows(key_gain)[:, None]
            ),
        ),
    )
    far_segments = swap_x(segment_ids)
    (first_pair,) = shards(
        [
            [
                (query_weight, True),
                (key_matrix, True),
                (value_matrix, True),
                (output_weight, True),
                (gains, False),
            ]
        ],
        3,
    )
    first = gather_line(first_pair)
    gate_up_pair, down_pair = shards(
        [
            [(after(gate_weight, first_pair), True), (up_weight, True)],
            [(down_weight, True)],
        ],
        4,
    )
    gate_up_w = gather_line(gate_up_pair)
    down_w = gather_line(down_pair)

    def own_quarter(value):
        return lax.dynamic_slice_in_dim(value.reshape(local, width), core * quarter, quarter, 0)

    own_tok, own_cot = own_quarter(tokens), own_quarter(cotangent)
    tok = gather8(after(own_tok, gate_up_pair))
    segments = jnp.concatenate([segment_ids, far_segments])
    seg_cols, seg_rows = segments[:, :, None], segments[:, None, :]
    cosine, sine = rope_tables(jnp.arange(length).astype(F32))
    meta = jnp.stack([place, core]).astype(jnp.int32)

    heads_q = query_weight.shape[1] // 4 // HEAD
    cols = (heads_q + 2) * HEAD
    qkv_w = first[:, :cols]
    out_w = first[:, cols : cols + heads_q * HEAD]
    gain_cols = first[:, cols + heads_q * HEAD :].astype(F32)
    in_gain, mid_gain = gain_cols[:, 0][None], gain_cols[:, 1][None]
    head_gains = gain_cols.reshape(count, block, HEAD)[:, :small, 2:4].reshape(HEAD, 2).T

    in_f = tok.astype(F32)
    cot_from = after(own_cot, tok)
    cot_x, cot_y = swap_x(cot_from), swap_ctx(cot_from)
    x_all = (in_f * inv_rms(in_f) * in_gain).astype(BF16)
    qkv = mm(x_all, qkv_w, 1, 0)
    attended = attend(meta, qkv, seg_cols, seg_rows, cosine, sine, head_gains)
    half = 4 * quarter
    cot_x, cot_y = after(cot_x, attended), after(cot_y, attended)
    eighth = quarter // 2
    cot_first, cot_second = swap_ctx(cot_x[:eighth]), swap_x(cot_y[eighth:])
    out_far = mm(attended[half:], out_w, 1, 1).astype(BF16)
    out_near = mm(attended[:half], out_w, 1, 1)
    middle = own_tok.astype(F32) + reduce8(out_near, out_far)
    inverse_mid = inv_rms(middle)
    scaled_mid = middle * inverse_mid
    y_own = (scaled_mid * mid_gain).astype(BF16)
    cot_first, cot_second = after(cot_first, y_own), after(cot_second, y_own)
    y_all, cot = gather8(y_own, (cot_from, cot_x, cot_y, cot_first, cot_second))

    ff = gate_up_w.shape[1] // 2
    gate_up = mm(y_all, gate_up_w, 1, 0)
    gate, up_value = gate_up[:, :ff], gate_up[:, ff:]
    sig = jax.nn.sigmoid(gate)
    active = gate * sig
    hidden = (active * up_value).astype(BF16)
    down_grad = mm(cot, hidden, 0, 0).astype(BF16)

    def finish_rows(own):
        pair = jnp.stack([own, swap_core(own)])
        return flip_if(core == 1, pair, 0).reshape(tokens.shape)

    grad_hidden = mm(after(cot, down_grad), down_w, 1, 0)
    grad_up = (grad_hidden * active).astype(BF16)
    grad_gate = (grad_hidden * up_value * (sig * (1.0 + gate * (1.0 - sig)))).astype(BF16)
    mid_grad, gate_up_grad = product_reduce8((grad_gate, grad_up), gate_up_w, 7, y_all)

    mlp_gain_part = jnp.sum(mid_grad * scaled_mid, axis=0)
    grad_middle = own_cot.astype(F32) + norm_back(mid_grad, scaled_mid, inverse_mid, mid_gain)
    grad_attn, mlp_kept, mlp_to_y, mlp_to_x = gather8_product(
        grad_middle.astype(BF16), hidden, down_w
    )
    out_grad = mm(grad_attn, attended, 0, 0).astype(BF16)
    grad_att = mm(grad_attn, out_w, 1, 0).astype(BF16)
    raw_grads, head_gain_parts = attend_back(
        meta, qkv, grad_att, seg_cols, seg_rows, cosine, sine, head_gains
    )
    mlp_first, mlp_second, mlp_came1, mlp_came2 = reduce4_links(
        mlp_kept, mlp_to_y, mlp_to_x, raw_grads
    )
    first_grad = mm(x_all, raw_grads, 0, 0).astype(BF16)
    first_grad = jnp.concatenate([first_grad, out_grad], axis=1)
    mlp_first = mlp_first + after(mlp_came1, first_grad).astype(F32)
    mlp_second = mlp_second + after(mlp_came2, first_grad).astype(F32)
    mlp_sum = (middle + jnp.concatenate([mlp_first, mlp_second])).astype(BF16)
    layer_out = finish_rows(mlp_sum)
    in_grad = product_reduce8((after(raw_grads, first_grad, mlp_sum),), qkv_w, 8)

    spot = jnp.stack([place, odd]).astype(jnp.int32)

    def owners(grad, sizes, *others):
        rows = scatter_line(grad)
        rows = after(rows, *others)
        kept = lax.dynamic_slice_in_dim(rows, odd * block, block, 0)
        sent = lax.dynamic_slice_in_dim(rows, (1 - odd) * block, block, 0)
        by_x, by_y = swap_x(sent), swap_ctx(kept)
        by_both = swap_ctx(by_x)
        return join_columns(spot, (kept, by_x, by_y, by_both), sizes)

    (down_share,) = owners(down_grad, (ff,))
    gate_share, up_share = owners(gate_up_grad, (ff, ff))
    query_share, key_share, value_share, out_share = owners(
        first_grad, (heads_q * HEAD, HEAD, HEAD, heads_q * HEAD)
    )

    own_in = own_tok.astype(F32)
    inverse_in = inv_rms(own_in)
    scaled_in = own_in * inverse_in
    norm_gain_part = jnp.sum(in_grad * scaled_in, axis=0)
    token_grad = finish_rows(
        (grad_middle + norm_back(in_grad, scaled_in, inverse_in, in_gain)).astype(BF16)
    )

    parts = jnp.concatenate([norm_gain_part, mlp_gain_part, head_gain_parts.reshape(-1)])
    sums = total(parts.reshape(-1, HEAD)).reshape(-1)
    norm_gain_grad = lax.dynamic_slice_in_dim(sums, mine * block, block, 0)
    mlp_gain_grad = lax.dynamic_slice_in_dim(sums, width + mine * block, block, 0)
    query_gain_grad = lax.dynamic_slice_in_dim(sums, 2 * width + mine * small, small, 0)
    key_gain_grad = lax.dynamic_slice_in_dim(sums, 2 * width + HEAD + mine * small, small, 0)
    return (
        layer_out,
        token_grad,
        norm_gain_grad,
        query_share,
        key_share,
        value_share,
        out_share,
        query_gain_grad,
        key_gain_grad,
        mlp_gain_grad,
        gate_share,
        up_share,
        down_share,
    )


def solution(mesh):
    in_specs = (
        P("fsdp", "ctx", None),
        P("fsdp", None),
        P("fsdp"),
        P("fsdp", "tp"),
        P("fsdp", "tp"),
        P("fsdp", "tp"),
        P("fsdp", "tp"),
        P("fsdp"),
        P("fsdp"),
        P("fsdp"),
        P("fsdp", "tp"),
        P("fsdp", "tp"),
        P("fsdp", "tp"),
        P("fsdp", "ctx", None),
    )
    out_specs = (
        P("fsdp", "ctx", None),
        P("fsdp", "ctx", None),
        P("fsdp"),
        P("fsdp", "tp"),
        P("fsdp", "tp"),
        P("fsdp", "tp"),
        P("fsdp", "tp"),
        P("fsdp"),
        P("fsdp"),
        P("fsdp"),
        P("fsdp", "tp"),
        P("fsdp", "tp"),
        P("fsdp", "tp"),
    )

    return jax.shard_map(body, mesh=mesh, in_specs=in_specs, out_specs=out_specs, check_vma=False)
```

```python
import functools
import math

import jax
import jax.numpy as jnp
from jax import lax
from jax.experimental import pallas as pl
from jax.experimental.pallas import tpu as pltpu
from jax.sharding import PartitionSpec as P


HEAD = 128
EPS = 1e-06
THETA = 1000000.0
MASKED = -1e30
MOST_DOC = 512
MESH = pl.DeviceIdType.MESH
F32 = jnp.float32
BF16 = jnp.bfloat16


def mm(left, right, left_dim, right_dim):
    return lax.dot_general(
        left, right, (((left_dim,), (right_dim,)), ((), ())), preferred_element_type=F32
    )


def swap_core(value):
    return lax.ppermute(value, "tp", [(0, 1), (1, 0)])


def swap_ctx(value):
    return lax.ppermute(value, "ctx", [(0, 1), (1, 0)])


def swap_x(value):
    count = lax.axis_size("fsdp")
    return lax.ppermute(value, "fsdp", [(i, i ^ 1) for i in range(count)])


def lines():
    count = lax.axis_size("fsdp")
    return [[i for i in range(count) if i % 2 == parity] for parity in (0, 1)]


def gather_line(value):
    return lax.all_gather(value, "fsdp", axis=0, tiled=True, axis_index_groups=lines())


def scatter_line(value):
    return lax.psum_scatter(
        value, "fsdp", scatter_dimension=0, tiled=True, axis_index_groups=lines()
    )


def flip_if(flag, value, axis):
    return jnp.where(flag, jnp.flip(value, axis), value)


def neighbours():
    mine = lax.axis_index("fsdp")
    return (
        {"fsdp": mine + 1 - 2 * lax.rem(mine, 2)},
        {"ctx": 1 - lax.axis_index("ctx")},
        {"tp": 1 - lax.axis_index("tp")},
    )


def greet(peers):
    barrier = pltpu.get_barrier_semaphore()
    for peer in peers:
        pl.semaphore_signal(barrier, inc=1, device_id=peer, device_id_type=MESH)
    pl.semaphore_wait(barrier, len(peers))


def remote_params(number, limit=None):
    return pltpu.CompilerParams(
        collective_id=number, has_side_effects=True, vmem_limit_bytes=limit
    )


def gather8_kernel(rows, spread, *refs):
    if spread:
        own_ref, kept_ref, x_ref, y_ref, first_ref, second_ref, out_ref, also_ref = refs[:8]
        send_sem, recv_sem, local_sem, stage, also_send, also_recv, also_in, also_out = refs[8:]
    else:
        own_ref, out_ref, send_sem, recv_sem, local_sem = refs
    x_peer, y_peer, c_peer = neighbours()

    def start_of(away_t, half, outer, inner):
        return pl.ds((away_t * 8 + half * 4 + outer * 2 + inner) * rows, rows)

    def slot(*block):
        return out_ref.at[start_of(*block)]

    also_loads, also_remote, also_stores = [], [], []
    if spread:
        top, low = pl.ds(0, rows), pl.ds(rows, rows)
        pieces = [
            ((0, 0, 0), kept_ref.at[top]),
            ((0, 0, 1), x_ref.at[top]),
            ((0, 1, 0), y_ref.at[top]),
            ((0, 1, 1), first_ref),
            ((1, 0, 0), kept_ref.at[low]),
            ((1, 0, 1), y_ref.at[low]),
            ((1, 1, 0), x_ref.at[low]),
            ((1, 1, 1), second_ref),
        ]
        for index, (block, source) in enumerate(pieces):
            also_loads.append(pltpu.make_async_copy(source, stage.at[index], also_in.at[index]))
            also_stores.append(
                pltpu.make_async_copy(
                    stage.at[index], also_ref.at[start_of(0, *block)], also_out.at[index]
                )
            )
            also_remote.append(
                pltpu.make_async_remote_copy(
                    src_ref=source,
                    dst_ref=also_ref.at[start_of(1, *block)],
                    send_sem=also_send.at[index],
                    recv_sem=also_recv.at[index],
                    device_id=c_peer,
                    device_id_type=MESH,
                )
            )
        for copy in also_loads:
            copy.start()
    greet((x_peer, y_peer, c_peer))

    number = iter(range(14))

    def send(source, target, peer):
        index = next(number)
        copy = pltpu.make_async_remote_copy(
            src_ref=source,
            dst_ref=target,
            send_sem=send_sem.at[index],
            recv_sem=recv_sem.at[index],
            device_id=peer,
            device_id_type=MESH,
        )
        copy.start()
        return copy

    first, second = own_ref.at[pl.ds(0, rows)], own_ref.at[pl.ds(rows, rows)]
    x1 = send(first, slot(0, 0, 0, 1), x_peer)
    y1 = send(second, slot(0, 1, 0, 1), y_peer)
    x2 = send(second, slot(0, 1, 1, 0), x_peer)
    y2 = send(first, slot(0, 0, 1, 0), y_peer)
    rest = [send(first, slot(1, 0, 0, 0), c_peer), send(second, slot(1, 1, 0, 0), c_peer)]
    kept = [
        pltpu.make_async_copy(first, slot(0, 0, 0, 0), local_sem.at[0]),
        pltpu.make_async_copy(second, slot(0, 1, 0, 0), local_sem.at[1]),
    ]
    for copy in kept:
        copy.start()
    for copy in also_remote:
        copy.start()
    for load, store in zip(also_loads, also_stores):
        load.wait()
        store.start()
    x1.wait_recv()
    y3 = send(slot(0, 0, 0, 1), slot(0, 0, 1, 1), y_peer)
    y1.wait_recv()
    x3 = send(slot(0, 1, 0, 1), slot(0, 1, 1, 1), x_peer)
    rest.append(send(slot(0, 0, 0, 1), slot(1, 0, 0, 1), c_peer))
    rest.append(send(slot(0, 1, 0, 1), slot(1, 1, 0, 1), c_peer))
    x2.wait_recv()
    rest.append(send(slot(0, 1, 1, 0), slot(1, 1, 1, 0), c_peer))
    y2.wait_recv()
    rest.append(send(slot(0, 0, 1, 0), slot(1, 0, 1, 0), c_peer))
    y3.wait_recv()
    rest.append(send(slot(0, 0, 1, 1), slot(1, 0, 1, 1), c_peer))
    x3.wait_recv()
    rest.append(send(slot(0, 1, 1, 1), slot(1, 1, 1, 1), c_peer))
    for copy in (x1, y1, x2, y2, y3, x3):
        copy.wait_send()
    for copy in rest + also_remote + kept + also_stores:
        copy.wait()


def gather8_product_kernel(
    rows,
    own_ref,
    acts_ref,
    weight_ref,
    out_ref,
    kept_ref,
    to_y_ref,
    to_x_ref,
    send_sem,
    recv_sem,
    local_sem,
    acts,
    weight,
    far,
    core_in,
    core_send,
    core_recv,
    load_sem,
):
    x_peer, y_peer, c_peer = neighbours()
    width = weight.shape[0]
    wide = 2 * rows
    loads = [
        pltpu.make_async_copy(weight_ref, weight, load_sem.at[0]),
        pltpu.make_async_copy(acts_ref, acts, load_sem.at[1]),
    ]
    for copy in loads:
        copy.start()
    greet((x_peer, y_peer, c_peer))

    def slot(away_t, half, outer, inner):
        return out_ref.at[pl.ds((away_t * 8 + half * 4 + outer * 2 + inner) * rows, rows)]

    number = iter(range(14))

    def send(source, target, peer):
        index = next(number)
        copy = pltpu.make_async_remote_copy(
            src_ref=source,
            dst_ref=target,
            send_sem=send_sem.at[index],
            recv_sem=recv_sem.at[index],
            device_id=peer,
            device_id_type=MESH,
        )
        copy.start()
        return copy

    core_copies = []

    def far_chunk(index):
        place = pl.ds(index * wide, wide)
        source = pl.ds(4 * wide + index * wide, wide)

        def step(cols):
            far[place, cols] = mm(acts[source, :], weight[cols, :], 1, 1).astype(BF16)
            return 0

        tiled(width, width // 2, step)
        copy = pltpu.make_async_remote_copy(
            src_ref=far.at[place],
            dst_ref=core_in.at[place],
            send_sem=core_send.at[index],
            recv_sem=core_recv.at[index],
            device_id=c_peer,
            device_id_type=MESH,
        )
        copy.start()
        core_copies.append(copy)

    def near_chunk(index, target_ref, start):
        core_copies[index].wait_recv()
        place = pl.ds(index * wide, wide)
        target = pl.ds(start, wide)

        def step(cols):
            value = mm(acts[place, :], weight[cols, :], 1, 1) + core_in[place, cols].astype(F32)
            target_ref[target, cols] = value.astype(target_ref.dtype)
            return 0

        tiled(width, width // 2, step)

    first, second = own_ref.at[pl.ds(0, rows)], own_ref.at[pl.ds(rows, rows)]
    x1 = send(first, slot(0, 0, 0, 1), x_peer)
    y1 = send(second, slot(0, 1, 0, 1), y_peer)
    x2 = send(second, slot(0, 1, 1, 0), x_peer)
    y2 = send(first, slot(0, 0, 1, 0), y_peer)
    rest = [send(first, slot(1, 0, 0, 0), c_peer), send(second, slot(1, 1, 0, 0), c_peer)]
    kept = [
        pltpu.make_async_copy(first, slot(0, 0, 0, 0), local_sem.at[0]),
        pltpu.make_async_copy(second, slot(0, 1, 0, 0), local_sem.at[1]),
    ]
    for copy in kept:
        copy.start()
    for copy in loads:
        copy.wait()
    for index in range(4):
        far_chunk(index)
    x1.wait_recv()
    y3 = send(slot(0, 0, 0, 1), slot(0, 0, 1, 1), y_peer)
    y1.wait_recv()
    x3 = send(slot(0, 1, 0, 1), slot(0, 1, 1, 1), x_peer)
    rest.append(send(slot(0, 0, 0, 1), slot(1, 0, 0, 1), c_peer))
    rest.append(send(slot(0, 1, 0, 1), slot(1, 1, 0, 1), c_peer))
    near_chunk(0, kept_ref, 0)
    near_chunk(1, to_y_ref, 0)
    near_chunk(2, kept_ref, wide)
    near_chunk(3, to_x_ref, 0)
    x2.wait_recv()
    rest.append(send(slot(0, 1, 1, 0), slot(1, 1, 1, 0), c_peer))
    y2.wait_recv()
    rest.append(send(slot(0, 0, 1, 0), slot(1, 0, 1, 0), c_peer))
    y3.wait_recv()
    rest.append(send(slot(0, 0, 1, 1), slot(1, 0, 1, 1), c_peer))
    x3.wait_recv()
    rest.append(send(slot(0, 1, 1, 1), slot(1, 1, 1, 1), c_peer))
    for copy in (x1, y1, x2, y2, y3, x3):
        copy.wait_send()
    for copy in core_copies:
        copy.wait_send()
    for copy in rest + kept:
        copy.wait()


def gather8_product(own, acts, weight):
    rows, width = own.shape[0] // 2, own.shape[1]
    hbm = pl.BlockSpec(memory_space=pl.ANY)
    vmem = pl.BlockSpec(memory_space=pltpu.VMEM)
    return pl.pallas_call(
        functools.partial(gather8_product_kernel, rows),
        out_shape=[
            jax.ShapeDtypeStruct((16 * rows, width), own.dtype),
            jax.ShapeDtypeStruct((4 * rows, width), F32),
            jax.ShapeDtypeStruct((2 * rows, width), BF16),
            jax.ShapeDtypeStruct((2 * rows, width), BF16),
        ],
        in_specs=[vmem, hbm, hbm],
        out_specs=[hbm, vmem, vmem, vmem],
        scratch_shapes=[
            pltpu.SemaphoreType.DMA((14,)),
            pltpu.SemaphoreType.DMA((14,)),
            pltpu.SemaphoreType.DMA((2,)),
            pltpu.VMEM(acts.shape, BF16),
            pltpu.VMEM(weight.shape, BF16),
            pltpu.VMEM((8 * rows, width), BF16),
            pltpu.VMEM((8 * rows, width), BF16),
            pltpu.SemaphoreType.DMA((4,)),
            pltpu.SemaphoreType.DMA((4,)),
            pltpu.SemaphoreType.DMA((2,)),
        ],
        compiler_params=remote_params(9, 48 * 1024 * 1024),
        cost_estimate=pl.CostEstimate(
            flops=2 * acts.size * width, bytes_accessed=16 * own.size, transcendentals=0
        ),
        name="gather8_product",
    )(own, acts, weight)


def gather8(own, also=()):
    rows, width = own.shape[0] // 2, own.shape[1]
    hbm = pl.BlockSpec(memory_space=pl.ANY)
    whole_shape = jax.ShapeDtypeStruct((16 * rows, width), own.dtype)
    sems = [
        pltpu.SemaphoreType.DMA((14,)),
        pltpu.SemaphoreType.DMA((14,)),
        pltpu.SemaphoreType.DMA((2,)),
    ]
    if also:
        sems += [pltpu.VMEM((8, rows, width), own.dtype)] + [pltpu.SemaphoreType.DMA((8,))] * 4
    outs = pl.pallas_call(
        functools.partial(gather8_kernel, rows, bool(also)),
        out_shape=[whole_shape] * (2 if also else 1),
        in_specs=[pl.BlockSpec(memory_space=pltpu.VMEM)] + [hbm] * len(also),
        out_specs=[hbm] * (2 if also else 1),
        scratch_shapes=sems,
        compiler_params=remote_params(6 if also else 1),
        name="gather8_also" if also else "gather8",
    )(own, *also)
    return outs if also else outs[0]


def reduce8_kernel(
    rows,
    near_ref,
    far_ref,
    out_ref,
    near,
    core_in,
    link_in,
    link_out,
    send_sem,
    recv_sem,
    local_sem,
):
    x_peer, y_peer, c_peer = neighbours()
    greet((x_peer, y_peer, c_peer))
    order = [(h, o, i) for o, i in ((1, 1), (1, 0), (0, 1), (0, 0)) for h in (0, 1)]
    core_copies, local_copies = {}, {}
    for number, (half, outer, inner) in enumerate(order):
        place = pl.ds((half * 4 + outer * 2 + inner) * rows, rows)
        core_copies[half, outer, inner] = pltpu.make_async_remote_copy(
            src_ref=far_ref.at[place],
            dst_ref=core_in.at[place],
            send_sem=send_sem.at[number],
            recv_sem=recv_sem.at[number],
            device_id=c_peer,
            device_id_type=MESH,
        )
        local_copies[half, outer, inner] = pltpu.make_async_copy(
            near_ref.at[place], near.at[place], local_sem.at[number]
        )
    for block in order:
        core_copies[block].start()
        local_copies[block].start()

    def partial_sum(block):
        half, outer, inner = block
        place = pl.ds((half * 4 + outer * 2 + inner) * rows, rows)
        core_copies[block].wait_recv()
        local_copies[block].wait()
        return near[place, :] + core_in[place, :].astype(F32)

    def link(index, value, peer):
        link_out[index] = value.astype(BF16)
        copy = pltpu.make_async_remote_copy(
            src_ref=link_out.at[index],
            dst_ref=link_in.at[index],
            send_sem=send_sem.at[8 + index],
            recv_sem=recv_sem.at[8 + index],
            device_id=peer,
            device_id_type=MESH,
        )
        copy.start()
        return copy

    y11 = link(0, partial_sum((0, 1, 1)), y_peer)
    x11 = link(1, partial_sum((1, 1, 1)), x_peer)
    y10 = link(2, partial_sum((0, 1, 0)), y_peer)
    x10 = link(3, partial_sum((1, 1, 0)), x_peer)
    first01, second01 = partial_sum((0, 0, 1)), partial_sum((1, 0, 1))
    y11.wait_recv()
    x01 = link(4, first01 + link_in[0].astype(F32), x_peer)
    x11.wait_recv()
    y01 = link(5, second01 + link_in[1].astype(F32), y_peer)
    first = partial_sum((0, 0, 0))
    second = partial_sum((1, 0, 0))
    y10.wait_recv()
    out_ref[pl.ds(0, rows), :] = first + link_in[2].astype(F32)
    x10.wait_recv()
    out_ref[pl.ds(rows, rows), :] = second + link_in[3].astype(F32)
    x01.wait_recv()
    out_ref[pl.ds(0, rows), :] += link_in[4].astype(F32)
    y01.wait_recv()
    out_ref[pl.ds(rows, rows), :] += link_in[5].astype(F32)
    for copy in (y11, x11, y10, x10, x01, y01):
        copy.wait_send()
    for copy in core_copies.values():
        copy.wait_send()


def reduce8(near, far):
    rows, width = near.shape[0] // 8, near.shape[1]
    return pl.pallas_call(
        functools.partial(reduce8_kernel, rows),
        out_shape=jax.ShapeDtypeStruct((2 * rows, width), F32),
        in_specs=[pl.BlockSpec(memory_space=pl.ANY), pl.BlockSpec(memory_space=pl.ANY)],
        out_specs=pl.BlockSpec(memory_space=pltpu.VMEM),
        scratch_shapes=[
            pltpu.VMEM(near.shape, F32),
            pltpu.VMEM(near.shape, BF16),
            pltpu.VMEM((6, rows, width), BF16),
            pltpu.VMEM((6, rows, width), BF16),
            pltpu.SemaphoreType.DMA((14,)),
            pltpu.SemaphoreType.DMA((14,)),
            pltpu.SemaphoreType.DMA((8,)),
        ],
        compiler_params=remote_params(2, 48 * 1024 * 1024),
        name="reduce8",
    )(near, far)


def tiled(count, tile, step):
    lax.fori_loop(0, count // tile, lambda i, _: step(pl.ds(pl.multiple_of(i * tile, tile), tile)), 0)


def product_reduce8_kernel(rows, groups, filler, *refs):
    acts_refs, refs = refs[:groups], refs[groups:]
    if filler:
        weight_ref, lhs_ref, out_ref, grad_ref, *refs = refs
    else:
        weight_ref, out_ref, *refs = refs
    acts, weight, far, near, core_in, link_in, link_out, send_sem, recv_sem, load_sem, *refs = refs
    x_peer, y_peer, c_peer = neighbours()
    width = weight.shape[0]
    wide = 2 * rows
    chunks = [(0, 1), (1, 1), (0, 0), (1, 0)]

    def where(chunk):
        return chunk[0] * 2 * wide + chunk[1] * wide

    half = width // 2
    load_weights = [
        pltpu.make_async_copy(
            weight_ref.at[pl.ds(part * half, half), pl.ds(0, weight.shape[1])],
            weight.at[pl.ds(part * half, half)],
            load_sem.at[part],
        )
        for part in (0, 1)
    ]
    loads = {}
    depth = weight.shape[1] // groups
    for number, chunk in enumerate(chunks):
        for side in (1, 0):
            place = pl.ds(side * 4 * wide + where(chunk), wide)
            loads[side, chunk] = [
                pltpu.make_async_copy(
                    acts_refs[group].at[place],
                    acts.at[place, pl.ds(group * depth, depth)],
                    load_sem.at[3 + (2 * number + side) * groups + group],
                )
                for group in range(groups)
            ]
    started = [loads[1, chunks[0]], [load_weights[0]], loads[1, chunks[1]], loads[0, chunks[0]]]
    started += [loads[0, chunks[1]], [load_weights[1]]]
    started += [loads[side, chunk] for chunk in chunks[2:] for side in (1, 0)]
    for group in started:
        for copy in group:
            copy.start()
    if filler:
        lhs, grad, grad_sem = refs
        load_lhs = pltpu.make_async_copy(lhs_ref, lhs, load_sem.at[2])
        load_lhs.start()
    greet((x_peer, y_peer, c_peer))

    core_copies, link_copies = {}, {}

    def product(chunk, side, part, target):
        place = pl.ds(where(chunk), wide)
        source = pl.ds(side * 4 * wide + where(chunk), wide)

        def step(index, _):
            cols = pl.ds(pl.multiple_of(part * half + index * (half // 2), half // 2), half // 2)
            target[place, cols] = mm(acts[source, :], weight[cols, :], 1, 1).astype(target.dtype)
            return 0

        lax.fori_loop(0, 2, step, 0)

    def remote(copies, key, number, source, target, peer):
        copies[key] = pltpu.make_async_remote_copy(
            src_ref=source,
            dst_ref=target,
            send_sem=send_sem.at[number],
            recv_sem=recv_sem.at[number],
            device_id=peer,
            device_id_type=MESH,
        )
        copies[key].start()

    def send_core(chunk, part):
        product(chunk, 1, part, far)
        here = (pl.ds(where(chunk), wide), pl.ds(part * half, half))
        number = 2 * chunks.index(chunk) + part
        remote(core_copies, (chunk, part), number, far.at[here], core_in.at[here], c_peer)

    def partial_sum(chunk, start, size, part):
        here = (pl.ds(where(chunk) + start, size), pl.ds(part * half, half))
        return near[here] + core_in[here].astype(F32)

    def link(hop, side, part, value, peer):
        size = value.shape[0]
        start = (side * 3 + hop * 2) * rows
        here = (pl.ds(start, size), pl.ds(part * half, half))
        link_out[here] = value.astype(BF16)
        number = 8 + hop * 4 + side * 2 + part
        remote(link_copies, (hop, side, part), number, link_out.at[here], link_in.at[here], peer)

    def came(hop, side, start, part):
        return link_in[
            pl.ds((side * 3 + hop * 2) * rows + start, rows), pl.ds(part * half, half)
        ].astype(F32)

    for chunk in chunks[:2]:
        for copy in loads[1, chunk]:
            copy.wait()
    for part in (0, 1):
        load_weights[part].wait()
        send_core((0, 1), part)
        send_core((1, 1), part)
        for side, peer in ((0, y_peer), (1, x_peer)):
            if part == 0:
                for copy in loads[0, (side, 1)]:
                    copy.wait()
            product((side, 1), 0, part, near)
            core_copies[(side, 1), part].wait_recv()
            link(0, side, part, partial_sum((side, 1), 0, wide, part), peer)
    for chunk in chunks[2:]:
        for side in (1, 0):
            for copy in loads[side, chunk]:
                copy.wait()
    for part in (0, 1):
        for chunk in chunks[2:]:
            send_core(chunk, part)
        for chunk in chunks[2:]:
            product(chunk, 0, part, near)
        for side, peer in ((0, x_peer), (1, y_peer)):
            core_copies[(side, 0), part].wait_recv()
            link_copies[0, side, part].wait_recv()
            link(1, side, part, partial_sum((side, 0), rows, rows, part) + came(0, side, rows, part), peer)
    if filler:
        load_lhs.wait()
        size = width // 4

        def fill(index, _):
            cols = pl.ds(pl.multiple_of(index * size, size), size)

            def step(columns):
                grad[cols, columns] = mm(lhs[:, cols], acts[:, columns], 0, 0).astype(BF16)
                return 0

            tiled(acts.shape[1], acts.shape[1] // 3, step)
            return 0

        lax.fori_loop(0, 4, fill, 0)
        grad_copy = pltpu.make_async_copy(grad, grad_ref, grad_sem.at[0])
        grad_copy.start()
    for side in (0, 1):
        for part in (0, 1):
            place = (pl.ds(side * rows, rows), pl.ds(part * half, half))
            kept = partial_sum((side, 0), 0, rows, part) + came(0, side, 0, part)
            link_copies[1, side, part].wait_recv()
            out_ref[place] = kept + came(1, side, 0, part)
    for copy in list(link_copies.values()) + list(core_copies.values()):
        copy.wait_send()
    if filler:
        grad_copy.wait()


def product_reduce8(columns, weight, number, lhs=None):
    depth, groups = sum(column.shape[1] for column in columns), len(columns)
    acts = jax.ShapeDtypeStruct((columns[0].shape[0], depth), BF16)
    rows, width = acts.shape[0] // 16, weight.shape[0]
    filler = lhs is not None
    hbm = pl.BlockSpec(memory_space=pl.ANY)
    scratch = [
        pltpu.VMEM(acts.shape, BF16),
        pltpu.VMEM((width, depth), BF16),
        pltpu.VMEM((8 * rows, width), BF16),
        pltpu.VMEM((8 * rows, width), F32),
        pltpu.VMEM((8 * rows, width), BF16),
        pltpu.VMEM((6 * rows, width), BF16),
        pltpu.VMEM((6 * rows, width), BF16),
        pltpu.SemaphoreType.DMA((16,)),
        pltpu.SemaphoreType.DMA((16,)),
        pltpu.SemaphoreType.DMA((3 + 8 * groups,)),
    ]
    out_shape = [jax.ShapeDtypeStruct((2 * rows, width), F32)]
    out_specs = [pl.BlockSpec(memory_space=pltpu.VMEM)]
    flops = 2 * acts.shape[0] * width * depth
    if filler:
        scratch += [
            pltpu.VMEM(lhs.shape, BF16),
            pltpu.VMEM((width, depth), BF16),
            pltpu.SemaphoreType.DMA((1,)),
        ]
        out_shape.append(jax.ShapeDtypeStruct((width, depth), BF16))
        out_specs.append(hbm)
        flops *= 2
    outs = pl.pallas_call(
        functools.partial(product_reduce8_kernel, rows, groups, filler),
        out_shape=out_shape,
        in_specs=[hbm] * (groups + (2 if filler else 1)),
        out_specs=out_specs,
        scratch_shapes=scratch,
        compiler_params=remote_params(number, 63 * 1024 * 1024),
        cost_estimate=pl.CostEstimate(
            flops=flops, bytes_accessed=4 * depth * (acts.shape[0] + width), transcendentals=0
        ),
        name="product_reduce8",
    )(*columns, weight, *((lhs,) if filler else ()))
    return outs if filler else outs[0]


def shard_kernel(plan, outs, *refs):
    ins, out_refs = refs[: len(plan)], refs[len(plan) : len(plan) + outs]
    stage = refs[len(plan) + outs : 2 * len(plan) + outs]
    send_sem, recv_sem, load_sem, store_sem = refs[2 * len(plan) + outs :]
    x_peer, _, _ = neighbours()
    odd = lax.rem(lax.axis_index("fsdp"), 2)
    column = 2 * lax.axis_index("ctx") + odd
    other = 2 * lax.axis_index("ctx") + 1 - odd
    greet((x_peer,))
    remote, loads, stores = [], [], []
    for number, (which, start, size, cut) in enumerate(plan):
        rows = ins[number].shape[0]
        place = pl.ds(pl.multiple_of(odd * rows, rows), rows)
        target = out_refs[which].at[place, pl.ds(start, size)]

        def source(index, ref=ins[number], size=size, cut=cut):
            if not cut:
                return ref
            return ref.at[:, pl.ds(pl.multiple_of(index * size, HEAD), size)]

        remote.append(
            pltpu.make_async_remote_copy(
                src_ref=source(other),
                dst_ref=target,
                send_sem=send_sem.at[number],
                recv_sem=recv_sem.at[number],
                device_id=x_peer,
                device_id_type=MESH,
            )
        )
        loads.append(pltpu.make_async_copy(source(column), stage[number], load_sem.at[number]))
        stores.append(pltpu.make_async_copy(stage[number], target, store_sem.at[number]))
    for copy in remote:
        copy.start()
    for copy in loads:
        copy.start()
    for load, store in zip(loads, stores):
        load.wait()
        store.start()
    for copy in stores:
        copy.wait()
    for copy in remote:
        copy.wait()


def shards(groups, number):
    plan, arrays, shapes = [], [], []
    for which, group in enumerate(groups):
        start = 0
        for array, cut in group:
            size = array.shape[1] // 4 if cut else array.shape[1]
            plan.append((which, start, size, cut))
            arrays.append(array)
            start += size
        shapes.append((2 * group[0][0].shape[0], start))
    hbm = pl.BlockSpec(memory_space=pl.ANY)
    return pl.pallas_call(
        functools.partial(shard_kernel, tuple(plan), len(groups)),
        out_shape=[jax.ShapeDtypeStruct(shape, BF16) for shape in shapes],
        in_specs=[hbm] * len(arrays),
        out_specs=[hbm] * len(groups),
        scratch_shapes=[
            pltpu.VMEM((array.shape[0], size), BF16)
            for array, (_, _, size, _) in zip(arrays, plan)
        ]
        + [pltpu.SemaphoreType.DMA((len(plan),))] * 4,
        compiler_params=remote_params(number),
        name="shards",
    )(*arrays)


def total_kernel(stages, part_ref, out_ref, inbox, outbox, send_sem, recv_sem):
    peers = []
    for axis, bit in stages:
        mine = lax.axis_index(axis)
        peers.append({axis: mine + bit * (1 - 2 * lax.rem(mine // bit, 2))})
    greet(peers)
    value = part_ref[...]
    copies = []
    for index, peer in enumerate(peers):
        outbox[index] = value
        copy = pltpu.make_async_remote_copy(
            src_ref=outbox.at[index],
            dst_ref=inbox.at[index],
            send_sem=send_sem.at[index],
            recv_sem=recv_sem.at[index],
            device_id=peer,
            device_id_type=MESH,
        )
        copy.start()
        copies.append(copy)
        copy.wait_recv()
        value = value + inbox[index]
    out_ref[...] = value
    for copy in copies:
        copy.wait_send()


def total(part):
    stages, bit = [], 2
    while bit < lax.axis_size("fsdp"):
        stages.append(("fsdp", bit))
        bit *= 2
    stages += [("tp", 1), ("fsdp", 1), ("ctx", 1)]
    return pl.pallas_call(
        functools.partial(total_kernel, tuple(stages)),
        out_shape=jax.ShapeDtypeStruct(part.shape, F32),
        in_specs=[pl.BlockSpec(memory_space=pltpu.VMEM)],
        out_specs=pl.BlockSpec(memory_space=pltpu.VMEM),
        scratch_shapes=[
            pltpu.VMEM((len(stages),) + part.shape, F32),
            pltpu.VMEM((len(stages),) + part.shape, F32),
            pltpu.SemaphoreType.DMA((len(stages),)),
            pltpu.SemaphoreType.DMA((len(stages),)),
        ],
        compiler_params=remote_params(5),
        name="total",
    )(part)


def join_kernel(sizes, spot_ref, kept_ref, x_ref, y_ref, both_ref, *out_refs):
    place, odd = spot_ref[0], spot_ref[1]
    parts = (
        (kept_ref, 2 * place + odd),
        (x_ref, 2 * place + 1 - odd),
        (y_ref, 2 - 2 * place + odd),
        (both_ref, 3 - 2 * place - odd),
    )
    for part, column in parts:
        start = 0
        for size, out_ref in zip(sizes, out_refs):
            target = pl.ds(pl.multiple_of(column * size, HEAD), size)
            out_ref[:, target] = part[:, start : start + size].astype(F32)
            start += size


def join_columns(spot, parts, sizes):
    rows = parts[0].shape[0]
    tile = min(rows, 64)
    return pl.pallas_call(
        functools.partial(join_kernel, sizes),
        out_shape=[jax.ShapeDtypeStruct((rows, 4 * size), F32) for size in sizes],
        grid_spec=pltpu.PrefetchScalarGridSpec(
            num_scalar_prefetch=1,
            grid=(rows // tile,),
            in_specs=[
                pl.BlockSpec((tile, part.shape[1]), lambda i, spot: (i, 0)) for part in parts
            ],
            out_specs=[pl.BlockSpec((tile, 4 * size), lambda i, spot: (i, 0)) for size in sizes],
        ),
        name="join",
    )(spot, *parts)


def after(value, *others):
    return lax.optimization_barrier((value,) + others)[0]


def reduce4_links(kept, to_y, to_x, *others):
    rows = kept.shape[0] // 4
    came_first, came_second = swap_ctx(to_y), swap_x(to_x)
    first = kept[: 2 * rows] + after(came_first, *others).astype(F32)
    second = kept[2 * rows :] + after(came_second, *others).astype(F32)
    came_first = swap_x(first[rows:].astype(BF16))
    came_second = swap_ctx(second[rows:].astype(BF16))
    return first[:rows], second[:rows], came_first, came_second


def rope_tables(positions):
    freqs = THETA ** (-(jnp.arange(HEAD // 2, dtype=F32) * 2.0) / HEAD)
    angle = positions[:, None] * freqs[None, :]
    cosine = jnp.concatenate([jnp.cos(angle), jnp.cos(angle)], axis=-1)
    sine = jnp.concatenate([-jnp.sin(angle), jnp.sin(angle)], axis=-1)
    return cosine, sine


def norm_back(grad, scaled, inverse, gain):
    weighted = grad * gain
    return inverse * (weighted - scaled * jnp.mean(weighted * scaled, axis=-1, keepdims=True))


def inv_rms(value):
    return lax.rsqrt(jnp.mean(value * value, axis=-1, keepdims=True) + EPS)


def block_row(meta_ref, seq, index, rows):
    away_c = lax.rem(meta_ref[0] + index // 4, 2)
    away_t = lax.rem(meta_ref[1] + (index // 2) % 2, 2)
    if index % 2 == 0:
        inner = away_c * 2 + seq
    else:
        inner = seq * 2 + away_c + 4
    return pl.multiple_of((away_t * 8 + inner) * rows, rows)


def scaled_of(raw):
    inverse = lax.rsqrt(jnp.mean(raw * raw, axis=-1, keepdims=True) + EPS)
    return raw * inverse, inverse


def load_heads(meta_ref, qkv_ref, cos_ref, sin_ref, gain_ref, q_scr, k_scr, v_scr, heads):
    seq = pl.program_id(0)
    rows = q_scr.shape[1] // 8
    for index in range(8):
        start = block_row(meta_ref, seq, index, rows)
        here = slice(index * rows, (index + 1) * rows)
        cosine, sine = cos_ref[here, :], sin_ref[here, :]
        for head in range(heads + 1):
            raw = qkv_ref[pl.ds(start, rows), head * HEAD : (head + 1) * HEAD]
            scaled, _ = scaled_of(raw)
            which = 0 if head < heads else 1
            value = scaled * gain_ref[which : which + 1, :]
            turned = value * cosine + pltpu.roll(value, HEAD // 2, 1) * sine
            if head < heads:
                q_scr[head, here, :] = turned.astype(BF16)
            else:
                k_scr[here, :] = turned.astype(BF16)
        v_scr[here, :] = qkv_ref[
            pl.ds(start, rows), (heads + 1) * HEAD : (heads + 2) * HEAD
        ].astype(BF16)


def key_span(index, tile):
    low = max(0, (index * tile - (MOST_DOC - 1)) // tile) * tile
    return low, (index + 1) * tile


def allowed_mask(segc_ref, segr_ref, index, tile):
    low, high = key_span(index, tile)
    shape = (tile, high - low)
    rows = lax.broadcasted_iota(jnp.int32, shape, 0) + index * tile
    cols = lax.broadcasted_iota(jnp.int32, shape, 1) + low
    same = segc_ref[0, index * tile : (index + 1) * tile, :] == segr_ref[0, :, low:high]
    return same & (cols <= rows)


def probs_of(query, keys, allowed, scale):
    scores = jnp.where(allowed, mm(query, keys, 1, 1) * scale, MASKED)
    weights = jnp.exp(scores - jnp.max(scores, axis=-1, keepdims=True))
    return weights * (1.0 / jnp.sum(weights, axis=-1, keepdims=True))


def attend_kernel(
    heads, tile, meta_ref, qkv_ref, segc_ref, segr_ref, cos_ref, sin_ref, gain_ref, out_ref, q_scr, k_scr, v_scr
):
    seq = pl.program_id(0)
    length = k_scr.shape[0]
    rows = length // 8
    scale = 1.0 / math.sqrt(HEAD)
    load_heads(meta_ref, qkv_ref, cos_ref, sin_ref, gain_ref, q_scr, k_scr, v_scr, heads)
    for index in range(length // tile):
        low, high = key_span(index, tile)
        allowed = allowed_mask(segc_ref, segr_ref, index, tile)
        for head in range(heads):
            query = q_scr[head, index * tile : (index + 1) * tile, :]
            probs = probs_of(query, k_scr[low:high, :], allowed, scale)
            mixed = mm(probs.astype(BF16), v_scr[low:high, :], 1, 0).astype(BF16)
            for piece in range(tile // rows):
                start = block_row(meta_ref, seq, index * (tile // rows) + piece, rows)
                out_ref[pl.ds(start, rows), head * HEAD : (head + 1) * HEAD] = mixed[
                    piece * rows : (piece + 1) * rows
                ]


def attend_back_kernel(
    heads,
    tile,
    meta_ref,
    qkv_ref,
    grad_ref,
    segc_ref,
    segr_ref,
    cos_ref,
    sin_ref,
    gain_ref,
    out_ref,
    gain_out_ref,
    q_scr,
    k_scr,
    v_scr,
    g_scr,
    dk_scr,
    dv_scr,
):
    seq = pl.program_id(0)
    length = k_scr.shape[0]
    rows = length // 8
    scale = 1.0 / math.sqrt(HEAD)
    load_heads(meta_ref, qkv_ref, cos_ref, sin_ref, gain_ref, q_scr, k_scr, v_scr, heads)
    for index in range(8):
        start = block_row(meta_ref, seq, index, rows)
        g_scr[index * rows : (index + 1) * rows, :] = grad_ref[pl.ds(start, rows), :]
    dk_scr[...] = jnp.zeros_like(dk_scr)
    dv_scr[...] = jnp.zeros_like(dv_scr)

    @pl.when(seq == 0)
    def _():
        gain_out_ref[...] = jnp.zeros_like(gain_out_ref)

    def finish(grad, index, head, which):
        here = slice(index * rows, (index + 1) * rows)
        start = block_row(meta_ref, seq, index, rows)
        grad = grad * cos_ref[here, :] - pltpu.roll(grad, HEAD // 2, 1) * sin_ref[here, :]
        raw = qkv_ref[pl.ds(start, rows), head * HEAD : (head + 1) * HEAD]
        scaled, inverse = scaled_of(raw)
        gain_out_ref[which : which + 1, :] += jnp.sum(grad * scaled, axis=0, keepdims=True)
        out = norm_back(grad, scaled, inverse, gain_ref[which : which + 1, :])
        out_ref[pl.ds(start, rows), head * HEAD : (head + 1) * HEAD] = out.astype(BF16)

    per = tile // rows
    for index in range(length // tile):
        low, high = key_span(index, tile)
        mine = slice(index * tile, (index + 1) * tile)
        allowed = allowed_mask(segc_ref, segr_ref, index, tile)
        for head in range(heads):
            query = q_scr[head, mine, :]
            keys = k_scr[low:high, :]
            probs = probs_of(query, keys, allowed, scale)
            grad = g_scr[mine, head * HEAD : (head + 1) * HEAD]
            grad_probs = mm(grad, v_scr[low:high, :], 1, 1)
            delta = jnp.sum(probs * grad_probs, axis=-1, keepdims=True)
            grad_scores = (probs * (grad_probs - delta)).astype(BF16)
            dv_scr[low:high, :] += mm(probs.astype(BF16), grad, 0, 0)
            dk_scr[low:high, :] += mm(grad_scores, query, 0, 0) * scale
            grad_query = mm(grad_scores, keys, 1, 0) * scale
            for piece in range(per):
                finish(
                    grad_query[piece * rows : (piece + 1) * rows], index * per + piece, head, 0
                )
    for index in range(8):
        here = slice(index * rows, (index + 1) * rows)
        start = block_row(meta_ref, seq, index, rows)
        finish(dk_scr[here, :], index, heads, 1)
        out_ref[pl.ds(start, rows), (heads + 1) * HEAD : (heads + 2) * HEAD] = dv_scr[
            here, :
        ].astype(BF16)


def whole(shape):
    return pl.BlockSpec(shape, lambda seq, meta: (0,) * len(shape))


def seg_specs(length):
    return [
        pl.BlockSpec((1, length, 1), lambda seq, meta: (seq, 0, 0)),
        pl.BlockSpec((1, 1, length), lambda seq, meta: (seq, 0, 0)),
    ]


def attend(meta, qkv, seg_cols, seg_rows, cosine, sine, gains):
    length = cosine.shape[0]
    tile = length // 4
    heads = qkv.shape[1] // HEAD - 2
    pairs = 2 * heads * length * length // 2
    return pl.pallas_call(
        functools.partial(attend_kernel, heads, tile),
        out_shape=jax.ShapeDtypeStruct((qkv.shape[0], heads * HEAD), BF16),
        grid_spec=pltpu.PrefetchScalarGridSpec(
            num_scalar_prefetch=1,
            grid=(2,),
            in_specs=[whole(qkv.shape)]
            + seg_specs(length)
            + [whole(cosine.shape), whole(sine.shape), whole(gains.shape)],
            out_specs=whole((qkv.shape[0], heads * HEAD)),
            scratch_shapes=[
                pltpu.VMEM((heads, length, HEAD), BF16),
                pltpu.VMEM((length, HEAD), BF16),
                pltpu.VMEM((length, HEAD), BF16),
            ],
        ),
        cost_estimate=pl.CostEstimate(
            flops=4 * pairs * HEAD, bytes_accessed=qkv.size * 4 + qkv.size, transcendentals=pairs
        ),
        name="attend",
    )(meta, qkv, seg_cols, seg_rows, cosine, sine, gains)


def attend_back(meta, qkv, grad, seg_cols, seg_rows, cosine, sine, gains):
    length = cosine.shape[0]
    tile = length // 4
    heads = qkv.shape[1] // HEAD - 2
    pairs = 2 * heads * length * length // 2
    return pl.pallas_call(
        functools.partial(attend_back_kernel, heads, tile),
        out_shape=(
            jax.ShapeDtypeStruct(qkv.shape, BF16),
            jax.ShapeDtypeStruct(gains.shape, F32),
        ),
        grid_spec=pltpu.PrefetchScalarGridSpec(
            num_scalar_prefetch=1,
            grid=(2,),
            in_specs=[whole(qkv.shape), whole(grad.shape)]
            + seg_specs(length)
            + [whole(cosine.shape), whole(sine.shape), whole(gains.shape)],
            out_specs=(whole(qkv.shape), whole(gains.shape)),
            scratch_shapes=[
                pltpu.VMEM((heads, length, HEAD), BF16),
                pltpu.VMEM((length, HEAD), BF16),
                pltpu.VMEM((length, HEAD), BF16),
                pltpu.VMEM((length, heads * HEAD), BF16),
                pltpu.VMEM((length, HEAD), F32),
                pltpu.VMEM((length, HEAD), F32),
            ],
        ),
        cost_estimate=pl.CostEstimate(
            flops=10 * pairs * HEAD, bytes_accessed=qkv.size * 8, transcendentals=pairs
        ),
        name="attend_back",
    )(meta, qkv, grad, seg_cols, seg_rows, cosine, sine, gains)


def body(
    tokens,
    segment_ids,
    norm_gain,
    query_weight,
    key_matrix,
    value_matrix,
    output_weight,
    query_gain,
    key_gain,
    mlp_gain,
    gate_weight,
    up_weight,
    down_weight,
    cotangent,
):
    local, width = tokens.shape[1], tokens.shape[2]
    length = 2 * local
    quarter = local // 2
    count = lax.axis_size("fsdp")
    block = width // count
    mine = lax.axis_index("fsdp")
    odd = mine % 2
    place = lax.axis_index("ctx")
    core = lax.axis_index("tp")

    small = query_gain.shape[0]
    lanes = jnp.arange(HEAD)[None, :]

    def pad_rows(vector):
        return jnp.concatenate([vector, jnp.zeros((block - small,), BF16)])

    gains = jnp.where(
        lanes == 0,
        norm_gain[:, None],
        jnp.where(
            lanes == 1,
            mlp_gain[:, None],
            jnp.where(
                lanes == 2, pad_rows(query_gain)[:, None], pad_rows(key_gain)[:, None]
            ),
        ),
    )
    far_segments = swap_x(segment_ids)
    (first_pair,) = shards(
        [
            [
                (query_weight, True),
                (key_matrix, True),
                (value_matrix, True),
                (output_weight, True),
                (gains, False),
            ]
        ],
        3,
    )
    first = gather_line(first_pair)
    gate_up_pair, down_pair = shards(
        [
            [(after(gate_weight, first_pair), True), (up_weight, True)],
            [(down_weight, True)],
        ],
        4,
    )
    gate_up_w = gather_line(gate_up_pair)
    down_w = gather_line(down_pair)

    def own_quarter(value):
        return lax.dynamic_slice_in_dim(value.reshape(local, width), core * quarter, quarter, 0)

    own_tok, own_cot = own_quarter(tokens), own_quarter(cotangent)
    tok = gather8(after(own_tok, gate_up_pair))
    segments = jnp.concatenate([segment_ids, far_segments])
    seg_cols, seg_rows = segments[:, :, None], segments[:, None, :]
    cosine, sine = rope_tables(jnp.arange(length).astype(F32))
    meta = jnp.stack([place, core]).astype(jnp.int32)

    heads_q = query_weight.shape[1] // 4 // HEAD
    cols = (heads_q + 2) * HEAD
    qkv_w = first[:, :cols]
    out_w = first[:, cols : cols + heads_q * HEAD]
    gain_cols = first[:, cols + heads_q * HEAD :].astype(F32)
    in_gain, mid_gain = gain_cols[:, 0][None], gain_cols[:, 1][None]
    head_gains = gain_cols.reshape(count, block, HEAD)[:, :small, 2:4].reshape(HEAD, 2).T

    in_f = tok.astype(F32)
    cot_from = after(own_cot, tok)
    cot_x, cot_y = swap_x(cot_from), swap_ctx(cot_from)
    x_all = (in_f * inv_rms(in_f) * in_gain).astype(BF16)
    qkv = mm(x_all, qkv_w, 1, 0)
    attended = attend(meta, qkv, seg_cols, seg_rows, cosine, sine, head_gains)
    half = 4 * quarter
    cot_x, cot_y = after(cot_x, attended), after(cot_y, attended)
    eighth = quarter // 2
    cot_first, cot_second = swap_ctx(cot_x[:eighth]), swap_x(cot_y[eighth:])
    out_far = mm(attended[half:], out_w, 1, 1).astype(BF16)
    out_near = mm(attended[:half], out_w, 1, 1)
    middle = own_tok.astype(F32) + reduce8(out_near, out_far)
    inverse_mid = inv_rms(middle)
    scaled_mid = middle * inverse_mid
    y_own = (scaled_mid * mid_gain).astype(BF16)
    cot_first, cot_second = after(cot_first, y_own), after(cot_second, y_own)
    y_all, cot = gather8(y_own, (cot_from, cot_x, cot_y, cot_first, cot_second))

    ff = gate_up_w.shape[1] // 2
    gate_up = mm(y_all, gate_up_w, 1, 0)
    gate, up_value = gate_up[:, :ff], gate_up[:, ff:]
    sig = jax.nn.sigmoid(gate)
    active = gate * sig
    hidden = (active * up_value).astype(BF16)
    down_grad = mm(cot, hidden, 0, 0).astype(BF16)

    def finish_rows(own):
        pair = jnp.stack([own, swap_core(own)])
        return flip_if(core == 1, pair, 0).reshape(tokens.shape)

    grad_hidden = mm(after(cot, down_grad), down_w, 1, 0)
    grad_up = (grad_hidden * active).astype(BF16)
    grad_gate = (grad_hidden * up_value * (sig * (1.0 + gate * (1.0 - sig)))).astype(BF16)
    mid_grad, gate_up_grad = product_reduce8((grad_gate, grad_up), gate_up_w, 7, y_all)

    mlp_gain_part = jnp.sum(mid_grad * scaled_mid, axis=0)
    grad_middle = own_cot.astype(F32) + norm_back(mid_grad, scaled_mid, inverse_mid, mid_gain)
    grad_attn, mlp_kept, mlp_to_y, mlp_to_x = gather8_product(
        grad_middle.astype(BF16), hidden, down_w
    )
    out_grad = mm(grad_attn, attended, 0, 0).astype(BF16)
    grad_att = mm(grad_attn, out_w, 1, 0).astype(BF16)
    raw_grads, head_gain_parts = attend_back(
        meta, qkv, grad_att, seg_cols, seg_rows, cosine, sine, head_gains
    )
    mlp_first, mlp_second, mlp_came1, mlp_came2 = reduce4_links(
        mlp_kept, mlp_to_y, mlp_to_x, raw_grads
    )
    first_grad = mm(x_all, raw_grads, 0, 0).astype(BF16)
    first_grad = jnp.concatenate([first_grad, out_grad], axis=1)
    mlp_first = mlp_first + after(mlp_came1, first_grad).astype(F32)
    mlp_second = mlp_second + after(mlp_came2, first_grad).astype(F32)
    mlp_sum = (middle + jnp.concatenate([mlp_first, mlp_second])).astype(BF16)
    layer_out = finish_rows(mlp_sum)
    in_grad = product_reduce8((after(raw_grads, first_grad, mlp_sum),), first, 8)

    spot = jnp.stack([place, odd]).astype(jnp.int32)

    def owners(grad, sizes, *others):
        rows = scatter_line(grad)
        rows = after(rows, *others)
        kept = lax.dynamic_slice_in_dim(rows, odd * block, block, 0)
        sent = lax.dynamic_slice_in_dim(rows, (1 - odd) * block, block, 0)
        by_x, by_y = swap_x(sent), swap_ctx(kept)
        by_both = swap_ctx(by_x)
        return join_columns(spot, (kept, by_x, by_y, by_both), sizes)

    (down_share,) = owners(down_grad, (ff,))
    gate_share, up_share = owners(gate_up_grad, (ff, ff))
    query_share, key_share, value_share, out_share = owners(
        first_grad, (heads_q * HEAD, HEAD, HEAD, heads_q * HEAD)
    )

    own_in = own_tok.astype(F32)
    inverse_in = inv_rms(own_in)
    scaled_in = own_in * inverse_in
    norm_gain_part = jnp.sum(in_grad * scaled_in, axis=0)
    token_grad = finish_rows(
        (grad_middle + norm_back(in_grad, scaled_in, inverse_in, in_gain)).astype(BF16)
    )

    parts = jnp.concatenate([norm_gain_part, mlp_gain_part, head_gain_parts.reshape(-1)])
    sums = total(parts.reshape(-1, HEAD)).reshape(-1)
    norm_gain_grad = lax.dynamic_slice_in_dim(sums, mine * block, block, 0)
    mlp_gain_grad = lax.dynamic_slice_in_dim(sums, width + mine * block, block, 0)
    query_gain_grad = lax.dynamic_slice_in_dim(sums, 2 * width + mine * small, small, 0)
    key_gain_grad = lax.dynamic_slice_in_dim(sums, 2 * width + HEAD + mine * small, small, 0)
    return (
        layer_out,
        token_grad,
        norm_gain_grad,
        query_share,
        key_share,
        value_share,
        out_share,
        query_gain_grad,
        key_gain_grad,
        mlp_gain_grad,
        gate_share,
        up_share,
        down_share,
    )


def solution(mesh):
    in_specs = (
        P("fsdp", "ctx", None),
        P("fsdp", None),
        P("fsdp"),
        P("fsdp", "tp"),
        P("fsdp", "tp"),
        P("fsdp", "tp"),
        P("fsdp", "tp"),
        P("fsdp"),
        P("fsdp"),
        P("fsdp"),
        P("fsdp", "tp"),
        P("fsdp", "tp"),
        P("fsdp", "tp"),
        P("fsdp", "ctx", None),
    )
    out_specs = (
        P("fsdp", "ctx", None),
        P("fsdp", "ctx", None),
        P("fsdp"),
        P("fsdp", "tp"),
        P("fsdp", "tp"),
        P("fsdp", "tp"),
        P("fsdp", "tp"),
        P("fsdp"),
        P("fsdp"),
        P("fsdp"),
        P("fsdp", "tp"),
        P("fsdp", "tp"),
        P("fsdp", "tp"),
    )

    return jax.shard_map(body, mesh=mesh, in_specs=in_specs, out_specs=out_specs, check_vma=False)
```

```python
import functools
import math

import jax
import jax.numpy as jnp
from jax import lax
from jax.experimental import pallas as pl
from jax.experimental.pallas import tpu as pltpu
from jax.sharding import PartitionSpec as P


HEAD = 128
EPS = 1e-06
THETA = 1000000.0
MASKED = -1e30
MOST_DOC = 512
MESH = pl.DeviceIdType.MESH
F32 = jnp.float32
BF16 = jnp.bfloat16


def mm(left, right, left_dim, right_dim):
    return lax.dot_general(
        left, right, (((left_dim,), (right_dim,)), ((), ())), preferred_element_type=F32
    )


def swap_core(value):
    return lax.ppermute(value, "tp", [(0, 1), (1, 0)])


def swap_ctx(value):
    return lax.ppermute(value, "ctx", [(0, 1), (1, 0)])


def swap_x(value):
    count = lax.axis_size("fsdp")
    return lax.ppermute(value, "fsdp", [(i, i ^ 1) for i in range(count)])


def lines():
    count = lax.axis_size("fsdp")
    return [[i for i in range(count) if i % 2 == parity] for parity in (0, 1)]


def gather_line(value):
    return lax.all_gather(value, "fsdp", axis=0, tiled=True, axis_index_groups=lines())


def scatter_line(value):
    return lax.psum_scatter(
        value, "fsdp", scatter_dimension=0, tiled=True, axis_index_groups=lines()
    )


def flip_if(flag, value, axis):
    return jnp.where(flag, jnp.flip(value, axis), value)


def neighbours():
    mine = lax.axis_index("fsdp")
    return (
        {"fsdp": mine + 1 - 2 * lax.rem(mine, 2)},
        {"ctx": 1 - lax.axis_index("ctx")},
        {"tp": 1 - lax.axis_index("tp")},
    )


def greet(peers):
    barrier = pltpu.get_barrier_semaphore()
    for peer in peers:
        pl.semaphore_signal(barrier, inc=1, device_id=peer, device_id_type=MESH)
    pl.semaphore_wait(barrier, len(peers))


def remote_params(number, limit=None):
    return pltpu.CompilerParams(
        collective_id=number, has_side_effects=True, vmem_limit_bytes=limit
    )


def gather8_kernel(rows, spread, *refs):
    if spread:
        own_ref, kept_ref, x_ref, y_ref, first_ref, second_ref, out_ref, also_ref = refs[:8]
        send_sem, recv_sem, local_sem, stage, also_send, also_recv, also_in, also_out = refs[8:]
    else:
        own_ref, out_ref, send_sem, recv_sem, local_sem = refs
    x_peer, y_peer, c_peer = neighbours()

    def start_of(away_t, half, outer, inner):
        return pl.ds((away_t * 8 + half * 4 + outer * 2 + inner) * rows, rows)

    def slot(*block):
        return out_ref.at[start_of(*block)]

    also_loads, also_remote, also_stores = [], [], []
    if spread:
        top, low = pl.ds(0, rows), pl.ds(rows, rows)
        pieces = [
            ((0, 0, 0), kept_ref.at[top]),
            ((0, 0, 1), x_ref.at[top]),
            ((0, 1, 0), y_ref.at[top]),
            ((0, 1, 1), first_ref),
            ((1, 0, 0), kept_ref.at[low]),
            ((1, 0, 1), y_ref.at[low]),
            ((1, 1, 0), x_ref.at[low]),
            ((1, 1, 1), second_ref),
        ]
        for index, (block, source) in enumerate(pieces):
            also_loads.append(pltpu.make_async_copy(source, stage.at[index], also_in.at[index]))
            also_stores.append(
                pltpu.make_async_copy(
                    stage.at[index], also_ref.at[start_of(0, *block)], also_out.at[index]
                )
            )
            also_remote.append(
                pltpu.make_async_remote_copy(
                    src_ref=source,
                    dst_ref=also_ref.at[start_of(1, *block)],
                    send_sem=also_send.at[index],
                    recv_sem=also_recv.at[index],
                    device_id=c_peer,
                    device_id_type=MESH,
                )
            )
        for copy in also_loads:
            copy.start()
    greet((x_peer, y_peer, c_peer))

    number = iter(range(14))

    def send(source, target, peer):
        index = next(number)
        copy = pltpu.make_async_remote_copy(
            src_ref=source,
            dst_ref=target,
            send_sem=send_sem.at[index],
            recv_sem=recv_sem.at[index],
            device_id=peer,
            device_id_type=MESH,
        )
        copy.start()
        return copy

    first, second = own_ref.at[pl.ds(0, rows)], own_ref.at[pl.ds(rows, rows)]
    x1 = send(first, slot(0, 0, 0, 1), x_peer)
    y1 = send(second, slot(0, 1, 0, 1), y_peer)
    x2 = send(second, slot(0, 1, 1, 0), x_peer)
    y2 = send(first, slot(0, 0, 1, 0), y_peer)
    rest = [send(first, slot(1, 0, 0, 0), c_peer), send(second, slot(1, 1, 0, 0), c_peer)]
    kept = [
        pltpu.make_async_copy(first, slot(0, 0, 0, 0), local_sem.at[0]),
        pltpu.make_async_copy(second, slot(0, 1, 0, 0), local_sem.at[1]),
    ]
    for copy in kept:
        copy.start()
    for copy in also_remote:
        copy.start()
    for load, store in zip(also_loads, also_stores):
        load.wait()
        store.start()
    x1.wait_recv()
    y3 = send(slot(0, 0, 0, 1), slot(0, 0, 1, 1), y_peer)
    y1.wait_recv()
    x3 = send(slot(0, 1, 0, 1), slot(0, 1, 1, 1), x_peer)
    rest.append(send(slot(0, 0, 0, 1), slot(1, 0, 0, 1), c_peer))
    rest.append(send(slot(0, 1, 0, 1), slot(1, 1, 0, 1), c_peer))
    x2.wait_recv()
    rest.append(send(slot(0, 1, 1, 0), slot(1, 1, 1, 0), c_peer))
    y2.wait_recv()
    rest.append(send(slot(0, 0, 1, 0), slot(1, 0, 1, 0), c_peer))
    y3.wait_recv()
    rest.append(send(slot(0, 0, 1, 1), slot(1, 0, 1, 1), c_peer))
    x3.wait_recv()
    rest.append(send(slot(0, 1, 1, 1), slot(1, 1, 1, 1), c_peer))
    for copy in (x1, y1, x2, y2, y3, x3):
        copy.wait_send()
    for copy in rest + also_remote + kept + also_stores:
        copy.wait()


def gather8_product_kernel(
    rows,
    own_ref,
    acts_ref,
    weight_ref,
    out_ref,
    kept_ref,
    to_y_ref,
    to_x_ref,
    send_sem,
    recv_sem,
    local_sem,
    acts,
    weight,
    far,
    core_in,
    core_send,
    core_recv,
    load_sem,
):
    x_peer, y_peer, c_peer = neighbours()
    width = weight.shape[0]
    wide = 2 * rows
    loads = [
        pltpu.make_async_copy(weight_ref, weight, load_sem.at[0]),
        pltpu.make_async_copy(acts_ref, acts, load_sem.at[1]),
    ]
    for copy in loads:
        copy.start()
    greet((x_peer, y_peer, c_peer))

    def slot(away_t, half, outer, inner):
        return out_ref.at[pl.ds((away_t * 8 + half * 4 + outer * 2 + inner) * rows, rows)]

    number = iter(range(14))

    def send(source, target, peer):
        index = next(number)
        copy = pltpu.make_async_remote_copy(
            src_ref=source,
            dst_ref=target,
            send_sem=send_sem.at[index],
            recv_sem=recv_sem.at[index],
            device_id=peer,
            device_id_type=MESH,
        )
        copy.start()
        return copy

    core_copies = []

    def far_chunk(index):
        place = pl.ds(index * wide, wide)
        source = pl.ds(4 * wide + index * wide, wide)

        def step(cols):
            far[place, cols] = mm(acts[source, :], weight[cols, :], 1, 1).astype(BF16)
            return 0

        tiled(width, width // 2, step)
        copy = pltpu.make_async_remote_copy(
            src_ref=far.at[place],
            dst_ref=core_in.at[place],
            send_sem=core_send.at[index],
            recv_sem=core_recv.at[index],
            device_id=c_peer,
            device_id_type=MESH,
        )
        copy.start()
        core_copies.append(copy)

    def near_chunk(index, target_ref, start):
        core_copies[index].wait_recv()
        place = pl.ds(index * wide, wide)
        target = pl.ds(start, wide)

        def step(cols):
            value = mm(acts[place, :], weight[cols, :], 1, 1) + core_in[place, cols].astype(F32)
            target_ref[target, cols] = value.astype(target_ref.dtype)
            return 0

        tiled(width, width // 2, step)

    first, second = own_ref.at[pl.ds(0, rows)], own_ref.at[pl.ds(rows, rows)]
    x1 = send(first, slot(0, 0, 0, 1), x_peer)
    y1 = send(second, slot(0, 1, 0, 1), y_peer)
    x2 = send(second, slot(0, 1, 1, 0), x_peer)
    y2 = send(first, slot(0, 0, 1, 0), y_peer)
    rest = [send(first, slot(1, 0, 0, 0), c_peer), send(second, slot(1, 1, 0, 0), c_peer)]
    kept = [
        pltpu.make_async_copy(first, slot(0, 0, 0, 0), local_sem.at[0]),
        pltpu.make_async_copy(second, slot(0, 1, 0, 0), local_sem.at[1]),
    ]
    for copy in kept:
        copy.start()
    for copy in loads:
        copy.wait()
    for index in range(4):
        far_chunk(index)
    x1.wait_recv()
    y3 = send(slot(0, 0, 0, 1), slot(0, 0, 1, 1), y_peer)
    y1.wait_recv()
    x3 = send(slot(0, 1, 0, 1), slot(0, 1, 1, 1), x_peer)
    rest.append(send(slot(0, 0, 0, 1), slot(1, 0, 0, 1), c_peer))
    rest.append(send(slot(0, 1, 0, 1), slot(1, 1, 0, 1), c_peer))
    near_chunk(0, kept_ref, 0)
    near_chunk(1, to_y_ref, 0)
    near_chunk(2, kept_ref, wide)
    near_chunk(3, to_x_ref, 0)
    x2.wait_recv()
    rest.append(send(slot(0, 1, 1, 0), slot(1, 1, 1, 0), c_peer))
    y2.wait_recv()
    rest.append(send(slot(0, 0, 1, 0), slot(1, 0, 1, 0), c_peer))
    y3.wait_recv()
    rest.append(send(slot(0, 0, 1, 1), slot(1, 0, 1, 1), c_peer))
    x3.wait_recv()
    rest.append(send(slot(0, 1, 1, 1), slot(1, 1, 1, 1), c_peer))
    for copy in (x1, y1, x2, y2, y3, x3):
        copy.wait_send()
    for copy in core_copies:
        copy.wait_send()
    for copy in rest + kept:
        copy.wait()


def gather8_product(own, acts, weight):
    rows, width = own.shape[0] // 2, own.shape[1]
    hbm = pl.BlockSpec(memory_space=pl.ANY)
    vmem = pl.BlockSpec(memory_space=pltpu.VMEM)
    return pl.pallas_call(
        functools.partial(gather8_product_kernel, rows),
        out_shape=[
            jax.ShapeDtypeStruct((16 * rows, width), own.dtype),
            jax.ShapeDtypeStruct((4 * rows, width), F32),
            jax.ShapeDtypeStruct((2 * rows, width), BF16),
            jax.ShapeDtypeStruct((2 * rows, width), BF16),
        ],
        in_specs=[vmem, hbm, hbm],
        out_specs=[hbm, vmem, vmem, vmem],
        scratch_shapes=[
            pltpu.SemaphoreType.DMA((14,)),
            pltpu.SemaphoreType.DMA((14,)),
            pltpu.SemaphoreType.DMA((2,)),
            pltpu.VMEM(acts.shape, BF16),
            pltpu.VMEM(weight.shape, BF16),
            pltpu.VMEM((8 * rows, width), BF16),
            pltpu.VMEM((8 * rows, width), BF16),
            pltpu.SemaphoreType.DMA((4,)),
            pltpu.SemaphoreType.DMA((4,)),
            pltpu.SemaphoreType.DMA((2,)),
        ],
        compiler_params=remote_params(9, 48 * 1024 * 1024),
        cost_estimate=pl.CostEstimate(
            flops=2 * acts.size * width, bytes_accessed=16 * own.size, transcendentals=0
        ),
        name="gather8_product",
    )(own, acts, weight)


def gather8(own, also=()):
    rows, width = own.shape[0] // 2, own.shape[1]
    hbm = pl.BlockSpec(memory_space=pl.ANY)
    whole_shape = jax.ShapeDtypeStruct((16 * rows, width), own.dtype)
    sems = [
        pltpu.SemaphoreType.DMA((14,)),
        pltpu.SemaphoreType.DMA((14,)),
        pltpu.SemaphoreType.DMA((2,)),
    ]
    if also:
        sems += [pltpu.VMEM((8, rows, width), own.dtype)] + [pltpu.SemaphoreType.DMA((8,))] * 4
    outs = pl.pallas_call(
        functools.partial(gather8_kernel, rows, bool(also)),
        out_shape=[whole_shape] * (2 if also else 1),
        in_specs=[pl.BlockSpec(memory_space=pltpu.VMEM)] + [hbm] * len(also),
        out_specs=[hbm] * (2 if also else 1),
        scratch_shapes=sems,
        compiler_params=remote_params(6 if also else 1),
        name="gather8_also" if also else "gather8",
    )(own, *also)
    return outs if also else outs[0]


def reduce8_kernel(
    rows,
    near_ref,
    far_ref,
    out_ref,
    near,
    core_in,
    link_in,
    link_out,
    send_sem,
    recv_sem,
    local_sem,
):
    x_peer, y_peer, c_peer = neighbours()
    greet((x_peer, y_peer, c_peer))
    order = [(h, o, i) for o, i in ((1, 1), (1, 0), (0, 1), (0, 0)) for h in (0, 1)]
    core_copies, local_copies = {}, {}
    for number, (half, outer, inner) in enumerate(order):
        place = pl.ds((half * 4 + outer * 2 + inner) * rows, rows)
        core_copies[half, outer, inner] = pltpu.make_async_remote_copy(
            src_ref=far_ref.at[place],
            dst_ref=core_in.at[place],
            send_sem=send_sem.at[number],
            recv_sem=recv_sem.at[number],
            device_id=c_peer,
            device_id_type=MESH,
        )
        local_copies[half, outer, inner] = pltpu.make_async_copy(
            near_ref.at[place], near.at[place], local_sem.at[number]
        )
    for block in order:
        core_copies[block].start()
        local_copies[block].start()

    def partial_sum(block):
        half, outer, inner = block
        place = pl.ds((half * 4 + outer * 2 + inner) * rows, rows)
        core_copies[block].wait_recv()
        local_copies[block].wait()
        return near[place, :] + core_in[place, :].astype(F32)

    def link(index, value, peer):
        link_out[index] = value.astype(BF16)
        copy = pltpu.make_async_remote_copy(
            src_ref=link_out.at[index],
            dst_ref=link_in.at[index],
            send_sem=send_sem.at[8 + index],
            recv_sem=recv_sem.at[8 + index],
            device_id=peer,
            device_id_type=MESH,
        )
        copy.start()
        return copy

    y11 = link(0, partial_sum((0, 1, 1)), y_peer)
    x11 = link(1, partial_sum((1, 1, 1)), x_peer)
    y10 = link(2, partial_sum((0, 1, 0)), y_peer)
    x10 = link(3, partial_sum((1, 1, 0)), x_peer)
    first01, second01 = partial_sum((0, 0, 1)), partial_sum((1, 0, 1))
    y11.wait_recv()
    x01 = link(4, first01 + link_in[0].astype(F32), x_peer)
    x11.wait_recv()
    y01 = link(5, second01 + link_in[1].astype(F32), y_peer)
    first = partial_sum((0, 0, 0))
    second = partial_sum((1, 0, 0))
    y10.wait_recv()
    out_ref[pl.ds(0, rows), :] = first + link_in[2].astype(F32)
    x10.wait_recv()
    out_ref[pl.ds(rows, rows), :] = second + link_in[3].astype(F32)
    x01.wait_recv()
    out_ref[pl.ds(0, rows), :] += link_in[4].astype(F32)
    y01.wait_recv()
    out_ref[pl.ds(rows, rows), :] += link_in[5].astype(F32)
    for copy in (y11, x11, y10, x10, x01, y01):
        copy.wait_send()
    for copy in core_copies.values():
        copy.wait_send()


def reduce8(near, far):
    rows, width = near.shape[0] // 8, near.shape[1]
    return pl.pallas_call(
        functools.partial(reduce8_kernel, rows),
        out_shape=jax.ShapeDtypeStruct((2 * rows, width), F32),
        in_specs=[pl.BlockSpec(memory_space=pl.ANY), pl.BlockSpec(memory_space=pl.ANY)],
        out_specs=pl.BlockSpec(memory_space=pltpu.VMEM),
        scratch_shapes=[
            pltpu.VMEM(near.shape, F32),
            pltpu.VMEM(near.shape, BF16),
            pltpu.VMEM((6, rows, width), BF16),
            pltpu.VMEM((6, rows, width), BF16),
            pltpu.SemaphoreType.DMA((14,)),
            pltpu.SemaphoreType.DMA((14,)),
            pltpu.SemaphoreType.DMA((8,)),
        ],
        compiler_params=remote_params(2, 48 * 1024 * 1024),
        name="reduce8",
    )(near, far)


def tiled(count, tile, step):
    lax.fori_loop(0, count // tile, lambda i, _: step(pl.ds(pl.multiple_of(i * tile, tile), tile)), 0)


def product_reduce8_kernel(rows, groups, filler, *refs):
    acts_refs, refs = refs[:groups], refs[groups:]
    if filler:
        weight_ref, lhs_ref, out_ref, grad_ref, *refs = refs
    else:
        weight_ref, out_ref, *refs = refs
    acts, weight, far, near, core_in, link_in, link_out, send_sem, recv_sem, load_sem, *refs = refs
    x_peer, y_peer, c_peer = neighbours()
    width = weight.shape[0]
    wide = 2 * rows
    chunks = [(0, 1), (1, 1), (0, 0), (1, 0)]

    def where(chunk):
        return chunk[0] * 2 * wide + chunk[1] * wide

    half = width // 2
    load_weights = [
        pltpu.make_async_copy(
            weight_ref.at[pl.ds(part * half, half), pl.ds(0, weight.shape[1])],
            weight.at[pl.ds(part * half, half)],
            load_sem.at[part],
        )
        for part in (0, 1)
    ]
    loads = {}
    depth = weight.shape[1] // groups
    for number, chunk in enumerate(chunks):
        for side in (1, 0):
            place = pl.ds(side * 4 * wide + where(chunk), wide)
            loads[side, chunk] = [
                pltpu.make_async_copy(
                    acts_refs[group].at[place],
                    acts.at[place, pl.ds(group * depth, depth)],
                    load_sem.at[3 + (2 * number + side) * groups + group],
                )
                for group in range(groups)
            ]
    started = [loads[1, chunks[0]], [load_weights[0]], loads[1, chunks[1]], loads[0, chunks[0]]]
    started += [loads[0, chunks[1]], [load_weights[1]]]
    started += [loads[side, chunk] for chunk in chunks[2:] for side in (1, 0)]
    for group in started:
        for copy in group:
            copy.start()
    if filler:
        lhs, grad, grad_sem = refs
        load_lhs = pltpu.make_async_copy(lhs_ref, lhs, load_sem.at[2])
        load_lhs.start()
    greet((x_peer, y_peer, c_peer))

    core_copies, link_copies = {}, {}

    def product(chunk, side, part, target):
        place = pl.ds(where(chunk), wide)
        source = pl.ds(side * 4 * wide + where(chunk), wide)

        cols = pl.ds(part * half, half)
        target[place, cols] = mm(acts[source, :], weight[cols, :], 1, 1).astype(target.dtype)

    def remote(copies, key, number, source, target, peer):
        copies[key] = pltpu.make_async_remote_copy(
            src_ref=source,
            dst_ref=target,
            send_sem=send_sem.at[number],
            recv_sem=recv_sem.at[number],
            device_id=peer,
            device_id_type=MESH,
        )
        copies[key].start()

    def send_core(chunk, part):
        product(chunk, 1, part, far)
        here = (pl.ds(where(chunk), wide), pl.ds(part * half, half))
        number = 2 * chunks.index(chunk) + part
        remote(core_copies, (chunk, part), number, far.at[here], core_in.at[here], c_peer)

    def partial_sum(chunk, start, size, part):
        here = (pl.ds(where(chunk) + start, size), pl.ds(part * half, half))
        return near[here] + core_in[here].astype(F32)

    def link(hop, side, part, value, peer):
        size = value.shape[0]
        start = (side * 3 + hop * 2) * rows
        here = (pl.ds(start, size), pl.ds(part * half, half))
        link_out[here] = value.astype(BF16)
        number = 8 + hop * 4 + side * 2 + part
        remote(link_copies, (hop, side, part), number, link_out.at[here], link_in.at[here], peer)

    def came(hop, side, start, part):
        return link_in[
            pl.ds((side * 3 + hop * 2) * rows + start, rows), pl.ds(part * half, half)
        ].astype(F32)

    for chunk in chunks[:2]:
        for copy in loads[1, chunk]:
            copy.wait()
    for part in (0, 1):
        load_weights[part].wait()
        send_core((0, 1), part)
        send_core((1, 1), part)
        for side, peer in ((0, y_peer), (1, x_peer)):
            if part == 0:
                for copy in loads[0, (side, 1)]:
                    copy.wait()
            product((side, 1), 0, part, near)
            core_copies[(side, 1), part].wait_recv()
            link(0, side, part, partial_sum((side, 1), 0, wide, part), peer)
    for chunk in chunks[2:]:
        for side in (1, 0):
            for copy in loads[side, chunk]:
                copy.wait()
    for part in (0, 1):
        for chunk in chunks[2:]:
            send_core(chunk, part)
        for chunk in chunks[2:]:
            product(chunk, 0, part, near)
        for side, peer in ((0, x_peer), (1, y_peer)):
            core_copies[(side, 0), part].wait_recv()
            link_copies[0, side, part].wait_recv()
            link(1, side, part, partial_sum((side, 0), rows, rows, part) + came(0, side, rows, part), peer)
    if filler:
        load_lhs.wait()
        size = width // 4

        def fill(index, _):
            cols = pl.ds(pl.multiple_of(index * size, size), size)

            def step(columns):
                grad[cols, columns] = mm(lhs[:, cols], acts[:, columns], 0, 0).astype(BF16)
                return 0

            tiled(acts.shape[1], acts.shape[1] // 3, step)
            return 0

        lax.fori_loop(0, 4, fill, 0)
        grad_copy = pltpu.make_async_copy(grad, grad_ref, grad_sem.at[0])
        grad_copy.start()
    for side in (0, 1):
        for part in (0, 1):
            place = (pl.ds(side * rows, rows), pl.ds(part * half, half))
            kept = partial_sum((side, 0), 0, rows, part) + came(0, side, 0, part)
            link_copies[1, side, part].wait_recv()
            out_ref[place] = kept + came(1, side, 0, part)
    for copy in list(link_copies.values()) + list(core_copies.values()):
        copy.wait_send()
    if filler:
        grad_copy.wait()


def product_reduce8(columns, weight, number, lhs=None):
    depth, groups = sum(column.shape[1] for column in columns), len(columns)
    acts = jax.ShapeDtypeStruct((columns[0].shape[0], depth), BF16)
    rows, width = acts.shape[0] // 16, weight.shape[0]
    filler = lhs is not None
    hbm = pl.BlockSpec(memory_space=pl.ANY)
    scratch = [
        pltpu.VMEM(acts.shape, BF16),
        pltpu.VMEM((width, depth), BF16),
        pltpu.VMEM((8 * rows, width), BF16),
        pltpu.VMEM((8 * rows, width), F32),
        pltpu.VMEM((8 * rows, width), BF16),
        pltpu.VMEM((6 * rows, width), BF16),
        pltpu.VMEM((6 * rows, width), BF16),
        pltpu.SemaphoreType.DMA((16,)),
        pltpu.SemaphoreType.DMA((16,)),
        pltpu.SemaphoreType.DMA((3 + 8 * groups,)),
    ]
    out_shape = [jax.ShapeDtypeStruct((2 * rows, width), F32)]
    out_specs = [pl.BlockSpec(memory_space=pltpu.VMEM)]
    flops = 2 * acts.shape[0] * width * depth
    if filler:
        scratch += [
            pltpu.VMEM(lhs.shape, BF16),
            pltpu.VMEM((width, depth), BF16),
            pltpu.SemaphoreType.DMA((1,)),
        ]
        out_shape.append(jax.ShapeDtypeStruct((width, depth), BF16))
        out_specs.append(hbm)
        flops *= 2
    outs = pl.pallas_call(
        functools.partial(product_reduce8_kernel, rows, groups, filler),
        out_shape=out_shape,
        in_specs=[hbm] * (groups + (2 if filler else 1)),
        out_specs=out_specs,
        scratch_shapes=scratch,
        compiler_params=remote_params(number, 63 * 1024 * 1024),
        cost_estimate=pl.CostEstimate(
            flops=flops, bytes_accessed=4 * depth * (acts.shape[0] + width), transcendentals=0
        ),
        name="product_reduce8",
    )(*columns, weight, *((lhs,) if filler else ()))
    return outs if filler else outs[0]


def shard_kernel(plan, outs, *refs):
    ins, out_refs = refs[: len(plan)], refs[len(plan) : len(plan) + outs]
    stage = refs[len(plan) + outs : 2 * len(plan) + outs]
    send_sem, recv_sem, load_sem, store_sem = refs[2 * len(plan) + outs :]
    x_peer, _, _ = neighbours()
    odd = lax.rem(lax.axis_index("fsdp"), 2)
    column = 2 * lax.axis_index("ctx") + odd
    other = 2 * lax.axis_index("ctx") + 1 - odd
    greet((x_peer,))
    remote, loads, stores = [], [], []
    for number, (which, start, size, cut) in enumerate(plan):
        rows = ins[number].shape[0]
        place = pl.ds(pl.multiple_of(odd * rows, rows), rows)
        target = out_refs[which].at[place, pl.ds(start, size)]

        def source(index, ref=ins[number], size=size, cut=cut):
            if not cut:
                return ref
            return ref.at[:, pl.ds(pl.multiple_of(index * size, HEAD), size)]

        remote.append(
            pltpu.make_async_remote_copy(
                src_ref=source(other),
                dst_ref=target,
                send_sem=send_sem.at[number],
                recv_sem=recv_sem.at[number],
                device_id=x_peer,
                device_id_type=MESH,
            )
        )
        loads.append(pltpu.make_async_copy(source(column), stage[number], load_sem.at[number]))
        stores.append(pltpu.make_async_copy(stage[number], target, store_sem.at[number]))
    for copy in remote:
        copy.start()
    for copy in loads:
        copy.start()
    for load, store in zip(loads, stores):
        load.wait()
        store.start()
    for copy in stores:
        copy.wait()
    for copy in remote:
        copy.wait()


def shards(groups, number):
    plan, arrays, shapes = [], [], []
    for which, group in enumerate(groups):
        start = 0
        for array, cut in group:
            size = array.shape[1] // 4 if cut else array.shape[1]
            plan.append((which, start, size, cut))
            arrays.append(array)
            start += size
        shapes.append((2 * group[0][0].shape[0], start))
    hbm = pl.BlockSpec(memory_space=pl.ANY)
    return pl.pallas_call(
        functools.partial(shard_kernel, tuple(plan), len(groups)),
        out_shape=[jax.ShapeDtypeStruct(shape, BF16) for shape in shapes],
        in_specs=[hbm] * len(arrays),
        out_specs=[hbm] * len(groups),
        scratch_shapes=[
            pltpu.VMEM((array.shape[0], size), BF16)
            for array, (_, _, size, _) in zip(arrays, plan)
        ]
        + [pltpu.SemaphoreType.DMA((len(plan),))] * 4,
        compiler_params=remote_params(number),
        name="shards",
    )(*arrays)


def total_kernel(stages, part_ref, out_ref, inbox, outbox, send_sem, recv_sem):
    peers = []
    for axis, bit in stages:
        mine = lax.axis_index(axis)
        peers.append({axis: mine + bit * (1 - 2 * lax.rem(mine // bit, 2))})
    greet(peers)
    value = part_ref[...]
    copies = []
    for index, peer in enumerate(peers):
        outbox[index] = value
        copy = pltpu.make_async_remote_copy(
            src_ref=outbox.at[index],
            dst_ref=inbox.at[index],
            send_sem=send_sem.at[index],
            recv_sem=recv_sem.at[index],
            device_id=peer,
            device_id_type=MESH,
        )
        copy.start()
        copies.append(copy)
        copy.wait_recv()
        value = value + inbox[index]
    out_ref[...] = value
    for copy in copies:
        copy.wait_send()


def total(part):
    stages, bit = [], 2
    while bit < lax.axis_size("fsdp"):
        stages.append(("fsdp", bit))
        bit *= 2
    stages += [("tp", 1), ("fsdp", 1)]
    return pl.pallas_call(
        functools.partial(total_kernel, tuple(stages)),
        out_shape=jax.ShapeDtypeStruct(part.shape, F32),
        in_specs=[pl.BlockSpec(memory_space=pltpu.VMEM)],
        out_specs=pl.BlockSpec(memory_space=pltpu.VMEM),
        scratch_shapes=[
            pltpu.VMEM((len(stages),) + part.shape, F32),
            pltpu.VMEM((len(stages),) + part.shape, F32),
            pltpu.SemaphoreType.DMA((len(stages),)),
            pltpu.SemaphoreType.DMA((len(stages),)),
        ],
        compiler_params=remote_params(5),
        name="total",
    )(part)


def join_kernel(sizes, spot_ref, kept_ref, x_ref, y_ref, both_ref, *out_refs):
    place, odd = spot_ref[0], spot_ref[1]
    parts = (
        (kept_ref, 2 * place + odd),
        (x_ref, 2 * place + 1 - odd),
        (y_ref, 2 - 2 * place + odd),
        (both_ref, 3 - 2 * place - odd),
    )
    for part, column in parts:
        start = 0
        for size, out_ref in zip(sizes, out_refs):
            target = pl.ds(pl.multiple_of(column * size, HEAD), size)
            out_ref[:, target] = part[:, start : start + size].astype(F32)
            start += size


def join_columns(spot, parts, sizes):
    rows = parts[0].shape[0]
    tile = min(rows, 64)
    return pl.pallas_call(
        functools.partial(join_kernel, sizes),
        out_shape=[jax.ShapeDtypeStruct((rows, 4 * size), F32) for size in sizes],
        grid_spec=pltpu.PrefetchScalarGridSpec(
            num_scalar_prefetch=1,
            grid=(rows // tile,),
            in_specs=[
                pl.BlockSpec((tile, part.shape[1]), lambda i, spot: (i, 0)) for part in parts
            ],
            out_specs=[pl.BlockSpec((tile, 4 * size), lambda i, spot: (i, 0)) for size in sizes],
        ),
        name="join",
    )(spot, *parts)


def after(value, *others):
    return lax.optimization_barrier((value,) + others)[0]


def reduce4_links(kept, to_y, to_x, *others):
    rows = kept.shape[0] // 4
    came_first, came_second = swap_ctx(to_y), swap_x(to_x)
    first = kept[: 2 * rows] + after(came_first, *others).astype(F32)
    second = kept[2 * rows :] + after(came_second, *others).astype(F32)
    came_first = swap_x(first[rows:].astype(BF16))
    came_second = swap_ctx(second[rows:].astype(BF16))
    return first[:rows], second[:rows], came_first, came_second


def rope_tables(positions):
    freqs = THETA ** (-(jnp.arange(HEAD // 2, dtype=F32) * 2.0) / HEAD)
    angle = positions[:, None] * freqs[None, :]
    cosine = jnp.concatenate([jnp.cos(angle), jnp.cos(angle)], axis=-1)
    sine = jnp.concatenate([-jnp.sin(angle), jnp.sin(angle)], axis=-1)
    return cosine, sine


def norm_back(grad, scaled, inverse, gain):
    weighted = grad * gain
    return inverse * (weighted - scaled * jnp.mean(weighted * scaled, axis=-1, keepdims=True))


def inv_rms(value):
    return lax.rsqrt(jnp.mean(value * value, axis=-1, keepdims=True) + EPS)


def block_row(meta_ref, seq, index, rows):
    away_c = lax.rem(meta_ref[0] + index // 4, 2)
    away_t = lax.rem(meta_ref[1] + (index // 2) % 2, 2)
    if index % 2 == 0:
        inner = away_c * 2 + seq
    else:
        inner = seq * 2 + away_c + 4
    return pl.multiple_of((away_t * 8 + inner) * rows, rows)


def scaled_of(raw):
    inverse = lax.rsqrt(jnp.mean(raw * raw, axis=-1, keepdims=True) + EPS)
    return raw * inverse, inverse


def load_heads(meta_ref, qkv_ref, cos_ref, sin_ref, gain_ref, q_scr, k_scr, v_scr, heads):
    seq = pl.program_id(0)
    rows = q_scr.shape[1] // 8
    for index in range(8):
        start = block_row(meta_ref, seq, index, rows)
        here = slice(index * rows, (index + 1) * rows)
        cosine, sine = cos_ref[here, :], sin_ref[here, :]
        for head in range(heads + 1):
            raw = qkv_ref[pl.ds(start, rows), head * HEAD : (head + 1) * HEAD]
            scaled, _ = scaled_of(raw)
            which = 0 if head < heads else 1
            value = scaled * gain_ref[which : which + 1, :]
            turned = value * cosine + pltpu.roll(value, HEAD // 2, 1) * sine
            if head < heads:
                q_scr[head, here, :] = turned.astype(BF16)
            else:
                k_scr[here, :] = turned.astype(BF16)
        v_scr[here, :] = qkv_ref[
            pl.ds(start, rows), (heads + 1) * HEAD : (heads + 2) * HEAD
        ].astype(BF16)


def key_span(index, tile):
    low = max(0, (index * tile - (MOST_DOC - 1)) // tile) * tile
    return low, (index + 1) * tile


def allowed_mask(segc_ref, segr_ref, index, tile):
    low, high = key_span(index, tile)
    shape = (tile, high - low)
    rows = lax.broadcasted_iota(jnp.int32, shape, 0) + index * tile
    cols = lax.broadcasted_iota(jnp.int32, shape, 1) + low
    same = segc_ref[0, index * tile : (index + 1) * tile, :] == segr_ref[0, :, low:high]
    return same & (cols <= rows)


def probs_of(query, keys, allowed, scale):
    scores = jnp.where(allowed, mm(query, keys, 1, 1) * scale, MASKED)
    weights = jnp.exp(scores - jnp.max(scores, axis=-1, keepdims=True))
    return weights * (1.0 / jnp.sum(weights, axis=-1, keepdims=True))


def attend_kernel(
    heads, tile, meta_ref, qkv_ref, segc_ref, segr_ref, cos_ref, sin_ref, gain_ref, out_ref, q_scr, k_scr, v_scr
):
    seq = pl.program_id(0)
    length = k_scr.shape[0]
    rows = length // 8
    scale = 1.0 / math.sqrt(HEAD)
    load_heads(meta_ref, qkv_ref, cos_ref, sin_ref, gain_ref, q_scr, k_scr, v_scr, heads)
    for index in range(length // tile):
        low, high = key_span(index, tile)
        allowed = allowed_mask(segc_ref, segr_ref, index, tile)
        for head in range(heads):
            query = q_scr[head, index * tile : (index + 1) * tile, :]
            probs = probs_of(query, k_scr[low:high, :], allowed, scale)
            mixed = mm(probs.astype(BF16), v_scr[low:high, :], 1, 0).astype(BF16)
            for piece in range(tile // rows):
                start = block_row(meta_ref, seq, index * (tile // rows) + piece, rows)
                out_ref[pl.ds(start, rows), head * HEAD : (head + 1) * HEAD] = mixed[
                    piece * rows : (piece + 1) * rows
                ]


def attend_back_kernel(
    heads,
    tile,
    meta_ref,
    qkv_ref,
    grad_ref,
    segc_ref,
    segr_ref,
    cos_ref,
    sin_ref,
    gain_ref,
    out_ref,
    gain_out_ref,
    q_scr,
    k_scr,
    v_scr,
    g_scr,
    dk_scr,
    dv_scr,
):
    seq = pl.program_id(0)
    length = k_scr.shape[0]
    rows = length // 8
    scale = 1.0 / math.sqrt(HEAD)
    load_heads(meta_ref, qkv_ref, cos_ref, sin_ref, gain_ref, q_scr, k_scr, v_scr, heads)
    for index in range(8):
        start = block_row(meta_ref, seq, index, rows)
        g_scr[index * rows : (index + 1) * rows, :] = grad_ref[pl.ds(start, rows), :]
    dk_scr[...] = jnp.zeros_like(dk_scr)
    dv_scr[...] = jnp.zeros_like(dv_scr)

    @pl.when(seq == 0)
    def _():
        gain_out_ref[...] = jnp.zeros_like(gain_out_ref)

    def finish(grad, index, head, which):
        here = slice(index * rows, (index + 1) * rows)
        start = block_row(meta_ref, seq, index, rows)
        grad = grad * cos_ref[here, :] - pltpu.roll(grad, HEAD // 2, 1) * sin_ref[here, :]
        raw = qkv_ref[pl.ds(start, rows), head * HEAD : (head + 1) * HEAD]
        scaled, inverse = scaled_of(raw)
        gain_out_ref[which : which + 1, :] += jnp.sum(grad * scaled, axis=0, keepdims=True)
        out = norm_back(grad, scaled, inverse, gain_ref[which : which + 1, :])
        out_ref[pl.ds(start, rows), head * HEAD : (head + 1) * HEAD] = out.astype(BF16)

    per = tile // rows
    for index in range(length // tile):
        low, high = key_span(index, tile)
        mine = slice(index * tile, (index + 1) * tile)
        allowed = allowed_mask(segc_ref, segr_ref, index, tile)
        for head in range(heads):
            query = q_scr[head, mine, :]
            keys = k_scr[low:high, :]
            probs = probs_of(query, keys, allowed, scale)
            grad = g_scr[mine, head * HEAD : (head + 1) * HEAD]
            grad_probs = mm(grad, v_scr[low:high, :], 1, 1)
            delta = jnp.sum(probs * grad_probs, axis=-1, keepdims=True)
            grad_scores = (probs * (grad_probs - delta)).astype(BF16)
            dv_scr[low:high, :] += mm(probs.astype(BF16), grad, 0, 0)
            dk_scr[low:high, :] += mm(grad_scores, query, 0, 0) * scale
            grad_query = mm(grad_scores, keys, 1, 0) * scale
            for piece in range(per):
                finish(
                    grad_query[piece * rows : (piece + 1) * rows], index * per + piece, head, 0
                )
    for index in range(8):
        here = slice(index * rows, (index + 1) * rows)
        start = block_row(meta_ref, seq, index, rows)
        finish(dk_scr[here, :], index, heads, 1)
        out_ref[pl.ds(start, rows), (heads + 1) * HEAD : (heads + 2) * HEAD] = dv_scr[
            here, :
        ].astype(BF16)


def whole(shape):
    return pl.BlockSpec(shape, lambda seq, meta: (0,) * len(shape))


def seg_specs(length):
    return [
        pl.BlockSpec((1, length, 1), lambda seq, meta: (seq, 0, 0)),
        pl.BlockSpec((1, 1, length), lambda seq, meta: (seq, 0, 0)),
    ]


def attend(meta, qkv, seg_cols, seg_rows, cosine, sine, gains):
    length = cosine.shape[0]
    tile = length // 4
    heads = qkv.shape[1] // HEAD - 2
    pairs = 2 * heads * length * length // 2
    return pl.pallas_call(
        functools.partial(attend_kernel, heads, tile),
        out_shape=jax.ShapeDtypeStruct((qkv.shape[0], heads * HEAD), BF16),
        grid_spec=pltpu.PrefetchScalarGridSpec(
            num_scalar_prefetch=1,
            grid=(2,),
            in_specs=[whole(qkv.shape)]
            + seg_specs(length)
            + [whole(cosine.shape), whole(sine.shape), whole(gains.shape)],
            out_specs=whole((qkv.shape[0], heads * HEAD)),
            scratch_shapes=[
                pltpu.VMEM((heads, length, HEAD), BF16),
                pltpu.VMEM((length, HEAD), BF16),
                pltpu.VMEM((length, HEAD), BF16),
            ],
        ),
        cost_estimate=pl.CostEstimate(
            flops=4 * pairs * HEAD, bytes_accessed=qkv.size * 4 + qkv.size, transcendentals=pairs
        ),
        name="attend",
    )(meta, qkv, seg_cols, seg_rows, cosine, sine, gains)


def attend_back(meta, qkv, grad, seg_cols, seg_rows, cosine, sine, gains):
    length = cosine.shape[0]
    tile = length // 4
    heads = qkv.shape[1] // HEAD - 2
    pairs = 2 * heads * length * length // 2
    return pl.pallas_call(
        functools.partial(attend_back_kernel, heads, tile),
        out_shape=(
            jax.ShapeDtypeStruct(qkv.shape, BF16),
            jax.ShapeDtypeStruct(gains.shape, F32),
        ),
        grid_spec=pltpu.PrefetchScalarGridSpec(
            num_scalar_prefetch=1,
            grid=(2,),
            in_specs=[whole(qkv.shape), whole(grad.shape)]
            + seg_specs(length)
            + [whole(cosine.shape), whole(sine.shape), whole(gains.shape)],
            out_specs=(whole(qkv.shape), whole(gains.shape)),
            scratch_shapes=[
                pltpu.VMEM((heads, length, HEAD), BF16),
                pltpu.VMEM((length, HEAD), BF16),
                pltpu.VMEM((length, HEAD), BF16),
                pltpu.VMEM((length, heads * HEAD), BF16),
                pltpu.VMEM((length, HEAD), F32),
                pltpu.VMEM((length, HEAD), F32),
            ],
        ),
        cost_estimate=pl.CostEstimate(
            flops=10 * pairs * HEAD, bytes_accessed=qkv.size * 8, transcendentals=pairs
        ),
        name="attend_back",
    )(meta, qkv, grad, seg_cols, seg_rows, cosine, sine, gains)


def body(
    tokens,
    segment_ids,
    norm_gain,
    query_weight,
    key_matrix,
    value_matrix,
    output_weight,
    query_gain,
    key_gain,
    mlp_gain,
    gate_weight,
    up_weight,
    down_weight,
    cotangent,
):
    local, width = tokens.shape[1], tokens.shape[2]
    length = 2 * local
    quarter = local // 2
    count = lax.axis_size("fsdp")
    block = width // count
    mine = lax.axis_index("fsdp")
    odd = mine % 2
    place = lax.axis_index("ctx")
    core = lax.axis_index("tp")

    small = query_gain.shape[0]
    lanes = jnp.arange(HEAD)[None, :]

    def pad_rows(vector):
        return jnp.concatenate([vector, jnp.zeros((block - small,), BF16)])

    gains = jnp.where(
        lanes == 0,
        norm_gain[:, None],
        jnp.where(
            lanes == 1,
            mlp_gain[:, None],
            jnp.where(
                lanes == 2, pad_rows(query_gain)[:, None], pad_rows(key_gain)[:, None]
            ),
        ),
    )
    far_segments = swap_x(segment_ids)
    (first_pair,) = shards(
        [
            [
                (query_weight, True),
                (key_matrix, True),
                (value_matrix, True),
                (output_weight, True),
                (gains, False),
            ]
        ],
        3,
    )
    first = gather_line(first_pair)
    gate_up_pair, down_pair = shards(
        [
            [(after(gate_weight, first_pair), True), (up_weight, True)],
            [(down_weight, True)],
        ],
        4,
    )
    gate_up_w = gather_line(gate_up_pair)
    down_w = gather_line(down_pair)

    def own_quarter(value):
        return lax.dynamic_slice_in_dim(value.reshape(local, width), core * quarter, quarter, 0)

    own_tok, own_cot = own_quarter(tokens), own_quarter(cotangent)
    tok = gather8(after(own_tok, gate_up_pair))
    segments = jnp.concatenate([segment_ids, far_segments])
    seg_cols, seg_rows = segments[:, :, None], segments[:, None, :]
    cosine, sine = rope_tables(jnp.arange(length).astype(F32))
    meta = jnp.stack([place, core]).astype(jnp.int32)

    heads_q = query_weight.shape[1] // 4 // HEAD
    cols = (heads_q + 2) * HEAD
    qkv_w = first[:, :cols]
    out_w = first[:, cols : cols + heads_q * HEAD]
    gain_cols = first[:, cols + heads_q * HEAD :].astype(F32)
    in_gain, mid_gain = gain_cols[:, 0][None], gain_cols[:, 1][None]
    head_gains = gain_cols.reshape(count, block, HEAD)[:, :small, 2:4].reshape(HEAD, 2).T

    in_f = tok.astype(F32)
    cot_from = after(own_cot, tok)
    cot_x, cot_y = swap_x(cot_from), swap_ctx(cot_from)
    x_all = (in_f * inv_rms(in_f) * in_gain).astype(BF16)
    qkv = mm(x_all, qkv_w, 1, 0)
    attended = attend(meta, qkv, seg_cols, seg_rows, cosine, sine, head_gains)
    half = 4 * quarter
    cot_x, cot_y = after(cot_x, attended), after(cot_y, attended)
    eighth = quarter // 2
    cot_first, cot_second = swap_ctx(cot_x[:eighth]), swap_x(cot_y[eighth:])
    out_far = mm(attended[half:], out_w, 1, 1).astype(BF16)
    out_near = mm(attended[:half], out_w, 1, 1)
    middle = own_tok.astype(F32) + reduce8(out_near, out_far)
    inverse_mid = inv_rms(middle)
    scaled_mid = middle * inverse_mid
    y_own = (scaled_mid * mid_gain).astype(BF16)
    cot_first, cot_second = after(cot_first, y_own), after(cot_second, y_own)
    y_all, cot = gather8(y_own, (cot_from, cot_x, cot_y, cot_first, cot_second))

    ff = gate_up_w.shape[1] // 2
    gate_up = mm(y_all, gate_up_w, 1, 0)
    gate, up_value = gate_up[:, :ff], gate_up[:, ff:]
    sig = jax.nn.sigmoid(gate)
    active = gate * sig
    hidden = (active * up_value).astype(BF16)
    down_grad = mm(cot, hidden, 0, 0).astype(BF16)

    def finish_rows(own):
        pair = jnp.stack([own, swap_core(own)])
        return flip_if(core == 1, pair, 0).reshape(tokens.shape)

    grad_hidden = mm(after(cot, down_grad), down_w, 1, 0)
    grad_up = (grad_hidden * active).astype(BF16)
    grad_gate = (grad_hidden * up_value * (sig * (1.0 + gate * (1.0 - sig)))).astype(BF16)
    mid_grad, gate_up_grad = product_reduce8((grad_gate, grad_up), gate_up_w, 7, y_all)

    mlp_gain_part = jnp.sum(mid_grad * scaled_mid, axis=0)
    grad_middle = own_cot.astype(F32) + norm_back(mid_grad, scaled_mid, inverse_mid, mid_gain)
    grad_attn, mlp_kept, mlp_to_y, mlp_to_x = gather8_product(
        grad_middle.astype(BF16), hidden, down_w
    )
    out_grad = mm(grad_attn, attended, 0, 0).astype(BF16)
    grad_att = mm(grad_attn, out_w, 1, 0).astype(BF16)
    raw_grads, head_gain_parts = attend_back(
        meta, qkv, grad_att, seg_cols, seg_rows, cosine, sine, head_gains
    )
    mlp_first, mlp_second, mlp_came1, mlp_came2 = reduce4_links(
        mlp_kept, mlp_to_y, mlp_to_x, raw_grads
    )
    first_grad = mm(x_all, raw_grads, 0, 0).astype(BF16)
    first_grad = jnp.concatenate([first_grad, out_grad], axis=1)
    mlp_first = mlp_first + after(mlp_came1, first_grad).astype(F32)
    mlp_second = mlp_second + after(mlp_came2, first_grad).astype(F32)
    mlp_sum = (middle + jnp.concatenate([mlp_first, mlp_second])).astype(BF16)
    layer_out = finish_rows(mlp_sum)
    in_grad = product_reduce8((after(raw_grads, first_grad, mlp_sum),), first, 8)

    spot = jnp.stack([place, odd]).astype(jnp.int32)

    def owners(grad, sizes, *others):
        rows = scatter_line(grad)
        rows = after(rows, *others)
        kept = lax.dynamic_slice_in_dim(rows, odd * block, block, 0)
        sent = lax.dynamic_slice_in_dim(rows, (1 - odd) * block, block, 0)
        by_x, by_y = swap_x(sent), swap_ctx(kept)
        by_both = swap_ctx(by_x)
        return join_columns(spot, (kept, by_x, by_y, by_both), sizes)

    (down_share,) = owners(down_grad, (ff,))
    gate_share, up_share = owners(gate_up_grad, (ff, ff))
    query_share, key_share, value_share, out_share = owners(
        first_grad, (heads_q * HEAD, HEAD, HEAD, heads_q * HEAD)
    )

    own_in = own_tok.astype(F32)
    inverse_in = inv_rms(own_in)
    scaled_in = own_in * inverse_in
    norm_gain_part = jnp.sum(in_grad * scaled_in, axis=0)
    own_token_grad = (grad_middle + norm_back(in_grad, scaled_in, inverse_in, in_gain)).astype(BF16)
    token_grad = finish_rows(own_token_grad)

    parts = jnp.concatenate([norm_gain_part, mlp_gain_part, head_gain_parts.reshape(-1)])
    parts = parts.reshape(-1, HEAD)
    far_parts = swap_ctx(parts)
    sums = total(parts + after(far_parts, token_grad)).reshape(-1)
    norm_gain_grad = lax.dynamic_slice_in_dim(sums, mine * block, block, 0)
    mlp_gain_grad = lax.dynamic_slice_in_dim(sums, width + mine * block, block, 0)
    query_gain_grad = lax.dynamic_slice_in_dim(sums, 2 * width + mine * small, small, 0)
    key_gain_grad = lax.dynamic_slice_in_dim(sums, 2 * width + HEAD + mine * small, small, 0)
    return (
        layer_out,
        token_grad,
        norm_gain_grad,
        query_share,
        key_share,
        value_share,
        out_share,
        query_gain_grad,
        key_gain_grad,
        mlp_gain_grad,
        gate_share,
        up_share,
        down_share,
    )


def solution(mesh):
    in_specs = (
        P("fsdp", "ctx", None),
        P("fsdp", None),
        P("fsdp"),
        P("fsdp", "tp"),
        P("fsdp", "tp"),
        P("fsdp", "tp"),
        P("fsdp", "tp"),
        P("fsdp"),
        P("fsdp"),
        P("fsdp"),
        P("fsdp", "tp"),
        P("fsdp", "tp"),
        P("fsdp", "tp"),
        P("fsdp", "ctx", None),
    )
    out_specs = (
        P("fsdp", "ctx", None),
        P("fsdp", "ctx", None),
        P("fsdp"),
        P("fsdp", "tp"),
        P("fsdp", "tp"),
        P("fsdp", "tp"),
        P("fsdp", "tp"),
        P("fsdp"),
        P("fsdp"),
        P("fsdp"),
        P("fsdp", "tp"),
        P("fsdp", "tp"),
        P("fsdp", "tp"),
    )

    return jax.shard_map(body, mesh=mesh, in_specs=in_specs, out_specs=out_specs, check_vma=False)
```

```python
import functools
import math

import jax
import jax.numpy as jnp
from jax import lax
from jax.experimental import pallas as pl
from jax.experimental.pallas import tpu as pltpu
from jax.sharding import PartitionSpec as P


HEAD = 128
EPS = 1e-06
THETA = 1000000.0
MASKED = -1e30
MOST_DOC = 512
MESH = pl.DeviceIdType.MESH
F32 = jnp.float32
BF16 = jnp.bfloat16


def mm(left, right, left_dim, right_dim):
    return lax.dot_general(
        left, right, (((left_dim,), (right_dim,)), ((), ())), preferred_element_type=F32
    )


def swap_core(value):
    return lax.ppermute(value, "tp", [(0, 1), (1, 0)])


def swap_ctx(value):
    return lax.ppermute(value, "ctx", [(0, 1), (1, 0)])


def swap_x(value):
    count = lax.axis_size("fsdp")
    return lax.ppermute(value, "fsdp", [(i, i ^ 1) for i in range(count)])


def lines():
    count = lax.axis_size("fsdp")
    return [[i for i in range(count) if i % 2 == parity] for parity in (0, 1)]


def gather_line(value):
    return lax.all_gather(value, "fsdp", axis=0, tiled=True, axis_index_groups=lines())


def scatter_line(value):
    return lax.psum_scatter(
        value, "fsdp", scatter_dimension=0, tiled=True, axis_index_groups=lines()
    )


def neighbours():
    mine = lax.axis_index("fsdp")
    return (
        {"fsdp": mine + 1 - 2 * lax.rem(mine, 2)},
        {"ctx": 1 - lax.axis_index("ctx")},
        {"tp": 1 - lax.axis_index("tp")},
    )


def greet(peers):
    barrier = pltpu.get_barrier_semaphore()
    for peer in peers:
        pl.semaphore_signal(barrier, inc=1, device_id=peer, device_id_type=MESH)
    pl.semaphore_wait(barrier, len(peers))


def remote_params(number, limit=None):
    return pltpu.CompilerParams(
        collective_id=number, has_side_effects=True, vmem_limit_bytes=limit
    )


def gather8_kernel(rows, spread, *refs):
    if spread:
        own_ref, kept_ref, x_ref, y_ref, first_ref, second_ref, out_ref, also_ref = refs[:8]
        send_sem, recv_sem, local_sem, stage, also_send, also_recv, also_in, also_out = refs[8:]
    else:
        own_ref, out_ref, send_sem, recv_sem, local_sem = refs
    x_peer, y_peer, c_peer = neighbours()

    def start_of(away_t, half, outer, inner):
        return pl.ds((away_t * 8 + half * 4 + outer * 2 + inner) * rows, rows)

    def slot(*block):
        return out_ref.at[start_of(*block)]

    also_loads, also_remote, also_stores = [], [], []
    if spread:
        top, low = pl.ds(0, rows), pl.ds(rows, rows)
        pieces = [
            ((0, 0, 0), kept_ref.at[top]),
            ((0, 0, 1), x_ref.at[top]),
            ((0, 1, 0), y_ref.at[top]),
            ((0, 1, 1), first_ref),
            ((1, 0, 0), kept_ref.at[low]),
            ((1, 0, 1), y_ref.at[low]),
            ((1, 1, 0), x_ref.at[low]),
            ((1, 1, 1), second_ref),
        ]
        for index, (block, source) in enumerate(pieces):
            also_loads.append(pltpu.make_async_copy(source, stage.at[index], also_in.at[index]))
            also_stores.append(
                pltpu.make_async_copy(
                    stage.at[index], also_ref.at[start_of(0, *block)], also_out.at[index]
                )
            )
            also_remote.append(
                pltpu.make_async_remote_copy(
                    src_ref=source,
                    dst_ref=also_ref.at[start_of(1, *block)],
                    send_sem=also_send.at[index],
                    recv_sem=also_recv.at[index],
                    device_id=c_peer,
                    device_id_type=MESH,
                )
            )
        for copy in also_loads:
            copy.start()
    greet((x_peer, y_peer, c_peer))

    number = iter(range(14))

    def send(source, target, peer):
        index = next(number)
        copy = pltpu.make_async_remote_copy(
            src_ref=source,
            dst_ref=target,
            send_sem=send_sem.at[index],
            recv_sem=recv_sem.at[index],
            device_id=peer,
            device_id_type=MESH,
        )
        copy.start()
        return copy

    first, second = own_ref.at[pl.ds(0, rows)], own_ref.at[pl.ds(rows, rows)]
    x1 = send(first, slot(0, 0, 0, 1), x_peer)
    y1 = send(second, slot(0, 1, 0, 1), y_peer)
    x2 = send(second, slot(0, 1, 1, 0), x_peer)
    y2 = send(first, slot(0, 0, 1, 0), y_peer)
    rest = [send(first, slot(1, 0, 0, 0), c_peer), send(second, slot(1, 1, 0, 0), c_peer)]
    kept = [
        pltpu.make_async_copy(first, slot(0, 0, 0, 0), local_sem.at[0]),
        pltpu.make_async_copy(second, slot(0, 1, 0, 0), local_sem.at[1]),
    ]
    for copy in kept:
        copy.start()
    for copy in also_remote:
        copy.start()
    for load, store in zip(also_loads, also_stores):
        load.wait()
        store.start()
    x1.wait_recv()
    y3 = send(slot(0, 0, 0, 1), slot(0, 0, 1, 1), y_peer)
    y1.wait_recv()
    x3 = send(slot(0, 1, 0, 1), slot(0, 1, 1, 1), x_peer)
    rest.append(send(slot(0, 0, 0, 1), slot(1, 0, 0, 1), c_peer))
    rest.append(send(slot(0, 1, 0, 1), slot(1, 1, 0, 1), c_peer))
    x2.wait_recv()
    rest.append(send(slot(0, 1, 1, 0), slot(1, 1, 1, 0), c_peer))
    y2.wait_recv()
    rest.append(send(slot(0, 0, 1, 0), slot(1, 0, 1, 0), c_peer))
    y3.wait_recv()
    rest.append(send(slot(0, 0, 1, 1), slot(1, 0, 1, 1), c_peer))
    x3.wait_recv()
    rest.append(send(slot(0, 1, 1, 1), slot(1, 1, 1, 1), c_peer))
    for copy in (x1, y1, x2, y2, y3, x3):
        copy.wait_send()
    for copy in rest + also_remote + kept + also_stores:
        copy.wait()


def gather8_product_kernel(
    rows,
    own_ref,
    acts_ref,
    weight_ref,
    out_ref,
    kept_ref,
    to_y_ref,
    to_x_ref,
    send_sem,
    recv_sem,
    local_sem,
    acts,
    weight,
    far,
    core_in,
    core_send,
    core_recv,
    load_sem,
):
    x_peer, y_peer, c_peer = neighbours()
    width = weight.shape[0]
    wide = 2 * rows
    loads = [
        pltpu.make_async_copy(weight_ref, weight, load_sem.at[0]),
        pltpu.make_async_copy(acts_ref, acts, load_sem.at[1]),
    ]
    for copy in loads:
        copy.start()
    greet((x_peer, y_peer, c_peer))

    def slot(away_t, half, outer, inner):
        return out_ref.at[pl.ds((away_t * 8 + half * 4 + outer * 2 + inner) * rows, rows)]

    number = iter(range(14))

    def send(source, target, peer):
        index = next(number)
        copy = pltpu.make_async_remote_copy(
            src_ref=source,
            dst_ref=target,
            send_sem=send_sem.at[index],
            recv_sem=recv_sem.at[index],
            device_id=peer,
            device_id_type=MESH,
        )
        copy.start()
        return copy

    core_copies = []

    def far_chunk(index):
        place = pl.ds(index * wide, wide)
        source = pl.ds(4 * wide + index * wide, wide)

        def step(cols):
            far[place, cols] = mm(acts[source, :], weight[cols, :], 1, 1).astype(BF16)
            return 0

        tiled(width, width // 2, step)
        copy = pltpu.make_async_remote_copy(
            src_ref=far.at[place],
            dst_ref=core_in.at[place],
            send_sem=core_send.at[index],
            recv_sem=core_recv.at[index],
            device_id=c_peer,
            device_id_type=MESH,
        )
        copy.start()
        core_copies.append(copy)

    def near_chunk(index, target_ref, start):
        core_copies[index].wait_recv()
        place = pl.ds(index * wide, wide)
        target = pl.ds(start, wide)

        def step(cols):
            value = mm(acts[place, :], weight[cols, :], 1, 1) + core_in[place, cols].astype(F32)
            target_ref[target, cols] = value.astype(target_ref.dtype)
            return 0

        tiled(width, width // 2, step)

    first, second = own_ref.at[pl.ds(0, rows)], own_ref.at[pl.ds(rows, rows)]
    x1 = send(first, slot(0, 0, 0, 1), x_peer)
    y1 = send(second, slot(0, 1, 0, 1), y_peer)
    x2 = send(second, slot(0, 1, 1, 0), x_peer)
    y2 = send(first, slot(0, 0, 1, 0), y_peer)
    rest = [send(first, slot(1, 0, 0, 0), c_peer), send(second, slot(1, 1, 0, 0), c_peer)]
    kept = [
        pltpu.make_async_copy(first, slot(0, 0, 0, 0), local_sem.at[0]),
        pltpu.make_async_copy(second, slot(0, 1, 0, 0), local_sem.at[1]),
    ]
    for copy in kept:
        copy.start()
    for copy in loads:
        copy.wait()
    for index in range(4):
        far_chunk(index)
    x1.wait_recv()
    y3 = send(slot(0, 0, 0, 1), slot(0, 0, 1, 1), y_peer)
    y1.wait_recv()
    x3 = send(slot(0, 1, 0, 1), slot(0, 1, 1, 1), x_peer)
    rest.append(send(slot(0, 0, 0, 1), slot(1, 0, 0, 1), c_peer))
    rest.append(send(slot(0, 1, 0, 1), slot(1, 1, 0, 1), c_peer))
    near_chunk(0, kept_ref, 0)
    near_chunk(1, to_y_ref, 0)
    near_chunk(2, kept_ref, wide)
    near_chunk(3, to_x_ref, 0)
    x2.wait_recv()
    rest.append(send(slot(0, 1, 1, 0), slot(1, 1, 1, 0), c_peer))
    y2.wait_recv()
    rest.append(send(slot(0, 0, 1, 0), slot(1, 0, 1, 0), c_peer))
    y3.wait_recv()
    rest.append(send(slot(0, 0, 1, 1), slot(1, 0, 1, 1), c_peer))
    x3.wait_recv()
    rest.append(send(slot(0, 1, 1, 1), slot(1, 1, 1, 1), c_peer))
    for copy in (x1, y1, x2, y2, y3, x3):
        copy.wait_send()
    for copy in core_copies:
        copy.wait_send()
    for copy in rest + kept:
        copy.wait()


def gather8_product(own, acts, weight):
    rows, width = own.shape[0] // 2, own.shape[1]
    hbm = pl.BlockSpec(memory_space=pl.ANY)
    vmem = pl.BlockSpec(memory_space=pltpu.VMEM)
    return pl.pallas_call(
        functools.partial(gather8_product_kernel, rows),
        out_shape=[
            jax.ShapeDtypeStruct((16 * rows, width), own.dtype),
            jax.ShapeDtypeStruct((4 * rows, width), F32),
            jax.ShapeDtypeStruct((2 * rows, width), BF16),
            jax.ShapeDtypeStruct((2 * rows, width), BF16),
        ],
        in_specs=[vmem, hbm, hbm],
        out_specs=[hbm, vmem, vmem, vmem],
        scratch_shapes=[
            pltpu.SemaphoreType.DMA((14,)),
            pltpu.SemaphoreType.DMA((14,)),
            pltpu.SemaphoreType.DMA((2,)),
            pltpu.VMEM(acts.shape, BF16),
            pltpu.VMEM(weight.shape, BF16),
            pltpu.VMEM((8 * rows, width), BF16),
            pltpu.VMEM((8 * rows, width), BF16),
            pltpu.SemaphoreType.DMA((4,)),
            pltpu.SemaphoreType.DMA((4,)),
            pltpu.SemaphoreType.DMA((2,)),
        ],
        compiler_params=remote_params(9, 48 * 1024 * 1024),
        cost_estimate=pl.CostEstimate(
            flops=2 * acts.size * width, bytes_accessed=16 * own.size, transcendentals=0
        ),
        name="gather8_product",
    )(own, acts, weight)


def gather8(own, also=()):
    rows, width = own.shape[0] // 2, own.shape[1]
    hbm = pl.BlockSpec(memory_space=pl.ANY)
    whole_shape = jax.ShapeDtypeStruct((16 * rows, width), own.dtype)
    sems = [
        pltpu.SemaphoreType.DMA((14,)),
        pltpu.SemaphoreType.DMA((14,)),
        pltpu.SemaphoreType.DMA((2,)),
    ]
    if also:
        sems += [pltpu.VMEM((8, rows, width), own.dtype)] + [pltpu.SemaphoreType.DMA((8,))] * 4
    outs = pl.pallas_call(
        functools.partial(gather8_kernel, rows, bool(also)),
        out_shape=[whole_shape] * (2 if also else 1),
        in_specs=[pl.BlockSpec(memory_space=pltpu.VMEM)] + [hbm] * len(also),
        out_specs=[hbm] * (2 if also else 1),
        scratch_shapes=sems,
        compiler_params=remote_params(6 if also else 1),
        name="gather8_also" if also else "gather8",
    )(own, *also)
    return outs if also else outs[0]


def reduce8_kernel(
    rows,
    near_ref,
    far_ref,
    out_ref,
    near,
    core_in,
    link_in,
    link_out,
    send_sem,
    recv_sem,
    local_sem,
):
    x_peer, y_peer, c_peer = neighbours()
    greet((x_peer, y_peer, c_peer))
    order = [(h, o, i) for o, i in ((1, 1), (1, 0), (0, 1), (0, 0)) for h in (0, 1)]
    core_copies, local_copies = {}, {}
    for number, (half, outer, inner) in enumerate(order):
        place = pl.ds((half * 4 + outer * 2 + inner) * rows, rows)
        core_copies[half, outer, inner] = pltpu.make_async_remote_copy(
            src_ref=far_ref.at[place],
            dst_ref=core_in.at[place],
            send_sem=send_sem.at[number],
            recv_sem=recv_sem.at[number],
            device_id=c_peer,
            device_id_type=MESH,
        )
        local_copies[half, outer, inner] = pltpu.make_async_copy(
            near_ref.at[place], near.at[place], local_sem.at[number]
        )
    for block in order:
        core_copies[block].start()
        local_copies[block].start()

    def partial_sum(block):
        half, outer, inner = block
        place = pl.ds((half * 4 + outer * 2 + inner) * rows, rows)
        core_copies[block].wait_recv()
        local_copies[block].wait()
        return near[place, :] + core_in[place, :].astype(F32)

    def link(index, value, peer):
        link_out[index] = value.astype(BF16)
        copy = pltpu.make_async_remote_copy(
            src_ref=link_out.at[index],
            dst_ref=link_in.at[index],
            send_sem=send_sem.at[8 + index],
            recv_sem=recv_sem.at[8 + index],
            device_id=peer,
            device_id_type=MESH,
        )
        copy.start()
        return copy

    y11 = link(0, partial_sum((0, 1, 1)), y_peer)
    x11 = link(1, partial_sum((1, 1, 1)), x_peer)
    y10 = link(2, partial_sum((0, 1, 0)), y_peer)
    x10 = link(3, partial_sum((1, 1, 0)), x_peer)
    first01, second01 = partial_sum((0, 0, 1)), partial_sum((1, 0, 1))
    y11.wait_recv()
    x01 = link(4, first01 + link_in[0].astype(F32), x_peer)
    x11.wait_recv()
    y01 = link(5, second01 + link_in[1].astype(F32), y_peer)
    first = partial_sum((0, 0, 0))
    second = partial_sum((1, 0, 0))
    y10.wait_recv()
    out_ref[pl.ds(0, rows), :] = first + link_in[2].astype(F32)
    x10.wait_recv()
    out_ref[pl.ds(rows, rows), :] = second + link_in[3].astype(F32)
    x01.wait_recv()
    out_ref[pl.ds(0, rows), :] += link_in[4].astype(F32)
    y01.wait_recv()
    out_ref[pl.ds(rows, rows), :] += link_in[5].astype(F32)
    for copy in (y11, x11, y10, x10, x01, y01):
        copy.wait_send()
    for copy in core_copies.values():
        copy.wait_send()


def reduce8(near, far):
    rows, width = near.shape[0] // 8, near.shape[1]
    return pl.pallas_call(
        functools.partial(reduce8_kernel, rows),
        out_shape=jax.ShapeDtypeStruct((2 * rows, width), F32),
        in_specs=[pl.BlockSpec(memory_space=pl.ANY), pl.BlockSpec(memory_space=pl.ANY)],
        out_specs=pl.BlockSpec(memory_space=pltpu.VMEM),
        scratch_shapes=[
            pltpu.VMEM(near.shape, F32),
            pltpu.VMEM(near.shape, BF16),
            pltpu.VMEM((6, rows, width), BF16),
            pltpu.VMEM((6, rows, width), BF16),
            pltpu.SemaphoreType.DMA((14,)),
            pltpu.SemaphoreType.DMA((14,)),
            pltpu.SemaphoreType.DMA((8,)),
        ],
        compiler_params=remote_params(2, 48 * 1024 * 1024),
        name="reduce8",
    )(near, far)


def tiled(count, tile, step):
    lax.fori_loop(0, count // tile, lambda i, _: step(pl.ds(pl.multiple_of(i * tile, tile), tile)), 0)


def product_reduce8_kernel(rows, groups, filler, *refs):
    acts_refs, refs = refs[:groups], refs[groups:]
    if filler:
        weight_ref, lhs_ref, out_ref, grad_ref, *refs = refs
    else:
        weight_ref, out_ref, *refs = refs
    acts, weight, far, near, core_in, link_in, link_out, send_sem, recv_sem, load_sem, *refs = refs
    x_peer, y_peer, c_peer = neighbours()
    width = weight.shape[0]
    wide = 2 * rows
    chunks = [(0, 1), (1, 1), (0, 0), (1, 0)]

    def where(chunk):
        return chunk[0] * 2 * wide + chunk[1] * wide

    half = width // 2
    load_weights = [
        pltpu.make_async_copy(
            weight_ref.at[pl.ds(part * half, half), pl.ds(0, weight.shape[1])],
            weight.at[pl.ds(part * half, half)],
            load_sem.at[part],
        )
        for part in (0, 1)
    ]
    loads = {}
    depth = weight.shape[1] // groups
    for number, chunk in enumerate(chunks):
        for side in (1, 0):
            place = pl.ds(side * 4 * wide + where(chunk), wide)
            loads[side, chunk] = [
                pltpu.make_async_copy(
                    acts_refs[group].at[place],
                    acts.at[place, pl.ds(group * depth, depth)],
                    load_sem.at[3 + (2 * number + side) * groups + group],
                )
                for group in range(groups)
            ]
    started = [loads[1, chunks[0]], [load_weights[0]], loads[1, chunks[1]], loads[0, chunks[0]]]
    started += [loads[0, chunks[1]], [load_weights[1]]]
    started += [loads[side, chunk] for chunk in chunks[2:] for side in (1, 0)]
    for group in started:
        for copy in group:
            copy.start()
    if filler:
        lhs, grad, grad_sem = refs
        load_lhs = pltpu.make_async_copy(lhs_ref, lhs, load_sem.at[2])
        load_lhs.start()
    greet((x_peer, y_peer, c_peer))

    core_copies, link_copies = {}, {}

    def product(chunk, side, part, target):
        place = pl.ds(where(chunk), wide)
        source = pl.ds(side * 4 * wide + where(chunk), wide)

        cols = pl.ds(part * half, half)
        target[place, cols] = mm(acts[source, :], weight[cols, :], 1, 1).astype(target.dtype)

    def remote(copies, key, number, source, target, peer):
        copies[key] = pltpu.make_async_remote_copy(
            src_ref=source,
            dst_ref=target,
            send_sem=send_sem.at[number],
            recv_sem=recv_sem.at[number],
            device_id=peer,
            device_id_type=MESH,
        )
        copies[key].start()

    def send_core(chunk, part):
        product(chunk, 1, part, far)
        here = (pl.ds(where(chunk), wide), pl.ds(part * half, half))
        number = 2 * chunks.index(chunk) + part
        remote(core_copies, (chunk, part), number, far.at[here], core_in.at[here], c_peer)

    def partial_sum(chunk, start, size, part):
        here = (pl.ds(where(chunk) + start, size), pl.ds(part * half, half))
        return near[here] + core_in[here].astype(F32)

    def link(hop, side, part, value, peer):
        size = value.shape[0]
        start = (side * 3 + hop * 2) * rows
        here = (pl.ds(start, size), pl.ds(part * half, half))
        link_out[here] = value.astype(BF16)
        number = 8 + hop * 4 + side * 2 + part
        remote(link_copies, (hop, side, part), number, link_out.at[here], link_in.at[here], peer)

    def came(hop, side, start, part):
        return link_in[
            pl.ds((side * 3 + hop * 2) * rows + start, rows), pl.ds(part * half, half)
        ].astype(F32)

    for chunk in chunks[:2]:
        for copy in loads[1, chunk]:
            copy.wait()
    for part in (0, 1):
        load_weights[part].wait()
        send_core((0, 1), part)
        send_core((1, 1), part)
        for side, peer in ((0, y_peer), (1, x_peer)):
            if part == 0:
                for copy in loads[0, (side, 1)]:
                    copy.wait()
            product((side, 1), 0, part, near)
            core_copies[(side, 1), part].wait_recv()
            link(0, side, part, partial_sum((side, 1), 0, wide, part), peer)
    for chunk in chunks[2:]:
        for side in (1, 0):
            for copy in loads[side, chunk]:
                copy.wait()
    if filler:
        size = width // 4

        def fill(index, _):
            cols = pl.ds(pl.multiple_of(index * size, size), size)

            def step(columns):
                grad[cols, columns] = mm(lhs[:, cols], acts[:, columns], 0, 0).astype(BF16)
                return 0

            tiled(acts.shape[1], acts.shape[1] // 3, step)
            return 0

    for part in (0, 1):
        for chunk in chunks[2:]:
            send_core(chunk, part)
        for chunk in chunks[2:]:
            product(chunk, 0, part, near)
        for side, peer in ((0, x_peer), (1, y_peer)):
            core_copies[(side, 0), part].wait_recv()
            link_copies[0, side, part].wait_recv()
            link(1, side, part, partial_sum((side, 0), rows, rows, part) + came(0, side, rows, part), peer)
        if filler and part == 0:
            load_lhs.wait()
            lax.fori_loop(0, 1, fill, 0)
    if filler:
        lax.fori_loop(1, 4, fill, 0)
        grad_copy = pltpu.make_async_copy(grad, grad_ref, grad_sem.at[0])
        grad_copy.start()
    for side in (0, 1):
        for part in (0, 1):
            place = (pl.ds(side * rows, rows), pl.ds(part * half, half))
            kept = partial_sum((side, 0), 0, rows, part) + came(0, side, 0, part)
            link_copies[1, side, part].wait_recv()
            out_ref[place] = kept + came(1, side, 0, part)
    for copy in list(link_copies.values()) + list(core_copies.values()):
        copy.wait_send()
    if filler:
        grad_copy.wait()


def product_reduce8(columns, weight, number, lhs=None):
    depth, groups = sum(column.shape[1] for column in columns), len(columns)
    acts = jax.ShapeDtypeStruct((columns[0].shape[0], depth), BF16)
    rows, width = acts.shape[0] // 16, weight.shape[0]
    filler = lhs is not None
    hbm = pl.BlockSpec(memory_space=pl.ANY)
    scratch = [
        pltpu.VMEM(acts.shape, BF16),
        pltpu.VMEM((width, depth), BF16),
        pltpu.VMEM((8 * rows, width), BF16),
        pltpu.VMEM((8 * rows, width), F32),
        pltpu.VMEM((8 * rows, width), BF16),
        pltpu.VMEM((6 * rows, width), BF16),
        pltpu.VMEM((6 * rows, width), BF16),
        pltpu.SemaphoreType.DMA((16,)),
        pltpu.SemaphoreType.DMA((16,)),
        pltpu.SemaphoreType.DMA((3 + 8 * groups,)),
    ]
    out_shape = [jax.ShapeDtypeStruct((2 * rows, width), F32)]
    out_specs = [pl.BlockSpec(memory_space=pltpu.VMEM)]
    flops = 2 * acts.shape[0] * width * depth
    if filler:
        scratch += [
            pltpu.VMEM(lhs.shape, BF16),
            pltpu.VMEM((width, depth), BF16),
            pltpu.SemaphoreType.DMA((1,)),
        ]
        out_shape.append(jax.ShapeDtypeStruct((width, depth), BF16))
        out_specs.append(hbm)
        flops *= 2
    outs = pl.pallas_call(
        functools.partial(product_reduce8_kernel, rows, groups, filler),
        out_shape=out_shape,
        in_specs=[hbm] * (groups + (2 if filler else 1)),
        out_specs=out_specs,
        scratch_shapes=scratch,
        compiler_params=remote_params(number, 63 * 1024 * 1024),
        cost_estimate=pl.CostEstimate(
            flops=flops, bytes_accessed=4 * depth * (acts.shape[0] + width), transcendentals=0
        ),
        name="product_reduce8",
    )(*columns, weight, *((lhs,) if filler else ()))
    return outs if filler else outs[0]


def shard_kernel(plan, outs, *refs):
    ins, out_refs = refs[: len(plan)], refs[len(plan) : len(plan) + outs]
    stage = refs[len(plan) + outs : 2 * len(plan) + outs]
    send_sem, recv_sem, load_sem, store_sem = refs[2 * len(plan) + outs :]
    x_peer, _, _ = neighbours()
    odd = lax.rem(lax.axis_index("fsdp"), 2)
    column = 2 * lax.axis_index("ctx") + odd
    other = 2 * lax.axis_index("ctx") + 1 - odd
    greet((x_peer,))
    remote, loads, stores = [], [], []
    for number, (which, start, size, cut) in enumerate(plan):
        rows = ins[number].shape[0]
        place = pl.ds(pl.multiple_of(odd * rows, rows), rows)
        target = out_refs[which].at[place, pl.ds(start, size)]

        def source(index, ref=ins[number], size=size, cut=cut):
            if not cut:
                return ref
            return ref.at[:, pl.ds(pl.multiple_of(index * size, HEAD), size)]

        remote.append(
            pltpu.make_async_remote_copy(
                src_ref=source(other),
                dst_ref=target,
                send_sem=send_sem.at[number],
                recv_sem=recv_sem.at[number],
                device_id=x_peer,
                device_id_type=MESH,
            )
        )
        loads.append(pltpu.make_async_copy(source(column), stage[number], load_sem.at[number]))
        stores.append(pltpu.make_async_copy(stage[number], target, store_sem.at[number]))
    for copy in remote:
        copy.start()
    for copy in loads:
        copy.start()
    for load, store in zip(loads, stores):
        load.wait()
        store.start()
    for copy in stores:
        copy.wait()
    for copy in remote:
        copy.wait()


def shards(groups, number):
    plan, arrays, shapes = [], [], []
    for which, group in enumerate(groups):
        start = 0
        for array, cut in group:
            size = array.shape[1] // 4 if cut else array.shape[1]
            plan.append((which, start, size, cut))
            arrays.append(array)
            start += size
        shapes.append((2 * group[0][0].shape[0], start))
    hbm = pl.BlockSpec(memory_space=pl.ANY)
    return pl.pallas_call(
        functools.partial(shard_kernel, tuple(plan), len(groups)),
        out_shape=[jax.ShapeDtypeStruct(shape, BF16) for shape in shapes],
        in_specs=[hbm] * len(arrays),
        out_specs=[hbm] * len(groups),
        scratch_shapes=[
            pltpu.VMEM((array.shape[0], size), BF16)
            for array, (_, _, size, _) in zip(arrays, plan)
        ]
        + [pltpu.SemaphoreType.DMA((len(plan),))] * 4,
        compiler_params=remote_params(number),
        name="shards",
    )(*arrays)


def total_kernel(stages, part_ref, out_ref, inbox, outbox, send_sem, recv_sem):
    peers = []
    for axis, bit in stages:
        mine = lax.axis_index(axis)
        peers.append({axis: mine + bit * (1 - 2 * lax.rem(mine // bit, 2))})
    greet(peers)
    value = part_ref[...]
    copies = []
    for index, peer in enumerate(peers):
        outbox[index] = value
        copy = pltpu.make_async_remote_copy(
            src_ref=outbox.at[index],
            dst_ref=inbox.at[index],
            send_sem=send_sem.at[index],
            recv_sem=recv_sem.at[index],
            device_id=peer,
            device_id_type=MESH,
        )
        copy.start()
        copies.append(copy)
        copy.wait_recv()
        value = value + inbox[index]
    out_ref[...] = value
    for copy in copies:
        copy.wait_send()


def total(part):
    stages, bit = [], 2
    while bit < lax.axis_size("fsdp"):
        stages.append(("fsdp", bit))
        bit *= 2
    stages += [("tp", 1), ("fsdp", 1)]
    return pl.pallas_call(
        functools.partial(total_kernel, tuple(stages)),
        out_shape=jax.ShapeDtypeStruct(part.shape, F32),
        in_specs=[pl.BlockSpec(memory_space=pltpu.VMEM)],
        out_specs=pl.BlockSpec(memory_space=pltpu.VMEM),
        scratch_shapes=[
            pltpu.VMEM((len(stages),) + part.shape, F32),
            pltpu.VMEM((len(stages),) + part.shape, F32),
            pltpu.SemaphoreType.DMA((len(stages),)),
            pltpu.SemaphoreType.DMA((len(stages),)),
        ],
        compiler_params=remote_params(5),
        name="total",
    )(part)


def stack_kernel(spot_ref, own_ref, other_ref, out_ref):
    @pl.when(pl.program_id(0) == 0)
    def _():
        out_ref[...] = own_ref[...]

    @pl.when(pl.program_id(0) == 1)
    def _():
        out_ref[...] = other_ref[...]


def stack_rows(spot, own, other):
    block = pl.BlockSpec(own.shape, lambda i, spot: (0, 0))
    return pl.pallas_call(
        stack_kernel,
        out_shape=jax.ShapeDtypeStruct((2 * own.shape[0], own.shape[1]), own.dtype),
        grid_spec=pltpu.PrefetchScalarGridSpec(
            num_scalar_prefetch=1,
            grid=(2,),
            in_specs=[block, block],
            out_specs=pl.BlockSpec(own.shape, lambda i, spot: (lax.rem(spot[1] + i, 2), 0)),
        ),
        name="stack",
    )(spot, own, other)


def join_kernel(sizes, spot_ref, kept_ref, x_ref, y_ref, both_ref, *out_refs):
    place, odd = spot_ref[0], spot_ref[1]
    parts = (
        (kept_ref, 2 * place + odd),
        (x_ref, 2 * place + 1 - odd),
        (y_ref, 2 - 2 * place + odd),
        (both_ref, 3 - 2 * place - odd),
    )
    for part, column in parts:
        start = 0
        for size, out_ref in zip(sizes, out_refs):
            target = pl.ds(pl.multiple_of(column * size, HEAD), size)
            out_ref[:, target] = part[:, start : start + size].astype(F32)
            start += size


def join_columns(spot, parts, sizes):
    rows = parts[0].shape[0]
    tile = min(rows, 64)
    return pl.pallas_call(
        functools.partial(join_kernel, sizes),
        out_shape=[jax.ShapeDtypeStruct((rows, 4 * size), F32) for size in sizes],
        grid_spec=pltpu.PrefetchScalarGridSpec(
            num_scalar_prefetch=1,
            grid=(rows // tile,),
            in_specs=[
                pl.BlockSpec((tile, part.shape[1]), lambda i, spot: (i, 0)) for part in parts
            ],
            out_specs=[pl.BlockSpec((tile, 4 * size), lambda i, spot: (i, 0)) for size in sizes],
        ),
        name="join",
    )(spot, *parts)


def after(value, *others):
    return lax.optimization_barrier((value,) + others)[0]


def reduce4_links(kept, to_y, to_x, *others):
    rows = kept.shape[0] // 4
    came_first, came_second = swap_ctx(to_y), swap_x(to_x)
    first = kept[: 2 * rows] + after(came_first, *others).astype(F32)
    second = kept[2 * rows :] + after(came_second, *others).astype(F32)
    came_first = swap_x(first[rows:].astype(BF16))
    came_second = swap_ctx(second[rows:].astype(BF16))
    return first[:rows], second[:rows], came_first, came_second


def rope_tables(positions):
    freqs = THETA ** (-(jnp.arange(HEAD // 2, dtype=F32) * 2.0) / HEAD)
    angle = positions[:, None] * freqs[None, :]
    cosine = jnp.concatenate([jnp.cos(angle), jnp.cos(angle)], axis=-1)
    sine = jnp.concatenate([-jnp.sin(angle), jnp.sin(angle)], axis=-1)
    return cosine, sine


def norm_back(grad, scaled, inverse, gain):
    weighted = grad * gain
    return inverse * (weighted - scaled * jnp.mean(weighted * scaled, axis=-1, keepdims=True))


def inv_rms(value):
    return lax.rsqrt(jnp.mean(value * value, axis=-1, keepdims=True) + EPS)


def block_row(meta_ref, seq, index, rows):
    away_c = lax.rem(meta_ref[0] + index // 4, 2)
    away_t = lax.rem(meta_ref[1] + (index // 2) % 2, 2)
    if index % 2 == 0:
        inner = away_c * 2 + seq
    else:
        inner = seq * 2 + away_c + 4
    return pl.multiple_of((away_t * 8 + inner) * rows, rows)


def scaled_of(raw):
    inverse = lax.rsqrt(jnp.mean(raw * raw, axis=-1, keepdims=True) + EPS)
    return raw * inverse, inverse


def load_heads(meta_ref, qkv_ref, cos_ref, sin_ref, gain_ref, q_scr, k_scr, v_scr, heads):
    seq = pl.program_id(0)
    rows = q_scr.shape[1] // 8
    for index in range(8):
        start = block_row(meta_ref, seq, index, rows)
        here = slice(index * rows, (index + 1) * rows)
        cosine, sine = cos_ref[here, :], sin_ref[here, :]
        for head in range(heads + 1):
            raw = qkv_ref[pl.ds(start, rows), head * HEAD : (head + 1) * HEAD]
            scaled, _ = scaled_of(raw)
            which = 0 if head < heads else 1
            value = scaled * gain_ref[which : which + 1, :]
            turned = value * cosine + pltpu.roll(value, HEAD // 2, 1) * sine
            if head < heads:
                q_scr[head, here, :] = turned.astype(BF16)
            else:
                k_scr[here, :] = turned.astype(BF16)
        v_scr[here, :] = qkv_ref[
            pl.ds(start, rows), (heads + 1) * HEAD : (heads + 2) * HEAD
        ].astype(BF16)


def key_span(index, tile):
    low = max(0, (index * tile - (MOST_DOC - 1)) // tile) * tile
    return low, (index + 1) * tile


def allowed_mask(segc_ref, segr_ref, index, tile):
    low, high = key_span(index, tile)
    shape = (tile, high - low)
    rows = lax.broadcasted_iota(jnp.int32, shape, 0) + index * tile
    cols = lax.broadcasted_iota(jnp.int32, shape, 1) + low
    same = segc_ref[0, index * tile : (index + 1) * tile, :] == segr_ref[0, :, low:high]
    return same & (cols <= rows)


def probs_of(query, keys, allowed, scale):
    scores = jnp.where(allowed, mm(query, keys, 1, 1) * scale, MASKED)
    weights = jnp.exp(scores - jnp.max(scores, axis=-1, keepdims=True))
    return weights * (1.0 / jnp.sum(weights, axis=-1, keepdims=True))


def attend_kernel(
    heads, tile, meta_ref, qkv_ref, segc_ref, segr_ref, cos_ref, sin_ref, gain_ref, out_ref, q_scr, k_scr, v_scr
):
    seq = pl.program_id(0)
    length = k_scr.shape[0]
    rows = length // 8
    scale = 1.0 / math.sqrt(HEAD)
    load_heads(meta_ref, qkv_ref, cos_ref, sin_ref, gain_ref, q_scr, k_scr, v_scr, heads)
    for index in range(length // tile):
        low, high = key_span(index, tile)
        allowed = allowed_mask(segc_ref, segr_ref, index, tile)
        for head in range(heads):
            query = q_scr[head, index * tile : (index + 1) * tile, :]
            probs = probs_of(query, k_scr[low:high, :], allowed, scale)
            mixed = mm(probs.astype(BF16), v_scr[low:high, :], 1, 0).astype(BF16)
            for piece in range(tile // rows):
                start = block_row(meta_ref, seq, index * (tile // rows) + piece, rows)
                out_ref[pl.ds(start, rows), head * HEAD : (head + 1) * HEAD] = mixed[
                    piece * rows : (piece + 1) * rows
                ]


def attend_back_kernel(
    heads,
    tile,
    meta_ref,
    qkv_ref,
    grad_ref,
    segc_ref,
    segr_ref,
    cos_ref,
    sin_ref,
    gain_ref,
    out_ref,
    gain_out_ref,
    q_scr,
    k_scr,
    v_scr,
    g_scr,
    dk_scr,
    dv_scr,
):
    seq = pl.program_id(0)
    length = k_scr.shape[0]
    rows = length // 8
    scale = 1.0 / math.sqrt(HEAD)
    load_heads(meta_ref, qkv_ref, cos_ref, sin_ref, gain_ref, q_scr, k_scr, v_scr, heads)
    for index in range(8):
        start = block_row(meta_ref, seq, index, rows)
        g_scr[index * rows : (index + 1) * rows, :] = grad_ref[pl.ds(start, rows), :]
    dk_scr[...] = jnp.zeros_like(dk_scr)
    dv_scr[...] = jnp.zeros_like(dv_scr)

    @pl.when(seq == 0)
    def _():
        gain_out_ref[...] = jnp.zeros_like(gain_out_ref)

    def finish(grad, index, head, which):
        here = slice(index * rows, (index + 1) * rows)
        start = block_row(meta_ref, seq, index, rows)
        grad = grad * cos_ref[here, :] - pltpu.roll(grad, HEAD // 2, 1) * sin_ref[here, :]
        raw = qkv_ref[pl.ds(start, rows), head * HEAD : (head + 1) * HEAD]
        scaled, inverse = scaled_of(raw)
        gain_out_ref[which : which + 1, :] += jnp.sum(grad * scaled, axis=0, keepdims=True)
        out = norm_back(grad, scaled, inverse, gain_ref[which : which + 1, :])
        out_ref[pl.ds(start, rows), head * HEAD : (head + 1) * HEAD] = out.astype(BF16)

    per = tile // rows
    for index in range(length // tile):
        low, high = key_span(index, tile)
        mine = slice(index * tile, (index + 1) * tile)
        allowed = allowed_mask(segc_ref, segr_ref, index, tile)
        for head in range(heads):
            query = q_scr[head, mine, :]
            keys = k_scr[low:high, :]
            probs = probs_of(query, keys, allowed, scale)
            grad = g_scr[mine, head * HEAD : (head + 1) * HEAD]
            grad_probs = mm(grad, v_scr[low:high, :], 1, 1)
            delta = jnp.sum(probs * grad_probs, axis=-1, keepdims=True)
            grad_scores = (probs * (grad_probs - delta)).astype(BF16)
            dv_scr[low:high, :] += mm(probs.astype(BF16), grad, 0, 0)
            dk_scr[low:high, :] += mm(grad_scores, query, 0, 0) * scale
            grad_query = mm(grad_scores, keys, 1, 0) * scale
            for piece in range(per):
                finish(
                    grad_query[piece * rows : (piece + 1) * rows], index * per + piece, head, 0
                )
    for index in range(8):
        here = slice(index * rows, (index + 1) * rows)
        start = block_row(meta_ref, seq, index, rows)
        finish(dk_scr[here, :], index, heads, 1)
        out_ref[pl.ds(start, rows), (heads + 1) * HEAD : (heads + 2) * HEAD] = dv_scr[
            here, :
        ].astype(BF16)


def whole(shape):
    return pl.BlockSpec(shape, lambda seq, meta: (0,) * len(shape))


def seg_specs(length):
    return [
        pl.BlockSpec((1, length, 1), lambda seq, meta: (seq, 0, 0)),
        pl.BlockSpec((1, 1, length), lambda seq, meta: (seq, 0, 0)),
    ]


def attend(meta, qkv, seg_cols, seg_rows, cosine, sine, gains):
    length = cosine.shape[0]
    tile = length // 4
    heads = qkv.shape[1] // HEAD - 2
    pairs = 2 * heads * length * length // 2
    return pl.pallas_call(
        functools.partial(attend_kernel, heads, tile),
        out_shape=jax.ShapeDtypeStruct((qkv.shape[0], heads * HEAD), BF16),
        grid_spec=pltpu.PrefetchScalarGridSpec(
            num_scalar_prefetch=1,
            grid=(2,),
            in_specs=[whole(qkv.shape)]
            + seg_specs(length)
            + [whole(cosine.shape), whole(sine.shape), whole(gains.shape)],
            out_specs=whole((qkv.shape[0], heads * HEAD)),
            scratch_shapes=[
                pltpu.VMEM((heads, length, HEAD), BF16),
                pltpu.VMEM((length, HEAD), BF16),
                pltpu.VMEM((length, HEAD), BF16),
            ],
        ),
        cost_estimate=pl.CostEstimate(
            flops=4 * pairs * HEAD, bytes_accessed=qkv.size * 4 + qkv.size, transcendentals=pairs
        ),
        name="attend",
    )(meta, qkv, seg_cols, seg_rows, cosine, sine, gains)


def attend_back(meta, qkv, grad, seg_cols, seg_rows, cosine, sine, gains):
    length = cosine.shape[0]
    tile = length // 4
    heads = qkv.shape[1] // HEAD - 2
    pairs = 2 * heads * length * length // 2
    return pl.pallas_call(
        functools.partial(attend_back_kernel, heads, tile),
        out_shape=(
            jax.ShapeDtypeStruct(qkv.shape, BF16),
            jax.ShapeDtypeStruct(gains.shape, F32),
        ),
        grid_spec=pltpu.PrefetchScalarGridSpec(
            num_scalar_prefetch=1,
            grid=(2,),
            in_specs=[whole(qkv.shape), whole(grad.shape)]
            + seg_specs(length)
            + [whole(cosine.shape), whole(sine.shape), whole(gains.shape)],
            out_specs=(whole(qkv.shape), whole(gains.shape)),
            scratch_shapes=[
                pltpu.VMEM((heads, length, HEAD), BF16),
                pltpu.VMEM((length, HEAD), BF16),
                pltpu.VMEM((length, HEAD), BF16),
                pltpu.VMEM((length, heads * HEAD), BF16),
                pltpu.VMEM((length, HEAD), F32),
                pltpu.VMEM((length, HEAD), F32),
            ],
        ),
        cost_estimate=pl.CostEstimate(
            flops=10 * pairs * HEAD, bytes_accessed=qkv.size * 8, transcendentals=pairs
        ),
        name="attend_back",
    )(meta, qkv, grad, seg_cols, seg_rows, cosine, sine, gains)


def body(
    tokens,
    segment_ids,
    norm_gain,
    query_weight,
    key_matrix,
    value_matrix,
    output_weight,
    query_gain,
    key_gain,
    mlp_gain,
    gate_weight,
    up_weight,
    down_weight,
    cotangent,
):
    local, width = tokens.shape[1], tokens.shape[2]
    length = 2 * local
    quarter = local // 2
    count = lax.axis_size("fsdp")
    block = width // count
    mine = lax.axis_index("fsdp")
    odd = mine % 2
    place = lax.axis_index("ctx")
    core = lax.axis_index("tp")

    small = query_gain.shape[0]
    lanes = jnp.arange(HEAD)[None, :]

    def pad_rows(vector):
        return jnp.concatenate([vector, jnp.zeros((block - small,), BF16)])

    gains = jnp.where(
        lanes == 0,
        norm_gain[:, None],
        jnp.where(
            lanes == 1,
            mlp_gain[:, None],
            jnp.where(
                lanes == 2, pad_rows(query_gain)[:, None], pad_rows(key_gain)[:, None]
            ),
        ),
    )
    far_segments = swap_x(segment_ids)
    (first_pair,) = shards(
        [
            [
                (query_weight, True),
                (key_matrix, True),
                (value_matrix, True),
                (output_weight, True),
                (gains, False),
            ]
        ],
        3,
    )
    first = gather_line(first_pair)
    gate_up_pair, down_pair = shards(
        [
            [(after(gate_weight, first_pair), True), (up_weight, True)],
            [(down_weight, True)],
        ],
        4,
    )
    gate_up_w = gather_line(gate_up_pair)
    down_w = gather_line(down_pair)

    def own_quarter(value):
        return lax.dynamic_slice_in_dim(value.reshape(local, width), core * quarter, quarter, 0)

    own_tok, own_cot = own_quarter(tokens), own_quarter(cotangent)
    tok = gather8(after(own_tok, gate_up_pair))
    segments = jnp.concatenate([segment_ids, far_segments])
    seg_cols, seg_rows = segments[:, :, None], segments[:, None, :]
    cosine, sine = rope_tables(jnp.arange(length).astype(F32))
    meta = jnp.stack([place, core]).astype(jnp.int32)

    heads_q = query_weight.shape[1] // 4 // HEAD
    cols = (heads_q + 2) * HEAD
    qkv_w = first[:, :cols]
    out_w = first[:, cols : cols + heads_q * HEAD]
    gain_cols = first[:, cols + heads_q * HEAD :].astype(F32)
    in_gain, mid_gain = gain_cols[:, 0][None], gain_cols[:, 1][None]
    head_gains = gain_cols.reshape(count, block, HEAD)[:, :small, 2:4].reshape(HEAD, 2).T

    in_f = tok.astype(F32)
    cot_from = after(own_cot, tok)
    cot_x, cot_y = swap_x(cot_from), swap_ctx(cot_from)
    x_all = (in_f * inv_rms(in_f) * in_gain).astype(BF16)
    qkv = mm(x_all, qkv_w, 1, 0)
    attended = attend(meta, qkv, seg_cols, seg_rows, cosine, sine, head_gains)
    half = 4 * quarter
    cot_x, cot_y = after(cot_x, attended), after(cot_y, attended)
    eighth = quarter // 2
    cot_first, cot_second = swap_ctx(cot_x[:eighth]), swap_x(cot_y[eighth:])
    out_far = mm(attended[half:], out_w, 1, 1).astype(BF16)
    out_near = mm(attended[:half], out_w, 1, 1)
    middle = own_tok.astype(F32) + reduce8(out_near, out_far)
    inverse_mid = inv_rms(middle)
    scaled_mid = middle * inverse_mid
    y_own = (scaled_mid * mid_gain).astype(BF16)
    cot_first, cot_second = after(cot_first, y_own), after(cot_second, y_own)
    y_all, cot = gather8(y_own, (cot_from, cot_x, cot_y, cot_first, cot_second))

    ff = gate_up_w.shape[1] // 2
    gate_up = mm(y_all, gate_up_w, 1, 0)
    gate, up_value = gate_up[:, :ff], gate_up[:, ff:]
    sig = jax.nn.sigmoid(gate)
    active = gate * sig
    hidden = (active * up_value).astype(BF16)
    down_grad = mm(cot, hidden, 0, 0).astype(BF16)

    def finish_rows(own):
        return stack_rows(meta, own, swap_core(own)).reshape(tokens.shape)

    grad_hidden = mm(after(cot, down_grad), down_w, 1, 0)
    grad_up = (grad_hidden * active).astype(BF16)
    grad_gate = (grad_hidden * up_value * (sig * (1.0 + gate * (1.0 - sig)))).astype(BF16)
    mid_grad, gate_up_grad = product_reduce8((grad_gate, grad_up), gate_up_w, 7, y_all)

    mlp_gain_part = jnp.sum(mid_grad * scaled_mid, axis=0)
    grad_middle = own_cot.astype(F32) + norm_back(mid_grad, scaled_mid, inverse_mid, mid_gain)
    grad_attn, mlp_kept, mlp_to_y, mlp_to_x = gather8_product(
        grad_middle.astype(BF16), hidden, down_w
    )
    out_grad = mm(grad_attn, attended, 0, 0).astype(BF16)
    grad_att = mm(grad_attn, out_w, 1, 0).astype(BF16)
    raw_grads, head_gain_parts = attend_back(
        meta, qkv, grad_att, seg_cols, seg_rows, cosine, sine, head_gains
    )
    mlp_first, mlp_second, mlp_came1, mlp_came2 = reduce4_links(
        mlp_kept, mlp_to_y, mlp_to_x, raw_grads
    )
    first_grad = mm(x_all, raw_grads, 0, 0).astype(BF16)
    first_grad = jnp.concatenate([first_grad, out_grad], axis=1)
    mlp_first = mlp_first + after(mlp_came1, first_grad).astype(F32)
    mlp_second = mlp_second + after(mlp_came2, first_grad).astype(F32)
    mlp_sum = (middle + jnp.concatenate([mlp_first, mlp_second])).astype(BF16)
    layer_out = finish_rows(mlp_sum)
    in_grad = product_reduce8((after(raw_grads, first_grad, mlp_sum),), first, 8)

    spot = jnp.stack([place, odd]).astype(jnp.int32)

    def owners(grad, sizes, *others):
        rows = scatter_line(grad)
        rows = after(rows, *others)
        kept = lax.dynamic_slice_in_dim(rows, odd * block, block, 0)
        sent = lax.dynamic_slice_in_dim(rows, (1 - odd) * block, block, 0)
        by_x, by_y = swap_x(sent), swap_ctx(kept)
        by_both = swap_ctx(by_x)
        return join_columns(spot, (kept, by_x, by_y, by_both), sizes)

    (down_share,) = owners(down_grad, (ff,))
    gate_share, up_share = owners(gate_up_grad, (ff, ff))
    query_share, key_share, value_share, out_share = owners(
        first_grad, (heads_q * HEAD, HEAD, HEAD, heads_q * HEAD)
    )

    own_in = own_tok.astype(F32)
    inverse_in = inv_rms(own_in)
    scaled_in = own_in * inverse_in
    norm_gain_part = jnp.sum(in_grad * scaled_in, axis=0)
    own_token_grad = (grad_middle + norm_back(in_grad, scaled_in, inverse_in, in_gain)).astype(BF16)
    token_grad = finish_rows(own_token_grad)

    parts = jnp.concatenate([norm_gain_part, mlp_gain_part, head_gain_parts.reshape(-1)])
    parts = parts.reshape(-1, HEAD)
    far_parts = swap_ctx(parts)
    sums = total(parts + after(far_parts, token_grad)).reshape(-1)
    norm_gain_grad = lax.dynamic_slice_in_dim(sums, mine * block, block, 0)
    mlp_gain_grad = lax.dynamic_slice_in_dim(sums, width + mine * block, block, 0)
    query_gain_grad = lax.dynamic_slice_in_dim(sums, 2 * width + mine * small, small, 0)
    key_gain_grad = lax.dynamic_slice_in_dim(sums, 2 * width + HEAD + mine * small, small, 0)
    return (
        layer_out,
        token_grad,
        norm_gain_grad,
        query_share,
        key_share,
        value_share,
        out_share,
        query_gain_grad,
        key_gain_grad,
        mlp_gain_grad,
        gate_share,
        up_share,
        down_share,
    )


def solution(mesh):
    in_specs = (
        P("fsdp", "ctx", None),
        P("fsdp", None),
        P("fsdp"),
        P("fsdp", "tp"),
        P("fsdp", "tp"),
        P("fsdp", "tp"),
        P("fsdp", "tp"),
        P("fsdp"),
        P("fsdp"),
        P("fsdp"),
        P("fsdp", "tp"),
        P("fsdp", "tp"),
        P("fsdp", "tp"),
        P("fsdp", "ctx", None),
    )
    out_specs = (
        P("fsdp", "ctx", None),
        P("fsdp", "ctx", None),
        P("fsdp"),
        P("fsdp", "tp"),
        P("fsdp", "tp"),
        P("fsdp", "tp"),
        P("fsdp", "tp"),
        P("fsdp"),
        P("fsdp"),
        P("fsdp"),
        P("fsdp", "tp"),
        P("fsdp", "tp"),
        P("fsdp", "tp"),
    )

    return jax.shard_map(body, mesh=mesh, in_specs=in_specs, out_specs=out_specs, check_vma=False)
```

```python
import functools
import math

import jax
import jax.numpy as jnp
from jax import lax
from jax.experimental import pallas as pl
from jax.experimental.pallas import tpu as pltpu
from jax.sharding import PartitionSpec as P


HEAD = 128
EPS = 1e-06
THETA = 1000000.0
MASKED = -1e30
MOST_DOC = 512
MESH = pl.DeviceIdType.MESH
F32 = jnp.float32
BF16 = jnp.bfloat16


def mm(left, right, left_dim, right_dim):
    return lax.dot_general(
        left, right, (((left_dim,), (right_dim,)), ((), ())), preferred_element_type=F32
    )


def swap_core(value):
    return lax.ppermute(value, "tp", [(0, 1), (1, 0)])


def swap_ctx(value):
    return lax.ppermute(value, "ctx", [(0, 1), (1, 0)])


def swap_x(value):
    count = lax.axis_size("fsdp")
    return lax.ppermute(value, "fsdp", [(i, i ^ 1) for i in range(count)])


def lines():
    count = lax.axis_size("fsdp")
    return [[i for i in range(count) if i % 2 == parity] for parity in (0, 1)]


def gather_line(value):
    return lax.all_gather(value, "fsdp", axis=0, tiled=True, axis_index_groups=lines())


def scatter_line(value):
    return lax.psum_scatter(
        value, "fsdp", scatter_dimension=0, tiled=True, axis_index_groups=lines()
    )


def neighbours():
    mine = lax.axis_index("fsdp")
    return (
        {"fsdp": mine + 1 - 2 * lax.rem(mine, 2)},
        {"ctx": 1 - lax.axis_index("ctx")},
        {"tp": 1 - lax.axis_index("tp")},
    )


def greet(peers):
    barrier = pltpu.get_barrier_semaphore()
    for peer in peers:
        pl.semaphore_signal(barrier, inc=1, device_id=peer, device_id_type=MESH)
    pl.semaphore_wait(barrier, len(peers))


def remote_params(number, limit=None):
    return pltpu.CompilerParams(
        collective_id=number, has_side_effects=True, vmem_limit_bytes=limit
    )


def gather8_kernel(rows, spread, *refs):
    if spread:
        own_ref, kept_ref, x_ref, y_ref, first_ref, second_ref, out_ref, also_ref = refs[:8]
        send_sem, recv_sem, local_sem, stage, also_send, also_recv, also_in, also_out = refs[8:]
    else:
        own_ref, out_ref, send_sem, recv_sem, local_sem = refs
    x_peer, y_peer, c_peer = neighbours()

    def start_of(away_t, half, outer, inner):
        return pl.ds((away_t * 8 + half * 4 + outer * 2 + inner) * rows, rows)

    def slot(*block):
        return out_ref.at[start_of(*block)]

    also_loads, also_remote, also_stores = [], [], []
    if spread:
        top, low = pl.ds(0, rows), pl.ds(rows, rows)
        pieces = [
            ((0, 0, 0), kept_ref.at[top]),
            ((0, 0, 1), x_ref.at[top]),
            ((0, 1, 0), y_ref.at[top]),
            ((0, 1, 1), first_ref),
            ((1, 0, 0), kept_ref.at[low]),
            ((1, 0, 1), y_ref.at[low]),
            ((1, 1, 0), x_ref.at[low]),
            ((1, 1, 1), second_ref),
        ]
        for index, (block, source) in enumerate(pieces):
            also_loads.append(pltpu.make_async_copy(source, stage.at[index], also_in.at[index]))
            also_stores.append(
                pltpu.make_async_copy(
                    stage.at[index], also_ref.at[start_of(0, *block)], also_out.at[index]
                )
            )
            also_remote.append(
                pltpu.make_async_remote_copy(
                    src_ref=source,
                    dst_ref=also_ref.at[start_of(1, *block)],
                    send_sem=also_send.at[index],
                    recv_sem=also_recv.at[index],
                    device_id=c_peer,
                    device_id_type=MESH,
                )
            )
        for copy in also_loads:
            copy.start()
    greet((x_peer, y_peer, c_peer))

    number = iter(range(14))

    def send(source, target, peer):
        index = next(number)
        copy = pltpu.make_async_remote_copy(
            src_ref=source,
            dst_ref=target,
            send_sem=send_sem.at[index],
            recv_sem=recv_sem.at[index],
            device_id=peer,
            device_id_type=MESH,
        )
        copy.start()
        return copy

    first, second = own_ref.at[pl.ds(0, rows)], own_ref.at[pl.ds(rows, rows)]
    x1 = send(first, slot(0, 0, 0, 1), x_peer)
    y1 = send(second, slot(0, 1, 0, 1), y_peer)
    x2 = send(second, slot(0, 1, 1, 0), x_peer)
    y2 = send(first, slot(0, 0, 1, 0), y_peer)
    rest = [send(first, slot(1, 0, 0, 0), c_peer), send(second, slot(1, 1, 0, 0), c_peer)]
    kept = [
        pltpu.make_async_copy(first, slot(0, 0, 0, 0), local_sem.at[0]),
        pltpu.make_async_copy(second, slot(0, 1, 0, 0), local_sem.at[1]),
    ]
    for copy in kept:
        copy.start()
    for copy in also_remote:
        copy.start()
    for load, store in zip(also_loads, also_stores):
        load.wait()
        store.start()
    x1.wait_recv()
    y3 = send(slot(0, 0, 0, 1), slot(0, 0, 1, 1), y_peer)
    y1.wait_recv()
    x3 = send(slot(0, 1, 0, 1), slot(0, 1, 1, 1), x_peer)
    rest.append(send(slot(0, 0, 0, 1), slot(1, 0, 0, 1), c_peer))
    rest.append(send(slot(0, 1, 0, 1), slot(1, 1, 0, 1), c_peer))
    x2.wait_recv()
    rest.append(send(slot(0, 1, 1, 0), slot(1, 1, 1, 0), c_peer))
    y2.wait_recv()
    rest.append(send(slot(0, 0, 1, 0), slot(1, 0, 1, 0), c_peer))
    y3.wait_recv()
    rest.append(send(slot(0, 0, 1, 1), slot(1, 0, 1, 1), c_peer))
    x3.wait_recv()
    rest.append(send(slot(0, 1, 1, 1), slot(1, 1, 1, 1), c_peer))
    for copy in (x1, y1, x2, y2, y3, x3):
        copy.wait_send()
    for copy in rest + also_remote + kept + also_stores:
        copy.wait()


def gather8_product_kernel(
    rows,
    own_ref,
    acts_ref,
    weight_ref,
    out_ref,
    kept_ref,
    to_y_ref,
    to_x_ref,
    send_sem,
    recv_sem,
    local_sem,
    acts,
    weight,
    far,
    core_in,
    core_send,
    core_recv,
    load_sem,
):
    x_peer, y_peer, c_peer = neighbours()
    width = weight.shape[0]
    wide = 2 * rows
    loads = [
        pltpu.make_async_copy(weight_ref, weight, load_sem.at[0]),
        pltpu.make_async_copy(acts_ref, acts, load_sem.at[1]),
    ]
    for copy in loads:
        copy.start()
    greet((x_peer, y_peer, c_peer))

    def slot(away_t, half, outer, inner):
        return out_ref.at[pl.ds((away_t * 8 + half * 4 + outer * 2 + inner) * rows, rows)]

    number = iter(range(14))

    def send(source, target, peer):
        index = next(number)
        copy = pltpu.make_async_remote_copy(
            src_ref=source,
            dst_ref=target,
            send_sem=send_sem.at[index],
            recv_sem=recv_sem.at[index],
            device_id=peer,
            device_id_type=MESH,
        )
        copy.start()
        return copy

    core_copies = []

    def far_chunk(index):
        place = pl.ds(index * wide, wide)
        source = pl.ds(4 * wide + index * wide, wide)

        def step(cols):
            far[place, cols] = mm(acts[source, :], weight[cols, :], 1, 1).astype(BF16)
            return 0

        tiled(width, width // 2, step)
        copy = pltpu.make_async_remote_copy(
            src_ref=far.at[place],
            dst_ref=core_in.at[place],
            send_sem=core_send.at[index],
            recv_sem=core_recv.at[index],
            device_id=c_peer,
            device_id_type=MESH,
        )
        copy.start()
        core_copies.append(copy)

    def near_chunk(index, target_ref, start):
        core_copies[index].wait_recv()
        place = pl.ds(index * wide, wide)
        target = pl.ds(start, wide)

        def step(cols):
            value = mm(acts[place, :], weight[cols, :], 1, 1) + core_in[place, cols].astype(F32)
            target_ref[target, cols] = value.astype(target_ref.dtype)
            return 0

        tiled(width, width // 2, step)

    first, second = own_ref.at[pl.ds(0, rows)], own_ref.at[pl.ds(rows, rows)]
    x1 = send(first, slot(0, 0, 0, 1), x_peer)
    y1 = send(second, slot(0, 1, 0, 1), y_peer)
    x2 = send(second, slot(0, 1, 1, 0), x_peer)
    y2 = send(first, slot(0, 0, 1, 0), y_peer)
    rest = [send(first, slot(1, 0, 0, 0), c_peer), send(second, slot(1, 1, 0, 0), c_peer)]
    kept = [
        pltpu.make_async_copy(first, slot(0, 0, 0, 0), local_sem.at[0]),
        pltpu.make_async_copy(second, slot(0, 1, 0, 0), local_sem.at[1]),
    ]
    for copy in kept:
        copy.start()
    for copy in loads:
        copy.wait()
    for index in range(4):
        far_chunk(index)
    x1.wait_recv()
    y3 = send(slot(0, 0, 0, 1), slot(0, 0, 1, 1), y_peer)
    y1.wait_recv()
    x3 = send(slot(0, 1, 0, 1), slot(0, 1, 1, 1), x_peer)
    rest.append(send(slot(0, 0, 0, 1), slot(1, 0, 0, 1), c_peer))
    rest.append(send(slot(0, 1, 0, 1), slot(1, 1, 0, 1), c_peer))
    near_chunk(0, kept_ref, 0)
    near_chunk(1, to_y_ref, 0)
    near_chunk(2, kept_ref, wide)
    near_chunk(3, to_x_ref, 0)
    x2.wait_recv()
    rest.append(send(slot(0, 1, 1, 0), slot(1, 1, 1, 0), c_peer))
    y2.wait_recv()
    rest.append(send(slot(0, 0, 1, 0), slot(1, 0, 1, 0), c_peer))
    y3.wait_recv()
    rest.append(send(slot(0, 0, 1, 1), slot(1, 0, 1, 1), c_peer))
    x3.wait_recv()
    rest.append(send(slot(0, 1, 1, 1), slot(1, 1, 1, 1), c_peer))
    for copy in (x1, y1, x2, y2, y3, x3):
        copy.wait_send()
    for copy in core_copies:
        copy.wait_send()
    for copy in rest + kept:
        copy.wait()


def gather8_product(own, acts, weight):
    rows, width = own.shape[0] // 2, own.shape[1]
    hbm = pl.BlockSpec(memory_space=pl.ANY)
    vmem = pl.BlockSpec(memory_space=pltpu.VMEM)
    return pl.pallas_call(
        functools.partial(gather8_product_kernel, rows),
        out_shape=[
            jax.ShapeDtypeStruct((16 * rows, width), own.dtype),
            jax.ShapeDtypeStruct((4 * rows, width), F32),
            jax.ShapeDtypeStruct((2 * rows, width), BF16),
            jax.ShapeDtypeStruct((2 * rows, width), BF16),
        ],
        in_specs=[vmem, hbm, hbm],
        out_specs=[hbm, vmem, vmem, vmem],
        scratch_shapes=[
            pltpu.SemaphoreType.DMA((14,)),
            pltpu.SemaphoreType.DMA((14,)),
            pltpu.SemaphoreType.DMA((2,)),
            pltpu.VMEM(acts.shape, BF16),
            pltpu.VMEM(weight.shape, BF16),
            pltpu.VMEM((8 * rows, width), BF16),
            pltpu.VMEM((8 * rows, width), BF16),
            pltpu.SemaphoreType.DMA((4,)),
            pltpu.SemaphoreType.DMA((4,)),
            pltpu.SemaphoreType.DMA((2,)),
        ],
        compiler_params=remote_params(9, 48 * 1024 * 1024),
        cost_estimate=pl.CostEstimate(
            flops=2 * acts.size * width, bytes_accessed=16 * own.size, transcendentals=0
        ),
        name="gather8_product",
    )(own, acts, weight)


def gather8(own, also=()):
    rows, width = own.shape[0] // 2, own.shape[1]
    hbm = pl.BlockSpec(memory_space=pl.ANY)
    whole_shape = jax.ShapeDtypeStruct((16 * rows, width), own.dtype)
    sems = [
        pltpu.SemaphoreType.DMA((14,)),
        pltpu.SemaphoreType.DMA((14,)),
        pltpu.SemaphoreType.DMA((2,)),
    ]
    if also:
        sems += [pltpu.VMEM((8, rows, width), own.dtype)] + [pltpu.SemaphoreType.DMA((8,))] * 4
    outs = pl.pallas_call(
        functools.partial(gather8_kernel, rows, bool(also)),
        out_shape=[whole_shape] * (2 if also else 1),
        in_specs=[pl.BlockSpec(memory_space=pltpu.VMEM)] + [hbm] * len(also),
        out_specs=[hbm] * (2 if also else 1),
        scratch_shapes=sems,
        compiler_params=remote_params(6 if also else 1),
        name="gather8_also" if also else "gather8",
    )(own, *also)
    return outs if also else outs[0]


def reduce8_kernel(
    rows,
    near_ref,
    far_ref,
    out_ref,
    near,
    core_in,
    link_in,
    link_out,
    send_sem,
    recv_sem,
    local_sem,
):
    x_peer, y_peer, c_peer = neighbours()
    greet((x_peer, y_peer, c_peer))
    order = [(h, o, i) for o, i in ((1, 1), (1, 0), (0, 1), (0, 0)) for h in (0, 1)]
    core_copies, local_copies = {}, {}
    for number, (half, outer, inner) in enumerate(order):
        place = pl.ds((half * 4 + outer * 2 + inner) * rows, rows)
        core_copies[half, outer, inner] = pltpu.make_async_remote_copy(
            src_ref=far_ref.at[place],
            dst_ref=core_in.at[place],
            send_sem=send_sem.at[number],
            recv_sem=recv_sem.at[number],
            device_id=c_peer,
            device_id_type=MESH,
        )
        local_copies[half, outer, inner] = pltpu.make_async_copy(
            near_ref.at[place], near.at[place], local_sem.at[number]
        )
    for block in order:
        core_copies[block].start()
        local_copies[block].start()

    def partial_sum(block):
        half, outer, inner = block
        place = pl.ds((half * 4 + outer * 2 + inner) * rows, rows)
        core_copies[block].wait_recv()
        local_copies[block].wait()
        return near[place, :] + core_in[place, :].astype(F32)

    def link(index, value, peer):
        link_out[index] = value.astype(BF16)
        copy = pltpu.make_async_remote_copy(
            src_ref=link_out.at[index],
            dst_ref=link_in.at[index],
            send_sem=send_sem.at[8 + index],
            recv_sem=recv_sem.at[8 + index],
            device_id=peer,
            device_id_type=MESH,
        )
        copy.start()
        return copy

    y11 = link(0, partial_sum((0, 1, 1)), y_peer)
    x11 = link(1, partial_sum((1, 1, 1)), x_peer)
    y10 = link(2, partial_sum((0, 1, 0)), y_peer)
    x10 = link(3, partial_sum((1, 1, 0)), x_peer)
    first01, second01 = partial_sum((0, 0, 1)), partial_sum((1, 0, 1))
    y11.wait_recv()
    x01 = link(4, first01 + link_in[0].astype(F32), x_peer)
    x11.wait_recv()
    y01 = link(5, second01 + link_in[1].astype(F32), y_peer)
    first = partial_sum((0, 0, 0))
    second = partial_sum((1, 0, 0))
    y10.wait_recv()
    out_ref[pl.ds(0, rows), :] = first + link_in[2].astype(F32)
    x10.wait_recv()
    out_ref[pl.ds(rows, rows), :] = second + link_in[3].astype(F32)
    x01.wait_recv()
    out_ref[pl.ds(0, rows), :] += link_in[4].astype(F32)
    y01.wait_recv()
    out_ref[pl.ds(rows, rows), :] += link_in[5].astype(F32)
    for copy in (y11, x11, y10, x10, x01, y01):
        copy.wait_send()
    for copy in core_copies.values():
        copy.wait_send()


def reduce8(near, far):
    rows, width = near.shape[0] // 8, near.shape[1]
    return pl.pallas_call(
        functools.partial(reduce8_kernel, rows),
        out_shape=jax.ShapeDtypeStruct((2 * rows, width), F32),
        in_specs=[pl.BlockSpec(memory_space=pl.ANY), pl.BlockSpec(memory_space=pl.ANY)],
        out_specs=pl.BlockSpec(memory_space=pltpu.VMEM),
        scratch_shapes=[
            pltpu.VMEM(near.shape, F32),
            pltpu.VMEM(near.shape, BF16),
            pltpu.VMEM((6, rows, width), BF16),
            pltpu.VMEM((6, rows, width), BF16),
            pltpu.SemaphoreType.DMA((14,)),
            pltpu.SemaphoreType.DMA((14,)),
            pltpu.SemaphoreType.DMA((8,)),
        ],
        compiler_params=remote_params(2, 48 * 1024 * 1024),
        name="reduce8",
    )(near, far)


def tiled(count, tile, step):
    lax.fori_loop(0, count // tile, lambda i, _: step(pl.ds(pl.multiple_of(i * tile, tile), tile)), 0)


def product_reduce8_kernel(rows, groups, filler, *refs):
    acts_refs, refs = refs[:groups], refs[groups:]
    if filler:
        weight_ref, lhs_ref, out_ref, grad_ref, *refs = refs
    else:
        weight_ref, out_ref, *refs = refs
    acts, weight, far, near, core_in, link_in, link_out, send_sem, recv_sem, load_sem, *refs = refs
    x_peer, y_peer, c_peer = neighbours()
    width = weight.shape[0]
    wide = 2 * rows
    chunks = [(0, 1), (1, 1), (0, 0), (1, 0)]

    def where(chunk):
        return chunk[0] * 2 * wide + chunk[1] * wide

    half = width // 2
    load_weights = [
        pltpu.make_async_copy(
            weight_ref.at[pl.ds(part * half, half), pl.ds(0, weight.shape[1])],
            weight.at[pl.ds(part * half, half)],
            load_sem.at[part],
        )
        for part in (0, 1)
    ]
    loads = {}
    depth = weight.shape[1] // groups
    for number, chunk in enumerate(chunks):
        for side in (1, 0):
            place = pl.ds(side * 4 * wide + where(chunk), wide)
            loads[side, chunk] = [
                pltpu.make_async_copy(
                    acts_refs[group].at[place],
                    acts.at[place, pl.ds(group * depth, depth)],
                    load_sem.at[3 + (2 * number + side) * groups + group],
                )
                for group in range(groups)
            ]
    started = [loads[1, chunks[0]], [load_weights[0]], loads[1, chunks[1]], loads[0, chunks[0]]]
    started += [loads[0, chunks[1]], [load_weights[1]]]
    started += [loads[side, chunk] for chunk in chunks[2:] for side in (1, 0)]
    for group in started:
        for copy in group:
            copy.start()
    if filler:
        lhs, grad, grad_sem = refs
        load_lhs = pltpu.make_async_copy(lhs_ref, lhs, load_sem.at[2])
        load_lhs.start()
    greet((x_peer, y_peer, c_peer))

    core_copies, link_copies = {}, {}

    def product(chunk, side, part, target):
        place = pl.ds(where(chunk), wide)
        source = pl.ds(side * 4 * wide + where(chunk), wide)

        cols = pl.ds(part * half, half)
        target[place, cols] = mm(acts[source, :], weight[cols, :], 1, 1).astype(target.dtype)

    def remote(copies, key, number, source, target, peer):
        copies[key] = pltpu.make_async_remote_copy(
            src_ref=source,
            dst_ref=target,
            send_sem=send_sem.at[number],
            recv_sem=recv_sem.at[number],
            device_id=peer,
            device_id_type=MESH,
        )
        copies[key].start()

    def send_core(chunk, part):
        product(chunk, 1, part, far)
        here = (pl.ds(where(chunk), wide), pl.ds(part * half, half))
        number = 2 * chunks.index(chunk) + part
        remote(core_copies, (chunk, part), number, far.at[here], core_in.at[here], c_peer)

    def partial_sum(chunk, start, size, part):
        here = (pl.ds(where(chunk) + start, size), pl.ds(part * half, half))
        return near[here] + core_in[here].astype(F32)

    def link(hop, side, part, value, peer):
        size = value.shape[0]
        start = (side * 3 + hop * 2) * rows
        here = (pl.ds(start, size), pl.ds(part * half, half))
        link_out[here] = value.astype(BF16)
        number = 8 + hop * 4 + side * 2 + part
        remote(link_copies, (hop, side, part), number, link_out.at[here], link_in.at[here], peer)

    def came(hop, side, start, part):
        return link_in[
            pl.ds((side * 3 + hop * 2) * rows + start, rows), pl.ds(part * half, half)
        ].astype(F32)

    for chunk in chunks[:2]:
        for copy in loads[1, chunk]:
            copy.wait()
    for part in (0, 1):
        load_weights[part].wait()
        send_core((0, 1), part)
        send_core((1, 1), part)
        for side, peer in ((0, y_peer), (1, x_peer)):
            if part == 0:
                for copy in loads[0, (side, 1)]:
                    copy.wait()
            product((side, 1), 0, part, near)
            core_copies[(side, 1), part].wait_recv()
            link(0, side, part, partial_sum((side, 1), 0, wide, part), peer)
    for chunk in chunks[2:]:
        for side in (1, 0):
            for copy in loads[side, chunk]:
                copy.wait()
    if filler:
        size = width // 4

        def fill(index, _):
            cols = pl.ds(pl.multiple_of(index * size, size), size)

            def step(columns):
                grad[cols, columns] = mm(lhs[:, cols], acts[:, columns], 0, 0).astype(BF16)
                return 0

            tiled(acts.shape[1], acts.shape[1] // 3, step)
            return 0

    for part in (0, 1):
        for chunk in chunks[2:]:
            send_core(chunk, part)
        for chunk in chunks[2:]:
            product(chunk, 0, part, near)
        for side, peer in ((0, x_peer), (1, y_peer)):
            core_copies[(side, 0), part].wait_recv()
            link_copies[0, side, part].wait_recv()
            link(1, side, part, partial_sum((side, 0), rows, rows, part) + came(0, side, rows, part), peer)
        if filler and part == 0:
            load_lhs.wait()
            lax.fori_loop(0, 1, fill, 0)
    if filler:
        lax.fori_loop(1, 4, fill, 0)
        grad_copy = pltpu.make_async_copy(grad, grad_ref, grad_sem.at[0])
        grad_copy.start()
    for side in (0, 1):
        for part in (0, 1):
            place = (pl.ds(side * rows, rows), pl.ds(part * half, half))
            kept = partial_sum((side, 0), 0, rows, part) + came(0, side, 0, part)
            link_copies[1, side, part].wait_recv()
            out_ref[place] = kept + came(1, side, 0, part)
    for copy in list(link_copies.values()) + list(core_copies.values()):
        copy.wait_send()
    if filler:
        grad_copy.wait()


def product_reduce8(columns, weight, number, lhs=None):
    depth, groups = sum(column.shape[1] for column in columns), len(columns)
    acts = jax.ShapeDtypeStruct((columns[0].shape[0], depth), BF16)
    rows, width = acts.shape[0] // 16, weight.shape[0]
    filler = lhs is not None
    hbm = pl.BlockSpec(memory_space=pl.ANY)
    scratch = [
        pltpu.VMEM(acts.shape, BF16),
        pltpu.VMEM((width, depth), BF16),
        pltpu.VMEM((8 * rows, width), BF16),
        pltpu.VMEM((8 * rows, width), F32),
        pltpu.VMEM((8 * rows, width), BF16),
        pltpu.VMEM((6 * rows, width), BF16),
        pltpu.VMEM((6 * rows, width), BF16),
        pltpu.SemaphoreType.DMA((16,)),
        pltpu.SemaphoreType.DMA((16,)),
        pltpu.SemaphoreType.DMA((3 + 8 * groups,)),
    ]
    out_shape = [jax.ShapeDtypeStruct((2 * rows, width), F32)]
    out_specs = [pl.BlockSpec(memory_space=pltpu.VMEM)]
    flops = 2 * acts.shape[0] * width * depth
    if filler:
        scratch += [
            pltpu.VMEM(lhs.shape, BF16),
            pltpu.VMEM((width, depth), BF16),
            pltpu.SemaphoreType.DMA((1,)),
        ]
        out_shape.append(jax.ShapeDtypeStruct((width, depth), BF16))
        out_specs.append(hbm)
        flops *= 2
    outs = pl.pallas_call(
        functools.partial(product_reduce8_kernel, rows, groups, filler),
        out_shape=out_shape,
        in_specs=[hbm] * (groups + (2 if filler else 1)),
        out_specs=out_specs,
        scratch_shapes=scratch,
        compiler_params=remote_params(number, 63 * 1024 * 1024),
        cost_estimate=pl.CostEstimate(
            flops=flops, bytes_accessed=4 * depth * (acts.shape[0] + width), transcendentals=0
        ),
        name="product_reduce8",
    )(*columns, weight, *((lhs,) if filler else ()))
    return outs if filler else outs[0]


def shard_copies(plan, ins, out_refs, stage, sems):
    send_sem, recv_sem, load_sem, store_sem = sems
    x_peer, _, _ = neighbours()
    odd = lax.rem(lax.axis_index("fsdp"), 2)
    column = 2 * lax.axis_index("ctx") + odd
    other = 2 * lax.axis_index("ctx") + 1 - odd
    remote, loads, stores = [], [], []
    for number, (which, start, size) in enumerate(plan):
        rows = ins[number].shape[0]
        place = pl.ds(pl.multiple_of(odd * rows, rows), rows)
        target = out_refs[which].at[place, pl.ds(start, size)]

        def source(index, ref=ins[number], size=size):
            return ref.at[:, pl.ds(pl.multiple_of(index * size, HEAD), size)]

        remote.append(
            pltpu.make_async_remote_copy(
                src_ref=source(other),
                dst_ref=target,
                send_sem=send_sem.at[number],
                recv_sem=recv_sem.at[number],
                device_id=x_peer,
                device_id_type=MESH,
            )
        )
        loads.append(pltpu.make_async_copy(source(column), stage[number], load_sem.at[number]))
        stores.append(pltpu.make_async_copy(stage[number], target, store_sem.at[number]))
    return remote, loads, stores


def shard_plan(groups):
    plan, arrays, shapes = [], [], []
    for which, group in enumerate(groups):
        start = 0
        for array in group:
            size = array.shape[1] // 4
            plan.append((which, start, size))
            arrays.append(array)
            start += size
        shapes.append(jax.ShapeDtypeStruct((2 * group[0].shape[0], start), BF16))
    return tuple(plan), arrays, shapes


def shard_scratch(plan, arrays):
    return [
        pltpu.VMEM((array.shape[0], size), BF16) for array, (_, _, size) in zip(arrays, plan)
    ] + [pltpu.SemaphoreType.DMA((len(plan),))] * 4


def bit_peer(axis, bit):
    mine = lax.axis_index(axis)
    return {axis: mine + bit * (1 - 2 * lax.rem(mine // bit, 2))}


def sum_over(stages, value, inbox, outbox, send_sem, recv_sem):
    copies = []
    for index, (axis, bit) in enumerate(stages):
        outbox[index] = value
        copy = pltpu.make_async_remote_copy(
            src_ref=outbox.at[index],
            dst_ref=inbox.at[index],
            send_sem=send_sem.at[index],
            recv_sem=recv_sem.at[index],
            device_id=bit_peer(axis, bit),
            device_id_type=MESH,
        )
        copy.start()
        copies.append(copy)
        copy.wait_recv()
        value = value + inbox[index]
    return value, copies


def fsdp_stages():
    stages, bit = [], 2
    while bit < lax.axis_size("fsdp"):
        stages.append(("fsdp", bit))
        bit *= 2
    return stages


def first_kernel(plan, stages, *refs):
    count = len(plan)
    ins, row_ref, out_ref, gain_ref = refs[:count], refs[count], refs[count + 1], refs[count + 2]
    stage, sems = refs[count + 3 : 2 * count + 3], refs[2 * count + 3 : 2 * count + 7]
    inbox, outbox, gain_send, gain_recv = refs[2 * count + 7 :]
    remote, loads, stores = shard_copies(plan, ins, [out_ref], stage, sems)
    for copy in loads:
        copy.start()
    greet([bit_peer(axis, bit) for axis, bit in stages])
    for copy in remote:
        copy.start()
    for load, store in zip(loads, stores):
        load.wait()
        store.start()
    member = lax.broadcasted_iota(jnp.int32, gain_ref.shape, 0)
    value = jnp.where(
        member == lax.axis_index("fsdp"), jnp.broadcast_to(row_ref[...], gain_ref.shape), 0.0
    )
    value, copies = sum_over(stages, value, inbox, outbox, gain_send, gain_recv)
    gain_ref[...] = value
    for copy in copies:
        copy.wait_send()
    for copy in stores + remote:
        copy.wait()


def first_shards(arrays, row, count):
    plan, arrays, shapes = shard_plan([arrays])
    stages = fsdp_stages() + [("fsdp", 1)]
    hbm = pl.BlockSpec(memory_space=pl.ANY)
    vmem = pl.BlockSpec(memory_space=pltpu.VMEM)
    gains = jax.ShapeDtypeStruct((count, row.shape[1]), F32)
    box = pltpu.VMEM((len(stages),) + gains.shape, F32)
    sem = pltpu.SemaphoreType.DMA((len(stages),))
    return pl.pallas_call(
        functools.partial(first_kernel, plan, tuple(stages)),
        out_shape=shapes + [gains],
        in_specs=[hbm] * len(arrays) + [vmem],
        out_specs=[hbm, vmem],
        scratch_shapes=shard_scratch(plan, arrays) + [box, box, sem, sem],
        compiler_params=remote_params(3),
        name="first_shards",
    )(*arrays, row)


def second_kernel(plan, outs, rows, *refs):
    count = len(plan)
    ins, token_ref, out_ref = refs[:count], refs[count], refs[count + 1]
    pair_refs, refs = refs[count + 2 : count + 2 + outs], refs[count + 2 + outs :]
    stage, sems = refs[:count], refs[count : count + 4]
    own, own_sem, send_sem, recv_sem, local_sem = refs[count + 4 :]
    x_peer, y_peer, c_peer = neighbours()
    core = lax.axis_index("tp")
    load_own = pltpu.make_async_copy(
        token_ref.at[pl.ds(pl.multiple_of(core * 2 * rows, 2 * rows), 2 * rows)], own, own_sem
    )
    load_own.start()
    remote, loads, stores = shard_copies(plan, ins, pair_refs, stage, sems)
    for copy in loads:
        copy.start()
    load_own.wait()
    greet((x_peer, y_peer, c_peer))

    def slot(away_t, half, outer, inner):
        return out_ref.at[pl.ds((away_t * 8 + half * 4 + outer * 2 + inner) * rows, rows)]

    number = iter(range(14))

    def send(source, target, peer):
        index = next(number)
        copy = pltpu.make_async_remote_copy(
            src_ref=source,
            dst_ref=target,
            send_sem=send_sem.at[index],
            recv_sem=recv_sem.at[index],
            device_id=peer,
            device_id_type=MESH,
        )
        copy.start()
        return copy

    first, second = own.at[pl.ds(0, rows)], own.at[pl.ds(rows, rows)]
    x1 = send(first, slot(0, 0, 0, 1), x_peer)
    y1 = send(second, slot(0, 1, 0, 1), y_peer)
    x2 = send(second, slot(0, 1, 1, 0), x_peer)
    y2 = send(first, slot(0, 0, 1, 0), y_peer)
    rest = [send(first, slot(1, 0, 0, 0), c_peer), send(second, slot(1, 1, 0, 0), c_peer)]
    kept = [
        pltpu.make_async_copy(first, slot(0, 0, 0, 0), local_sem.at[0]),
        pltpu.make_async_copy(second, slot(0, 1, 0, 0), local_sem.at[1]),
    ]
    for copy in kept:
        copy.start()
    for load, store in zip(loads, stores):
        load.wait()
        store.start()
    x1.wait_recv()
    y3 = send(slot(0, 0, 0, 1), slot(0, 0, 1, 1), y_peer)
    y1.wait_recv()
    x3 = send(slot(0, 1, 0, 1), slot(0, 1, 1, 1), x_peer)
    for copy in remote:
        copy.start()
    rest.append(send(slot(0, 0, 0, 1), slot(1, 0, 0, 1), c_peer))
    rest.append(send(slot(0, 1, 0, 1), slot(1, 1, 0, 1), c_peer))
    x2.wait_recv()
    rest.append(send(slot(0, 1, 1, 0), slot(1, 1, 1, 0), c_peer))
    y2.wait_recv()
    rest.append(send(slot(0, 0, 1, 0), slot(1, 0, 1, 0), c_peer))
    y3.wait_recv()
    rest.append(send(slot(0, 0, 1, 1), slot(1, 0, 1, 1), c_peer))
    x3.wait_recv()
    rest.append(send(slot(0, 1, 1, 1), slot(1, 1, 1, 1), c_peer))
    for copy in (x1, y1, x2, y2, y3, x3):
        copy.wait_send()
    for copy in rest + kept + stores + remote:
        copy.wait()


def second_shards(groups, tokens):
    plan, arrays, shapes = shard_plan(groups)
    rows, width = tokens.shape[0] // 4, tokens.shape[1]
    hbm = pl.BlockSpec(memory_space=pl.ANY)
    return pl.pallas_call(
        functools.partial(second_kernel, plan, len(groups), rows),
        out_shape=[jax.ShapeDtypeStruct((16 * rows, width), tokens.dtype)] + shapes,
        in_specs=[hbm] * (len(arrays) + 1),
        out_specs=[hbm] * (len(groups) + 1),
        scratch_shapes=shard_scratch(plan, arrays)
        + [
            pltpu.VMEM((2 * rows, width), tokens.dtype),
            pltpu.SemaphoreType.DMA,
            pltpu.SemaphoreType.DMA((14,)),
            pltpu.SemaphoreType.DMA((14,)),
            pltpu.SemaphoreType.DMA((2,)),
        ],
        compiler_params=remote_params(4),
        name="second_shards",
    )(*arrays, tokens)


def total_kernel(stages, part_ref, out_ref, inbox, outbox, send_sem, recv_sem):
    greet([bit_peer(axis, bit) for axis, bit in stages])
    value, copies = sum_over(stages, part_ref[...], inbox, outbox, send_sem, recv_sem)
    out_ref[...] = value
    for copy in copies:
        copy.wait_send()


def total(part):
    stages = fsdp_stages() + [("tp", 1), ("fsdp", 1)]
    return pl.pallas_call(
        functools.partial(total_kernel, tuple(stages)),
        out_shape=jax.ShapeDtypeStruct(part.shape, F32),
        in_specs=[pl.BlockSpec(memory_space=pltpu.VMEM)],
        out_specs=pl.BlockSpec(memory_space=pltpu.VMEM),
        scratch_shapes=[
            pltpu.VMEM((len(stages),) + part.shape, F32),
            pltpu.VMEM((len(stages),) + part.shape, F32),
            pltpu.SemaphoreType.DMA((len(stages),)),
            pltpu.SemaphoreType.DMA((len(stages),)),
        ],
        compiler_params=remote_params(5),
        name="total",
    )(part)


def stack_kernel(spot_ref, own_ref, other_ref, out_ref):
    @pl.when(pl.program_id(0) == 0)
    def _():
        out_ref[...] = own_ref[...]

    @pl.when(pl.program_id(0) == 1)
    def _():
        out_ref[...] = other_ref[...]


def stack_rows(spot, own, other):
    block = pl.BlockSpec(own.shape, lambda i, spot: (0, 0))
    return pl.pallas_call(
        stack_kernel,
        out_shape=jax.ShapeDtypeStruct((2 * own.shape[0], own.shape[1]), own.dtype),
        grid_spec=pltpu.PrefetchScalarGridSpec(
            num_scalar_prefetch=1,
            grid=(2,),
            in_specs=[block, block],
            out_specs=pl.BlockSpec(own.shape, lambda i, spot: (lax.rem(spot[1] + i, 2), 0)),
        ),
        name="stack",
    )(spot, own, other)


def join_kernel(sizes, spot_ref, kept_ref, x_ref, y_ref, both_ref, *out_refs):
    place, odd = spot_ref[0], spot_ref[1]
    parts = (
        (kept_ref, 2 * place + odd),
        (x_ref, 2 * place + 1 - odd),
        (y_ref, 2 - 2 * place + odd),
        (both_ref, 3 - 2 * place - odd),
    )
    for part, column in parts:
        start = 0
        for size, out_ref in zip(sizes, out_refs):
            target = pl.ds(pl.multiple_of(column * size, HEAD), size)
            out_ref[:, target] = part[:, start : start + size].astype(F32)
            start += size


def join_columns(spot, parts, sizes):
    rows = parts[0].shape[0]
    tile = min(rows, 64)
    return pl.pallas_call(
        functools.partial(join_kernel, sizes),
        out_shape=[jax.ShapeDtypeStruct((rows, 4 * size), F32) for size in sizes],
        grid_spec=pltpu.PrefetchScalarGridSpec(
            num_scalar_prefetch=1,
            grid=(rows // tile,),
            in_specs=[
                pl.BlockSpec((tile, part.shape[1]), lambda i, spot: (i, 0)) for part in parts
            ],
            out_specs=[pl.BlockSpec((tile, 4 * size), lambda i, spot: (i, 0)) for size in sizes],
        ),
        name="join",
    )(spot, *parts)


def after(value, *others):
    return lax.optimization_barrier((value,) + others)[0]


def reduce4_links(kept, to_y, to_x, *others):
    rows = kept.shape[0] // 4
    came_first, came_second = swap_ctx(to_y), swap_x(to_x)
    first = kept[: 2 * rows] + after(came_first, *others).astype(F32)
    second = kept[2 * rows :] + after(came_second, *others).astype(F32)
    came_first = swap_x(first[rows:].astype(BF16))
    came_second = swap_ctx(second[rows:].astype(BF16))
    return first[:rows], second[:rows], came_first, came_second


def rope_tables(positions):
    freqs = THETA ** (-(jnp.arange(HEAD // 2, dtype=F32) * 2.0) / HEAD)
    angle = positions[:, None] * freqs[None, :]
    cosine = jnp.concatenate([jnp.cos(angle), jnp.cos(angle)], axis=-1)
    sine = jnp.concatenate([-jnp.sin(angle), jnp.sin(angle)], axis=-1)
    return cosine, sine


def norm_back(grad, scaled, inverse, gain):
    weighted = grad * gain
    return inverse * (weighted - scaled * jnp.mean(weighted * scaled, axis=-1, keepdims=True))


def inv_rms(value):
    return lax.rsqrt(jnp.mean(value * value, axis=-1, keepdims=True) + EPS)


def block_row(meta_ref, seq, index, rows):
    away_c = lax.rem(meta_ref[0] + index // 4, 2)
    away_t = lax.rem(meta_ref[1] + (index // 2) % 2, 2)
    if index % 2 == 0:
        inner = away_c * 2 + seq
    else:
        inner = seq * 2 + away_c + 4
    return pl.multiple_of((away_t * 8 + inner) * rows, rows)


def scaled_of(raw):
    inverse = lax.rsqrt(jnp.mean(raw * raw, axis=-1, keepdims=True) + EPS)
    return raw * inverse, inverse


def load_heads(meta_ref, qkv_ref, cos_ref, sin_ref, gain_ref, q_scr, k_scr, v_scr, heads):
    seq = pl.program_id(0)
    rows = q_scr.shape[1] // 8
    for index in range(8):
        start = block_row(meta_ref, seq, index, rows)
        here = slice(index * rows, (index + 1) * rows)
        cosine, sine = cos_ref[here, :], sin_ref[here, :]
        for head in range(heads + 1):
            raw = qkv_ref[pl.ds(start, rows), head * HEAD : (head + 1) * HEAD]
            scaled, _ = scaled_of(raw)
            which = 0 if head < heads else 1
            value = scaled * gain_ref[which : which + 1, :]
            turned = value * cosine + pltpu.roll(value, HEAD // 2, 1) * sine
            if head < heads:
                q_scr[head, here, :] = turned.astype(BF16)
            else:
                k_scr[here, :] = turned.astype(BF16)
        v_scr[here, :] = qkv_ref[
            pl.ds(start, rows), (heads + 1) * HEAD : (heads + 2) * HEAD
        ].astype(BF16)


def key_span(index, tile):
    low = max(0, (index * tile - (MOST_DOC - 1)) // tile) * tile
    return low, (index + 1) * tile


def allowed_mask(segc_ref, segr_ref, index, tile):
    low, high = key_span(index, tile)
    shape = (tile, high - low)
    rows = lax.broadcasted_iota(jnp.int32, shape, 0) + index * tile
    cols = lax.broadcasted_iota(jnp.int32, shape, 1) + low
    same = segc_ref[0, index * tile : (index + 1) * tile, :] == segr_ref[0, :, low:high]
    return same & (cols <= rows)


def probs_of(query, keys, allowed, scale):
    scores = jnp.where(allowed, mm(query, keys, 1, 1) * scale, MASKED)
    weights = jnp.exp(scores - jnp.max(scores, axis=-1, keepdims=True))
    return weights * (1.0 / jnp.sum(weights, axis=-1, keepdims=True))


def attend_kernel(
    heads, tile, meta_ref, qkv_ref, segc_ref, segr_ref, cos_ref, sin_ref, gain_ref, out_ref, q_scr, k_scr, v_scr
):
    seq = pl.program_id(0)
    length = k_scr.shape[0]
    rows = length // 8
    scale = 1.0 / math.sqrt(HEAD)
    load_heads(meta_ref, qkv_ref, cos_ref, sin_ref, gain_ref, q_scr, k_scr, v_scr, heads)
    for index in range(length // tile):
        low, high = key_span(index, tile)
        allowed = allowed_mask(segc_ref, segr_ref, index, tile)
        for head in range(heads):
            query = q_scr[head, index * tile : (index + 1) * tile, :]
            probs = probs_of(query, k_scr[low:high, :], allowed, scale)
            mixed = mm(probs.astype(BF16), v_scr[low:high, :], 1, 0).astype(BF16)
            for piece in range(tile // rows):
                start = block_row(meta_ref, seq, index * (tile // rows) + piece, rows)
                out_ref[pl.ds(start, rows), head * HEAD : (head + 1) * HEAD] = mixed[
                    piece * rows : (piece + 1) * rows
                ]


def attend_back_kernel(
    heads,
    tile,
    meta_ref,
    qkv_ref,
    grad_ref,
    segc_ref,
    segr_ref,
    cos_ref,
    sin_ref,
    gain_ref,
    out_ref,
    gain_out_ref,
    q_scr,
    k_scr,
    v_scr,
    g_scr,
    dk_scr,
    dv_scr,
):
    seq = pl.program_id(0)
    length = k_scr.shape[0]
    rows = length // 8
    scale = 1.0 / math.sqrt(HEAD)
    load_heads(meta_ref, qkv_ref, cos_ref, sin_ref, gain_ref, q_scr, k_scr, v_scr, heads)
    for index in range(8):
        start = block_row(meta_ref, seq, index, rows)
        g_scr[index * rows : (index + 1) * rows, :] = grad_ref[pl.ds(start, rows), :]
    dk_scr[...] = jnp.zeros_like(dk_scr)
    dv_scr[...] = jnp.zeros_like(dv_scr)

    @pl.when(seq == 0)
    def _():
        gain_out_ref[...] = jnp.zeros_like(gain_out_ref)

    def finish(grad, index, head, which):
        here = slice(index * rows, (index + 1) * rows)
        start = block_row(meta_ref, seq, index, rows)
        grad = grad * cos_ref[here, :] - pltpu.roll(grad, HEAD // 2, 1) * sin_ref[here, :]
        raw = qkv_ref[pl.ds(start, rows), head * HEAD : (head + 1) * HEAD]
        scaled, inverse = scaled_of(raw)
        gain_out_ref[which : which + 1, :] += jnp.sum(grad * scaled, axis=0, keepdims=True)
        out = norm_back(grad, scaled, inverse, gain_ref[which : which + 1, :])
        out_ref[pl.ds(start, rows), head * HEAD : (head + 1) * HEAD] = out.astype(BF16)

    per = tile // rows
    for index in range(length // tile):
        low, high = key_span(index, tile)
        mine = slice(index * tile, (index + 1) * tile)
        allowed = allowed_mask(segc_ref, segr_ref, index, tile)
        for head in range(heads):
            query = q_scr[head, mine, :]
            keys = k_scr[low:high, :]
            probs = probs_of(query, keys, allowed, scale)
            grad = g_scr[mine, head * HEAD : (head + 1) * HEAD]
            grad_probs = mm(grad, v_scr[low:high, :], 1, 1)
            delta = jnp.sum(probs * grad_probs, axis=-1, keepdims=True)
            grad_scores = (probs * (grad_probs - delta)).astype(BF16)
            dv_scr[low:high, :] += mm(probs.astype(BF16), grad, 0, 0)
            dk_scr[low:high, :] += mm(grad_scores, query, 0, 0) * scale
            grad_query = mm(grad_scores, keys, 1, 0) * scale
            for piece in range(per):
                finish(
                    grad_query[piece * rows : (piece + 1) * rows], index * per + piece, head, 0
                )
    for index in range(8):
        here = slice(index * rows, (index + 1) * rows)
        start = block_row(meta_ref, seq, index, rows)
        finish(dk_scr[here, :], index, heads, 1)
        out_ref[pl.ds(start, rows), (heads + 1) * HEAD : (heads + 2) * HEAD] = dv_scr[
            here, :
        ].astype(BF16)


def whole(shape):
    return pl.BlockSpec(shape, lambda seq, meta: (0,) * len(shape))


def seg_specs(length):
    return [
        pl.BlockSpec((1, length, 1), lambda seq, meta: (seq, 0, 0)),
        pl.BlockSpec((1, 1, length), lambda seq, meta: (seq, 0, 0)),
    ]


def attend(meta, qkv, seg_cols, seg_rows, cosine, sine, gains):
    length = cosine.shape[0]
    tile = length // 4
    heads = qkv.shape[1] // HEAD - 2
    pairs = 2 * heads * length * length // 2
    return pl.pallas_call(
        functools.partial(attend_kernel, heads, tile),
        out_shape=jax.ShapeDtypeStruct((qkv.shape[0], heads * HEAD), BF16),
        grid_spec=pltpu.PrefetchScalarGridSpec(
            num_scalar_prefetch=1,
            grid=(2,),
            in_specs=[whole(qkv.shape)]
            + seg_specs(length)
            + [whole(cosine.shape), whole(sine.shape), whole(gains.shape)],
            out_specs=whole((qkv.shape[0], heads * HEAD)),
            scratch_shapes=[
                pltpu.VMEM((heads, length, HEAD), BF16),
                pltpu.VMEM((length, HEAD), BF16),
                pltpu.VMEM((length, HEAD), BF16),
            ],
        ),
        cost_estimate=pl.CostEstimate(
            flops=4 * pairs * HEAD, bytes_accessed=qkv.size * 4 + qkv.size, transcendentals=pairs
        ),
        name="attend",
    )(meta, qkv, seg_cols, seg_rows, cosine, sine, gains)


def attend_back(meta, qkv, grad, seg_cols, seg_rows, cosine, sine, gains):
    length = cosine.shape[0]
    tile = length // 4
    heads = qkv.shape[1] // HEAD - 2
    pairs = 2 * heads * length * length // 2
    return pl.pallas_call(
        functools.partial(attend_back_kernel, heads, tile),
        out_shape=(
            jax.ShapeDtypeStruct(qkv.shape, BF16),
            jax.ShapeDtypeStruct(gains.shape, F32),
        ),
        grid_spec=pltpu.PrefetchScalarGridSpec(
            num_scalar_prefetch=1,
            grid=(2,),
            in_specs=[whole(qkv.shape), whole(grad.shape)]
            + seg_specs(length)
            + [whole(cosine.shape), whole(sine.shape), whole(gains.shape)],
            out_specs=(whole(qkv.shape), whole(gains.shape)),
            scratch_shapes=[
                pltpu.VMEM((heads, length, HEAD), BF16),
                pltpu.VMEM((length, HEAD), BF16),
                pltpu.VMEM((length, HEAD), BF16),
                pltpu.VMEM((length, heads * HEAD), BF16),
                pltpu.VMEM((length, HEAD), F32),
                pltpu.VMEM((length, HEAD), F32),
            ],
        ),
        cost_estimate=pl.CostEstimate(
            flops=10 * pairs * HEAD, bytes_accessed=qkv.size * 8, transcendentals=pairs
        ),
        name="attend_back",
    )(meta, qkv, grad, seg_cols, seg_rows, cosine, sine, gains)


def body(
    tokens,
    segment_ids,
    norm_gain,
    query_weight,
    key_matrix,
    value_matrix,
    output_weight,
    query_gain,
    key_gain,
    mlp_gain,
    gate_weight,
    up_weight,
    down_weight,
    cotangent,
):
    local, width = tokens.shape[1], tokens.shape[2]
    length = 2 * local
    quarter = local // 2
    count = lax.axis_size("fsdp")
    block = width // count
    mine = lax.axis_index("fsdp")
    odd = mine % 2
    place = lax.axis_index("ctx")
    core = lax.axis_index("tp")

    small = query_gain.shape[0]
    members = [norm_gain, mlp_gain, query_gain, key_gain]
    used = sum(member.shape[0] for member in members)
    lanes = -(-used // HEAD) * HEAD
    row = jnp.concatenate(members + [jnp.zeros((lanes - used,), BF16)]).astype(F32)[None]
    far_segments = swap_x(segment_ids)
    first_pair, all_gains = first_shards(
        [query_weight, key_matrix, value_matrix, output_weight], row, count
    )
    first = gather_line(first_pair)
    tok, gate_up_pair, down_pair = second_shards(
        [[after(gate_weight, first_pair), up_weight], [down_weight]],
        tokens.reshape(local, width),
    )
    gate_up_w = gather_line(gate_up_pair)
    down_w = gather_line(down_pair)

    def own_quarter(value):
        return lax.dynamic_slice_in_dim(value.reshape(local, width), core * quarter, quarter, 0)

    own_tok, own_cot = own_quarter(tokens), own_quarter(cotangent)
    segments = jnp.concatenate([segment_ids, far_segments])
    seg_cols, seg_rows = segments[:, :, None], segments[:, None, :]
    cosine, sine = rope_tables(jnp.arange(length).astype(F32))
    meta = jnp.stack([place, core]).astype(jnp.int32)

    heads_q = query_weight.shape[1] // 4 // HEAD
    cols = (heads_q + 2) * HEAD
    qkv_w = first[:, :cols]
    out_w = first[:, cols : cols + heads_q * HEAD]
    in_gain = all_gains[:, :block].reshape(1, width)
    mid_gain = all_gains[:, block : 2 * block].reshape(1, width)
    head_gains = all_gains[:, 2 * block : 2 * block + 2 * small].reshape(count, 2, small)
    head_gains = jnp.moveaxis(head_gains, 0, 1).reshape(2, HEAD)

    in_f = tok.astype(F32)
    cot_from = after(own_cot, tok)
    cot_x, cot_y = swap_x(cot_from), swap_ctx(cot_from)
    x_all = (in_f * inv_rms(in_f) * in_gain).astype(BF16)
    qkv = mm(x_all, qkv_w, 1, 0)
    attended = attend(meta, qkv, seg_cols, seg_rows, cosine, sine, head_gains)
    half = 4 * quarter
    cot_x, cot_y = after(cot_x, attended), after(cot_y, attended)
    eighth = quarter // 2
    cot_first, cot_second = swap_ctx(cot_x[:eighth]), swap_x(cot_y[eighth:])
    out_far = mm(attended[half:], out_w, 1, 1).astype(BF16)
    out_near = mm(attended[:half], out_w, 1, 1)
    middle = own_tok.astype(F32) + reduce8(out_near, out_far)
    inverse_mid = inv_rms(middle)
    scaled_mid = middle * inverse_mid
    y_own = (scaled_mid * mid_gain).astype(BF16)
    cot_first, cot_second = after(cot_first, y_own), after(cot_second, y_own)
    y_all, cot = gather8(y_own, (cot_from, cot_x, cot_y, cot_first, cot_second))

    ff = gate_up_w.shape[1] // 2
    gate_up = mm(y_all, gate_up_w, 1, 0)
    gate, up_value = gate_up[:, :ff], gate_up[:, ff:]
    sig = jax.nn.sigmoid(gate)
    active = gate * sig
    hidden = (active * up_value).astype(BF16)
    down_grad = mm(cot, hidden, 0, 0).astype(BF16)

    def finish_rows(own):
        return stack_rows(meta, own, swap_core(own)).reshape(tokens.shape)

    grad_hidden = mm(after(cot, down_grad), down_w, 1, 0)
    grad_up = (grad_hidden * active).astype(BF16)
    grad_gate = (grad_hidden * up_value * (sig * (1.0 + gate * (1.0 - sig)))).astype(BF16)
    mid_grad, gate_up_grad = product_reduce8((grad_gate, grad_up), gate_up_w, 7, y_all)

    mlp_gain_part = jnp.sum(mid_grad * scaled_mid, axis=0)
    grad_middle = own_cot.astype(F32) + norm_back(mid_grad, scaled_mid, inverse_mid, mid_gain)
    grad_attn, mlp_kept, mlp_to_y, mlp_to_x = gather8_product(
        grad_middle.astype(BF16), hidden, down_w
    )
    out_grad = mm(grad_attn, attended, 0, 0).astype(BF16)
    grad_att = mm(grad_attn, out_w, 1, 0).astype(BF16)
    raw_grads, head_gain_parts = attend_back(
        meta, qkv, grad_att, seg_cols, seg_rows, cosine, sine, head_gains
    )
    mlp_first, mlp_second, mlp_came1, mlp_came2 = reduce4_links(
        mlp_kept, mlp_to_y, mlp_to_x, raw_grads
    )
    first_grad = mm(x_all, raw_grads, 0, 0).astype(BF16)
    first_grad = jnp.concatenate([first_grad, out_grad], axis=1)
    mlp_first = mlp_first + after(mlp_came1, first_grad).astype(F32)
    mlp_second = mlp_second + after(mlp_came2, first_grad).astype(F32)
    mlp_sum = (middle + jnp.concatenate([mlp_first, mlp_second])).astype(BF16)
    layer_out = finish_rows(mlp_sum)
    in_grad = product_reduce8((after(raw_grads, first_grad, mlp_sum),), first, 8)

    spot = jnp.stack([place, odd]).astype(jnp.int32)

    def owners(grad, sizes, *others):
        rows = scatter_line(grad)
        rows = after(rows, *others)
        kept = lax.dynamic_slice_in_dim(rows, odd * block, block, 0)
        sent = lax.dynamic_slice_in_dim(rows, (1 - odd) * block, block, 0)
        by_x, by_y = swap_x(sent), swap_ctx(kept)
        by_both = swap_ctx(by_x)
        return join_columns(spot, (kept, by_x, by_y, by_both), sizes)

    (down_share,) = owners(down_grad, (ff,))
    gate_share, up_share = owners(gate_up_grad, (ff, ff))
    query_share, key_share, value_share, out_share = owners(
        first_grad, (heads_q * HEAD, HEAD, HEAD, heads_q * HEAD)
    )

    own_in = own_tok.astype(F32)
    inverse_in = inv_rms(own_in)
    scaled_in = own_in * inverse_in
    norm_gain_part = jnp.sum(in_grad * scaled_in, axis=0)
    own_token_grad = (grad_middle + norm_back(in_grad, scaled_in, inverse_in, in_gain)).astype(BF16)
    token_grad = finish_rows(own_token_grad)

    parts = jnp.concatenate([norm_gain_part, mlp_gain_part, head_gain_parts.reshape(-1)])
    parts = parts.reshape(-1, HEAD)
    far_parts = swap_ctx(parts)
    sums = total(parts + after(far_parts, token_grad)).reshape(-1)
    norm_gain_grad = lax.dynamic_slice_in_dim(sums, mine * block, block, 0)
    mlp_gain_grad = lax.dynamic_slice_in_dim(sums, width + mine * block, block, 0)
    query_gain_grad = lax.dynamic_slice_in_dim(sums, 2 * width + mine * small, small, 0)
    key_gain_grad = lax.dynamic_slice_in_dim(sums, 2 * width + HEAD + mine * small, small, 0)
    return (
        layer_out,
        token_grad,
        norm_gain_grad,
        query_share,
        key_share,
        value_share,
        out_share,
        query_gain_grad,
        key_gain_grad,
        mlp_gain_grad,
        gate_share,
        up_share,
        down_share,
    )


def solution(mesh):
    in_specs = (
        P("fsdp", "ctx", None),
        P("fsdp", None),
        P("fsdp"),
        P("fsdp", "tp"),
        P("fsdp", "tp"),
        P("fsdp", "tp"),
        P("fsdp", "tp"),
        P("fsdp"),
        P("fsdp"),
        P("fsdp"),
        P("fsdp", "tp"),
        P("fsdp", "tp"),
        P("fsdp", "tp"),
        P("fsdp", "ctx", None),
    )
    out_specs = (
        P("fsdp", "ctx", None),
        P("fsdp", "ctx", None),
        P("fsdp"),
        P("fsdp", "tp"),
        P("fsdp", "tp"),
        P("fsdp", "tp"),
        P("fsdp", "tp"),
        P("fsdp"),
        P("fsdp"),
        P("fsdp"),
        P("fsdp", "tp"),
        P("fsdp", "tp"),
        P("fsdp", "tp"),
    )

    return jax.shard_map(body, mesh=mesh, in_specs=in_specs, out_specs=out_specs, check_vma=False)
```

```python
import functools
import math

import jax
import jax.numpy as jnp
from jax import lax
from jax.experimental import pallas as pl
from jax.experimental.pallas import tpu as pltpu
from jax.sharding import PartitionSpec as P


HEAD = 128
EPS = 1e-06
THETA = 1000000.0
MASKED = -1e30
MOST_DOC = 512
MESH = pl.DeviceIdType.MESH
F32 = jnp.float32
BF16 = jnp.bfloat16


def mm(left, right, left_dim, right_dim):
    return lax.dot_general(
        left, right, (((left_dim,), (right_dim,)), ((), ())), preferred_element_type=F32
    )


def swap_core(value):
    return lax.ppermute(value, "tp", [(0, 1), (1, 0)])


def swap_ctx(value):
    return lax.ppermute(value, "ctx", [(0, 1), (1, 0)])


def swap_x(value):
    count = lax.axis_size("fsdp")
    return lax.ppermute(value, "fsdp", [(i, i ^ 1) for i in range(count)])


def lines():
    count = lax.axis_size("fsdp")
    return [[i for i in range(count) if i % 2 == parity] for parity in (0, 1)]


def gather_line(value):
    return lax.all_gather(value, "fsdp", axis=0, tiled=True, axis_index_groups=lines())


def scatter_line(value):
    return lax.psum_scatter(
        value, "fsdp", scatter_dimension=0, tiled=True, axis_index_groups=lines()
    )


def neighbours():
    mine = lax.axis_index("fsdp")
    return (
        {"fsdp": mine + 1 - 2 * lax.rem(mine, 2)},
        {"ctx": 1 - lax.axis_index("ctx")},
        {"tp": 1 - lax.axis_index("tp")},
    )


def greet(peers):
    barrier = pltpu.get_barrier_semaphore()
    for peer in peers:
        pl.semaphore_signal(barrier, inc=1, device_id=peer, device_id_type=MESH)
    pl.semaphore_wait(barrier, len(peers))


def remote_params(number, limit=None):
    return pltpu.CompilerParams(
        collective_id=number, has_side_effects=True, vmem_limit_bytes=limit
    )


def gather8_kernel(rows, spread, *refs):
    if spread:
        own_ref, kept_ref, x_ref, y_ref, first_ref, second_ref, out_ref, also_ref = refs[:8]
        send_sem, recv_sem, local_sem, stage, also_send, also_recv, also_in, also_out = refs[8:]
    else:
        own_ref, out_ref, send_sem, recv_sem, local_sem = refs
    x_peer, y_peer, c_peer = neighbours()

    def start_of(away_t, half, outer, inner):
        return pl.ds((away_t * 8 + half * 4 + outer * 2 + inner) * rows, rows)

    def slot(*block):
        return out_ref.at[start_of(*block)]

    also_loads, also_remote, also_stores = [], [], []
    if spread:
        top, low = pl.ds(0, rows), pl.ds(rows, rows)
        pieces = [
            ((0, 0, 0), kept_ref.at[top]),
            ((0, 0, 1), x_ref.at[top]),
            ((0, 1, 0), y_ref.at[top]),
            ((0, 1, 1), first_ref),
            ((1, 0, 0), kept_ref.at[low]),
            ((1, 0, 1), y_ref.at[low]),
            ((1, 1, 0), x_ref.at[low]),
            ((1, 1, 1), second_ref),
        ]
        for index, (block, source) in enumerate(pieces):
            also_loads.append(pltpu.make_async_copy(source, stage.at[index], also_in.at[index]))
            also_stores.append(
                pltpu.make_async_copy(
                    stage.at[index], also_ref.at[start_of(0, *block)], also_out.at[index]
                )
            )
            also_remote.append(
                pltpu.make_async_remote_copy(
                    src_ref=source,
                    dst_ref=also_ref.at[start_of(1, *block)],
                    send_sem=also_send.at[index],
                    recv_sem=also_recv.at[index],
                    device_id=c_peer,
                    device_id_type=MESH,
                )
            )
        for copy in also_loads:
            copy.start()
    greet((x_peer, y_peer, c_peer))

    number = iter(range(14))

    def send(source, target, peer):
        index = next(number)
        copy = pltpu.make_async_remote_copy(
            src_ref=source,
            dst_ref=target,
            send_sem=send_sem.at[index],
            recv_sem=recv_sem.at[index],
            device_id=peer,
            device_id_type=MESH,
        )
        copy.start()
        return copy

    first, second = own_ref.at[pl.ds(0, rows)], own_ref.at[pl.ds(rows, rows)]
    x1 = send(first, slot(0, 0, 0, 1), x_peer)
    y1 = send(second, slot(0, 1, 0, 1), y_peer)
    x2 = send(second, slot(0, 1, 1, 0), x_peer)
    y2 = send(first, slot(0, 0, 1, 0), y_peer)
    rest = [send(first, slot(1, 0, 0, 0), c_peer), send(second, slot(1, 1, 0, 0), c_peer)]
    kept = [
        pltpu.make_async_copy(first, slot(0, 0, 0, 0), local_sem.at[0]),
        pltpu.make_async_copy(second, slot(0, 1, 0, 0), local_sem.at[1]),
    ]
    for copy in kept:
        copy.start()
    for copy in also_remote:
        copy.start()
    for load, store in zip(also_loads, also_stores):
        load.wait()
        store.start()
    x1.wait_recv()
    y3 = send(slot(0, 0, 0, 1), slot(0, 0, 1, 1), y_peer)
    y1.wait_recv()
    x3 = send(slot(0, 1, 0, 1), slot(0, 1, 1, 1), x_peer)
    rest.append(send(slot(0, 0, 0, 1), slot(1, 0, 0, 1), c_peer))
    rest.append(send(slot(0, 1, 0, 1), slot(1, 1, 0, 1), c_peer))
    x2.wait_recv()
    rest.append(send(slot(0, 1, 1, 0), slot(1, 1, 1, 0), c_peer))
    y2.wait_recv()
    rest.append(send(slot(0, 0, 1, 0), slot(1, 0, 1, 0), c_peer))
    y3.wait_recv()
    rest.append(send(slot(0, 0, 1, 1), slot(1, 0, 1, 1), c_peer))
    x3.wait_recv()
    rest.append(send(slot(0, 1, 1, 1), slot(1, 1, 1, 1), c_peer))
    for copy in (x1, y1, x2, y2, y3, x3):
        copy.wait_send()
    for copy in rest + also_remote + kept + also_stores:
        copy.wait()


def gather8_product_kernel(
    rows,
    own_ref,
    acts_ref,
    weight_ref,
    out_ref,
    kept_ref,
    to_y_ref,
    to_x_ref,
    send_sem,
    recv_sem,
    local_sem,
    acts,
    weight,
    far,
    core_in,
    core_send,
    core_recv,
    load_sem,
):
    x_peer, y_peer, c_peer = neighbours()
    width = weight.shape[0]
    wide = 2 * rows
    loads = [
        pltpu.make_async_copy(weight_ref, weight, load_sem.at[0]),
        pltpu.make_async_copy(acts_ref, acts, load_sem.at[1]),
    ]
    for copy in loads:
        copy.start()
    greet((x_peer, y_peer, c_peer))

    def slot(away_t, half, outer, inner):
        return out_ref.at[pl.ds((away_t * 8 + half * 4 + outer * 2 + inner) * rows, rows)]

    number = iter(range(14))

    def send(source, target, peer):
        index = next(number)
        copy = pltpu.make_async_remote_copy(
            src_ref=source,
            dst_ref=target,
            send_sem=send_sem.at[index],
            recv_sem=recv_sem.at[index],
            device_id=peer,
            device_id_type=MESH,
        )
        copy.start()
        return copy

    core_copies = []

    def far_chunk(index):
        place = pl.ds(index * wide, wide)
        source = pl.ds(4 * wide + index * wide, wide)

        def step(cols):
            far[place, cols] = mm(acts[source, :], weight[cols, :], 1, 1).astype(BF16)
            return 0

        tiled(width, width // 2, step)
        copy = pltpu.make_async_remote_copy(
            src_ref=far.at[place],
            dst_ref=core_in.at[place],
            send_sem=core_send.at[index],
            recv_sem=core_recv.at[index],
            device_id=c_peer,
            device_id_type=MESH,
        )
        copy.start()
        core_copies.append(copy)

    def near_chunk(index, target_ref, start):
        core_copies[index].wait_recv()
        place = pl.ds(index * wide, wide)
        target = pl.ds(start, wide)

        def step(cols):
            value = mm(acts[place, :], weight[cols, :], 1, 1) + core_in[place, cols].astype(F32)
            target_ref[target, cols] = value.astype(target_ref.dtype)
            return 0

        tiled(width, width // 2, step)

    first, second = own_ref.at[pl.ds(0, rows)], own_ref.at[pl.ds(rows, rows)]
    x1 = send(first, slot(0, 0, 0, 1), x_peer)
    y1 = send(second, slot(0, 1, 0, 1), y_peer)
    x2 = send(second, slot(0, 1, 1, 0), x_peer)
    y2 = send(first, slot(0, 0, 1, 0), y_peer)
    rest = [send(first, slot(1, 0, 0, 0), c_peer), send(second, slot(1, 1, 0, 0), c_peer)]
    kept = [
        pltpu.make_async_copy(first, slot(0, 0, 0, 0), local_sem.at[0]),
        pltpu.make_async_copy(second, slot(0, 1, 0, 0), local_sem.at[1]),
    ]
    for copy in kept:
        copy.start()
    for copy in loads:
        copy.wait()
    for index in range(4):
        far_chunk(index)
    x1.wait_recv()
    y3 = send(slot(0, 0, 0, 1), slot(0, 0, 1, 1), y_peer)
    y1.wait_recv()
    x3 = send(slot(0, 1, 0, 1), slot(0, 1, 1, 1), x_peer)
    rest.append(send(slot(0, 0, 0, 1), slot(1, 0, 0, 1), c_peer))
    rest.append(send(slot(0, 1, 0, 1), slot(1, 1, 0, 1), c_peer))
    near_chunk(0, kept_ref, 0)
    near_chunk(1, to_y_ref, 0)
    near_chunk(2, kept_ref, wide)
    near_chunk(3, to_x_ref, 0)
    x2.wait_recv()
    rest.append(send(slot(0, 1, 1, 0), slot(1, 1, 1, 0), c_peer))
    y2.wait_recv()
    rest.append(send(slot(0, 0, 1, 0), slot(1, 0, 1, 0), c_peer))
    y3.wait_recv()
    rest.append(send(slot(0, 0, 1, 1), slot(1, 0, 1, 1), c_peer))
    x3.wait_recv()
    rest.append(send(slot(0, 1, 1, 1), slot(1, 1, 1, 1), c_peer))
    for copy in (x1, y1, x2, y2, y3, x3):
        copy.wait_send()
    for copy in core_copies:
        copy.wait_send()
    for copy in rest + kept:
        copy.wait()


def gather8_product(own, acts, weight):
    rows, width = own.shape[0] // 2, own.shape[1]
    hbm = pl.BlockSpec(memory_space=pl.ANY)
    vmem = pl.BlockSpec(memory_space=pltpu.VMEM)
    return pl.pallas_call(
        functools.partial(gather8_product_kernel, rows),
        out_shape=[
            jax.ShapeDtypeStruct((16 * rows, width), own.dtype),
            jax.ShapeDtypeStruct((4 * rows, width), F32),
            jax.ShapeDtypeStruct((2 * rows, width), BF16),
            jax.ShapeDtypeStruct((2 * rows, width), BF16),
        ],
        in_specs=[vmem, hbm, hbm],
        out_specs=[hbm, vmem, vmem, vmem],
        scratch_shapes=[
            pltpu.SemaphoreType.DMA((14,)),
            pltpu.SemaphoreType.DMA((14,)),
            pltpu.SemaphoreType.DMA((2,)),
            pltpu.VMEM(acts.shape, BF16),
            pltpu.VMEM(weight.shape, BF16),
            pltpu.VMEM((8 * rows, width), BF16),
            pltpu.VMEM((8 * rows, width), BF16),
            pltpu.SemaphoreType.DMA((4,)),
            pltpu.SemaphoreType.DMA((4,)),
            pltpu.SemaphoreType.DMA((2,)),
        ],
        compiler_params=remote_params(9, 48 * 1024 * 1024),
        cost_estimate=pl.CostEstimate(
            flops=2 * acts.size * width, bytes_accessed=16 * own.size, transcendentals=0
        ),
        name="gather8_product",
    )(own, acts, weight)


def gather8(own, also=()):
    rows, width = own.shape[0] // 2, own.shape[1]
    hbm = pl.BlockSpec(memory_space=pl.ANY)
    whole_shape = jax.ShapeDtypeStruct((16 * rows, width), own.dtype)
    sems = [
        pltpu.SemaphoreType.DMA((14,)),
        pltpu.SemaphoreType.DMA((14,)),
        pltpu.SemaphoreType.DMA((2,)),
    ]
    if also:
        sems += [pltpu.VMEM((8, rows, width), own.dtype)] + [pltpu.SemaphoreType.DMA((8,))] * 4
    outs = pl.pallas_call(
        functools.partial(gather8_kernel, rows, bool(also)),
        out_shape=[whole_shape] * (2 if also else 1),
        in_specs=[pl.BlockSpec(memory_space=pltpu.VMEM)] + [hbm] * len(also),
        out_specs=[hbm] * (2 if also else 1),
        scratch_shapes=sems,
        compiler_params=remote_params(6 if also else 1),
        name="gather8_also" if also else "gather8",
    )(own, *also)
    return outs if also else outs[0]


def reduce8_kernel(
    rows,
    near_ref,
    far_ref,
    out_ref,
    near,
    core_in,
    link_in,
    link_out,
    send_sem,
    recv_sem,
    local_sem,
):
    x_peer, y_peer, c_peer = neighbours()
    greet((x_peer, y_peer, c_peer))
    order = [(h, o, i) for o, i in ((1, 1), (1, 0), (0, 1), (0, 0)) for h in (0, 1)]
    core_copies, local_copies = {}, {}
    for number, (half, outer, inner) in enumerate(order):
        place = pl.ds((half * 4 + outer * 2 + inner) * rows, rows)
        core_copies[half, outer, inner] = pltpu.make_async_remote_copy(
            src_ref=far_ref.at[place],
            dst_ref=core_in.at[place],
            send_sem=send_sem.at[number],
            recv_sem=recv_sem.at[number],
            device_id=c_peer,
            device_id_type=MESH,
        )
        local_copies[half, outer, inner] = pltpu.make_async_copy(
            near_ref.at[place], near.at[place], local_sem.at[number]
        )
    for block in order:
        core_copies[block].start()
        local_copies[block].start()

    def partial_sum(block):
        half, outer, inner = block
        place = pl.ds((half * 4 + outer * 2 + inner) * rows, rows)
        core_copies[block].wait_recv()
        local_copies[block].wait()
        return near[place, :] + core_in[place, :].astype(F32)

    def link(index, value, peer):
        link_out[index] = value.astype(BF16)
        copy = pltpu.make_async_remote_copy(
            src_ref=link_out.at[index],
            dst_ref=link_in.at[index],
            send_sem=send_sem.at[8 + index],
            recv_sem=recv_sem.at[8 + index],
            device_id=peer,
            device_id_type=MESH,
        )
        copy.start()
        return copy

    y11 = link(0, partial_sum((0, 1, 1)), y_peer)
    x11 = link(1, partial_sum((1, 1, 1)), x_peer)
    y10 = link(2, partial_sum((0, 1, 0)), y_peer)
    x10 = link(3, partial_sum((1, 1, 0)), x_peer)
    first01, second01 = partial_sum((0, 0, 1)), partial_sum((1, 0, 1))
    y11.wait_recv()
    x01 = link(4, first01 + link_in[0].astype(F32), x_peer)
    x11.wait_recv()
    y01 = link(5, second01 + link_in[1].astype(F32), y_peer)
    first = partial_sum((0, 0, 0))
    second = partial_sum((1, 0, 0))
    y10.wait_recv()
    out_ref[pl.ds(0, rows), :] = first + link_in[2].astype(F32)
    x10.wait_recv()
    out_ref[pl.ds(rows, rows), :] = second + link_in[3].astype(F32)
    x01.wait_recv()
    out_ref[pl.ds(0, rows), :] += link_in[4].astype(F32)
    y01.wait_recv()
    out_ref[pl.ds(rows, rows), :] += link_in[5].astype(F32)
    for copy in (y11, x11, y10, x10, x01, y01):
        copy.wait_send()
    for copy in core_copies.values():
        copy.wait_send()


def reduce8(near, far):
    rows, width = near.shape[0] // 8, near.shape[1]
    return pl.pallas_call(
        functools.partial(reduce8_kernel, rows),
        out_shape=jax.ShapeDtypeStruct((2 * rows, width), F32),
        in_specs=[pl.BlockSpec(memory_space=pl.ANY), pl.BlockSpec(memory_space=pl.ANY)],
        out_specs=pl.BlockSpec(memory_space=pltpu.VMEM),
        scratch_shapes=[
            pltpu.VMEM(near.shape, F32),
            pltpu.VMEM(near.shape, BF16),
            pltpu.VMEM((6, rows, width), BF16),
            pltpu.VMEM((6, rows, width), BF16),
            pltpu.SemaphoreType.DMA((14,)),
            pltpu.SemaphoreType.DMA((14,)),
            pltpu.SemaphoreType.DMA((8,)),
        ],
        compiler_params=remote_params(2, 48 * 1024 * 1024),
        name="reduce8",
    )(near, far)


def tiled(count, tile, step):
    lax.fori_loop(0, count // tile, lambda i, _: step(pl.ds(pl.multiple_of(i * tile, tile), tile)), 0)


def product_reduce8_kernel(rows, groups, filler, *refs):
    acts_refs, refs = refs[:groups], refs[groups:]
    if filler:
        weight_ref, lhs_ref, out_ref, grad_ref, *refs = refs
    else:
        weight_ref, out_ref, *refs = refs
    acts, weight, far, near, core_in, link_in, link_out, send_sem, recv_sem, load_sem, *refs = refs
    x_peer, y_peer, c_peer = neighbours()
    width = weight.shape[0]
    wide = 2 * rows
    chunks = [(0, 1), (1, 1), (0, 0), (1, 0)]

    def where(chunk):
        return chunk[0] * 2 * wide + chunk[1] * wide

    half = width // 2
    load_weights = [
        pltpu.make_async_copy(
            weight_ref.at[pl.ds(part * half, half), pl.ds(0, weight.shape[1])],
            weight.at[pl.ds(part * half, half)],
            load_sem.at[part],
        )
        for part in (0, 1)
    ]
    loads = {}
    depth = weight.shape[1] // groups
    for number, chunk in enumerate(chunks):
        for side in (1, 0):
            place = pl.ds(side * 4 * wide + where(chunk), wide)
            loads[side, chunk] = [
                pltpu.make_async_copy(
                    acts_refs[group].at[place],
                    acts.at[place, pl.ds(group * depth, depth)],
                    load_sem.at[3 + (2 * number + side) * groups + group],
                )
                for group in range(groups)
            ]
    started = [loads[1, chunks[0]], [load_weights[0]], loads[1, chunks[1]], loads[0, chunks[0]]]
    started += [loads[0, chunks[1]], [load_weights[1]]]
    started += [loads[side, chunk] for chunk in chunks[2:] for side in (1, 0)]
    for group in started:
        for copy in group:
            copy.start()
    if filler:
        lhs, grad, grad_sem = refs
        load_lhs = pltpu.make_async_copy(lhs_ref, lhs, load_sem.at[2])
        load_lhs.start()
    greet((x_peer, y_peer, c_peer))

    core_copies, link_copies = {}, {}

    def product(chunk, side, part, target):
        place = pl.ds(where(chunk), wide)
        source = pl.ds(side * 4 * wide + where(chunk), wide)

        cols = pl.ds(part * half, half)
        target[place, cols] = mm(acts[source, :], weight[cols, :], 1, 1).astype(target.dtype)

    def remote(copies, key, number, source, target, peer):
        copies[key] = pltpu.make_async_remote_copy(
            src_ref=source,
            dst_ref=target,
            send_sem=send_sem.at[number],
            recv_sem=recv_sem.at[number],
            device_id=peer,
            device_id_type=MESH,
        )
        copies[key].start()

    def send_core(chunk, part):
        product(chunk, 1, part, far)
        here = (pl.ds(where(chunk), wide), pl.ds(part * half, half))
        number = 2 * chunks.index(chunk) + part
        remote(core_copies, (chunk, part), number, far.at[here], core_in.at[here], c_peer)

    def partial_sum(chunk, start, size, part):
        here = (pl.ds(where(chunk) + start, size), pl.ds(part * half, half))
        return near[here] + core_in[here].astype(F32)

    def link(hop, side, part, value, peer):
        size = value.shape[0]
        start = (side * 3 + hop * 2) * rows
        here = (pl.ds(start, size), pl.ds(part * half, half))
        link_out[here] = value.astype(BF16)
        number = 8 + hop * 4 + side * 2 + part
        remote(link_copies, (hop, side, part), number, link_out.at[here], link_in.at[here], peer)

    def came(hop, side, start, part):
        return link_in[
            pl.ds((side * 3 + hop * 2) * rows + start, rows), pl.ds(part * half, half)
        ].astype(F32)

    for chunk in chunks[:2]:
        for copy in loads[1, chunk]:
            copy.wait()
    for part in (0, 1):
        load_weights[part].wait()
        send_core((0, 1), part)
        send_core((1, 1), part)
        for side, peer in ((0, y_peer), (1, x_peer)):
            if part == 0:
                for copy in loads[0, (side, 1)]:
                    copy.wait()
            product((side, 1), 0, part, near)
            core_copies[(side, 1), part].wait_recv()
            link(0, side, part, partial_sum((side, 1), 0, wide, part), peer)
    for chunk in chunks[2:]:
        for side in (1, 0):
            for copy in loads[side, chunk]:
                copy.wait()
    if filler:
        size = width // 4

        def fill(index, _):
            cols = pl.ds(pl.multiple_of(index * size, size), size)

            def step(columns):
                grad[cols, columns] = mm(lhs[:, cols], acts[:, columns], 0, 0).astype(BF16)
                return 0

            tiled(acts.shape[1], acts.shape[1] // 3, step)
            return 0

    for part in (0, 1):
        for chunk in chunks[2:]:
            send_core(chunk, part)
        for chunk in chunks[2:]:
            product(chunk, 0, part, near)
        for side, peer in ((0, x_peer), (1, y_peer)):
            core_copies[(side, 0), part].wait_recv()
            link_copies[0, side, part].wait_recv()
            link(1, side, part, partial_sum((side, 0), rows, rows, part) + came(0, side, rows, part), peer)
        if filler and part == 0:
            load_lhs.wait()
            lax.fori_loop(0, 1, fill, 0)
    if filler:
        lax.fori_loop(1, 4, fill, 0)
        grad_copy = pltpu.make_async_copy(grad, grad_ref, grad_sem.at[0])
        grad_copy.start()
    for side in (0, 1):
        for part in (0, 1):
            place = (pl.ds(side * rows, rows), pl.ds(part * half, half))
            kept = partial_sum((side, 0), 0, rows, part) + came(0, side, 0, part)
            link_copies[1, side, part].wait_recv()
            out_ref[place] = kept + came(1, side, 0, part)
    for copy in list(link_copies.values()) + list(core_copies.values()):
        copy.wait_send()
    if filler:
        grad_copy.wait()


def product_reduce8(columns, weight, number, lhs=None):
    depth, groups = sum(column.shape[1] for column in columns), len(columns)
    acts = jax.ShapeDtypeStruct((columns[0].shape[0], depth), BF16)
    rows, width = acts.shape[0] // 16, weight.shape[0]
    filler = lhs is not None
    hbm = pl.BlockSpec(memory_space=pl.ANY)
    scratch = [
        pltpu.VMEM(acts.shape, BF16),
        pltpu.VMEM((width, depth), BF16),
        pltpu.VMEM((8 * rows, width), BF16),
        pltpu.VMEM((8 * rows, width), F32),
        pltpu.VMEM((8 * rows, width), BF16),
        pltpu.VMEM((6 * rows, width), BF16),
        pltpu.VMEM((6 * rows, width), BF16),
        pltpu.SemaphoreType.DMA((16,)),
        pltpu.SemaphoreType.DMA((16,)),
        pltpu.SemaphoreType.DMA((3 + 8 * groups,)),
    ]
    out_shape = [jax.ShapeDtypeStruct((2 * rows, width), F32)]
    out_specs = [pl.BlockSpec(memory_space=pltpu.VMEM)]
    flops = 2 * acts.shape[0] * width * depth
    if filler:
        scratch += [
            pltpu.VMEM(lhs.shape, BF16),
            pltpu.VMEM((width, depth), BF16),
            pltpu.SemaphoreType.DMA((1,)),
        ]
        out_shape.append(jax.ShapeDtypeStruct((width, depth), BF16))
        out_specs.append(hbm)
        flops *= 2
    outs = pl.pallas_call(
        functools.partial(product_reduce8_kernel, rows, groups, filler),
        out_shape=out_shape,
        in_specs=[hbm] * (groups + (2 if filler else 1)),
        out_specs=out_specs,
        scratch_shapes=scratch,
        compiler_params=remote_params(number, 63 * 1024 * 1024),
        cost_estimate=pl.CostEstimate(
            flops=flops, bytes_accessed=4 * depth * (acts.shape[0] + width), transcendentals=0
        ),
        name="product_reduce8",
    )(*columns, weight, *((lhs,) if filler else ()))
    return outs if filler else outs[0]


def shard_copies(plan, ins, out_refs, stage, sems):
    send_sem, recv_sem, load_sem, store_sem = sems
    x_peer, _, _ = neighbours()
    odd = lax.rem(lax.axis_index("fsdp"), 2)
    column = 2 * lax.axis_index("ctx") + odd
    other = 2 * lax.axis_index("ctx") + 1 - odd
    remote, loads, stores = [], [], []
    for number, (which, start, size) in enumerate(plan):
        rows = ins[number].shape[0]
        place = pl.ds(pl.multiple_of(odd * rows, rows), rows)
        target = out_refs[which].at[place, pl.ds(start, size)]

        def source(index, ref=ins[number], size=size):
            return ref.at[:, pl.ds(pl.multiple_of(index * size, HEAD), size)]

        remote.append(
            pltpu.make_async_remote_copy(
                src_ref=source(other),
                dst_ref=target,
                send_sem=send_sem.at[number],
                recv_sem=recv_sem.at[number],
                device_id=x_peer,
                device_id_type=MESH,
            )
        )
        loads.append(pltpu.make_async_copy(source(column), stage[number], load_sem.at[number]))
        stores.append(pltpu.make_async_copy(stage[number], target, store_sem.at[number]))
    return remote, loads, stores


def shard_plan(groups):
    plan, arrays, shapes = [], [], []
    for which, group in enumerate(groups):
        start = 0
        for array in group:
            size = array.shape[1] // 4
            plan.append((which, start, size))
            arrays.append(array)
            start += size
        shapes.append(jax.ShapeDtypeStruct((2 * group[0].shape[0], start), BF16))
    return tuple(plan), arrays, shapes


def shard_scratch(plan, arrays):
    return [
        pltpu.VMEM((array.shape[0], size), BF16) for array, (_, _, size) in zip(arrays, plan)
    ] + [pltpu.SemaphoreType.DMA((len(plan),))] * 4


def bit_peer(axis, bit):
    mine = lax.axis_index(axis)
    return {axis: mine + bit * (1 - 2 * lax.rem(mine // bit, 2))}


def sum_over(stages, value, inbox, outbox, send_sem, recv_sem, behind=()):
    copies = []
    for index, (axis, bit) in enumerate(stages):
        outbox[index] = value
        copy = pltpu.make_async_remote_copy(
            src_ref=outbox.at[index],
            dst_ref=inbox.at[index],
            send_sem=send_sem.at[index],
            recv_sem=recv_sem.at[index],
            device_id=bit_peer(axis, bit),
            device_id_type=MESH,
        )
        copy.start()
        copies.append(copy)
        if index == 0:
            for later in behind:
                later.start()
        copy.wait_recv()
        value = value + inbox[index]
    return value, copies


def fsdp_stages():
    stages, bit = [], 2
    while bit < lax.axis_size("fsdp"):
        stages.append(("fsdp", bit))
        bit *= 2
    return stages


def first_kernel(plan, stages, *refs):
    count = len(plan)
    ins, row_ref, out_ref, gain_ref = refs[:count], refs[count], refs[count + 1], refs[count + 2]
    stage, sems = refs[count + 3 : 2 * count + 3], refs[2 * count + 3 : 2 * count + 7]
    inbox, outbox, gain_send, gain_recv = refs[2 * count + 7 :]
    remote, loads, stores = shard_copies(plan, ins, [out_ref], stage, sems)
    for copy in loads:
        copy.start()
    greet([bit_peer(axis, bit) for axis, bit in stages])
    for load, store in zip(loads, stores):
        load.wait()
        store.start()
    member = lax.broadcasted_iota(jnp.int32, gain_ref.shape, 0)
    value = jnp.where(
        member == lax.axis_index("fsdp"), jnp.broadcast_to(row_ref[...], gain_ref.shape), 0.0
    )
    value, copies = sum_over(stages, value, inbox, outbox, gain_send, gain_recv, remote)
    gain_ref[...] = value
    for copy in copies:
        copy.wait_send()
    for copy in stores + remote:
        copy.wait()


def first_shards(arrays, row, count):
    plan, arrays, shapes = shard_plan([arrays])
    stages = [("fsdp", 1)] + fsdp_stages()
    hbm = pl.BlockSpec(memory_space=pl.ANY)
    vmem = pl.BlockSpec(memory_space=pltpu.VMEM)
    gains = jax.ShapeDtypeStruct((count, row.shape[1]), F32)
    box = pltpu.VMEM((len(stages),) + gains.shape, F32)
    sem = pltpu.SemaphoreType.DMA((len(stages),))
    return pl.pallas_call(
        functools.partial(first_kernel, plan, tuple(stages)),
        out_shape=shapes + [gains],
        in_specs=[hbm] * len(arrays) + [vmem],
        out_specs=[hbm, vmem],
        scratch_shapes=shard_scratch(plan, arrays) + [box, box, sem, sem],
        compiler_params=remote_params(3),
        name="first_shards",
    )(*arrays, row)


def second_kernel(plan, outs, rows, *refs):
    count = len(plan)
    ins, token_ref, out_ref = refs[:count], refs[count], refs[count + 1]
    pair_refs, refs = refs[count + 2 : count + 2 + outs], refs[count + 2 + outs :]
    stage, sems = refs[:count], refs[count : count + 4]
    own, own_sem, send_sem, recv_sem, local_sem = refs[count + 4 :]
    x_peer, y_peer, c_peer = neighbours()
    core = lax.axis_index("tp")
    load_own = pltpu.make_async_copy(
        token_ref.at[pl.ds(pl.multiple_of(core * 2 * rows, 2 * rows), 2 * rows)], own, own_sem
    )
    load_own.start()
    remote, loads, stores = shard_copies(plan, ins, pair_refs, stage, sems)
    for copy in loads:
        copy.start()
    load_own.wait()
    greet((x_peer, y_peer, c_peer))

    def slot(away_t, half, outer, inner):
        return out_ref.at[pl.ds((away_t * 8 + half * 4 + outer * 2 + inner) * rows, rows)]

    number = iter(range(14))

    def send(source, target, peer):
        index = next(number)
        copy = pltpu.make_async_remote_copy(
            src_ref=source,
            dst_ref=target,
            send_sem=send_sem.at[index],
            recv_sem=recv_sem.at[index],
            device_id=peer,
            device_id_type=MESH,
        )
        copy.start()
        return copy

    first, second = own.at[pl.ds(0, rows)], own.at[pl.ds(rows, rows)]
    x1 = send(first, slot(0, 0, 0, 1), x_peer)
    y1 = send(second, slot(0, 1, 0, 1), y_peer)
    x2 = send(second, slot(0, 1, 1, 0), x_peer)
    y2 = send(first, slot(0, 0, 1, 0), y_peer)
    rest = [send(first, slot(1, 0, 0, 0), c_peer), send(second, slot(1, 1, 0, 0), c_peer)]
    kept = [
        pltpu.make_async_copy(first, slot(0, 0, 0, 0), local_sem.at[0]),
        pltpu.make_async_copy(second, slot(0, 1, 0, 0), local_sem.at[1]),
    ]
    for copy in kept:
        copy.start()
    for load, store in zip(loads, stores):
        load.wait()
        store.start()
    x1.wait_recv()
    y3 = send(slot(0, 0, 0, 1), slot(0, 0, 1, 1), y_peer)
    y1.wait_recv()
    x3 = send(slot(0, 1, 0, 1), slot(0, 1, 1, 1), x_peer)
    for copy in remote:
        copy.start()
    rest.append(send(slot(0, 0, 0, 1), slot(1, 0, 0, 1), c_peer))
    rest.append(send(slot(0, 1, 0, 1), slot(1, 1, 0, 1), c_peer))
    x2.wait_recv()
    rest.append(send(slot(0, 1, 1, 0), slot(1, 1, 1, 0), c_peer))
    y2.wait_recv()
    rest.append(send(slot(0, 0, 1, 0), slot(1, 0, 1, 0), c_peer))
    y3.wait_recv()
    rest.append(send(slot(0, 0, 1, 1), slot(1, 0, 1, 1), c_peer))
    x3.wait_recv()
    rest.append(send(slot(0, 1, 1, 1), slot(1, 1, 1, 1), c_peer))
    for copy in (x1, y1, x2, y2, y3, x3):
        copy.wait_send()
    for copy in rest + kept + stores + remote:
        copy.wait()


def second_shards(groups, tokens):
    plan, arrays, shapes = shard_plan(groups)
    rows, width = tokens.shape[0] // 4, tokens.shape[1]
    hbm = pl.BlockSpec(memory_space=pl.ANY)
    return pl.pallas_call(
        functools.partial(second_kernel, plan, len(groups), rows),
        out_shape=[jax.ShapeDtypeStruct((16 * rows, width), tokens.dtype)] + shapes,
        in_specs=[hbm] * (len(arrays) + 1),
        out_specs=[hbm] * (len(groups) + 1),
        scratch_shapes=shard_scratch(plan, arrays)
        + [
            pltpu.VMEM((2 * rows, width), tokens.dtype),
            pltpu.SemaphoreType.DMA,
            pltpu.SemaphoreType.DMA((14,)),
            pltpu.SemaphoreType.DMA((14,)),
            pltpu.SemaphoreType.DMA((2,)),
        ],
        compiler_params=remote_params(4),
        name="second_shards",
    )(*arrays, tokens)


def total_kernel(stages, part_ref, *refs):
    row_refs, (out_ref, first_ref, second_ref), refs = refs[:4], refs[4:7], refs[7:]
    inbox, outbox, send_sem, recv_sem, stage, load_sem, store_sem = refs
    core = lax.axis_index("tp")
    rows = stage.shape[1]
    loads, stores = [], []
    for index, row_ref in enumerate(row_refs):
        side = core if index % 2 == 0 else 1 - core
        place = pl.ds(pl.multiple_of(side * rows, rows), rows)
        target = (first_ref, second_ref)[index // 2]
        loads.append(pltpu.make_async_copy(row_ref, stage.at[index], load_sem.at[index]))
        stores.append(
            pltpu.make_async_copy(stage.at[index], target.at[place], store_sem.at[index])
        )
    for copy in loads:
        copy.start()
    greet([bit_peer(axis, bit) for axis, bit in stages])
    for load, store in zip(loads, stores):
        load.wait()
        store.start()
    value, copies = sum_over(stages, part_ref[...], inbox, outbox, send_sem, recv_sem)
    out_ref[...] = value
    for copy in copies:
        copy.wait_send()
    for copy in stores:
        copy.wait()


def total(part, first, second):
    stages = fsdp_stages() + [("tp", 1), ("fsdp", 1)]
    rows, width = first[0].shape
    hbm = pl.BlockSpec(memory_space=pl.ANY)
    vmem = pl.BlockSpec(memory_space=pltpu.VMEM)
    both = jax.ShapeDtypeStruct((2 * rows, width), BF16)
    return pl.pallas_call(
        functools.partial(total_kernel, tuple(stages)),
        out_shape=[jax.ShapeDtypeStruct(part.shape, F32), both, both],
        in_specs=[vmem] + [hbm] * 4,
        out_specs=[vmem, hbm, hbm],
        scratch_shapes=[
            pltpu.VMEM((len(stages),) + part.shape, F32),
            pltpu.VMEM((len(stages),) + part.shape, F32),
            pltpu.SemaphoreType.DMA((len(stages),)),
            pltpu.SemaphoreType.DMA((len(stages),)),
            pltpu.VMEM((4, rows, width), BF16),
            pltpu.SemaphoreType.DMA((4,)),
            pltpu.SemaphoreType.DMA((4,)),
        ],
        compiler_params=remote_params(5),
        name="total",
    )(part, *first, *second)


def join_kernel(sizes, spot_ref, kept_ref, x_ref, y_ref, both_ref, *out_refs):
    place, odd = spot_ref[0], spot_ref[1]
    parts = (
        (kept_ref, 2 * place + odd),
        (x_ref, 2 * place + 1 - odd),
        (y_ref, 2 - 2 * place + odd),
        (both_ref, 3 - 2 * place - odd),
    )
    for part, column in parts:
        start = 0
        for size, out_ref in zip(sizes, out_refs):
            target = pl.ds(pl.multiple_of(column * size, HEAD), size)
            out_ref[:, target] = part[:, start : start + size].astype(F32)
            start += size


def join_columns(spot, parts, sizes):
    rows = parts[0].shape[0]
    tile = min(rows, 64)
    return pl.pallas_call(
        functools.partial(join_kernel, sizes),
        out_shape=[jax.ShapeDtypeStruct((rows, 4 * size), F32) for size in sizes],
        grid_spec=pltpu.PrefetchScalarGridSpec(
            num_scalar_prefetch=1,
            grid=(rows // tile,),
            in_specs=[
                pl.BlockSpec((tile, part.shape[1]), lambda i, spot: (i, 0)) for part in parts
            ],
            out_specs=[pl.BlockSpec((tile, 4 * size), lambda i, spot: (i, 0)) for size in sizes],
        ),
        name="join",
    )(spot, *parts)


def after(value, *others):
    return lax.optimization_barrier((value,) + others)[0]


def reduce4_links(kept, to_y, to_x, *others):
    rows = kept.shape[0] // 4
    came_first, came_second = swap_ctx(to_y), swap_x(to_x)
    first = kept[: 2 * rows] + after(came_first, *others).astype(F32)
    second = kept[2 * rows :] + after(came_second, *others).astype(F32)
    came_first = swap_x(first[rows:].astype(BF16))
    came_second = swap_ctx(second[rows:].astype(BF16))
    return first[:rows], second[:rows], came_first, came_second


def rope_tables(positions):
    freqs = THETA ** (-(jnp.arange(HEAD // 2, dtype=F32) * 2.0) / HEAD)
    angle = positions[:, None] * freqs[None, :]
    cosine = jnp.concatenate([jnp.cos(angle), jnp.cos(angle)], axis=-1)
    sine = jnp.concatenate([-jnp.sin(angle), jnp.sin(angle)], axis=-1)
    return cosine, sine


def norm_back(grad, scaled, inverse, gain):
    weighted = grad * gain
    return inverse * (weighted - scaled * jnp.mean(weighted * scaled, axis=-1, keepdims=True))


def inv_rms(value):
    return lax.rsqrt(jnp.mean(value * value, axis=-1, keepdims=True) + EPS)


def block_row(meta_ref, seq, index, rows):
    away_c = lax.rem(meta_ref[0] + index // 4, 2)
    away_t = lax.rem(meta_ref[1] + (index // 2) % 2, 2)
    if index % 2 == 0:
        inner = away_c * 2 + seq
    else:
        inner = seq * 2 + away_c + 4
    return pl.multiple_of((away_t * 8 + inner) * rows, rows)


def scaled_of(raw):
    inverse = lax.rsqrt(jnp.mean(raw * raw, axis=-1, keepdims=True) + EPS)
    return raw * inverse, inverse


def load_heads(meta_ref, qkv_ref, cos_ref, sin_ref, gain_ref, q_scr, k_scr, v_scr, heads):
    seq = pl.program_id(0)
    rows = q_scr.shape[1] // 8
    for index in range(8):
        start = block_row(meta_ref, seq, index, rows)
        here = slice(index * rows, (index + 1) * rows)
        cosine, sine = cos_ref[here, :], sin_ref[here, :]
        for head in range(heads + 1):
            raw = qkv_ref[pl.ds(start, rows), head * HEAD : (head + 1) * HEAD]
            scaled, _ = scaled_of(raw)
            which = 0 if head < heads else 1
            value = scaled * gain_ref[which : which + 1, :]
            turned = value * cosine + pltpu.roll(value, HEAD // 2, 1) * sine
            if head < heads:
                q_scr[head, here, :] = turned.astype(BF16)
            else:
                k_scr[here, :] = turned.astype(BF16)
        v_scr[here, :] = qkv_ref[
            pl.ds(start, rows), (heads + 1) * HEAD : (heads + 2) * HEAD
        ].astype(BF16)


def key_span(index, tile):
    low = max(0, (index * tile - (MOST_DOC - 1)) // tile) * tile
    return low, (index + 1) * tile


def allowed_mask(segc_ref, segr_ref, index, tile):
    low, high = key_span(index, tile)
    shape = (tile, high - low)
    rows = lax.broadcasted_iota(jnp.int32, shape, 0) + index * tile
    cols = lax.broadcasted_iota(jnp.int32, shape, 1) + low
    same = segc_ref[0, index * tile : (index + 1) * tile, :] == segr_ref[0, :, low:high]
    return same & (cols <= rows)


def probs_of(query, keys, allowed, scale):
    scores = jnp.where(allowed, mm(query, keys, 1, 1) * scale, MASKED)
    weights = jnp.exp(scores - jnp.max(scores, axis=-1, keepdims=True))
    return weights * (1.0 / jnp.sum(weights, axis=-1, keepdims=True))


def attend_kernel(
    heads, tile, meta_ref, qkv_ref, segc_ref, segr_ref, cos_ref, sin_ref, gain_ref, out_ref, q_scr, k_scr, v_scr
):
    seq = pl.program_id(0)
    length = k_scr.shape[0]
    rows = length // 8
    scale = 1.0 / math.sqrt(HEAD)
    load_heads(meta_ref, qkv_ref, cos_ref, sin_ref, gain_ref, q_scr, k_scr, v_scr, heads)
    for index in range(length // tile):
        low, high = key_span(index, tile)
        allowed = allowed_mask(segc_ref, segr_ref, index, tile)
        for head in range(heads):
            query = q_scr[head, index * tile : (index + 1) * tile, :]
            probs = probs_of(query, k_scr[low:high, :], allowed, scale)
            mixed = mm(probs.astype(BF16), v_scr[low:high, :], 1, 0).astype(BF16)
            for piece in range(tile // rows):
                start = block_row(meta_ref, seq, index * (tile // rows) + piece, rows)
                out_ref[pl.ds(start, rows), head * HEAD : (head + 1) * HEAD] = mixed[
                    piece * rows : (piece + 1) * rows
                ]


def attend_back_kernel(
    heads,
    tile,
    meta_ref,
    qkv_ref,
    grad_ref,
    segc_ref,
    segr_ref,
    cos_ref,
    sin_ref,
    gain_ref,
    out_ref,
    gain_out_ref,
    q_scr,
    k_scr,
    v_scr,
    g_scr,
    dk_scr,
    dv_scr,
):
    seq = pl.program_id(0)
    length = k_scr.shape[0]
    rows = length // 8
    scale = 1.0 / math.sqrt(HEAD)
    load_heads(meta_ref, qkv_ref, cos_ref, sin_ref, gain_ref, q_scr, k_scr, v_scr, heads)
    for index in range(8):
        start = block_row(meta_ref, seq, index, rows)
        g_scr[index * rows : (index + 1) * rows, :] = grad_ref[pl.ds(start, rows), :]
    dk_scr[...] = jnp.zeros_like(dk_scr)
    dv_scr[...] = jnp.zeros_like(dv_scr)

    @pl.when(seq == 0)
    def _():
        gain_out_ref[...] = jnp.zeros_like(gain_out_ref)

    def finish(grad, index, head, which):
        here = slice(index * rows, (index + 1) * rows)
        start = block_row(meta_ref, seq, index, rows)
        grad = grad * cos_ref[here, :] - pltpu.roll(grad, HEAD // 2, 1) * sin_ref[here, :]
        raw = qkv_ref[pl.ds(start, rows), head * HEAD : (head + 1) * HEAD]
        scaled, inverse = scaled_of(raw)
        gain_out_ref[which : which + 1, :] += jnp.sum(grad * scaled, axis=0, keepdims=True)
        out = norm_back(grad, scaled, inverse, gain_ref[which : which + 1, :])
        out_ref[pl.ds(start, rows), head * HEAD : (head + 1) * HEAD] = out.astype(BF16)

    per = tile // rows
    for index in range(length // tile):
        low, high = key_span(index, tile)
        mine = slice(index * tile, (index + 1) * tile)
        allowed = allowed_mask(segc_ref, segr_ref, index, tile)
        for head in range(heads):
            query = q_scr[head, mine, :]
            keys = k_scr[low:high, :]
            probs = probs_of(query, keys, allowed, scale)
            grad = g_scr[mine, head * HEAD : (head + 1) * HEAD]
            grad_probs = mm(grad, v_scr[low:high, :], 1, 1)
            delta = jnp.sum(probs * grad_probs, axis=-1, keepdims=True)
            grad_scores = (probs * (grad_probs - delta)).astype(BF16)
            dv_scr[low:high, :] += mm(probs.astype(BF16), grad, 0, 0)
            dk_scr[low:high, :] += mm(grad_scores, query, 0, 0) * scale
            grad_query = mm(grad_scores, keys, 1, 0) * scale
            for piece in range(per):
                finish(
                    grad_query[piece * rows : (piece + 1) * rows], index * per + piece, head, 0
                )
    for index in range(8):
        here = slice(index * rows, (index + 1) * rows)
        start = block_row(meta_ref, seq, index, rows)
        finish(dk_scr[here, :], index, heads, 1)
        out_ref[pl.ds(start, rows), (heads + 1) * HEAD : (heads + 2) * HEAD] = dv_scr[
            here, :
        ].astype(BF16)


def whole(shape):
    return pl.BlockSpec(shape, lambda seq, meta: (0,) * len(shape))


def seg_specs(length):
    return [
        pl.BlockSpec((1, length, 1), lambda seq, meta: (seq, 0, 0)),
        pl.BlockSpec((1, 1, length), lambda seq, meta: (seq, 0, 0)),
    ]


def attend(meta, qkv, seg_cols, seg_rows, cosine, sine, gains):
    length = cosine.shape[0]
    tile = length // 4
    heads = qkv.shape[1] // HEAD - 2
    pairs = 2 * heads * length * length // 2
    return pl.pallas_call(
        functools.partial(attend_kernel, heads, tile),
        out_shape=jax.ShapeDtypeStruct((qkv.shape[0], heads * HEAD), BF16),
        grid_spec=pltpu.PrefetchScalarGridSpec(
            num_scalar_prefetch=1,
            grid=(2,),
            in_specs=[whole(qkv.shape)]
            + seg_specs(length)
            + [whole(cosine.shape), whole(sine.shape), whole(gains.shape)],
            out_specs=whole((qkv.shape[0], heads * HEAD)),
            scratch_shapes=[
                pltpu.VMEM((heads, length, HEAD), BF16),
                pltpu.VMEM((length, HEAD), BF16),
                pltpu.VMEM((length, HEAD), BF16),
            ],
        ),
        cost_estimate=pl.CostEstimate(
            flops=4 * pairs * HEAD, bytes_accessed=qkv.size * 4 + qkv.size, transcendentals=pairs
        ),
        name="attend",
    )(meta, qkv, seg_cols, seg_rows, cosine, sine, gains)


def attend_back(meta, qkv, grad, seg_cols, seg_rows, cosine, sine, gains):
    length = cosine.shape[0]
    tile = length // 4
    heads = qkv.shape[1] // HEAD - 2
    pairs = 2 * heads * length * length // 2
    return pl.pallas_call(
        functools.partial(attend_back_kernel, heads, tile),
        out_shape=(
            jax.ShapeDtypeStruct(qkv.shape, BF16),
            jax.ShapeDtypeStruct(gains.shape, F32),
        ),
        grid_spec=pltpu.PrefetchScalarGridSpec(
            num_scalar_prefetch=1,
            grid=(2,),
            in_specs=[whole(qkv.shape), whole(grad.shape)]
            + seg_specs(length)
            + [whole(cosine.shape), whole(sine.shape), whole(gains.shape)],
            out_specs=(whole(qkv.shape), whole(gains.shape)),
            scratch_shapes=[
                pltpu.VMEM((heads, length, HEAD), BF16),
                pltpu.VMEM((length, HEAD), BF16),
                pltpu.VMEM((length, HEAD), BF16),
                pltpu.VMEM((length, heads * HEAD), BF16),
                pltpu.VMEM((length, HEAD), F32),
                pltpu.VMEM((length, HEAD), F32),
            ],
        ),
        cost_estimate=pl.CostEstimate(
            flops=10 * pairs * HEAD, bytes_accessed=qkv.size * 8, transcendentals=pairs
        ),
        name="attend_back",
    )(meta, qkv, grad, seg_cols, seg_rows, cosine, sine, gains)


def body(
    tokens,
    segment_ids,
    norm_gain,
    query_weight,
    key_matrix,
    value_matrix,
    output_weight,
    query_gain,
    key_gain,
    mlp_gain,
    gate_weight,
    up_weight,
    down_weight,
    cotangent,
):
    local, width = tokens.shape[1], tokens.shape[2]
    length = 2 * local
    quarter = local // 2
    count = lax.axis_size("fsdp")
    block = width // count
    mine = lax.axis_index("fsdp")
    odd = mine % 2
    place = lax.axis_index("ctx")
    core = lax.axis_index("tp")

    small = query_gain.shape[0]
    members = [norm_gain, mlp_gain, query_gain, key_gain]
    used = sum(member.shape[0] for member in members)
    lanes = -(-used // HEAD) * HEAD
    row = jnp.concatenate(members + [jnp.zeros((lanes - used,), BF16)]).astype(F32)[None]
    far_segments = swap_x(segment_ids)
    first_pair, all_gains = first_shards(
        [query_weight, key_matrix, value_matrix, output_weight], row, count
    )
    first = gather_line(first_pair)
    tok, gate_up_pair, down_pair = second_shards(
        [[after(gate_weight, first_pair), up_weight], [down_weight]],
        tokens.reshape(local, width),
    )
    gate_up_w = gather_line(gate_up_pair)
    down_w = gather_line(down_pair)

    def own_quarter(value):
        return lax.dynamic_slice_in_dim(value.reshape(local, width), core * quarter, quarter, 0)

    own_tok, own_cot = own_quarter(tokens), own_quarter(cotangent)
    segments = jnp.concatenate([segment_ids, far_segments])
    seg_cols, seg_rows = segments[:, :, None], segments[:, None, :]
    cosine, sine = rope_tables(jnp.arange(length).astype(F32))
    meta = jnp.stack([place, core]).astype(jnp.int32)

    heads_q = query_weight.shape[1] // 4 // HEAD
    cols = (heads_q + 2) * HEAD
    qkv_w = first[:, :cols]
    out_w = first[:, cols : cols + heads_q * HEAD]
    in_gain = all_gains[:, :block].reshape(1, width)
    mid_gain = all_gains[:, block : 2 * block].reshape(1, width)
    head_gains = all_gains[:, 2 * block : 2 * block + 2 * small].reshape(count, 2, small)
    head_gains = jnp.moveaxis(head_gains, 0, 1).reshape(2, HEAD)

    in_f = tok.astype(F32)
    cot_from = after(own_cot, tok)
    cot_x, cot_y = swap_x(cot_from), swap_ctx(cot_from)
    x_all = (in_f * inv_rms(in_f) * in_gain).astype(BF16)
    qkv = mm(x_all, qkv_w, 1, 0)
    attended = attend(meta, qkv, seg_cols, seg_rows, cosine, sine, head_gains)
    half = 4 * quarter
    cot_x, cot_y = after(cot_x, attended), after(cot_y, attended)
    eighth = quarter // 2
    cot_first, cot_second = swap_ctx(cot_x[:eighth]), swap_x(cot_y[eighth:])
    out_far = mm(attended[half:], out_w, 1, 1).astype(BF16)
    out_near = mm(attended[:half], out_w, 1, 1)
    middle = own_tok.astype(F32) + reduce8(out_near, out_far)
    inverse_mid = inv_rms(middle)
    scaled_mid = middle * inverse_mid
    y_own = (scaled_mid * mid_gain).astype(BF16)
    cot_first, cot_second = after(cot_first, y_own), after(cot_second, y_own)
    y_all, cot = gather8(y_own, (cot_from, cot_x, cot_y, cot_first, cot_second))

    ff = gate_up_w.shape[1] // 2
    gate_up = mm(y_all, gate_up_w, 1, 0)
    gate, up_value = gate_up[:, :ff], gate_up[:, ff:]
    sig = jax.nn.sigmoid(gate)
    active = gate * sig
    hidden = (active * up_value).astype(BF16)
    down_grad = mm(cot, hidden, 0, 0).astype(BF16)

    grad_hidden = mm(after(cot, down_grad), down_w, 1, 0)
    grad_up = (grad_hidden * active).astype(BF16)
    grad_gate = (grad_hidden * up_value * (sig * (1.0 + gate * (1.0 - sig)))).astype(BF16)
    mid_grad, gate_up_grad = product_reduce8((grad_gate, grad_up), gate_up_w, 7, y_all)

    mlp_gain_part = jnp.sum(mid_grad * scaled_mid, axis=0)
    grad_middle = own_cot.astype(F32) + norm_back(mid_grad, scaled_mid, inverse_mid, mid_gain)
    grad_attn, mlp_kept, mlp_to_y, mlp_to_x = gather8_product(
        grad_middle.astype(BF16), hidden, down_w
    )
    out_grad = mm(grad_attn, attended, 0, 0).astype(BF16)
    grad_att = mm(grad_attn, out_w, 1, 0).astype(BF16)
    raw_grads, head_gain_parts = attend_back(
        meta, qkv, grad_att, seg_cols, seg_rows, cosine, sine, head_gains
    )
    mlp_first, mlp_second, mlp_came1, mlp_came2 = reduce4_links(
        mlp_kept, mlp_to_y, mlp_to_x, raw_grads
    )
    first_grad = mm(x_all, raw_grads, 0, 0).astype(BF16)
    first_grad = jnp.concatenate([first_grad, out_grad], axis=1)
    mlp_first = mlp_first + after(mlp_came1, first_grad).astype(F32)
    mlp_second = mlp_second + after(mlp_came2, first_grad).astype(F32)
    mlp_sum = (middle + jnp.concatenate([mlp_first, mlp_second])).astype(BF16)
    far_sum = swap_core(mlp_sum)
    in_grad = product_reduce8((after(raw_grads, first_grad, mlp_sum),), first, 8)

    spot = jnp.stack([place, odd]).astype(jnp.int32)

    def owners(grad, sizes, *others):
        rows = scatter_line(grad)
        rows = after(rows, *others)
        kept = lax.dynamic_slice_in_dim(rows, odd * block, block, 0)
        sent = lax.dynamic_slice_in_dim(rows, (1 - odd) * block, block, 0)
        by_x, by_y = swap_x(sent), swap_ctx(kept)
        by_both = swap_ctx(by_x)
        return join_columns(spot, (kept, by_x, by_y, by_both), sizes)

    (down_share,) = owners(down_grad, (ff,))
    gate_share, up_share = owners(gate_up_grad, (ff, ff))
    query_share, key_share, value_share, out_share = owners(
        first_grad, (heads_q * HEAD, HEAD, HEAD, heads_q * HEAD)
    )

    own_in = own_tok.astype(F32)
    inverse_in = inv_rms(own_in)
    scaled_in = own_in * inverse_in
    norm_gain_part = jnp.sum(in_grad * scaled_in, axis=0)
    own_token_grad = (grad_middle + norm_back(in_grad, scaled_in, inverse_in, in_gain)).astype(BF16)
    far_token_grad = swap_core(own_token_grad)

    parts = jnp.concatenate([norm_gain_part, mlp_gain_part, head_gain_parts.reshape(-1)])
    parts = parts.reshape(-1, HEAD)
    far_parts = swap_ctx(parts)
    sums, layer_out, token_grad = total(
        parts + after(far_parts, far_token_grad),
        (mlp_sum, far_sum),
        (own_token_grad, far_token_grad),
    )
    sums = sums.reshape(-1)
    layer_out, token_grad = layer_out.reshape(tokens.shape), token_grad.reshape(tokens.shape)
    norm_gain_grad = lax.dynamic_slice_in_dim(sums, mine * block, block, 0)
    mlp_gain_grad = lax.dynamic_slice_in_dim(sums, width + mine * block, block, 0)
    query_gain_grad = lax.dynamic_slice_in_dim(sums, 2 * width + mine * small, small, 0)
    key_gain_grad = lax.dynamic_slice_in_dim(sums, 2 * width + HEAD + mine * small, small, 0)
    return (
        layer_out,
        token_grad,
        norm_gain_grad,
        query_share,
        key_share,
        value_share,
        out_share,
        query_gain_grad,
        key_gain_grad,
        mlp_gain_grad,
        gate_share,
        up_share,
        down_share,
    )


def solution(mesh):
    in_specs = (
        P("fsdp", "ctx", None),
        P("fsdp", None),
        P("fsdp"),
        P("fsdp", "tp"),
        P("fsdp", "tp"),
        P("fsdp", "tp"),
        P("fsdp", "tp"),
        P("fsdp"),
        P("fsdp"),
        P("fsdp"),
        P("fsdp", "tp"),
        P("fsdp", "tp"),
        P("fsdp", "tp"),
        P("fsdp", "ctx", None),
    )
    out_specs = (
        P("fsdp", "ctx", None),
        P("fsdp", "ctx", None),
        P("fsdp"),
        P("fsdp", "tp"),
        P("fsdp", "tp"),
        P("fsdp", "tp"),
        P("fsdp", "tp"),
        P("fsdp"),
        P("fsdp"),
        P("fsdp"),
        P("fsdp", "tp"),
        P("fsdp", "tp"),
        P("fsdp", "tp"),
    )

    return jax.shard_map(body, mesh=mesh, in_specs=in_specs, out_specs=out_specs, check_vma=False)
```
